32 devices in a mesh: section: 2 (over x), fsdp: 4 (over y, core), tp: 4 (over z).
Axes of the slice: x: 2, y: 2, z: 4, core: 2. Of those that a mesh axis runs over, the one named last changes fastest.
Arguments:
- ends_in: bfloat16 [2, 2, 1024, 2048], P('section', None, ('fsdp', 'tp')), may hold values from -6 to 6
- segments: int32 [2, 1024], P(None, 'fsdp'), may hold values from 0 to 15, never falling along the last dimension, each value on 1 to 256 neighbouring positions
- ln_gain: bfloat16 [2, 2048], P('section', ('fsdp', 'tp')), may hold values from 0.5 to 1.5
- ln_bias: bfloat16 [2, 2048], P('section', ('fsdp', 'tp')), may hold values from -3 to 3
- w_qkv: bfloat16 [2, 2048, 3, 2048], P('section', 'fsdp', None, 'tp'), may hold values from -2 to 2
- w_out: bfloat16 [2, 2048, 2048], P('section', 'fsdp', 'tp'), may hold values from -0.375 to 0.375
- w_fc1: bfloat16 [2, 2048, 8192], P('section', 'fsdp', 'tp'), may hold values from -0.125 to 0.125
- w_fc2: bfloat16 [2, 2048, 8192], P('section', 'fsdp', 'tp'), may hold values from -0.0625 to 0.0625
- bias_qkv: bfloat16 [2, 3, 2048], P('section', None, ('fsdp', 'tp')), may hold values from -3 to 3
- bias_out: bfloat16 [2, 2048], P('section', ('fsdp', 'tp')), may hold values from -3 to 3
- bias_fc1: bfloat16 [2, 8192], P('section', ('fsdp', 'tp')), may hold values from -3 to 3
- bias_fc2: bfloat16 [2, 2048], P('section', ('fsdp', 'tp')), may hold values from -3 to 3
Outputs:
- ends_out: float32 [2, 2, 1024, 2048], P('section', None, ('fsdp', 'tp'))
- grad_gain: float32 [2, 2048], P('section', ('fsdp', 'tp'))
- grad_bias: float32 [2, 2048], P('section', ('fsdp', 'tp'))
- grad_qkv: float32 [2, 2048, 3, 2048], P('section', 'fsdp', None, 'tp')
- grad_out: float32 [2, 2048, 2048], P('section', 'fsdp', 'tp')
- grad_fc1: float32 [2, 2048, 8192], P('section', 'fsdp', 'tp')
- grad_fc2: float32 [2, 2048, 8192], P('section', 'fsdp', 'tp')
- grad_bias_qkv: float32 [2, 3, 2048], P('section', None, ('fsdp', 'tp'))
- grad_bias_out: float32 [2, 2048], P('section', ('fsdp', 'tp'))
- grad_bias_fc1: float32 [2, 8192], P('section', ('fsdp', 'tp'))
- grad_bias_fc2: float32 [2, 2048], P('section', ('fsdp', 'tp'))
The draws below stay inside these ranges and needn't reach their ends.
Inputs may be any that keep to these rules, and one draw needn't show every extreme that they name: `segments`: segment ids never fall along a row; a run of equal ids is one document.
All inputs are finite; a program needn't handle non-finite values.
Results may differ from the reference program's by a relative error of at most 0.015.
Values may be sent and summed in bfloat16 or wider, within the bound.
A program may use at most 256 MiB of HBM per device.

```python
import math
import jax
import jax.numpy as jnp
import numpy as np
from jax import lax

D = 2048
HEADS = 32
FF = 8192
HEAD_DIM = 64
ROT_DIM = 32
SEQ = 256
MICRO = 2
TOKENS = 1024
N_FSDP = 4


def draw_w_qkv(key, part):
    base = jax.random.truncated_normal(key, -4.0, 4.0, (2, D, 3, D), jnp.float32)
    return (base * D ** (-0.5)).astype(jnp.bfloat16)


def levels(rng, dims, shards, least, high):
    def one(axis_at, blocks):
        draws = jax.random.uniform(jax.random.fold_in(jax.random.fold_in(rng, 6), axis_at), (blocks,), jnp.float32, least / len(shards), high / len(shards))
        return jnp.repeat(jnp.exp(draws), dims[axis_at] // blocks).reshape((-1,) + (1,) * (len(dims) - axis_at - 1))

    gain = one(*shards[0])
    for cut in shards[1:]:
        gain = gain * one(*cut)
    return gain


def split_up(amount, total, limit, lean):
    loads = [(1 << 20) // math.isqrt(grade ** lean) + 1 for grade in range(2, amount + 1)]
    rest, given = total - limit - (amount - 1), [1] * (amount - 1)
    while rest > 0:
        candidates = [i for i in range(amount - 1) if given[i] < limit]
        mass, budget = sum([loads[i] for i in candidates]), rest
        for i in candidates:
            extra = min(limit - given[i], max(1, budget * loads[i] // mass), rest)
            given[i] = given[i] + extra
            rest = rest - extra
    return np.array([limit] + given)


def ragged_sizes(key, amount, total, limit, skew):
    if amount == 2:
        one = jax.random.randint(key, (), max(1, total - limit), min(limit, total - 1) + 1)
        return jnp.stack([one, total - one])
    lengths = jnp.asarray(split_up(amount, total, limit, skew), jnp.int32)
    twos = (amount - 1) // 2
    source_of, sink = lengths[1:1 + 2 * twos:2], lengths[2:2 + 2 * twos:2]
    margin = jnp.minimum(source_of - 1, limit - sink)
    shifted = jax.random.randint(jax.random.fold_in(key, 1), (twos,), 0, 1 << 20) % (margin + 1)
    lengths = lengths.at[1:1 + 2 * twos:2].set(source_of - shifted).at[2:2 + 2 * twos:2].set(sink + shifted)
    return lengths[jax.random.permutation(jax.random.fold_in(key, 2), amount)]


def noise(stream_key, shape, width, bound, shards=(), held_as=jnp.bfloat16):
    values = jax.random.normal(stream_key, shape, jnp.float32) * width
    if len(shards) > 0:
        values = levels(stream_key, shape, shards, -0.22, 0.18) * values
    return jnp.clip(values, min=-bound, max=bound).astype(held_as)


def setup_inputs(seed: int = 0) -> dict:
    key_of = jax.random.split(jax.random.key(seed), 13)
    ends_in = noise(key_of[0], (2, MICRO, TOKENS, D), 1.0, 6.0, ((0, 2), (2, 16)))
    segments = jax.vmap(lambda own: jnp.searchsorted(jnp.cumsum(ragged_sizes(own, 4 * N_FSDP, TOKENS, SEQ, 2)), jnp.arange(TOKENS), side="right"))(jax.random.split(key_of[1], MICRO)).reshape((MICRO, TOKENS)).astype(jnp.int32)
    ln_gain = jnp.clip(1.0 + 0.1 * jax.random.normal(key_of[2], (2, D), jnp.float32), 0.5, 1.5).astype(jnp.bfloat16)
    ln_bias = noise(key_of[3], (2, D), 0.5, 3.0, ((0, 2), (1, 16)))
    w_qkv = draw_w_qkv(jax.random.fold_in(key_of[12], 71), 0)
    w_out = noise(key_of[5], (2, D, D), (D // 8) ** -0.5, 0.375, ((0, 2), (1, 4), (2, 4)))
    w_fc1 = noise(key_of[6], (2, D, FF), D ** -0.5, 0.125, ((0, 2), (1, 4), (2, 4)))
    w_fc2 = noise(key_of[7], (2, D, FF), FF ** -0.5, 0.0625, ((0, 2), (1, 4), (2, 4)))
    bias_qkv = noise(key_of[8], (2, 3, D), 0.5, 3.0, ((0, 2), (2, 16)))
    bias_out = noise(key_of[9], (2, D), 0.5, 3.0, ((0, 2), (1, 16)))
    bias_fc1 = noise(key_of[10], (2, FF), 0.5, 3.0, ((0, 2), (1, 16)))
    bias_fc2 = noise(key_of[11], (2, D), 0.5, 3.0, ((0, 2), (1, 16)))
    return {"ends_in": ends_in, "segments": segments, "ln_gain": ln_gain, "ln_bias": ln_bias, "w_qkv": w_qkv, "w_out": w_out, "w_fc1": w_fc1, "w_fc2": w_fc2, "bias_qkv": bias_qkv, "bias_out": bias_out, "bias_fc1": bias_fc1, "bias_fc2": bias_fc2}


@jax.custom_vjp
def low(v):
    return lax.optimization_barrier(v.astype(jnp.bfloat16)).astype(jnp.float32)

@jax.custom_vjp
def low_back(v):
    return v

def low_keep(v):
    return (low(v), None)

def low_pass(kept, grad):
    return (grad,)

def back_keep(v):
    return (v, None)

def back_low(kept, grad):
    return (low(grad),)
low.defvjp(low_keep, low_pass)
low_back.defvjp(back_keep, back_low)
EPSILON = 1e-05
HIGHEST = lax.Precision.HIGHEST

def positions_of(segment_ids):
    length = segment_ids.shape[-1]
    places = jnp.arange(length, dtype=jnp.int32)
    before = jnp.concatenate([segment_ids[..., :1] - 1, segment_ids[..., :-1]], axis=-1)
    starts = jnp.where(segment_ids != before, places, 0).astype(jnp.int32)
    starts = lax.cummax(starts, axis=segment_ids.ndim - 1)
    return places - starts

def inverse_freq(rot_dim):
    half = rot_dim // 2
    return jnp.exp(-jnp.log(10000.0) * (2.0 * jnp.arange(half, dtype=jnp.float32)) / rot_dim)

def rotate(values_in, angles, rot_dim):
    half = rot_dim // 2
    cosine = jnp.cos(angles)[..., None, :]
    sine = jnp.sin(angles)[..., None, :]
    front = values_in[..., :half]
    second = values_in[..., half:rot_dim]
    return jnp.concatenate([front * cosine - second * sine, second * cosine + front * sine, values_in[..., rot_dim:]], axis=-1)

def layer(inputs, seg_packs, gains, biases, qkv_w, out_w, fc1_w, fc2_w, qkv_b, out_b, fc1_b, fc2_b):
    packs, length = (inputs.shape[0], inputs.shape[1])
    mean = lax.optimization_barrier(jnp.mean(inputs, axis=-1, keepdims=True))
    centred = inputs - mean
    variance = lax.optimization_barrier(jnp.mean(centred * centred, axis=-1, keepdims=True))
    normed = low(centred * lax.rsqrt(variance + EPSILON) * gains + biases)
    joined = low_back(jnp.einsum('psd,dce->psce', normed, qkv_w, precision=HIGHEST) + qkv_b)
    joined = joined.reshape(packs, length, 3, HEADS, HEAD_DIM)
    angles = positions_of(seg_packs).astype(jnp.float32)[..., None] * inverse_freq(ROT_DIM)
    query = low(rotate(joined[:, :, 0], angles, ROT_DIM))
    keys = low(rotate(joined[:, :, 1], angles, ROT_DIM))
    values = low(joined[:, :, 2])
    scores = low_back(jnp.einsum('pqhe,pkhe->phqk', query, keys, precision=HIGHEST) * HEAD_DIM ** (-0.5))
    places = jnp.arange(length, dtype=jnp.int32)
    allowed = (places[:, None] >= places[None, :])[None] & (seg_packs[:, :, None] == seg_packs[:, None, :])
    scores = jnp.where(allowed[:, None], scores, -1e+30)
    top = lax.optimization_barrier(jnp.max(scores, axis=-1, keepdims=True))
    expo = jnp.exp(scores - top)
    probs = low(expo / lax.optimization_barrier(jnp.sum(expo, axis=-1, keepdims=True)))
    attended = low(low_back(jnp.einsum('phqk,pkhe->pqhe', probs, values, precision=HIGHEST)))
    attended = attended.reshape(packs, length, HEADS * HEAD_DIM)
    attn_part = jnp.einsum('pse,de->psd', attended, out_w, precision=HIGHEST)
    upward = low_back(jnp.einsum('psd,df->psf', normed, fc1_w, precision=HIGHEST) + fc1_b)
    activated = low(jax.nn.gelu(upward, approximate=True))
    mlp_part = jnp.einsum('psf,df->psd', activated, fc2_w, precision=HIGHEST)
    return inputs + low_back(attn_part + mlp_part + out_b + fc2_b)

def forward(start, segments, gains, biases, qkv_w, out_w, fc1_w, fc2_w, qkv_b, out_b, fc1_b, fc2_b):
    packs = start.reshape(MICRO * N_FSDP, SEQ, D)
    seg_packs = segments.reshape(MICRO * N_FSDP, SEQ)
    middle = layer(packs, seg_packs, gains[0], biases[0], qkv_w[0], out_w[0], fc1_w[0], fc2_w[0], qkv_b[0], out_b[0], fc1_b[0], fc2_b[0])
    passed = low(low_back(middle))
    final = layer(passed, seg_packs, gains[1], biases[1], qkv_w[1], out_w[1], fc1_w[1], fc2_w[1], qkv_b[1], out_b[1], fc1_b[1], fc2_b[1])
    return final.reshape(MICRO, TOKENS, D)

def reference(ends_in, segments, ln_gain, ln_bias, w_qkv, w_out, w_fc1, w_fc2, bias_qkv, bias_out, bias_fc1, bias_fc2):
    start = ends_in[0].astype(jnp.float32)
    cotangent = ends_in[1].astype(jnp.float32)

    def whole(first_in, gains, biases, qkv_w, out_w, fc1_w, fc2_w, qkv_b, out_b, fc1_b, fc2_b):
        return forward(first_in, segments, gains, biases, qkv_w, out_w, fc1_w, fc2_w, qkv_b, out_b, fc1_b, fc2_b)
    result, pullback = jax.vjp(whole, start, ln_gain.astype(jnp.float32), ln_bias.astype(jnp.float32), w_qkv.astype(jnp.float32), w_out.astype(jnp.float32), w_fc1.astype(jnp.float32), w_fc2.astype(jnp.float32), bias_qkv.astype(jnp.float32), bias_out.astype(jnp.float32), bias_fc1.astype(jnp.float32), bias_fc2.astype(jnp.float32))
    grads = pullback(cotangent)
    ends_out = jnp.stack([grads[0], result])
    return (ends_out, grads[1], grads[2], grads[3], grads[4], grads[5], grads[6], grads[7], grads[8], grads[9], grads[10])
```

```python
import functools

import jax
import jax.numpy as jnp
from jax import lax
from jax.experimental import pallas as pl
from jax.experimental.pallas import tpu as pltpu
from jax.sharding import PartitionSpec as P

HEAD_DIM = 64
ROT_DIM = 32
EPSILON = 1e-05
LANES = 128
TILE = 256
MESH = pl.DeviceIdType.MESH
F32 = jnp.float32
BF16 = jnp.bfloat16
COLS = (((1,), (1,)), ((), ()))
ROWS = (((0,), (0,)), ((), ()))
VMEM_LIMIT = 62 * 1024 * 1024


def positions_of(segment_ids):
    length = segment_ids.shape[-1]
    places = jnp.arange(length, dtype=jnp.int32)
    before = jnp.concatenate([segment_ids[..., :1] - 1, segment_ids[..., :-1]], axis=-1)
    starts = jnp.where(segment_ids != before, places, 0)
    starts = lax.cummax(starts, axis=segment_ids.ndim - 1)
    return places - starts


def rope_tables(segments):
    half = ROT_DIM // 2
    freq = jnp.exp(-jnp.log(10000.0) * (2.0 * jnp.arange(half, dtype=F32)) / ROT_DIM)
    angles = positions_of(segments).astype(F32)[..., None] * freq
    cosine, sine = jnp.cos(angles), jnp.sin(angles)
    none = jnp.zeros_like(sine)
    rest = jnp.zeros(angles.shape[:-1] + (HEAD_DIM - ROT_DIM,), F32)
    keep = jnp.concatenate([cosine, cosine, rest + 1.0], axis=-1)
    ahead = jnp.concatenate([-sine, none, rest], axis=-1)
    behind = jnp.concatenate([none, sine, rest], axis=-1)
    tables = jnp.stack([keep, ahead, behind], axis=1)
    return jnp.concatenate([tables, tables], axis=-1)


def send(src, dst, send_sem, recv_sem, device):
    return pltpu.make_async_remote_copy(
        src_ref=src,
        dst_ref=dst,
        send_sem=send_sem,
        recv_sem=recv_sem,
        device_id=device,
        device_id_type=MESH,
    )


def greet(peers):
    barrier = pltpu.get_barrier_semaphore()
    for peer in peers:
        pl.semaphore_signal(barrier, inc=1, device_id=peer, device_id_type=MESH)
    pl.semaphore_wait(barrier, len(peers))


def group_peers(nf, nt):
    me = lax.axis_index("fsdp") * nt + lax.axis_index("tp")
    found = []
    for k in range(1, nf * nt):
        to = lax.rem(me + k, nf * nt)
        found.append((k, to, {"fsdp": to // nt, "tp": lax.rem(to, nt)}))
    return me, found


def gather_small_kernel(nf, nt, own, out, send_sems, recv_sems, local_sem):
    me, peers = group_peers(nf, nt)
    greet([peer for _, _, peer in peers])
    mine = pltpu.make_async_copy(own, out.at[me], local_sem)
    mine.start()
    copies = []
    for k, _, peer in peers:
        copy = send(own, out.at[me], send_sems.at[k], recv_sems.at[k], peer)
        copy.start()
        copies.append(copy)
    mine.wait()
    for copy in copies:
        copy.wait()


def gather_small(own, nf, nt):
    count = nf * nt
    return pl.pallas_call(
        functools.partial(gather_small_kernel, nf, nt),
        out_shape=jax.ShapeDtypeStruct((count,) + own.shape, own.dtype),
        in_specs=[pl.BlockSpec(memory_space=pltpu.VMEM)],
        out_specs=pl.BlockSpec(memory_space=pltpu.VMEM),
        scratch_shapes=[
            pltpu.SemaphoreType.DMA((count,)),
            pltpu.SemaphoreType.DMA((count,)),
            pltpu.SemaphoreType.DMA,
        ],
        compiler_params=pltpu.CompilerParams(collective_id=0, has_side_effects=True),
        name="gather_small",
    )(own)


def sum_small_kernel(nf, nt, own, out, got, send_sems, recv_sems):
    me, peers = group_peers(nf, nt)
    greet([peer for _, _, peer in peers])
    copies = []
    for k, to, peer in peers:
        copy = send(own.at[to], got.at[k], send_sems.at[k], recv_sems.at[k], peer)
        copy.start()
        copies.append(copy)
    total = own[me]
    for k, copy in enumerate(copies):
        copy.wait()
        total = total + got[k + 1]
    out[...] = total


def sum_small(own, nf, nt):
    count = nf * nt
    return pl.pallas_call(
        functools.partial(sum_small_kernel, nf, nt),
        out_shape=jax.ShapeDtypeStruct(own.shape[1:], own.dtype),
        in_specs=[pl.BlockSpec(memory_space=pltpu.VMEM)],
        out_specs=pl.BlockSpec(memory_space=pltpu.VMEM),
        scratch_shapes=[
            pltpu.VMEM(own.shape, own.dtype),
            pltpu.SemaphoreType.DMA((count,)),
            pltpu.SemaphoreType.DMA((count,)),
        ],
        compiler_params=pltpu.CompilerParams(collective_id=1, has_side_effects=True),
        name="sum_small",
    )(own)


def cols(n, width=TILE):
    return pl.ds(pl.multiple_of(n * width, width), width)


def loop(count, body):
    def step(i, carry):
        body(i)
        return carry

    lax.fori_loop(0, count, step, 0)


def turn(x, tables, sign):
    keep, ahead, behind = tables
    left = pltpu.roll(x, LANES - ROT_DIM // 2, 1)
    right = pltpu.roll(x, ROT_DIM // 2, 1)
    return x * keep + sign * (left * ahead + right * behind)


def low_half(length):
    return lax.broadcasted_iota(jnp.int32, (length, LANES), 1) < HEAD_DIM


def allowed_mask(segc, segr, m, length):
    query = lax.broadcasted_iota(jnp.int32, (length, length), 0)
    key = lax.broadcasted_iota(jnp.int32, (length, length), 1)
    return (query >= key) & (segc[m] == segr[m])


class Ring:
    def __init__(self, nt, rows):
        self.nt, self.rows = nt, rows
        self.me = lax.axis_index("tp")
        self.others = [(k, lax.rem(self.me + k, nt)) for k in range(1, nt)]

    def block(self, who):
        return pl.ds(pl.multiple_of(who * self.rows, self.rows), self.rows)

    def gather(self, buf, m, sems):
        return [
            send(
                buf.at[m, self.block(self.me)],
                buf.at[m, self.block(self.me)],
                sems[0].at[m, k],
                sems[1].at[m, k],
                {"tp": to},
            )
            for k, to in self.others
        ]

    def scatter(self, buf, got, m, sems, part=None):
        at = slice(None) if part is None else part
        return [
            send(
                buf.at[m, self.block(to), at],
                got.at[m, k, :, at],
                sems[0].at[m, k],
                sems[1].at[m, k],
                {"tp": to},
            )
            for k, to in self.others
        ]

    def total(self, buf, got, m):
        acc = buf[m, self.block(self.me)].astype(F32)
        for k, _ in self.others:
            acc = acc + got[m, k].astype(F32)
        return acc


def stats(rows):
    mean = jnp.mean(rows, axis=-1, keepdims=True)
    centred = rows - mean
    variance = jnp.mean(centred * centred, axis=-1, keepdims=True)
    inv_root = lax.rsqrt(variance + EPSILON)
    return centred * inv_root, inv_root


def forward_kernel(
    nt,
    rows_h, wq_h, wo_h, w1_h, w2_h, vec, qb, fb, rope, segc, segr,
    rows_o, xg_o, qkv_o, lse_o, att_o, gp_o, act_o, y_o,
    wq, wo, w1, w2, rin, xg, qkv, lse, att, gp, act, branch, got, out_f, out_b,
    w_sem, in_sem, o_sem, ag_s, ag_r, rs_s, rs_r, x_s, x_r,
):
    micro, length, width = xg.shape
    section = lax.axis_index("section")
    first, second = section == 0, section == 1
    ring = Ring(nt, length // nt)
    own = wo.shape[1]
    loads = []
    for i, (src, dst) in enumerate(((wq_h, wq), (w1_h, w1), (wo_h, wo), (w2_h, w2))):
        loads.append(pltpu.make_async_copy(src, dst, w_sem.at[i]))
        loads[-1].start()
    mine = pltpu.make_async_copy(rows_h, rin, in_sem)

    @pl.when(first)
    def _():
        mine.start()

    greet([{"tp": to} for _, to in ring.others] + [{"section": 1 - section}])

    @pl.when(first)
    def _():
        mine.wait()

    def hop(m):
        return send(out_b.at[m], rin.at[m], x_s.at[m], x_r.at[m], {"section": 1 - section})

    def front(m):
        unit, _ = stats(rin[m].astype(F32))
        normed = unit * vec[0:1, :] + vec[1:2, :]
        xg[m, ring.block(ring.me)] = normed.astype(BF16)
        for copy in ring.gather(xg, m, (ag_s, ag_r)):
            copy.start()

    def arrive(m):
        @pl.when(second)
        def _():
            hop(m).wait_recv()
            front(m)

    stores = []

    def store(src, dst, m, i):
        copy = pltpu.make_async_copy(src.at[m], dst.at[m], o_sem.at[m, i])
        copy.start()
        stores.append(copy)

    def body(m):
        for copy in ring.gather(xg, m, (ag_s, ag_r)):
            copy.wait()
        store(xg, xg_o, m, 0)
        store(rin, rows_o, m, 1)
        tables = (rope[m, 0], rope[m, 1], rope[m, 2])
        if m == 0:
            loads[0].wait()
        per = own // TILE
        for part in range(3):
            def qkv_tile(n, part=part):
                at = cols(n)
                acc = jnp.dot(xg[m], wq[part, :, at], preferred_element_type=F32)
                acc = acc + qb[part:part + 1, at]
                if part < 2:
                    acc = jnp.concatenate(
                        [
                            turn(acc[:, c:c + LANES], tables, 1.0)
                            for c in range(0, TILE, LANES)
                        ],
                        axis=1,
                    )
                qkv[m, part, :, at] = acc.astype(BF16)

            loop(per, qkv_tile)
        store(qkv, qkv_o, m, 2)
        allowed = allowed_mask(segc, segr, m, length)
        low = low_half(length)
        lane = lax.broadcasted_iota(jnp.int32, (length, LANES), 1)

        def pair(p):
            at = cols(p, LANES)
            query, key, value = qkv[m, 0, :, at], qkv[m, 1, :, at], qkv[m, 2, :, at]
            outs = []
            for h in range(2):
                mask = low if h == 0 else ~low
                one = jnp.where(mask, query, jnp.zeros_like(query))
                s = lax.dot_general(one, key, COLS, preferred_element_type=F32)
                s = jnp.where(allowed, s * HEAD_DIM ** (-0.5), -1e30)
                top = jnp.max(s, axis=-1, keepdims=True)
                e = jnp.exp(s - top)
                total = jnp.sum(e, axis=-1, keepdims=True)
                probs = (e / total).astype(BF16)
                outs.append(jnp.dot(probs, value, preferred_element_type=F32))
                lse[m] = jnp.where(lane == 2 * p + h, top + jnp.log(total), lse[m])
            att[m, :, at] = jnp.where(low, outs[0], outs[1]).astype(BF16)

        lse[m] = jnp.zeros((length, LANES), F32)
        loop(own // LANES, pair)
        store(lse, lse_o, m, 3)
        store(att, att_o, m, 4)
        if m == 0:
            loads[1].wait()

        def up_tile(n):
            at = cols(n)
            u = jnp.dot(xg[m], w1[:, at], preferred_element_type=F32) + fb[0:1, at]
            c = 0.7978845608028654
            square = u * u
            t = jnp.tanh(c * u * (1.0 + 0.044715 * square))
            act[m, :, at] = (0.5 * u * (1.0 + t)).astype(BF16)
            slope = 0.5 * (1.0 + t) + 0.5 * u * (1.0 - t * t) * (c * (1.0 + 3 * 0.044715 * square))
            gp[m, :, at] = slope.astype(BF16)

        loop(act.shape[2] // TILE, up_tile)
        store(act, act_o, m, 5)
        store(gp, gp_o, m, 6)
        if m == 0:
            loads[2].wait()
            loads[3].wait()

        def out_tile(n):
            at = cols(n)
            acc = lax.dot_general(att[m], wo[at, :], COLS, preferred_element_type=F32)
            acc = acc + lax.dot_general(act[m], w2[at, :], COLS, preferred_element_type=F32)
            branch[m, :, at] = acc.astype(BF16)
            for copy in ring.scatter(branch, got, m, (rs_s, rs_r), at):
                copy.start()

        loop(width // TILE, out_tile)

    def finish(m):
        for copy in ring.scatter(branch, got, m, (rs_s, rs_r)):
            copy.wait()
        y = rin[m].astype(F32) + ring.total(branch, got, m) + vec[2:3, :]
        out_f[m] = y
        out_b[m] = y.astype(BF16)
        store(out_f, y_o, m, 7)

        @pl.when(first)
        def _():
            hop(m).start()

    @pl.when(first)
    def _():
        for m in range(micro):
            front(m)

    for m in range(micro):
        arrive(m)
        body(m)
    for m in range(micro):
        finish(m)
    for copy in stores:
        copy.wait()

    @pl.when(first)
    def _():
        for m in range(micro):
            hop(m).wait_send()


def forward(rows, weights, vec, qb, fb, rope, segc, segr, nt):
    wq, wo, w1, w2 = weights
    micro, per, width = rows.shape
    length = per * nt
    own, hidden = wo.shape[1], w1.shape[1]
    anywhere = pl.BlockSpec(memory_space=pl.ANY)
    inside = pl.BlockSpec(memory_space=pltpu.VMEM)
    out_shape = [
        jax.ShapeDtypeStruct(rows.shape, BF16),
        jax.ShapeDtypeStruct((micro, length, width), BF16),
        jax.ShapeDtypeStruct((micro, 3, length, own), BF16),
        jax.ShapeDtypeStruct((micro, length, LANES), F32),
        jax.ShapeDtypeStruct((micro, length, own), BF16),
        jax.ShapeDtypeStruct((micro, length, hidden), BF16),
        jax.ShapeDtypeStruct((micro, length, hidden), BF16),
        jax.ShapeDtypeStruct(rows.shape, F32),
    ]
    dma = pltpu.SemaphoreType.DMA
    return pl.pallas_call(
        functools.partial(forward_kernel, nt),
        out_shape=out_shape,
        in_specs=[anywhere] * 5 + [inside] * 6,
        out_specs=[anywhere] * 8,
        scratch_shapes=[
            pltpu.VMEM(wq.shape, BF16),
            pltpu.VMEM(wo.shape, BF16),
            pltpu.VMEM(w1.shape, BF16),
            pltpu.VMEM(w2.shape, BF16),
            pltpu.VMEM(rows.shape, BF16),
            pltpu.VMEM((micro, length, width), BF16),
            pltpu.VMEM((micro, 3, length, own), BF16),
            pltpu.VMEM((micro, length, LANES), F32),
            pltpu.VMEM((micro, length, own), BF16),
            pltpu.VMEM((micro, length, hidden), BF16),
            pltpu.VMEM((micro, length, hidden), BF16),
            pltpu.VMEM((micro, length, width), BF16),
            pltpu.VMEM((micro, nt, per, width), BF16),
            pltpu.VMEM(rows.shape, F32),
            pltpu.VMEM(rows.shape, BF16),
            dma((4,)),
            dma,
            dma((micro, 8)),
            dma((micro, nt)),
            dma((micro, nt)),
            dma((micro, nt)),
            dma((micro, nt)),
            dma((micro,)),
            dma((micro,)),
        ],
        compiler_params=pltpu.CompilerParams(
            collective_id=2, has_side_effects=True, vmem_limit_bytes=VMEM_LIMIT
        ),
        name="forward",
    )(rows, wq, wo, w1, w2, vec, qb, fb, rope, segc, segr)


def backward_kernel(
    nt,
    dy_h, wq_h, wo_h, w1_h, w2_h, rows_h, qkv_h, lse_h, gp_h, vec, rope, segc, segr,
    gr_o, up_o, dj_o, dx_o, own_sums, head_sums, up_sums,
    wq, wo, w1, w2, dyr, rin, qkv, lse, gp, gr, gatt, up, dj, branch, got, out_f, out_b,
    w_sem, in_sem, o_sem, ag_s, ag_r, rs_s, rs_r, x_s, x_r,
):
    micro, length, width = gr.shape
    section = lax.axis_index("section")
    first, second = section == 0, section == 1
    ring = Ring(nt, length // nt)
    own = wo.shape[1]
    mine = pltpu.make_async_copy(dy_h, dyr, in_sem.at[4])

    @pl.when(second)
    def _():
        mine.start()

    loads = []
    for i, (src, dst) in enumerate(((wo_h, wo), (w2_h, w2), (wq_h, wq), (w1_h, w1))):
        loads.append(pltpu.make_async_copy(src, dst, w_sem.at[i]))
    kept = []
    for i, (src, dst) in enumerate(((qkv_h, qkv), (lse_h, lse), (gp_h, gp), (rows_h, rin))):
        kept.append(pltpu.make_async_copy(src, dst, in_sem.at[i]))
    for copy in (loads[0], kept[0], kept[1], loads[1], kept[2], loads[2], loads[3], kept[3]):
        copy.start()
    greet([{"tp": to} for _, to in ring.others] + [{"section": 1 - section}])

    @pl.when(second)
    def _():
        mine.wait()

    def hop(m):
        return send(out_b.at[m], dyr.at[m], x_s.at[m], x_r.at[m], {"section": 1 - section})

    def front(m):
        gr[m, ring.block(ring.me)] = dyr[m]
        for copy in ring.gather(gr, m, (ag_s, ag_r)):
            copy.start()

    def arrive(m):
        @pl.when(first)
        def _():
            hop(m).wait_recv()
            front(m)

    stores = []

    def store(src, dst, m, i):
        copy = pltpu.make_async_copy(src.at[m], dst.at[m], o_sem.at[m, i])
        copy.start()
        stores.append(copy)

    def body(m):
        for copy in ring.gather(gr, m, (ag_s, ag_r)):
            copy.wait()
        store(gr, gr_o, m, 0)
        if m == 0:
            loads[0].wait()

        def att_tile(n):
            at = cols(n)
            gatt[:, at] = jnp.dot(gr[m], wo[:, at], preferred_element_type=F32).astype(BF16)

        loop(own // TILE, att_tile)
        if m == 0:
            kept[0].wait()
            kept[1].wait()
        tables = (rope[m, 0], rope[m, 1], rope[m, 2])
        allowed = allowed_mask(segc, segr, m, length)
        low = low_half(length)
        lane = lax.broadcasted_iota(jnp.int32, (length, LANES), 1)
        factor = HEAD_DIM ** (-0.5)

        def pair(p):
            at = cols(p, LANES)
            query, key, value = qkv[m, 0, :, at], qkv[m, 1, :, at], qkv[m, 2, :, at]
            grad = gatt[:, at]
            dqs, dks, dvs = [], [], []
            for h in range(2):
                mask = low if h == 0 else ~low
                one = jnp.where(mask, query, jnp.zeros_like(query))
                s = lax.dot_general(one, key, COLS, preferred_element_type=F32)
                s = jnp.where(allowed, s * factor, -1e30)
                log_total = jnp.sum(
                    jnp.where(lane == 2 * p + h, lse[m], 0.0), axis=-1, keepdims=True
                )
                soft = jnp.exp(s - log_total)
                probs = soft.astype(BF16)
                one_grad = jnp.where(mask, grad, jnp.zeros_like(grad))
                dp = lax.dot_general(one_grad, value, COLS, preferred_element_type=F32)
                delta = jnp.sum(dp * soft, axis=-1, keepdims=True)
                ds = (soft * (dp - delta)).astype(BF16)
                dvs.append(lax.dot_general(probs, grad, ROWS, preferred_element_type=F32))
                dqs.append(jnp.dot(ds, key, preferred_element_type=F32))
                dks.append(lax.dot_general(ds, query, ROWS, preferred_element_type=F32))
            dq = jnp.where(low, dqs[0], dqs[1]) * factor
            dk = jnp.where(low, dks[0], dks[1]) * factor
            dj[m, 0, :, at] = turn(dq, tables, -1.0).astype(BF16)
            dj[m, 1, :, at] = turn(dk, tables, -1.0).astype(BF16)
            dj[m, 2, :, at] = jnp.where(low, dvs[0], dvs[1]).astype(BF16)

        loop(own // LANES, pair)
        store(dj, dj_o, m, 1)
        for part in range(3):
            sums = jnp.sum(dj[m, part].astype(F32), axis=0, keepdims=True)
            if m == 0:
                head_sums[part:part + 1, :] = sums
            else:
                head_sums[part:part + 1, :] += sums
        if m == 0:
            loads[1].wait()
            kept[2].wait()

        def up_tile(n):
            at = cols(n)
            acc = jnp.dot(gr[m], w2[:, at], preferred_element_type=F32)
            rounded = (acc * gp[m, :, at].astype(F32)).astype(BF16)
            up[m, :, at] = rounded
            sums = jnp.sum(rounded.astype(F32), axis=0, keepdims=True)
            if m == 0:
                up_sums[0:1, at] = sums
            else:
                up_sums[0:1, at] += sums

        loop(up.shape[2] // TILE, up_tile)
        store(up, up_o, m, 2)
        if m == 0:
            loads[2].wait()
            loads[3].wait()

        def norm_tile(n):
            at = cols(n)
            acc = lax.dot_general(up[m], w1[at, :], COLS, preferred_element_type=F32)
            for part in range(3):
                acc = acc + lax.dot_general(
                    dj[m, part], wq[part, at, :], COLS, preferred_element_type=F32
                )
            branch[m, :, at] = acc.astype(BF16)
            for copy in ring.scatter(branch, got, m, (rs_s, rs_r), at):
                copy.start()

        loop(width // TILE, norm_tile)

    def finish(m):
        for copy in ring.scatter(branch, got, m, (rs_s, rs_r)):
            copy.wait()
        if m == 0:
            kept[3].wait()
        grad_norm = ring.total(branch, got, m)
        unit, inv_root = stats(rin[m].astype(F32))
        scaled = grad_norm * vec[0:1, :]
        upstream = dyr[m].astype(F32)
        dx = upstream + inv_root * (
            scaled
            - jnp.mean(scaled, axis=-1, keepdims=True)
            - unit * jnp.mean(scaled * unit, axis=-1, keepdims=True)
        )
        out_f[m] = dx
        out_b[m] = dx.astype(BF16)

        @pl.when(second)
        def _():
            hop(m).start()

        store(out_f, dx_o, m, 3)
        for i, term in enumerate((grad_norm * unit, grad_norm, upstream)):
            sums = jnp.sum(term, axis=0, keepdims=True)
            if m == 0:
                own_sums[i:i + 1, :] = sums
            else:
                own_sums[i:i + 1, :] += sums

    @pl.when(second)
    def _():
        for m in range(micro):
            front(m)

    for m in range(micro):
        arrive(m)
        body(m)
    for m in range(micro):
        finish(m)
    for copy in stores:
        copy.wait()

    @pl.when(second)
    def _():
        for m in range(micro):
            hop(m).wait_send()


def backward(dy, weights, rows, qkv, lse, gp, vec, rope, segc, segr, nt):
    wq, wo, w1, w2 = weights
    micro, per, width = rows.shape
    length = per * nt
    own, hidden = wo.shape[1], w1.shape[1]
    anywhere = pl.BlockSpec(memory_space=pl.ANY)
    inside = pl.BlockSpec(memory_space=pltpu.VMEM)
    out_shape = [
        jax.ShapeDtypeStruct((micro, length, width), BF16),
        jax.ShapeDtypeStruct((micro, length, hidden), BF16),
        jax.ShapeDtypeStruct((micro, 3, length, own), BF16),
        jax.ShapeDtypeStruct(rows.shape, F32),
        jax.ShapeDtypeStruct((8, width), F32),
        jax.ShapeDtypeStruct((8, own), F32),
        jax.ShapeDtypeStruct((8, hidden), F32),
    ]
    dma = pltpu.SemaphoreType.DMA
    return pl.pallas_call(
        functools.partial(backward_kernel, nt),
        out_shape=out_shape,
        in_specs=[anywhere] * 9 + [inside] * 4,
        out_specs=[anywhere] * 4 + [inside] * 3,
        scratch_shapes=[
            pltpu.VMEM(wq.shape, BF16),
            pltpu.VMEM(wo.shape, BF16),
            pltpu.VMEM(w1.shape, BF16),
            pltpu.VMEM(w2.shape, BF16),
            pltpu.VMEM(rows.shape, BF16),
            pltpu.VMEM(rows.shape, BF16),
            pltpu.VMEM(qkv.shape, BF16),
            pltpu.VMEM(lse.shape, F32),
            pltpu.VMEM(gp.shape, BF16),
            pltpu.VMEM((micro, length, width), BF16),
            pltpu.VMEM((length, own), BF16),
            pltpu.VMEM((micro, length, hidden), BF16),
            pltpu.VMEM((micro, 3, length, own), BF16),
            pltpu.VMEM((micro, length, width), BF16),
            pltpu.VMEM((micro, nt, per, width), BF16),
            pltpu.VMEM(rows.shape, F32),
            pltpu.VMEM(rows.shape, BF16),
            dma((4,)),
            dma((5,)),
            dma((micro, 4)),
            dma((micro, nt)),
            dma((micro, nt)),
            dma((micro, nt)),
            dma((micro, nt)),
            dma((micro,)),
            dma((micro,)),
        ],
        compiler_params=pltpu.CompilerParams(
            collective_id=3, has_side_effects=True, vmem_limit_bytes=VMEM_LIMIT
        ),
        name="backward",
    )(dy, wq, wo, w1, w2, rows, qkv, lse, gp, vec, rope, segc, segr)


def padded(flat):
    size = -(-flat.shape[-1] // (8 * LANES)) * (8 * LANES)
    room = [(0, 0)] * (flat.ndim - 1) + [(0, size - flat.shape[-1])]
    flat = jnp.pad(flat, room)
    return flat.reshape(flat.shape[:-1] + (size // LANES, LANES))


def shards(
    ends_in, segments, ln_gain, ln_bias, w_qkv, w_out, w_fc1, w_fc2,
    bias_qkv, bias_out, bias_fc1, bias_fc2,
):
    nf, nt = lax.axis_size("fsdp"), lax.axis_size("tp")
    count = nf * nt
    section, tp_index = lax.axis_index("section"), lax.axis_index("tp")
    is_first = section == 0
    piece = ln_gain.shape[1]
    hidden_piece = bias_fc1.shape[1]
    own, hidden = w_out.shape[2], w_fc1.shape[2]
    width = piece * count

    pack = jnp.concatenate(
        [ln_gain[0], ln_bias[0], bias_out[0], bias_fc2[0], bias_qkv[0].reshape(-1), bias_fc1[0]]
    ).astype(F32)
    used = pack.shape[0]
    smalls = gather_small(padded(pack), nf, nt).reshape(count, -1)[:, :used]
    wide = smalls[:, :7 * piece].reshape(count, 7, piece).transpose(1, 0, 2).reshape(7, width)
    vec = jnp.stack([wide[0], wide[1], wide[2] + wide[3]])
    vec = jnp.pad(vec, ((0, 5), (0, 0)))
    qb = lax.dynamic_slice_in_dim(wide[4:7], tp_index * own, own, 1)
    qb = jnp.pad(qb, ((0, 5), (0, 0)))
    fb = lax.dynamic_slice_in_dim(smalls[:, 7 * piece:], tp_index * nf, nf, 0).reshape(1, hidden)
    fb = jnp.pad(fb, ((0, 7), (0, 0)))
    rope = rope_tables(segments)
    segc, segr = segments[:, :, None], segments[:, None, :]

    wq = lax.all_gather(w_qkv[0].transpose(1, 0, 2), "fsdp", axis=1, tiled=True)
    w1 = lax.all_gather(w_fc1[0], "fsdp", axis=0, tiled=True)
    wo = lax.all_gather(w_out[0], "fsdp", axis=0, tiled=True)
    w2 = lax.all_gather(w_fc2[0], "fsdp", axis=0, tiled=True)
    weights = (wq, wo, w1, w2)
    rows, xg, qkv, lse, att, gp, act, y = forward(
        ends_in[0], weights, vec, qb, fb, rope, segc, segr, nt
    )
    gr, up, dj, dx, own_sums, head_sums, up_sums = backward(
        ends_in[0], weights, rows, qkv, lse, gp, vec, rope, segc, segr, nt
    )

    def everywhere(arr):
        return lax.all_gather(arr, "fsdp", axis=arr.ndim - 2, tiled=True)

    def columns(arr):
        return lax.all_to_all(arr, "fsdp", split_axis=2, concat_axis=1, tiled=True)

    xc, gc = columns(xg), columns(gr)

    def product(left, right):
        return lax.dot_general(
            left, right, (((0, 1), (0, 1)), ((), ())), preferred_element_type=F32
        )

    act_all, att_all, up_all, dj_all = (everywhere(a) for a in (act, att, up, dj))
    grad_fc2 = product(gc, act_all)
    grad_out = product(gc, att_all)
    grad_fc1 = product(xc, up_all)
    grad_qkv = jnp.stack([product(xc, dj_all[:, part]) for part in range(3)], axis=1)

    mine = own_sums[:3].reshape(3, count, piece).transpose(1, 0, 2).reshape(count, 3 * piece)
    head = lax.dynamic_update_slice_in_dim(
        jnp.zeros((3, width), F32), head_sums[:3], tp_index * own, 1
    )
    head = head.reshape(3, count, piece).transpose(1, 0, 2).reshape(count, 3 * piece)
    ups = lax.dynamic_update_slice_in_dim(
        jnp.zeros((count, hidden_piece), F32),
        up_sums[0].reshape(nf, hidden_piece),
        tp_index * nf,
        0,
    )
    sums = sum_small(padded(jnp.concatenate([mine, head, ups], axis=1)), nf, nt).reshape(-1)
    gain_grad, bias_grad, row_grad = (sums[i * piece:(i + 1) * piece] for i in range(3))
    qkv_bias_grad = sums[3 * piece:6 * piece].reshape(3, piece)
    fc1_bias_grad = sums[6 * piece:6 * piece + hidden_piece]
    ends_out = jnp.where(is_first, dx, y)[None]
    return (
        ends_out,
        gain_grad[None],
        bias_grad[None],
        grad_qkv[None],
        grad_out[None],
        grad_fc1[None],
        grad_fc2[None],
        qkv_bias_grad[None],
        row_grad[None],
        fc1_bias_grad[None],
        row_grad[None],
    )


def solution(mesh):
    both = P("section", ("fsdp", "tp"))
    square = P("section", "fsdp", "tp")
    tokens = P("section", None, ("fsdp", "tp"), None)
    heads = P("section", "fsdp", None, "tp")
    bias3 = P("section", None, ("fsdp", "tp"))
    return jax.shard_map(
        shards,
        mesh=mesh,
        in_specs=(
            tokens, P(None, "fsdp"), both, both, heads, square, square, square,
            bias3, both, both, both,
        ),
        out_specs=(
            tokens, both, both, heads, square, square, square, bias3, both, both, both,
        ),
        check_vma=False,
    )
```

```python
import functools

import jax
import jax.numpy as jnp
from jax import lax
from jax.experimental import pallas as pl
from jax.experimental.pallas import tpu as pltpu
from jax.sharding import PartitionSpec as P

HEAD_DIM = 64
ROT_DIM = 32
EPSILON = 1e-05
LANES = 128
TILE = 256
MESH = pl.DeviceIdType.MESH
F32 = jnp.float32
BF16 = jnp.bfloat16
COLS = (((1,), (1,)), ((), ()))
ROWS = (((0,), (0,)), ((), ()))
VMEM_LIMIT = 62 * 1024 * 1024


def positions_of(segment_ids):
    length = segment_ids.shape[-1]
    places = jnp.arange(length, dtype=jnp.int32)
    before = jnp.concatenate([segment_ids[..., :1] - 1, segment_ids[..., :-1]], axis=-1)
    starts = jnp.where(segment_ids != before, places, 0)
    starts = lax.cummax(starts, axis=segment_ids.ndim - 1)
    return places - starts


def rope_tables(segments):
    half = ROT_DIM // 2
    freq = jnp.exp(-jnp.log(10000.0) * (2.0 * jnp.arange(half, dtype=F32)) / ROT_DIM)
    angles = positions_of(segments).astype(F32)[..., None] * freq
    cosine, sine = jnp.cos(angles), jnp.sin(angles)
    none = jnp.zeros_like(sine)
    rest = jnp.zeros(angles.shape[:-1] + (HEAD_DIM - ROT_DIM,), F32)
    keep = jnp.concatenate([cosine, cosine, rest + 1.0], axis=-1)
    ahead = jnp.concatenate([-sine, none, rest], axis=-1)
    behind = jnp.concatenate([none, sine, rest], axis=-1)
    tables = jnp.stack([keep, ahead, behind], axis=1)
    return jnp.concatenate([tables, tables], axis=-1)


def send(src, dst, send_sem, recv_sem, device):
    return pltpu.make_async_remote_copy(
        src_ref=src,
        dst_ref=dst,
        send_sem=send_sem,
        recv_sem=recv_sem,
        device_id=device,
        device_id_type=MESH,
    )


def greet(peers):
    barrier = pltpu.get_barrier_semaphore()
    for peer in peers:
        pl.semaphore_signal(barrier, inc=1, device_id=peer, device_id_type=MESH)
    pl.semaphore_wait(barrier, len(peers))


def group_peers(nf, nt):
    me = lax.axis_index("fsdp") * nt + lax.axis_index("tp")
    found = []
    for k in range(1, nf * nt):
        to = lax.rem(me + k, nf * nt)
        found.append((k, to, {"fsdp": to // nt, "tp": lax.rem(to, nt)}))
    return me, found


def gather_small_kernel(nf, nt, own, out, send_sems, recv_sems, local_sem):
    me, peers = group_peers(nf, nt)
    greet([peer for _, _, peer in peers])
    mine = pltpu.make_async_copy(own, out.at[me], local_sem)
    mine.start()
    copies = []
    for k, _, peer in peers:
        copy = send(own, out.at[me], send_sems.at[k], recv_sems.at[k], peer)
        copy.start()
        copies.append(copy)
    mine.wait()
    for copy in copies:
        copy.wait()


def gather_small(own, nf, nt):
    count = nf * nt
    return pl.pallas_call(
        functools.partial(gather_small_kernel, nf, nt),
        out_shape=jax.ShapeDtypeStruct((count,) + own.shape, own.dtype),
        in_specs=[pl.BlockSpec(memory_space=pltpu.VMEM)],
        out_specs=pl.BlockSpec(memory_space=pltpu.VMEM),
        scratch_shapes=[
            pltpu.SemaphoreType.DMA((count,)),
            pltpu.SemaphoreType.DMA((count,)),
            pltpu.SemaphoreType.DMA,
        ],
        compiler_params=pltpu.CompilerParams(collective_id=0, has_side_effects=True),
        name="gather_small",
    )(own)


def sum_small_kernel(nf, nt, own, out, got, send_sems, recv_sems):
    me, peers = group_peers(nf, nt)
    greet([peer for _, _, peer in peers])
    copies = []
    for k, to, peer in peers:
        copy = send(own.at[to], got.at[k], send_sems.at[k], recv_sems.at[k], peer)
        copy.start()
        copies.append(copy)
    total = own[me]
    for k, copy in enumerate(copies):
        copy.wait()
        total = total + got[k + 1]
    out[...] = total


def sum_small(own, nf, nt):
    count = nf * nt
    return pl.pallas_call(
        functools.partial(sum_small_kernel, nf, nt),
        out_shape=jax.ShapeDtypeStruct(own.shape[1:], own.dtype),
        in_specs=[pl.BlockSpec(memory_space=pltpu.VMEM)],
        out_specs=pl.BlockSpec(memory_space=pltpu.VMEM),
        scratch_shapes=[
            pltpu.VMEM(own.shape, own.dtype),
            pltpu.SemaphoreType.DMA((count,)),
            pltpu.SemaphoreType.DMA((count,)),
        ],
        compiler_params=pltpu.CompilerParams(collective_id=1, has_side_effects=True),
        name="sum_small",
    )(own)


def cols(n, width=TILE):
    return pl.ds(pl.multiple_of(n * width, width), width)


def loop(count, body):
    def step(i, carry):
        body(i)
        return carry

    lax.fori_loop(0, count, step, 0)


def turn(x, tables, sign):
    keep, ahead, behind = tables
    left = pltpu.roll(x, LANES - ROT_DIM // 2, 1)
    right = pltpu.roll(x, ROT_DIM // 2, 1)
    return x * keep + sign * (left * ahead + right * behind)


def low_half(length):
    return lax.broadcasted_iota(jnp.int32, (length, LANES), 1) < HEAD_DIM


def allowed_mask(segc, segr, m, length):
    query = lax.broadcasted_iota(jnp.int32, (length, length), 0)
    key = lax.broadcasted_iota(jnp.int32, (length, length), 1)
    return (query >= key) & (segc[m] == segr[m])


class Ring:
    def __init__(self, nt, rows):
        self.nt, self.rows = nt, rows
        self.me = lax.axis_index("tp")
        self.others = [(k, lax.rem(self.me + k, nt)) for k in range(1, nt)]

    def block(self, who):
        return pl.ds(pl.multiple_of(who * self.rows, self.rows), self.rows)

    def gather(self, buf, m, sems):
        return [
            send(
                buf.at[m, self.block(self.me)],
                buf.at[m, self.block(self.me)],
                sems[0].at[m, k],
                sems[1].at[m, k],
                {"tp": to},
            )
            for k, to in self.others
        ]

    def scatter(self, buf, got, m, sems, part=None):
        at = slice(None) if part is None else part
        return [
            send(
                buf.at[m, self.block(to), at],
                got.at[m, k, :, at],
                sems[0].at[m, k],
                sems[1].at[m, k],
                {"tp": to},
            )
            for k, to in self.others
        ]

    def total(self, buf, got, m):
        acc = buf[m, self.block(self.me)].astype(F32)
        for k, _ in self.others:
            acc = acc + got[m, k].astype(F32)
        return acc


def stats(rows):
    mean = jnp.mean(rows, axis=-1, keepdims=True)
    centred = rows - mean
    variance = jnp.mean(centred * centred, axis=-1, keepdims=True)
    inv_root = lax.rsqrt(variance + EPSILON)
    return centred * inv_root, inv_root


def forward_kernel(
    nt,
    rows_h, wq_h, wo_h, w1_h, w2_h, vec, qb, fb, rope, segc, segr,
    rows_o, xg_o, qkv_o, lse_o, att_o, gp_o, act_o, y_o,
    wq, wo, w1, w2, rin, xg, qkv, lse, att, gp, act, branch, got, out_f, out_b,
    w_sem, in_sem, o_sem, ag_s, ag_r, rs_s, rs_r, x_s, x_r,
):
    micro, length, width = xg.shape
    section = lax.axis_index("section")
    first, second = section == 0, section == 1
    ring = Ring(nt, length // nt)
    own = wo.shape[1]
    loads = []
    for i, (src, dst) in enumerate(((wq_h, wq), (w1_h, w1), (wo_h, wo), (w2_h, w2))):
        loads.append(pltpu.make_async_copy(src, dst, w_sem.at[i]))
        loads[-1].start()
    mine = pltpu.make_async_copy(rows_h, rin, in_sem)

    @pl.when(first)
    def _():
        mine.start()

    greet([{"tp": to} for _, to in ring.others] + [{"section": 1 - section}])

    @pl.when(first)
    def _():
        mine.wait()

    def hop(m):
        return send(out_b.at[m], rin.at[m], x_s.at[m], x_r.at[m], {"section": 1 - section})

    def front(m):
        unit, _ = stats(rin[m].astype(F32))
        normed = unit * vec[0:1, :] + vec[1:2, :]
        xg[m, ring.block(ring.me)] = normed.astype(BF16)
        for copy in ring.gather(xg, m, (ag_s, ag_r)):
            copy.start()

    def arrive(m):
        @pl.when(second)
        def _():
            hop(m).wait_recv()
            front(m)

    stores = []

    def store(src, dst, m, i):
        copy = pltpu.make_async_copy(src.at[m], dst.at[m], o_sem.at[m, i])
        copy.start()
        stores.append(copy)

    def body(m):
        for copy in ring.gather(xg, m, (ag_s, ag_r)):
            copy.wait()
        store(xg, xg_o, m, 0)
        store(rin, rows_o, m, 1)
        tables = (rope[m, 0], rope[m, 1], rope[m, 2])
        if m == 0:
            loads[0].wait()
        per = own // TILE
        for part in range(3):
            def qkv_tile(n, part=part):
                at = cols(n)
                acc = jnp.dot(xg[m], wq[part, :, at], preferred_element_type=F32)
                acc = acc + qb[part:part + 1, at]
                if part < 2:
                    acc = jnp.concatenate(
                        [
                            turn(acc[:, c:c + LANES], tables, 1.0)
                            for c in range(0, TILE, LANES)
                        ],
                        axis=1,
                    )
                qkv[m, part, :, at] = acc.astype(BF16)

            loop(per, qkv_tile)
        store(qkv, qkv_o, m, 2)
        allowed = allowed_mask(segc, segr, m, length)
        low = low_half(length)
        lane = lax.broadcasted_iota(jnp.int32, (length, LANES), 1)

        def pair(p):
            at = cols(p, LANES)
            query, key, value = qkv[m, 0, :, at], qkv[m, 1, :, at], qkv[m, 2, :, at]
            outs = []
            for h in range(2):
                mask = low if h == 0 else ~low
                one = jnp.where(mask, query, jnp.zeros_like(query))
                s = lax.dot_general(one, key, COLS, preferred_element_type=F32)
                s = jnp.where(allowed, s * HEAD_DIM ** (-0.5), -1e30)
                top = jnp.max(s, axis=-1, keepdims=True)
                e = jnp.exp(s - top)
                total = jnp.sum(e, axis=-1, keepdims=True)
                probs = (e / total).astype(BF16)
                outs.append(jnp.dot(probs, value, preferred_element_type=F32))
                lse[m] = jnp.where(lane == 2 * p + h, top + jnp.log(total), lse[m])
            att[m, :, at] = jnp.where(low, outs[0], outs[1]).astype(BF16)

        lse[m] = jnp.zeros((length, LANES), F32)
        loop(own // LANES, pair)
        store(lse, lse_o, m, 3)
        store(att, att_o, m, 4)
        if m == 0:
            loads[1].wait()

        def up_tile(n):
            at = cols(n)
            u = jnp.dot(xg[m], w1[:, at], preferred_element_type=F32) + fb[0:1, at]
            c = 0.7978845608028654
            square = u * u
            t = jnp.tanh(c * u * (1.0 + 0.044715 * square))
            act[m, :, at] = (0.5 * u * (1.0 + t)).astype(BF16)
            slope = 0.5 * (1.0 + t) + 0.5 * u * (1.0 - t * t) * (c * (1.0 + 3 * 0.044715 * square))
            gp[m, :, at] = slope.astype(BF16)

        loop(act.shape[2] // TILE, up_tile)
        store(act, act_o, m, 5)
        store(gp, gp_o, m, 6)
        if m == 0:
            loads[2].wait()
            loads[3].wait()

        def out_tile(n):
            at = cols(n)
            acc = lax.dot_general(att[m], wo[at, :], COLS, preferred_element_type=F32)
            acc = acc + lax.dot_general(act[m], w2[at, :], COLS, preferred_element_type=F32)
            branch[m, :, at] = acc.astype(BF16)
            for copy in ring.scatter(branch, got, m, (rs_s, rs_r), at):
                copy.start()

        loop(width // TILE, out_tile)

    def finish(m):
        for copy in ring.scatter(branch, got, m, (rs_s, rs_r)):
            copy.wait()
        y = rin[m].astype(F32) + ring.total(branch, got, m) + vec[2:3, :]
        out_f[m] = y
        out_b[m] = y.astype(BF16)
        store(out_f, y_o, m, 7)

        @pl.when(first)
        def _():
            hop(m).start()

    @pl.when(first)
    def _():
        for m in range(micro):
            front(m)

    for m in range(micro):
        arrive(m)
        body(m)
    for m in range(micro):
        finish(m)
    for copy in stores:
        copy.wait()

    @pl.when(first)
    def _():
        for m in range(micro):
            hop(m).wait_send()


def forward(rows, weights, vec, qb, fb, rope, segc, segr, nt):
    wq, wo, w1, w2 = weights
    micro, per, width = rows.shape
    length = per * nt
    own, hidden = wo.shape[1], w1.shape[1]
    anywhere = pl.BlockSpec(memory_space=pl.ANY)
    inside = pl.BlockSpec(memory_space=pltpu.VMEM)
    out_shape = [
        jax.ShapeDtypeStruct(rows.shape, BF16),
        jax.ShapeDtypeStruct((micro, length, width), BF16),
        jax.ShapeDtypeStruct((micro, 3, length, own), BF16),
        jax.ShapeDtypeStruct((micro, length, LANES), F32),
        jax.ShapeDtypeStruct((micro, length, own), BF16),
        jax.ShapeDtypeStruct((micro, length, hidden), BF16),
        jax.ShapeDtypeStruct((micro, length, hidden), BF16),
        jax.ShapeDtypeStruct(rows.shape, F32),
    ]
    dma = pltpu.SemaphoreType.DMA
    return pl.pallas_call(
        functools.partial(forward_kernel, nt),
        out_shape=out_shape,
        in_specs=[anywhere] * 5 + [inside] * 6,
        out_specs=[anywhere] * 8,
        scratch_shapes=[
            pltpu.VMEM(wq.shape, BF16),
            pltpu.VMEM(wo.shape, BF16),
            pltpu.VMEM(w1.shape, BF16),
            pltpu.VMEM(w2.shape, BF16),
            pltpu.VMEM(rows.shape, BF16),
            pltpu.VMEM((micro, length, width), BF16),
            pltpu.VMEM((micro, 3, length, own), BF16),
            pltpu.VMEM((micro, length, LANES), F32),
            pltpu.VMEM((micro, length, own), BF16),
            pltpu.VMEM((micro, length, hidden), BF16),
            pltpu.VMEM((micro, length, hidden), BF16),
            pltpu.VMEM((micro, length, width), BF16),
            pltpu.VMEM((micro, nt, per, width), BF16),
            pltpu.VMEM(rows.shape, F32),
            pltpu.VMEM(rows.shape, BF16),
            dma((4,)),
            dma,
            dma((micro, 8)),
            dma((micro, nt)),
            dma((micro, nt)),
            dma((micro, nt)),
            dma((micro, nt)),
            dma((micro,)),
            dma((micro,)),
        ],
        compiler_params=pltpu.CompilerParams(
            collective_id=2, has_side_effects=True, vmem_limit_bytes=VMEM_LIMIT
        ),
        name="forward",
    )(rows, wq, wo, w1, w2, vec, qb, fb, rope, segc, segr)


def backward_kernel(
    nt,
    dy_h, wq_h, wo_h, w1_h, w2_h, rows_h, qkv_h, lse_h, gp_h, vec, rope, segc, segr,
    gr_o, up_o, dj_o, dx_o, own_sums, head_sums, up_sums,
    wq, wo, w1, w2, dyr, rin, qkv, lse, gp, gr, gatt, up, dj, branch, got, out_f, out_b,
    w_sem, in_sem, o_sem, ag_s, ag_r, rs_s, rs_r, x_s, x_r,
):
    micro, length, width = gr.shape
    section = lax.axis_index("section")
    first, second = section == 0, section == 1
    ring = Ring(nt, length // nt)
    own = wo.shape[1]
    mine = pltpu.make_async_copy(dy_h, dyr, in_sem.at[4])

    @pl.when(second)
    def _():
        mine.start()

    loads = []
    for i, (src, dst) in enumerate(((wo_h, wo), (w2_h, w2), (wq_h, wq), (w1_h, w1))):
        loads.append(pltpu.make_async_copy(src, dst, w_sem.at[i]))
    kept = []
    for i, (src, dst) in enumerate(((qkv_h, qkv), (lse_h, lse), (gp_h, gp), (rows_h, rin))):
        kept.append(pltpu.make_async_copy(src, dst, in_sem.at[i]))
    for copy in (loads[0], kept[0], kept[1], loads[1], kept[2], loads[2], loads[3], kept[3]):
        copy.start()
    greet([{"tp": to} for _, to in ring.others] + [{"section": 1 - section}])

    @pl.when(second)
    def _():
        mine.wait()

    def hop(m):
        return send(out_b.at[m], dyr.at[m], x_s.at[m], x_r.at[m], {"section": 1 - section})

    def front(m):
        gr[m, ring.block(ring.me)] = dyr[m]
        for copy in ring.gather(gr, m, (ag_s, ag_r)):
            copy.start()

    def arrive(m):
        @pl.when(first)
        def _():
            hop(m).wait_recv()
            front(m)

    stores = []

    def store(src, dst, m, i):
        copy = pltpu.make_async_copy(src.at[m], dst.at[m], o_sem.at[m, i])
        copy.start()
        stores.append(copy)

    def body(m):
        for copy in ring.gather(gr, m, (ag_s, ag_r)):
            copy.wait()
        store(gr, gr_o, m, 0)
        if m == 0:
            loads[0].wait()

        def att_tile(n):
            at = cols(n)
            gatt[:, at] = jnp.dot(gr[m], wo[:, at], preferred_element_type=F32).astype(BF16)

        loop(own // TILE, att_tile)
        if m == 0:
            kept[0].wait()
            kept[1].wait()
        tables = (rope[m, 0], rope[m, 1], rope[m, 2])
        allowed = allowed_mask(segc, segr, m, length)
        low = low_half(length)
        lane = lax.broadcasted_iota(jnp.int32, (length, LANES), 1)
        factor = HEAD_DIM ** (-0.5)

        def pair(p):
            at = cols(p, LANES)
            query, key, value = qkv[m, 0, :, at], qkv[m, 1, :, at], qkv[m, 2, :, at]
            grad = gatt[:, at]
            dqs, dks, dvs = [], [], []
            for h in range(2):
                mask = low if h == 0 else ~low
                one = jnp.where(mask, query, jnp.zeros_like(query))
                s = lax.dot_general(one, key, COLS, preferred_element_type=F32)
                s = jnp.where(allowed, s * factor, -1e30)
                log_total = jnp.sum(
                    jnp.where(lane == 2 * p + h, lse[m], 0.0), axis=-1, keepdims=True
                )
                soft = jnp.exp(s - log_total)
                probs = soft.astype(BF16)
                one_grad = jnp.where(mask, grad, jnp.zeros_like(grad))
                dp = lax.dot_general(one_grad, value, COLS, preferred_element_type=F32)
                delta = jnp.sum(dp * soft, axis=-1, keepdims=True)
                ds = (soft * (dp - delta)).astype(BF16)
                dvs.append(lax.dot_general(probs, grad, ROWS, preferred_element_type=F32))
                dqs.append(jnp.dot(ds, key, preferred_element_type=F32))
                dks.append(lax.dot_general(ds, query, ROWS, preferred_element_type=F32))
            dq = jnp.where(low, dqs[0], dqs[1]) * factor
            dk = jnp.where(low, dks[0], dks[1]) * factor
            dj[m, 0, :, at] = turn(dq, tables, -1.0).astype(BF16)
            dj[m, 1, :, at] = turn(dk, tables, -1.0).astype(BF16)
            dj[m, 2, :, at] = jnp.where(low, dvs[0], dvs[1]).astype(BF16)

        loop(own // LANES, pair)
        store(dj, dj_o, m, 1)
        for part in range(3):
            sums = jnp.sum(dj[m, part].astype(F32), axis=0, keepdims=True)
            if m == 0:
                head_sums[part:part + 1, :] = sums
            else:
                head_sums[part:part + 1, :] += sums
        if m == 0:
            loads[1].wait()
            kept[2].wait()

        def up_tile(n):
            at = cols(n)
            acc = jnp.dot(gr[m], w2[:, at], preferred_element_type=F32)
            rounded = (acc * gp[m, :, at].astype(F32)).astype(BF16)
            up[m, :, at] = rounded
            sums = jnp.sum(rounded.astype(F32), axis=0, keepdims=True)
            if m == 0:
                up_sums[0:1, at] = sums
            else:
                up_sums[0:1, at] += sums

        loop(up.shape[2] // TILE, up_tile)
        store(up, up_o, m, 2)
        if m == 0:
            loads[2].wait()
            loads[3].wait()

        def norm_tile(n):
            at = cols(n)
            acc = lax.dot_general(up[m], w1[at, :], COLS, preferred_element_type=F32)
            for part in range(3):
                acc = acc + lax.dot_general(
                    dj[m, part], wq[part, at, :], COLS, preferred_element_type=F32
                )
            branch[m, :, at] = acc.astype(BF16)
            for copy in ring.scatter(branch, got, m, (rs_s, rs_r), at):
                copy.start()

        loop(width // TILE, norm_tile)

    def finish(m):
        for copy in ring.scatter(branch, got, m, (rs_s, rs_r)):
            copy.wait()
        if m == 0:
            kept[3].wait()
        grad_norm = ring.total(branch, got, m)
        unit, inv_root = stats(rin[m].astype(F32))
        scaled = grad_norm * vec[0:1, :]
        upstream = dyr[m].astype(F32)
        dx = upstream + inv_root * (
            scaled
            - jnp.mean(scaled, axis=-1, keepdims=True)
            - unit * jnp.mean(scaled * unit, axis=-1, keepdims=True)
        )
        out_f[m] = dx
        out_b[m] = dx.astype(BF16)

        @pl.when(second)
        def _():
            hop(m).start()

        store(out_f, dx_o, m, 3)
        for i, term in enumerate((grad_norm * unit, grad_norm, upstream)):
            sums = jnp.sum(term, axis=0, keepdims=True)
            if m == 0:
                own_sums[i:i + 1, :] = sums
            else:
                own_sums[i:i + 1, :] += sums

    @pl.when(second)
    def _():
        for m in range(micro):
            front(m)

    for m in range(micro):
        arrive(m)
        body(m)
    for m in range(micro):
        finish(m)
    for copy in stores:
        copy.wait()

    @pl.when(second)
    def _():
        for m in range(micro):
            hop(m).wait_send()


def backward(dy, weights, rows, qkv, lse, gp, vec, rope, segc, segr, nt):
    wq, wo, w1, w2 = weights
    micro, per, width = rows.shape
    length = per * nt
    own, hidden = wo.shape[1], w1.shape[1]
    anywhere = pl.BlockSpec(memory_space=pl.ANY)
    inside = pl.BlockSpec(memory_space=pltpu.VMEM)
    out_shape = [
        jax.ShapeDtypeStruct((micro, length, width), BF16),
        jax.ShapeDtypeStruct((micro, length, hidden), BF16),
        jax.ShapeDtypeStruct((micro, 3, length, own), BF16),
        jax.ShapeDtypeStruct(rows.shape, F32),
        jax.ShapeDtypeStruct((8, width), F32),
        jax.ShapeDtypeStruct((8, own), F32),
        jax.ShapeDtypeStruct((8, hidden), F32),
    ]
    dma = pltpu.SemaphoreType.DMA
    return pl.pallas_call(
        functools.partial(backward_kernel, nt),
        out_shape=out_shape,
        in_specs=[anywhere] * 9 + [inside] * 4,
        out_specs=[anywhere] * 4 + [inside] * 3,
        scratch_shapes=[
            pltpu.VMEM(wq.shape, BF16),
            pltpu.VMEM(wo.shape, BF16),
            pltpu.VMEM(w1.shape, BF16),
            pltpu.VMEM(w2.shape, BF16),
            pltpu.VMEM(rows.shape, BF16),
            pltpu.VMEM(rows.shape, BF16),
            pltpu.VMEM(qkv.shape, BF16),
            pltpu.VMEM(lse.shape, F32),
            pltpu.VMEM(gp.shape, BF16),
            pltpu.VMEM((micro, length, width), BF16),
            pltpu.VMEM((length, own), BF16),
            pltpu.VMEM((micro, length, hidden), BF16),
            pltpu.VMEM((micro, 3, length, own), BF16),
            pltpu.VMEM((micro, length, width), BF16),
            pltpu.VMEM((micro, nt, per, width), BF16),
            pltpu.VMEM(rows.shape, F32),
            pltpu.VMEM(rows.shape, BF16),
            dma((4,)),
            dma((5,)),
            dma((micro, 4)),
            dma((micro, nt)),
            dma((micro, nt)),
            dma((micro, nt)),
            dma((micro, nt)),
            dma((micro,)),
            dma((micro,)),
        ],
        compiler_params=pltpu.CompilerParams(
            collective_id=3, has_side_effects=True, vmem_limit_bytes=VMEM_LIMIT
        ),
        name="backward",
    )(dy, wq, wo, w1, w2, rows, qkv, lse, gp, vec, rope, segc, segr)


ROWS_OF_PACK = 16


def masks_of(nf):
    return range(nf)


def bits_below(mask, nf):
    low = mask & -mask if mask else nf
    return [(i, 1 << i) for i in range(nf.bit_length() - 1) if (1 << i) < low]


def flipped(index, mask, nf):
    for i in range(nf.bit_length() - 1):
        if mask >> i & 1:
            index = index + (1 << i) * (1 - 2 * lax.rem(index // (1 << i), 2))
    return index


def fused_kernel(
    nf, nt,
    ends_h, pack, wq_h, wo_h, w1_h, w2_h, rope, segc, segr,
    ends_o, sums_o, act_x, att_x, up_x, dj_x, xc_x, gc_x,
    wq, wo, w1, w2, packs, wide, fb, rin, dyr, xg, qkv, lse, att, gp, act,
    gr, gatt, up, dj, out_bf, out_got, in_bf, in_got, y_f, y_b, dx_f, dx_b,
    own_sums, head_sums, up_sums, s_src, s_got,
    in_sem, wl_sem, ws_sem, wr_sem, pk_s, pk_r, sm_s, sm_r,
    ag_s, ag_r, gg_s, gg_r, rs_s, rs_r, rb_s, rb_r, hx_s, hx_r, hb_s, hb_r,
    xl_sem, xs_s, xs_r, cl_sem, ca_s, ca_r, o_sem,
):
    micro, length, width = xg.shape
    section, f, t = (lax.axis_index(a) for a in ("section", "fsdp", "tp"))
    first, second = section == 0, section == 1
    ring = Ring(nt, length // nt)
    own, hidden = wo.shape[1], w1.shape[1]
    depth = width // nf
    count = nf * nt
    other = {"section": 1 - section}
    me, group = group_peers(nf, nt)
    fblock = [flipped(f, mask, nf) for mask in masks_of(nf)]

    def rows_at(block):
        return pl.ds(pl.multiple_of(block * depth, depth), depth)

    load_rows = pltpu.make_async_copy(ends_h, rin, in_sem)
    load_dy = pltpu.make_async_copy(ends_h, dyr, in_sem)

    @pl.when(first)
    def _():
        load_rows.start()

    @pl.when(second)
    def _():
        load_dy.start()

    greet([peer for _, _, peer in group] + [other])

    pack_local = pltpu.make_async_copy(pack, packs.at[me], pk_s.at[0])
    pack_copies = [
        send(pack, packs.at[me], pk_s.at[k], pk_r.at[k], peer) for k, _, peer in group
    ]
    pack_local.start()
    for copy in pack_copies:
        copy.start()

    table = ((wq_h, wq), (w1_h, w1), (wo_h, wo), (w2_h, w2))

    def w_at(ref, block):
        return ref.at[:, rows_at(block), :] if len(ref.shape) == 3 else ref.at[rows_at(block), :]

    def w_local(a):
        return pltpu.make_async_copy(table[a][0], w_at(table[a][1], f), wl_sem.at[a])

    def w_send(a, mask, i, bit):
        block = w_at(table[a][1], fblock[mask])
        src = table[a][0] if mask == 0 else block
        peer = {"fsdp": flipped(f, bit, nf)}
        return send(src, block, ws_sem.at[a, mask, i], wr_sem.at[a, mask | bit], peer)

    def w_recv(a, mask):
        block = w_at(table[a][1], fblock[mask])
        return send(block, block, ws_sem.at[a, mask, 0], wr_sem.at[a, mask], other)

    def w_start(a):
        w_local(a).start()
        for i, bit in reversed(bits_below(0, nf)):
            w_send(a, 0, i, bit).start()

    def w_ready(a, mask):
        if mask == 0:
            w_local(a).wait()
            return
        w_recv(a, mask).wait_recv()
        for i, bit in bits_below(mask, nf):
            w_send(a, mask, i, bit).start()

    order = sorted(masks_of(nf), key=lambda m: (m != 0, -(m & -m), m))
    out_order = list(masks_of(nf))
    w_start(0)
    w_start(1)

    pack_local.wait()
    for copy in pack_copies:
        copy.wait()
    for j in range(count):
        wide[:, j * LANES:(j + 1) * LANES] = packs[j]
    per_row = hidden // nf // LANES
    for j in range(nf):
        for r in range(per_row):
            c = (j * per_row + r) * LANES
            fb[0:1, c:c + LANES] = packs[t * nf + j, 6 + r:7 + r, :]

    def hop_out(m):
        return send(y_b.at[m], rin.at[m], hx_s.at[m], hx_r.at[m], other)

    def hop_back(m):
        return send(dx_b.at[m], dyr.at[m], hb_s.at[m], hb_r.at[m], other)

    def front(m):
        unit, _ = stats(rin[m].astype(F32))
        normed = unit * wide[0:1, :] + wide[1:2, :]
        xg[m, ring.block(ring.me)] = normed.astype(BF16)
        for copy in ring.gather(xg, m, (ag_s, ag_r)):
            copy.start()

    def front_back(m):
        gr[m, ring.block(ring.me)] = dyr[m]
        for copy in ring.gather(gr, m, (gg_s, gg_r)):
            copy.start()

    def x_dst(a, m, block):
        if a == 3:
            return dj_x.at[:, m, block]
        return (act_x, att_x, up_x)[a].at[m, block]

    def x_src(a, m):
        return (act, att, up, dj)[a].at[m]

    def x_local(a, m):
        return pltpu.make_async_copy(x_src(a, m), x_dst(a, m, f), xl_sem.at[a, m])

    def x_send(a, m, mask, i, bit):
        block = x_dst(a, m, fblock[mask])
        src = x_src(a, m) if mask == 0 else block
        peer = {"fsdp": flipped(f, bit, nf)}
        return send(src, block, xs_s.at[a, m, mask, i], xs_r.at[a, m, mask | bit], peer)

    def x_recv(a, m, mask):
        block = x_dst(a, m, fblock[mask])
        return send(block, block, xs_s.at[a, m, mask, 0], xs_r.at[a, m, mask], other)

    def x_start(a, m):
        x_local(a, m).start()
        for i, bit in reversed(bits_below(0, nf)):
            x_send(a, m, 0, i, bit).start()

    def x_relay(a, m):
        for mask in order[1:]:
            x_recv(a, m, mask).wait_recv()
            for i, bit in bits_below(mask, nf):
                x_send(a, m, mask, i, bit).start()

    def x_done(a, m):
        x_local(a, m).wait()
        for mask in masks_of(nf):
            for i, bit in bits_below(mask, nf):
                x_send(a, m, mask, i, bit).wait_send()

    def c_copies(which, m):
        src, dst = ((xg, xc_x), (gr, gc_x))[which]
        copies = []
        for k in range(1, nf):
            to = lax.rem(f + k, nf)
            copies.append(
                send(
                    src.at[m, :, rows_at(to)],
                    dst.at[m, f],
                    ca_s.at[which, m, k],
                    ca_r.at[which, m, k],
                    {"fsdp": to},
                )
            )
        return copies

    def c_local(which, m):
        src, dst = ((xg, xc_x), (gr, gc_x))[which]
        return pltpu.make_async_copy(src.at[m, :, rows_at(f)], dst.at[m, f], cl_sem.at[which, m])

    def c_start(which, m):
        c_local(which, m).start()
        for copy in c_copies(which, m):
            copy.start()

    def attention_masks(m):
        low = low_half(length)
        lane = lax.broadcasted_iota(jnp.int32, (length, LANES), 1)
        tables = (rope[m, 0], rope[m, 1], rope[m, 2])
        return low, lane, tables, allowed_mask(segc, segr, m, length)

    factor = HEAD_DIM ** (-0.5)

    def forward_stage(m, fresh):
        for copy in ring.gather(xg, m, (ag_s, ag_r)):
            copy.wait()
        c_start(0, m)

        @pl.when(fresh)
        def _():
            for mask in order:
                w_ready(0, mask)
            w_start(2)
            w_start(3)

        low, lane, tables, allowed = attention_masks(m)
        for part in range(3):
            def qkv_tile(n, part=part):
                at = cols(n)
                acc = jnp.dot(xg[m], wq[part, :, at], preferred_element_type=F32)
                acc = acc + wide[3 + part:4 + part, pl.ds(
                    pl.multiple_of(t * own + n * TILE, TILE), TILE)]
                if part < 2:
                    acc = jnp.concatenate(
                        [
                            turn(acc[:, c:c + LANES], tables, 1.0)
                            for c in range(0, TILE, LANES)
                        ],
                        axis=1,
                    )
                qkv[m, part, :, at] = acc.astype(BF16)

            loop(own // TILE, qkv_tile)

        def pair(p):
            at = cols(p, LANES)
            query, key, value = qkv[m, 0, :, at], qkv[m, 1, :, at], qkv[m, 2, :, at]
            outs = []
            for h in range(2):
                mask = low if h == 0 else ~low
                one = jnp.where(mask, query, jnp.zeros_like(query))
                s = lax.dot_general(one, key, COLS, preferred_element_type=F32)
                s = jnp.where(allowed, s * factor, -1e30)
                top = jnp.max(s, axis=-1, keepdims=True)
                e = jnp.exp(s - top)
                total = jnp.sum(e, axis=-1, keepdims=True)
                probs = (e / total).astype(BF16)
                outs.append(jnp.dot(probs, value, preferred_element_type=F32))
                lse[m] = jnp.where(lane == 2 * p + h, top + jnp.log(total), lse[m])
            att[m, :, at] = jnp.where(low, outs[0], outs[1]).astype(BF16)

        lse[m] = jnp.zeros((length, LANES), F32)
        loop(own // LANES, pair)
        x_start(1, m)

        @pl.when(fresh)
        def _():
            for mask in order:
                w_ready(1, mask)

        def up_tile(n):
            at = cols(n)
            u = jnp.dot(xg[m], w1[:, at], preferred_element_type=F32) + fb[0:1, at]
            c = 0.7978845608028654
            square = u * u
            th = jnp.tanh(c * u * (1.0 + 0.044715 * square))
            act[m, :, at] = (0.5 * u * (1.0 + th)).astype(BF16)
            slope = 0.5 * (1.0 + th)
            slope = slope + 0.5 * u * (1.0 - th * th) * (c * (1.0 + 3 * 0.044715 * square))
            gp[m, :, at] = slope.astype(BF16)

        loop(hidden // TILE, up_tile)
        x_start(0, m)

    def output_stage(m, fresh):
        for mask in out_order:
            @pl.when(fresh)
            def _(mask=mask):
                w_ready(2, mask)
                w_ready(3, mask)

            def out_tile(n, mask=mask):
                start = pl.multiple_of(fblock[mask] * depth + n * TILE, TILE)
                at = pl.ds(start, TILE)
                acc = lax.dot_general(att[m], wo[at, :], COLS, preferred_element_type=F32)
                acc = acc + lax.dot_general(act[m], w2[at, :], COLS, preferred_element_type=F32)
                out_bf[m, :, at] = acc.astype(BF16)
                for copy in ring.scatter(out_bf, out_got, m, (rs_s, rs_r), at):
                    copy.start()

            loop(depth // TILE, out_tile)

    def store_ends(src, m):
        return pltpu.make_async_copy(src.at[m], ends_o.at[m], o_sem.at[m])

    def output_finish(m):
        for copy in ring.scatter(out_bf, out_got, m, (rs_s, rs_r)):
            copy.wait()
        y = rin[m].astype(F32) + ring.total(out_bf, out_got, m) + wide[2:3, :]
        y_b[m] = y.astype(BF16)

        @pl.when(first)
        def _():
            hop_out(m).start()

        @pl.when(second)
        def _():
            y_f[m] = y
            store_ends(y_f, m).start()

    def backward_stage(m, k):
        @pl.when(first)
        def _():
            for copy in ring.gather(gr, m, (gg_s, gg_r)):
                copy.wait()
            c_start(1, m)

        def att_tile(n):
            at = cols(n)
            gatt[:, at] = jnp.dot(gr[m], wo[:, at], preferred_element_type=F32).astype(BF16)

        loop(own // TILE, att_tile)
        low, lane, tables, allowed = attention_masks(m)

        def pair(p):
            at = cols(p, LANES)
            query, key, value = qkv[m, 0, :, at], qkv[m, 1, :, at], qkv[m, 2, :, at]
            grad = gatt[:, at]
            dqs, dks, dvs = [], [], []
            for h in range(2):
                mask = low if h == 0 else ~low
                one = jnp.where(mask, query, jnp.zeros_like(query))
                s = lax.dot_general(one, key, COLS, preferred_element_type=F32)
                s = jnp.where(allowed, s * factor, -1e30)
                log_total = jnp.sum(
                    jnp.where(lane == 2 * p + h, lse[m], 0.0), axis=-1, keepdims=True
                )
                soft = jnp.exp(s - log_total)
                probs = soft.astype(BF16)
                one_grad = jnp.where(mask, grad, jnp.zeros_like(grad))
                dp = lax.dot_general(one_grad, value, COLS, preferred_element_type=F32)
                delta = jnp.sum(dp * soft, axis=-1, keepdims=True)
                ds = (soft * (dp - delta)).astype(BF16)
                dvs.append(lax.dot_general(probs, grad, ROWS, preferred_element_type=F32))
                dqs.append(jnp.dot(ds, key, preferred_element_type=F32))
                dks.append(lax.dot_general(ds, query, ROWS, preferred_element_type=F32))
            dq = jnp.where(low, dqs[0], dqs[1]) * factor
            dk = jnp.where(low, dks[0], dks[1]) * factor
            dj[m, 0, :, at] = turn(dq, tables, -1.0).astype(BF16)
            dj[m, 1, :, at] = turn(dk, tables, -1.0).astype(BF16)
            dj[m, 2, :, at] = jnp.where(low, dvs[0], dvs[1]).astype(BF16)

        loop(own // LANES, pair)
        x_start(3, m)

        @pl.when(second & (k == 3))
        def _():
            backward_finish(0)

        for part in range(3):
            head_sums[part:part + 1, :] += jnp.sum(
                dj[m, part].astype(F32), axis=0, keepdims=True
            )

        def up_tile(n):
            at = cols(n)
            acc = jnp.dot(gr[m], w2[:, at], preferred_element_type=F32)
            rounded = (acc * gp[m, :, at].astype(F32)).astype(BF16)
            up[m, :, at] = rounded
            up_sums[0:1, at] += jnp.sum(rounded.astype(F32), axis=0, keepdims=True)

        loop(hidden // TILE, up_tile)
        x_start(2, m)

        @pl.when(first & (k == 2))
        def _():
            hop_back(1).wait_recv()
            front_back(1)

        def norm_tile(n):
            at = cols(n)
            acc = lax.dot_general(up[m], w1[at, :], COLS, preferred_element_type=F32)
            for part in range(3):
                acc = acc + lax.dot_general(
                    dj[m, part], wq[part, at, :], COLS, preferred_element_type=F32
                )
            in_bf[m, :, at] = acc.astype(BF16)
            for copy in ring.scatter(in_bf, in_got, m, (rb_s, rb_r), at):
                copy.start()

        loop(width // TILE, norm_tile)

    def backward_finish(m):
        for copy in ring.scatter(in_bf, in_got, m, (rb_s, rb_r)):
            copy.wait()
        grad_norm = ring.total(in_bf, in_got, m)
        unit, inv_root = stats(rin[m].astype(F32))
        scaled = grad_norm * wide[0:1, :]
        upstream = dyr[m].astype(F32)
        dx = upstream + inv_root * (
            scaled
            - jnp.mean(scaled, axis=-1, keepdims=True)
            - unit * jnp.mean(scaled * unit, axis=-1, keepdims=True)
        )
        dx_b[m] = dx.astype(BF16)

        @pl.when(second)
        def _():
            hop_back(m).start()

        @pl.when(first)
        def _():
            dx_f[m] = dx
            store_ends(dx_f, m).start()

        for i, term in enumerate((grad_norm * unit, grad_norm, upstream)):
            own_sums[i:i + 1, :] += jnp.sum(term, axis=0, keepdims=True)

    own_sums[...] = jnp.zeros_like(own_sums)
    head_sums[...] = jnp.zeros_like(head_sums)
    up_sums[...] = jnp.zeros_like(up_sums)

    @pl.when(first)
    def _():
        load_rows.wait()
        loop(micro, front)

    @pl.when(second)
    def _():
        load_dy.wait()
        loop(micro, front_back)
        for mask in order:
            w_ready(0, mask)
        w_start(2)
        w_start(3)
        for a in (1, 2, 3):
            for mask in order:
                w_ready(a, mask)

        def columns_out(m):
            for copy in ring.gather(gr, m, (gg_s, gg_r)):
                copy.wait()
            c_start(1, m)

        loop(micro, columns_out)

    def slot(k):
        is_f = jnp.where(first, k < 2, (k == 0) | (k == 2))
        is_b = jnp.where(first, (k == 2) | (k == 3), (k == 1) | (k == 3))
        is_o = jnp.where(first, k < 2, k >= 4)
        fresh = first & (k == 0)
        m = jnp.where(first | (k >= 4), lax.rem(k, 2), k // 2)

        @pl.when(second & (k < 2))
        def _():
            hop_out(k).wait_recv()
            front(k)

        @pl.when(first & (k == 2))
        def _():
            for i in range(micro):
                for a in (1, 0):
                    x_relay(a, i)
            hop_back(0).wait_recv()
            front_back(0)

        @pl.when(is_f)
        def _():
            forward_stage(m, fresh)

        @pl.when(is_o)
        def _():
            output_stage(m, fresh)

        @pl.when(is_b)
        def _():
            backward_stage(m, k)

        @pl.when((first & (k == 1)) | (second & (k == 5)))
        def _():
            loop(micro, output_finish)

        @pl.when(first & (k == 3))
        def _():
            backward_finish(0)

        @pl.when(k == 3)
        def _():
            backward_finish(1)

    loop(6, slot)

    s_src[...] = jnp.zeros_like(s_src)
    for j in range(count):
        s_src[j, 0:3, :] = own_sums[0:3, j * LANES:(j + 1) * LANES]
    for j in range(nf):
        s_src[t * nf + j, 3:6, :] = head_sums[0:3, j * LANES:(j + 1) * LANES]
        for r in range(per_row):
            c = (j * per_row + r) * LANES
            s_src[t * nf + j, 6 + r:7 + r, :] = up_sums[0:1, c:c + LANES]
    small = [
        send(s_src.at[to], s_got.at[k], sm_s.at[k], sm_r.at[k], peer) for k, to, peer in group
    ]
    for copy in small:
        copy.start()

    @pl.when(second)
    def _():
        for a, m in ((1, 0), (0, 0), (3, 0), (2, 0), (1, 1), (0, 1), (3, 1), (2, 1)):
            x_relay(a, m)
        for m in range(micro):
            hop_back(m).wait_send()

    @pl.when(first)
    def _():
        for a, m in ((3, 0), (2, 0), (3, 1), (2, 1)):
            x_relay(a, m)
        for m in range(micro):
            hop_out(m).wait_send()

    total = s_src[me]
    for k, copy in enumerate(small):
        copy.wait()
        total = total + s_got[k + 1]
    sums_o[...] = total
    for m in range(micro):
        for a in range(4):
            x_done(a, m)
        for which in range(2):
            c_local(which, m).wait()
            for copy in c_copies(which, m):
                copy.wait()
        store_ends(y_f, m).wait()
    for a in range(4):
        for mask in masks_of(nf):
            for i, bit in bits_below(mask, nf):
                w_send(a, mask, i, bit).wait_send()


def fused(ends, pack, wq, wo, w1, w2, rope, segc, segr, nf, nt):
    micro, per, width = ends.shape
    length = per * nt
    own, hidden = wo.shape[1], w1.shape[1]
    depth = width // nf
    count = nf * nt
    bits = nf.bit_length() - 1
    anywhere = pl.BlockSpec(memory_space=pl.ANY)
    inside = pl.BlockSpec(memory_space=pltpu.VMEM)
    dma = pltpu.SemaphoreType.DMA
    vm = pltpu.VMEM
    small = (count,) + pack.shape
    tokens = (micro, length)
    out_shape = [
        jax.ShapeDtypeStruct(ends.shape, F32),
        jax.ShapeDtypeStruct(pack.shape, F32),
        jax.ShapeDtypeStruct((micro, nf, length, hidden), BF16),
        jax.ShapeDtypeStruct((micro, nf, length, own), BF16),
        jax.ShapeDtypeStruct((micro, nf, length, hidden), BF16),
        jax.ShapeDtypeStruct((3, micro, nf, length, own), BF16),
        jax.ShapeDtypeStruct((micro, nf, length, depth), BF16),
        jax.ShapeDtypeStruct((micro, nf, length, depth), BF16),
    ]
    scratch = [
        vm((3, width, own), BF16), vm((width, own), BF16),
        vm((width, hidden), BF16), vm((width, hidden), BF16),
        vm(small, F32), vm((pack.shape[0], width), F32), vm((8, hidden), F32),
        vm(ends.shape, BF16), vm(ends.shape, BF16),
        vm(tokens + (width,), BF16), vm((micro, 3, length, own), BF16),
        vm(tokens + (LANES,), F32), vm(tokens + (own,), BF16),
        vm(tokens + (hidden,), BF16), vm(tokens + (hidden,), BF16),
        vm(tokens + (width,), BF16), vm((length, own), BF16),
        vm(tokens + (hidden,), BF16), vm((micro, 3, length, own), BF16),
        vm(tokens + (width,), BF16), vm((micro, nt, per, width), BF16),
        vm(tokens + (width,), BF16), vm((micro, nt, per, width), BF16),
        vm(ends.shape, F32), vm(ends.shape, BF16),
        vm(ends.shape, F32), vm(ends.shape, BF16),
        vm((8, width), F32), vm((8, own), F32), vm((8, hidden), F32),
        vm(small, F32), vm(small, F32),
        dma, dma((4,)), dma((4, nf, bits)), dma((4, nf)),
        dma((count,)), dma((count,)), dma((count,)), dma((count,)),
        dma((micro, nt)), dma((micro, nt)), dma((micro, nt)), dma((micro, nt)),
        dma((micro, nt)), dma((micro, nt)), dma((micro, nt)), dma((micro, nt)),
        dma((micro,)), dma((micro,)), dma((micro,)), dma((micro,)),
        dma((4, micro)), dma((4, micro, nf, bits)), dma((4, micro, nf)),
        dma((2, micro)), dma((2, micro, nf)), dma((2, micro, nf)), dma((micro,)),
    ]
    return pl.pallas_call(
        functools.partial(fused_kernel, nf, nt),
        out_shape=out_shape,
        in_specs=[anywhere, inside] + [anywhere] * 4 + [inside] * 3,
        out_specs=[anywhere, inside] + [anywhere] * 6,
        scratch_shapes=scratch,
        compiler_params=pltpu.CompilerParams(
            collective_id=4, has_side_effects=True, vmem_limit_bytes=VMEM_LIMIT
        ),
        name="fused",
    )(ends, pack, wq, wo, w1, w2, rope, segc, segr)


def padded(flat):
    size = -(-flat.shape[-1] // (8 * LANES)) * (8 * LANES)
    room = [(0, 0)] * (flat.ndim - 1) + [(0, size - flat.shape[-1])]
    flat = jnp.pad(flat, room)
    return flat.reshape(flat.shape[:-1] + (size // LANES, LANES))


def split_shards(
    ends_in, segments, ln_gain, ln_bias, w_qkv, w_out, w_fc1, w_fc2,
    bias_qkv, bias_out, bias_fc1, bias_fc2,
):
    nf, nt = lax.axis_size("fsdp"), lax.axis_size("tp")
    count = nf * nt
    section, tp_index = lax.axis_index("section"), lax.axis_index("tp")
    is_first = section == 0
    piece = ln_gain.shape[1]
    hidden_piece = bias_fc1.shape[1]
    own, hidden = w_out.shape[2], w_fc1.shape[2]
    width = piece * count

    pack = jnp.concatenate(
        [ln_gain[0], ln_bias[0], bias_out[0], bias_fc2[0], bias_qkv[0].reshape(-1), bias_fc1[0]]
    ).astype(F32)
    used = pack.shape[0]
    smalls = gather_small(padded(pack), nf, nt).reshape(count, -1)[:, :used]
    wide = smalls[:, :7 * piece].reshape(count, 7, piece).transpose(1, 0, 2).reshape(7, width)
    vec = jnp.stack([wide[0], wide[1], wide[2] + wide[3]])
    vec = jnp.pad(vec, ((0, 5), (0, 0)))
    qb = lax.dynamic_slice_in_dim(wide[4:7], tp_index * own, own, 1)
    qb = jnp.pad(qb, ((0, 5), (0, 0)))
    fb = lax.dynamic_slice_in_dim(smalls[:, 7 * piece:], tp_index * nf, nf, 0).reshape(1, hidden)
    fb = jnp.pad(fb, ((0, 7), (0, 0)))
    rope = rope_tables(segments)
    segc, segr = segments[:, :, None], segments[:, None, :]

    wq = lax.all_gather(w_qkv[0].transpose(1, 0, 2), "fsdp", axis=1, tiled=True)
    w1 = lax.all_gather(w_fc1[0], "fsdp", axis=0, tiled=True)
    wo = lax.all_gather(w_out[0], "fsdp", axis=0, tiled=True)
    w2 = lax.all_gather(w_fc2[0], "fsdp", axis=0, tiled=True)
    weights = (wq, wo, w1, w2)
    rows, xg, qkv, lse, att, gp, act, y = forward(
        ends_in[0], weights, vec, qb, fb, rope, segc, segr, nt
    )
    gr, up, dj, dx, own_sums, head_sums, up_sums = backward(
        ends_in[0], weights, rows, qkv, lse, gp, vec, rope, segc, segr, nt
    )

    def everywhere(arr):
        return lax.all_gather(arr, "fsdp", axis=arr.ndim - 2, tiled=True)

    def columns(arr):
        return lax.all_to_all(arr, "fsdp", split_axis=2, concat_axis=1, tiled=True)

    xc, gc = columns(xg), columns(gr)

    def product(left, right):
        return lax.dot_general(
            left, right, (((0, 1), (0, 1)), ((), ())), preferred_element_type=F32
        )

    act_all, att_all, up_all, dj_all = (everywhere(a) for a in (act, att, up, dj))
    grad_fc2 = product(gc, act_all)
    grad_out = product(gc, att_all)
    grad_fc1 = product(xc, up_all)
    grad_qkv = jnp.stack([product(xc, dj_all[:, part]) for part in range(3)], axis=1)

    mine = own_sums[:3].reshape(3, count, piece).transpose(1, 0, 2).reshape(count, 3 * piece)
    head = lax.dynamic_update_slice_in_dim(
        jnp.zeros((3, width), F32), head_sums[:3], tp_index * own, 1
    )
    head = head.reshape(3, count, piece).transpose(1, 0, 2).reshape(count, 3 * piece)
    ups = lax.dynamic_update_slice_in_dim(
        jnp.zeros((count, hidden_piece), F32),
        up_sums[0].reshape(nf, hidden_piece),
        tp_index * nf,
        0,
    )
    sums = sum_small(padded(jnp.concatenate([mine, head, ups], axis=1)), nf, nt).reshape(-1)
    gain_grad, bias_grad, row_grad = (sums[i * piece:(i + 1) * piece] for i in range(3))
    qkv_bias_grad = sums[3 * piece:6 * piece].reshape(3, piece)
    fc1_bias_grad = sums[6 * piece:6 * piece + hidden_piece]
    ends_out = jnp.where(is_first, dx, y)[None]
    return (
        ends_out,
        gain_grad[None],
        bias_grad[None],
        grad_qkv[None],
        grad_out[None],
        grad_fc1[None],
        grad_fc2[None],
        qkv_bias_grad[None],
        row_grad[None],
        fc1_bias_grad[None],
        row_grad[None],
    )


def fused_shards(
    ends_in, segments, ln_gain, ln_bias, w_qkv, w_out, w_fc1, w_fc2,
    bias_qkv, bias_out, bias_fc1, bias_fc2,
):
    nf, nt = lax.axis_size("fsdp"), lax.axis_size("tp")
    pack = jnp.concatenate(
        [
            ln_gain, ln_bias, (bias_out.astype(F32) + bias_fc2.astype(F32)),
            bias_qkv[0], bias_fc1[0].reshape(-1, LANES),
        ]
    ).astype(F32)
    used = pack.shape[0]
    pack = jnp.pad(pack, ((0, ROWS_OF_PACK - used), (0, 0)))
    ends_out, sums, act_x, att_x, up_x, dj_x, xc, gc = fused(
        ends_in[0], pack, w_qkv[0].transpose(1, 0, 2), w_out[0], w_fc1[0], w_fc2[0],
        rope_tables(segments), segments[:, :, None], segments[:, None, :], nf, nt,
    )

    def product(left, right):
        left = left.reshape(-1, left.shape[-1])
        right = right.reshape(-1, right.shape[-1])
        return lax.dot_general(left, right, ROWS, preferred_element_type=F32)

    grad_fc2 = product(gc, act_x)
    grad_out = product(gc, att_x)
    grad_fc1 = product(xc, up_x)
    grad_qkv = jnp.stack([product(xc, dj_x[part]) for part in range(3)], axis=1)
    row_grad = sums[2:3]
    return (
        ends_out[None],
        sums[0:1],
        sums[1:2],
        grad_qkv[None],
        grad_out[None],
        grad_fc1[None],
        grad_fc2[None],
        sums[3:6][None],
        row_grad,
        sums[6:used].reshape(1, -1),
        row_grad,
    )


def shards(*args):
    rows, piece = args[0].shape[2], args[2].shape[1]
    small = rows * lax.axis_size("tp") <= 256
    tidy = piece == LANES and args[10].shape[1] // LANES <= ROWS_OF_PACK - 6
    return (fused_shards if small and tidy else split_shards)(*args)


def solution(mesh):
    both = P("section", ("fsdp", "tp"))
    square = P("section", "fsdp", "tp")
    tokens = P("section", None, ("fsdp", "tp"), None)
    heads = P("section", "fsdp", None, "tp")
    bias3 = P("section", None, ("fsdp", "tp"))
    return jax.shard_map(
        shards,
        mesh=mesh,
        in_specs=(
            tokens, P(None, "fsdp"), both, both, heads, square, square, square,
            bias3, both, both, both,
        ),
        out_specs=(
            tokens, both, both, heads, square, square, square, bias3, both, both, both,
        ),
        check_vma=False,
    )
```

```python
import functools

import jax
import jax.numpy as jnp
from jax import lax
from jax.experimental import pallas as pl
from jax.experimental.pallas import tpu as pltpu
from jax.sharding import PartitionSpec as P

HEAD_DIM = 64
ROT_DIM = 32
EPSILON = 1e-05
LANES = 128
TILE = 256
MESH = pl.DeviceIdType.MESH
F32 = jnp.float32
BF16 = jnp.bfloat16
COLS = (((1,), (1,)), ((), ()))
ROWS = (((0,), (0,)), ((), ()))
VMEM_LIMIT = 66_900_000


def positions_of(segment_ids):
    length = segment_ids.shape[-1]
    places = jnp.arange(length, dtype=jnp.int32)
    before = jnp.concatenate([segment_ids[..., :1] - 1, segment_ids[..., :-1]], axis=-1)
    starts = jnp.where(segment_ids != before, places, 0)
    starts = lax.cummax(starts, axis=segment_ids.ndim - 1)
    return places - starts


def rope_tables(segments):
    half = ROT_DIM // 2
    freq = jnp.exp(-jnp.log(10000.0) * (2.0 * jnp.arange(half, dtype=F32)) / ROT_DIM)
    angles = positions_of(segments).astype(F32)[..., None] * freq
    cosine, sine = jnp.cos(angles), jnp.sin(angles)
    none = jnp.zeros_like(sine)
    rest = jnp.zeros(angles.shape[:-1] + (HEAD_DIM - ROT_DIM,), F32)
    keep = jnp.concatenate([cosine, cosine, rest + 1.0], axis=-1)
    ahead = jnp.concatenate([-sine, none, rest], axis=-1)
    behind = jnp.concatenate([none, sine, rest], axis=-1)
    tables = jnp.stack([keep, ahead, behind], axis=1)
    return jnp.concatenate([tables, tables], axis=-1)


def send(src, dst, send_sem, recv_sem, device):
    return pltpu.make_async_remote_copy(
        src_ref=src,
        dst_ref=dst,
        send_sem=send_sem,
        recv_sem=recv_sem,
        device_id=device,
        device_id_type=MESH,
    )


def greet(peers):
    barrier = pltpu.get_barrier_semaphore()
    for peer in peers:
        pl.semaphore_signal(barrier, inc=1, device_id=peer, device_id_type=MESH)
    pl.semaphore_wait(barrier, len(peers))


def group_peers(nf, nt):
    me = lax.axis_index("fsdp") * nt + lax.axis_index("tp")
    found = []
    for k in range(1, nf * nt):
        to = lax.rem(me + k, nf * nt)
        found.append((k, to, {"fsdp": to // nt, "tp": lax.rem(to, nt)}))
    return me, found


def gather_small_kernel(nf, nt, own, out, send_sems, recv_sems, local_sem):
    me, peers = group_peers(nf, nt)
    greet([peer for _, _, peer in peers])
    mine = pltpu.make_async_copy(own, out.at[me], local_sem)
    mine.start()
    copies = []
    for k, _, peer in peers:
        copy = send(own, out.at[me], send_sems.at[k], recv_sems.at[k], peer)
        copy.start()
        copies.append(copy)
    mine.wait()
    for copy in copies:
        copy.wait()


def gather_small(own, nf, nt):
    count = nf * nt
    return pl.pallas_call(
        functools.partial(gather_small_kernel, nf, nt),
        out_shape=jax.ShapeDtypeStruct((count,) + own.shape, own.dtype),
        in_specs=[pl.BlockSpec(memory_space=pltpu.VMEM)],
        out_specs=pl.BlockSpec(memory_space=pltpu.VMEM),
        scratch_shapes=[
            pltpu.SemaphoreType.DMA((count,)),
            pltpu.SemaphoreType.DMA((count,)),
            pltpu.SemaphoreType.DMA,
        ],
        compiler_params=pltpu.CompilerParams(collective_id=0, has_side_effects=True),
        name="gather_small",
    )(own)


def sum_small_kernel(nf, nt, own, out, got, send_sems, recv_sems):
    me, peers = group_peers(nf, nt)
    greet([peer for _, _, peer in peers])
    copies = []
    for k, to, peer in peers:
        copy = send(own.at[to], got.at[k], send_sems.at[k], recv_sems.at[k], peer)
        copy.start()
        copies.append(copy)
    total = own[me]
    for k, copy in enumerate(copies):
        copy.wait()
        total = total + got[k + 1]
    out[...] = total


def sum_small(own, nf, nt):
    count = nf * nt
    return pl.pallas_call(
        functools.partial(sum_small_kernel, nf, nt),
        out_shape=jax.ShapeDtypeStruct(own.shape[1:], own.dtype),
        in_specs=[pl.BlockSpec(memory_space=pltpu.VMEM)],
        out_specs=pl.BlockSpec(memory_space=pltpu.VMEM),
        scratch_shapes=[
            pltpu.VMEM(own.shape, own.dtype),
            pltpu.SemaphoreType.DMA((count,)),
            pltpu.SemaphoreType.DMA((count,)),
        ],
        compiler_params=pltpu.CompilerParams(collective_id=1, has_side_effects=True),
        name="sum_small",
    )(own)


def cols(n, width=TILE):
    return pl.ds(pl.multiple_of(n * width, width), width)


def loop(count, body):
    def step(i, carry):
        body(i)
        return carry

    lax.fori_loop(0, count, step, 0)


def turn(x, tables, sign):
    keep, ahead, behind = tables
    left = pltpu.roll(x, LANES - ROT_DIM // 2, 1)
    right = pltpu.roll(x, ROT_DIM // 2, 1)
    return x * keep + sign * (left * ahead + right * behind)


def low_half(length):
    return lax.broadcasted_iota(jnp.int32, (length, LANES), 1) < HEAD_DIM


def allowed_mask(segc, segr, m, length):
    query = lax.broadcasted_iota(jnp.int32, (length, length), 0)
    key = lax.broadcasted_iota(jnp.int32, (length, length), 1)
    return (query >= key) & (segc[m] == segr[m])


class Ring:
    def __init__(self, nt, rows):
        self.nt, self.rows = nt, rows
        self.me = lax.axis_index("tp")
        self.others = [(k, lax.rem(self.me + k, nt)) for k in range(1, nt)]

    def block(self, who):
        return pl.ds(pl.multiple_of(who * self.rows, self.rows), self.rows)

    def gather(self, buf, m, sems):
        return [
            send(
                buf.at[m, self.block(self.me)],
                buf.at[m, self.block(self.me)],
                sems[0].at[m, k],
                sems[1].at[m, k],
                {"tp": to},
            )
            for k, to in self.others
        ]

    def scatter(self, buf, got, m, sems, part=None):
        at = slice(None) if part is None else part
        return [
            send(
                buf.at[m, self.block(to), at],
                got.at[m, k - 1, :, at],
                sems[0].at[m, k],
                sems[1].at[m, k],
                {"tp": to},
            )
            for k, to in self.others
        ]

    def total(self, buf, got, m):
        acc = buf[m, self.block(self.me)].astype(F32)
        for k, _ in self.others:
            acc = acc + got[m, k - 1].astype(F32)
        return acc


def stats(rows):
    mean = jnp.mean(rows, axis=-1, keepdims=True)
    centred = rows - mean
    variance = jnp.mean(centred * centred, axis=-1, keepdims=True)
    inv_root = lax.rsqrt(variance + EPSILON)
    return centred * inv_root, inv_root


def forward_kernel(
    nt,
    rows_h, wq_h, wo_h, w1_h, w2_h, vec, qb, fb, rope, segc, segr,
    rows_o, xg_o, qkv_o, lse_o, att_o, gp_o, act_o, y_o,
    wq, wo, w1, w2, rin, xg, qkv, lse, att, gp, act, branch, got, out_f, out_b,
    w_sem, in_sem, o_sem, ag_s, ag_r, rs_s, rs_r, x_s, x_r,
):
    micro, length, width = xg.shape
    section = lax.axis_index("section")
    first, second = section == 0, section == 1
    ring = Ring(nt, length // nt)
    own = wo.shape[1]
    loads = []
    for i, (src, dst) in enumerate(((wq_h, wq), (w1_h, w1), (wo_h, wo), (w2_h, w2))):
        loads.append(pltpu.make_async_copy(src, dst, w_sem.at[i]))
        loads[-1].start()
    mine = pltpu.make_async_copy(rows_h, rin, in_sem)

    @pl.when(first)
    def _():
        mine.start()

    greet([{"tp": to} for _, to in ring.others] + [{"section": 1 - section}])

    @pl.when(first)
    def _():
        mine.wait()

    def hop(m):
        return send(out_b.at[m], rin.at[m], x_s.at[m], x_r.at[m], {"section": 1 - section})

    def front(m):
        unit, _ = stats(rin[m].astype(F32))
        normed = unit * vec[0:1, :] + vec[1:2, :]
        xg[m, ring.block(ring.me)] = normed.astype(BF16)
        for copy in ring.gather(xg, m, (ag_s, ag_r)):
            copy.start()

    def arrive(m):
        @pl.when(second)
        def _():
            hop(m).wait_recv()
            front(m)

    stores = []

    def store(src, dst, m, i):
        copy = pltpu.make_async_copy(src.at[m], dst.at[m], o_sem.at[m, i])
        copy.start()
        stores.append(copy)

    def body(m):
        for copy in ring.gather(xg, m, (ag_s, ag_r)):
            copy.wait()
        store(xg, xg_o, m, 0)
        store(rin, rows_o, m, 1)
        tables = (rope[m, 0], rope[m, 1], rope[m, 2])
        if m == 0:
            loads[0].wait()
        per = own // TILE
        for part in range(3):
            def qkv_tile(n, part=part):
                at = cols(n)
                acc = jnp.dot(xg[m], wq[part, :, at], preferred_element_type=F32)
                acc = acc + qb[part:part + 1, at]
                if part < 2:
                    acc = jnp.concatenate(
                        [
                            turn(acc[:, c:c + LANES], tables, 1.0)
                            for c in range(0, TILE, LANES)
                        ],
                        axis=1,
                    )
                qkv[m, part, :, at] = acc.astype(BF16)

            loop(per, qkv_tile)
        store(qkv, qkv_o, m, 2)
        allowed = allowed_mask(segc, segr, m, length)
        low = low_half(length)
        lane = lax.broadcasted_iota(jnp.int32, (length, LANES), 1)

        def pair(p):
            at = cols(p, LANES)
            query, key, value = qkv[m, 0, :, at], qkv[m, 1, :, at], qkv[m, 2, :, at]
            outs = []
            for h in range(2):
                mask = low if h == 0 else ~low
                one = jnp.where(mask, query, jnp.zeros_like(query))
                s = lax.dot_general(one, key, COLS, preferred_element_type=F32)
                s = jnp.where(allowed, s * HEAD_DIM ** (-0.5), -1e30)
                top = jnp.max(s, axis=-1, keepdims=True)
                e = jnp.exp(s - top)
                total = jnp.sum(e, axis=-1, keepdims=True)
                probs = (e / total).astype(BF16)
                outs.append(jnp.dot(probs, value, preferred_element_type=F32))
                lse[m] = jnp.where(lane == 2 * p + h, top + jnp.log(total), lse[m])
            att[m, :, at] = jnp.where(low, outs[0], outs[1]).astype(BF16)

        lse[m] = jnp.zeros((length, LANES), F32)
        loop(own // LANES, pair)
        store(lse, lse_o, m, 3)
        store(att, att_o, m, 4)
        if m == 0:
            loads[1].wait()

        def up_tile(n):
            at = cols(n)
            u = jnp.dot(xg[m], w1[:, at], preferred_element_type=F32) + fb[0:1, at]
            c = 0.7978845608028654
            square = u * u
            t = jnp.tanh(c * u * (1.0 + 0.044715 * square))
            act[m, :, at] = (0.5 * u * (1.0 + t)).astype(BF16)
            slope = 0.5 * (1.0 + t) + 0.5 * u * (1.0 - t * t) * (c * (1.0 + 3 * 0.044715 * square))
            gp[m, :, at] = slope.astype(BF16)

        loop(act.shape[2] // TILE, up_tile)
        store(act, act_o, m, 5)
        store(gp, gp_o, m, 6)
        if m == 0:
            loads[2].wait()
            loads[3].wait()

        def out_tile(n):
            at = cols(n)
            acc = lax.dot_general(att[m], wo[at, :], COLS, preferred_element_type=F32)
            acc = acc + lax.dot_general(act[m], w2[at, :], COLS, preferred_element_type=F32)
            branch[m, :, at] = acc.astype(BF16)
            for copy in ring.scatter(branch, got, m, (rs_s, rs_r), at):
                copy.start()

        loop(width // TILE, out_tile)

    def finish(m):
        for copy in ring.scatter(branch, got, m, (rs_s, rs_r)):
            copy.wait()
        y = rin[m].astype(F32) + ring.total(branch, got, m) + vec[2:3, :]
        out_f[m] = y
        out_b[m] = y.astype(BF16)
        store(out_f, y_o, m, 7)

        @pl.when(first)
        def _():
            hop(m).start()

    @pl.when(first)
    def _():
        for m in range(micro):
            front(m)

    for m in range(micro):
        arrive(m)
        body(m)
    for m in range(micro):
        finish(m)
    for copy in stores:
        copy.wait()

    @pl.when(first)
    def _():
        for m in range(micro):
            hop(m).wait_send()


def forward(rows, weights, vec, qb, fb, rope, segc, segr, nt):
    wq, wo, w1, w2 = weights
    micro, per, width = rows.shape
    length = per * nt
    own, hidden = wo.shape[1], w1.shape[1]
    anywhere = pl.BlockSpec(memory_space=pl.ANY)
    inside = pl.BlockSpec(memory_space=pltpu.VMEM)
    out_shape = [
        jax.ShapeDtypeStruct(rows.shape, BF16),
        jax.ShapeDtypeStruct((micro, length, width), BF16),
        jax.ShapeDtypeStruct((micro, 3, length, own), BF16),
        jax.ShapeDtypeStruct((micro, length, LANES), F32),
        jax.ShapeDtypeStruct((micro, length, own), BF16),
        jax.ShapeDtypeStruct((micro, length, hidden), BF16),
        jax.ShapeDtypeStruct((micro, length, hidden), BF16),
        jax.ShapeDtypeStruct(rows.shape, F32),
    ]
    dma = pltpu.SemaphoreType.DMA
    return pl.pallas_call(
        functools.partial(forward_kernel, nt),
        out_shape=out_shape,
        in_specs=[anywhere] * 5 + [inside] * 6,
        out_specs=[anywhere] * 8,
        scratch_shapes=[
            pltpu.VMEM(wq.shape, BF16),
            pltpu.VMEM(wo.shape, BF16),
            pltpu.VMEM(w1.shape, BF16),
            pltpu.VMEM(w2.shape, BF16),
            pltpu.VMEM(rows.shape, BF16),
            pltpu.VMEM((micro, length, width), BF16),
            pltpu.VMEM((micro, 3, length, own), BF16),
            pltpu.VMEM((micro, length, LANES), F32),
            pltpu.VMEM((micro, length, own), BF16),
            pltpu.VMEM((micro, length, hidden), BF16),
            pltpu.VMEM((micro, length, hidden), BF16),
            pltpu.VMEM((micro, length, width), BF16),
            pltpu.VMEM((micro, nt - 1, per, width), BF16),
            pltpu.VMEM(rows.shape, F32),
            pltpu.VMEM(rows.shape, BF16),
            dma((4,)),
            dma,
            dma((micro, 8)),
            dma((micro, nt)),
            dma((micro, nt)),
            dma((micro, nt)),
            dma((micro, nt)),
            dma((micro,)),
            dma((micro,)),
        ],
        compiler_params=pltpu.CompilerParams(
            collective_id=2, has_side_effects=True, vmem_limit_bytes=VMEM_LIMIT
        ),
        name="forward",
    )(rows, wq, wo, w1, w2, vec, qb, fb, rope, segc, segr)


def backward_kernel(
    nt,
    dy_h, wq_h, wo_h, w1_h, w2_h, rows_h, qkv_h, lse_h, gp_h, vec, rope, segc, segr,
    gr_o, up_o, dj_o, dx_o, own_sums, head_sums, up_sums,
    wq, wo, w1, w2, dyr, rin, qkv, lse, gp, gr, gatt, up, dj, branch, got, out_f, out_b,
    w_sem, in_sem, o_sem, ag_s, ag_r, rs_s, rs_r, x_s, x_r,
):
    micro, length, width = gr.shape
    section = lax.axis_index("section")
    first, second = section == 0, section == 1
    ring = Ring(nt, length // nt)
    own = wo.shape[1]
    mine = pltpu.make_async_copy(dy_h, dyr, in_sem.at[4])

    @pl.when(second)
    def _():
        mine.start()

    loads = []
    for i, (src, dst) in enumerate(((wo_h, wo), (w2_h, w2), (wq_h, wq), (w1_h, w1))):
        loads.append(pltpu.make_async_copy(src, dst, w_sem.at[i]))
    kept = []
    for i, (src, dst) in enumerate(((qkv_h, qkv), (lse_h, lse), (gp_h, gp), (rows_h, rin))):
        kept.append(pltpu.make_async_copy(src, dst, in_sem.at[i]))
    for copy in (loads[0], kept[0], kept[1], loads[1], kept[2], loads[2], loads[3], kept[3]):
        copy.start()
    greet([{"tp": to} for _, to in ring.others] + [{"section": 1 - section}])

    @pl.when(second)
    def _():
        mine.wait()

    def hop(m):
        return send(out_b.at[m], dyr.at[m], x_s.at[m], x_r.at[m], {"section": 1 - section})

    def front(m):
        gr[m, ring.block(ring.me)] = dyr[m]
        for copy in ring.gather(gr, m, (ag_s, ag_r)):
            copy.start()

    def arrive(m):
        @pl.when(first)
        def _():
            hop(m).wait_recv()
            front(m)

    stores = []

    def store(src, dst, m, i):
        copy = pltpu.make_async_copy(src.at[m], dst.at[m], o_sem.at[m, i])
        copy.start()
        stores.append(copy)

    def body(m):
        for copy in ring.gather(gr, m, (ag_s, ag_r)):
            copy.wait()
        store(gr, gr_o, m, 0)
        if m == 0:
            loads[0].wait()

        def att_tile(n):
            at = cols(n)
            gatt[:, at] = jnp.dot(gr[m], wo[:, at], preferred_element_type=F32).astype(BF16)

        loop(own // TILE, att_tile)
        if m == 0:
            kept[0].wait()
            kept[1].wait()
        tables = (rope[m, 0], rope[m, 1], rope[m, 2])
        allowed = allowed_mask(segc, segr, m, length)
        low = low_half(length)
        lane = lax.broadcasted_iota(jnp.int32, (length, LANES), 1)
        factor = HEAD_DIM ** (-0.5)

        def pair(p):
            at = cols(p, LANES)
            query, key, value = qkv[m, 0, :, at], qkv[m, 1, :, at], qkv[m, 2, :, at]
            grad = gatt[:, at]
            dqs, dks, dvs = [], [], []
            for h in range(2):
                mask = low if h == 0 else ~low
                one = jnp.where(mask, query, jnp.zeros_like(query))
                s = lax.dot_general(one, key, COLS, preferred_element_type=F32)
                s = jnp.where(allowed, s * factor, -1e30)
                log_total = jnp.sum(
                    jnp.where(lane == 2 * p + h, lse[m], 0.0), axis=-1, keepdims=True
                )
                soft = jnp.exp(s - log_total)
                probs = soft.astype(BF16)
                one_grad = jnp.where(mask, grad, jnp.zeros_like(grad))
                dp = lax.dot_general(one_grad, value, COLS, preferred_element_type=F32)
                delta = jnp.sum(dp * soft, axis=-1, keepdims=True)
                ds = (soft * (dp - delta)).astype(BF16)
                dvs.append(lax.dot_general(probs, grad, ROWS, preferred_element_type=F32))
                dqs.append(jnp.dot(ds, key, preferred_element_type=F32))
                dks.append(lax.dot_general(ds, query, ROWS, preferred_element_type=F32))
            dq = jnp.where(low, dqs[0], dqs[1]) * factor
            dk = jnp.where(low, dks[0], dks[1]) * factor
            dj[m, 0, :, at] = turn(dq, tables, -1.0).astype(BF16)
            dj[m, 1, :, at] = turn(dk, tables, -1.0).astype(BF16)
            dj[m, 2, :, at] = jnp.where(low, dvs[0], dvs[1]).astype(BF16)

        loop(own // LANES, pair)
        store(dj, dj_o, m, 1)
        for part in range(3):
            sums = jnp.sum(dj[m, part].astype(F32), axis=0, keepdims=True)
            if m == 0:
                head_sums[part:part + 1, :] = sums
            else:
                head_sums[part:part + 1, :] += sums
        if m == 0:
            loads[1].wait()
            kept[2].wait()

        def up_tile(n):
            at = cols(n)
            acc = jnp.dot(gr[m], w2[:, at], preferred_element_type=F32)
            rounded = (acc * gp[m, :, at].astype(F32)).astype(BF16)
            up[m, :, at] = rounded
            sums = jnp.sum(rounded.astype(F32), axis=0, keepdims=True)
            if m == 0:
                up_sums[0:1, at] = sums
            else:
                up_sums[0:1, at] += sums

        loop(up.shape[2] // TILE, up_tile)
        store(up, up_o, m, 2)
        if m == 0:
            loads[2].wait()
            loads[3].wait()

        def norm_tile(n):
            at = cols(n)
            acc = lax.dot_general(up[m], w1[at, :], COLS, preferred_element_type=F32)
            for part in range(3):
                acc = acc + lax.dot_general(
                    dj[m, part], wq[part, at, :], COLS, preferred_element_type=F32
                )
            branch[m, :, at] = acc.astype(BF16)
            for copy in ring.scatter(branch, got, m, (rs_s, rs_r), at):
                copy.start()

        loop(width // TILE, norm_tile)

    def finish(m):
        for copy in ring.scatter(branch, got, m, (rs_s, rs_r)):
            copy.wait()
        if m == 0:
            kept[3].wait()
        grad_norm = ring.total(branch, got, m)
        unit, inv_root = stats(rin[m].astype(F32))
        scaled = grad_norm * vec[0:1, :]
        upstream = dyr[m].astype(F32)
        dx = upstream + inv_root * (
            scaled
            - jnp.mean(scaled, axis=-1, keepdims=True)
            - unit * jnp.mean(scaled * unit, axis=-1, keepdims=True)
        )
        out_f[m] = dx
        out_b[m] = dx.astype(BF16)

        @pl.when(second)
        def _():
            hop(m).start()

        store(out_f, dx_o, m, 3)
        for i, term in enumerate((grad_norm * unit, grad_norm, upstream)):
            sums = jnp.sum(term, axis=0, keepdims=True)
            if m == 0:
                own_sums[i:i + 1, :] = sums
            else:
                own_sums[i:i + 1, :] += sums

    @pl.when(second)
    def _():
        for m in range(micro):
            front(m)

    for m in range(micro):
        arrive(m)
        body(m)
    for m in range(micro):
        finish(m)
    for copy in stores:
        copy.wait()

    @pl.when(second)
    def _():
        for m in range(micro):
            hop(m).wait_send()


def backward(dy, weights, rows, qkv, lse, gp, vec, rope, segc, segr, nt):
    wq, wo, w1, w2 = weights
    micro, per, width = rows.shape
    length = per * nt
    own, hidden = wo.shape[1], w1.shape[1]
    anywhere = pl.BlockSpec(memory_space=pl.ANY)
    inside = pl.BlockSpec(memory_space=pltpu.VMEM)
    out_shape = [
        jax.ShapeDtypeStruct((micro, length, width), BF16),
        jax.ShapeDtypeStruct((micro, length, hidden), BF16),
        jax.ShapeDtypeStruct((micro, 3, length, own), BF16),
        jax.ShapeDtypeStruct(rows.shape, F32),
        jax.ShapeDtypeStruct((8, width), F32),
        jax.ShapeDtypeStruct((8, own), F32),
        jax.ShapeDtypeStruct((8, hidden), F32),
    ]
    dma = pltpu.SemaphoreType.DMA
    return pl.pallas_call(
        functools.partial(backward_kernel, nt),
        out_shape=out_shape,
        in_specs=[anywhere] * 9 + [inside] * 4,
        out_specs=[anywhere] * 4 + [inside] * 3,
        scratch_shapes=[
            pltpu.VMEM(wq.shape, BF16),
            pltpu.VMEM(wo.shape, BF16),
            pltpu.VMEM(w1.shape, BF16),
            pltpu.VMEM(w2.shape, BF16),
            pltpu.VMEM(rows.shape, BF16),
            pltpu.VMEM(rows.shape, BF16),
            pltpu.VMEM(qkv.shape, BF16),
            pltpu.VMEM(lse.shape, F32),
            pltpu.VMEM(gp.shape, BF16),
            pltpu.VMEM((micro, length, width), BF16),
            pltpu.VMEM((length, own), BF16),
            pltpu.VMEM((micro, length, hidden), BF16),
            pltpu.VMEM((micro, 3, length, own), BF16),
            pltpu.VMEM((micro, length, width), BF16),
            pltpu.VMEM((micro, nt - 1, per, width), BF16),
            pltpu.VMEM(rows.shape, F32),
            pltpu.VMEM(rows.shape, BF16),
            dma((4,)),
            dma((5,)),
            dma((micro, 4)),
            dma((micro, nt)),
            dma((micro, nt)),
            dma((micro, nt)),
            dma((micro, nt)),
            dma((micro,)),
            dma((micro,)),
        ],
        compiler_params=pltpu.CompilerParams(
            collective_id=3, has_side_effects=True, vmem_limit_bytes=VMEM_LIMIT
        ),
        name="backward",
    )(dy, wq, wo, w1, w2, rows, qkv, lse, gp, vec, rope, segc, segr)


ROWS_OF_PACK = 16


def twist(x, tables, sign):
    keep, sine, ahead = tables
    left = pltpu.roll(x, LANES - ROT_DIM // 2, 1)
    right = pltpu.roll(x, ROT_DIM // 2, 1)
    return x * keep + jnp.where(ahead, left, right) * (sign * sine)


def masks_of(nf):
    return range(nf)


def bits_below(mask, nf):
    low = mask & -mask if mask else nf
    return [(i, 1 << i) for i in range(nf.bit_length() - 1) if (1 << i) < low]


def flipped(index, mask, nf):
    for i in range(nf.bit_length() - 1):
        if mask >> i & 1:
            index = index + (1 << i) * (1 - 2 * lax.rem(index // (1 << i), 2))
    return index


def fused_kernel(
    nf, nt,
    ends_h, gain, shift, b_out, b_fc2, b_qkv, b_fc1, seg_in, wq_h, wo_h, w1_h, w2_h,
    ends_o, sums_o, act_x, att_x, up_x, dj_x, xc_x, gc_x,
    wq, wo, w1, w2, pack, packs, wide, fb, segs, rope, rin, dyr, xg, qkv, lse, att, gp, act,
    gr, gatt, up, dj, out_bf, out_got, in_bf, in_got, y_f, y_b,
    own_sums, head_sums, up_sums, s_src, s_got,
    in_sem, wl_sem, ws_sem, wr_sem, pk_s, pk_r, sm_s, sm_r,
    ag_s, ag_r, gg_s, gg_r, rs_s, rs_r, rb_s, rb_r, hx_s, hx_r, hb_s, hb_r,
    xl_sem, xs_s, xs_r, cl_sem, ca_s, ca_r, mx_s, mx_r, o_sem,
):
    micro, per, width = rin.shape
    length = per * nt
    section, f, t = (lax.axis_index(a) for a in ("section", "fsdp", "tp"))
    first, second = section == 0, section == 1
    ring = Ring(nt, per)
    own, hidden = wo.shape[1], w1.shape[1]
    depth = width // nf
    mirror, sibling = {"fsdp": flipped(f, 2, nf)}, {"fsdp": flipped(f, 1, nf)}
    count = nf * nt
    other = {"section": 1 - section}
    me, group = group_peers(nf, nt)
    fblock = [flipped(f, mask, nf) for mask in masks_of(nf)]

    def rows_at(block):
        return pl.ds(pl.multiple_of(block * depth, depth), depth)

    load_rows = pltpu.make_async_copy(ends_h, rin, in_sem)
    load_dy = pltpu.make_async_copy(ends_h, dyr, in_sem)

    @pl.when(first)
    def _():
        load_rows.start()

    @pl.when(second)
    def _():
        load_dy.start()

    greet([peer for _, _, peer in group] + [other])

    per_row = hidden // nf // LANES
    segs[0] = jnp.zeros((8, length), F32)
    segs[0, 0:micro, :] = seg_in[...].astype(F32)
    pack[...] = jnp.zeros_like(pack)
    pack[0:1, :] = gain[...].astype(F32)
    pack[1:2, :] = shift[...].astype(F32)
    pack[2:3, :] = b_out[...].astype(F32) + b_fc2[...].astype(F32)
    pack[3:6, :] = b_qkv[...].astype(F32)
    for r in range(per_row):
        pack[6 + r:7 + r, :] = b_fc1[:, r * LANES:(r + 1) * LANES].astype(F32)
    seg_copy = send(segs.at[0], segs.at[1], mx_s.at[2, 0], mx_r.at[2, 0], mirror)
    pack_local = pltpu.make_async_copy(pack, packs.at[me], pk_s.at[0])
    pack_copies = [
        send(pack, packs.at[me], pk_s.at[k], pk_r.at[k], peer) for k, _, peer in group
    ]
    pack_local.start()
    seg_copy.start()
    for copy in pack_copies:
        copy.start()

    table = ((wq_h, wq), (w1_h, w1), (wo_h, wo), (w2_h, w2))

    def w_at(ref, block):
        return ref.at[:, rows_at(block), :] if len(ref.shape) == 3 else ref.at[rows_at(block), :]

    def w_local(a):
        return pltpu.make_async_copy(table[a][0], w_at(table[a][1], f), wl_sem.at[a])

    def w_send(a, mask, i, bit):
        block = w_at(table[a][1], fblock[mask])
        src = table[a][0] if mask == 0 else block
        peer = {"fsdp": flipped(f, bit, nf)}
        return send(src, block, ws_sem.at[a, mask, i], wr_sem.at[a, mask | bit], peer)

    def w_recv(a, mask):
        block = w_at(table[a][1], fblock[mask])
        return send(block, block, ws_sem.at[a, mask, 0], wr_sem.at[a, mask], other)

    def w_start(a):
        w_local(a).start()
        for i, bit in reversed(bits_below(0, nf)):
            w_send(a, 0, i, bit).start()

    def w_ready(a, mask):
        if mask == 0:
            w_local(a).wait()
            return
        w_recv(a, mask).wait_recv()
        for i, bit in bits_below(mask, nf):
            w_send(a, mask, i, bit).start()

    order = sorted(masks_of(nf), key=lambda m: (m != 0, -(m & -m), m))
    out_order = list(masks_of(nf))
    w_start(0)
    w_start(1)

    pack_local.wait()
    for copy in pack_copies:
        copy.wait()
    for j in range(count):
        wide[:, j * LANES:(j + 1) * LANES] = packs[j]
    for j in range(nf):
        for r in range(per_row):
            c = (j * per_row + r) * LANES
            fb[0:1, c:c + LANES] = packs[t * nf + j, 6 + r:7 + r, :]

    def segment_parts(q):
        row = segs[q // micro, pl.ds(lax.rem(q, micro), 1), :]
        query = lax.broadcasted_iota(jnp.int32, (length, length), 0)
        key = lax.broadcasted_iota(jnp.int32, (length, length), 1)
        column = jnp.sum(jnp.where(query == key, row, 0.0), axis=1, keepdims=True)
        return row, column, query >= key

    def allowed_of(q):
        row, column, causal = segment_parts(q)
        return causal & (row == column)

    def rope_of(q):
        row, column, _ = segment_parts(q)
        before = jnp.sum(jnp.where(row < column, 1.0, 0.0), axis=1, keepdims=True)
        lane = lax.rem(lax.broadcasted_iota(jnp.int32, (length, LANES), 1), HEAD_DIM)
        place = lax.broadcasted_iota(jnp.int32, (length, LANES), 0).astype(F32) - before
        half = ROT_DIM // 2
        power = lax.rem(lane, half).astype(F32)
        freq = jnp.exp(-jnp.log(10000.0) * (2.0 * power) / ROT_DIM)
        angles = place * freq
        rope[q, 0] = jnp.where(lane < ROT_DIM, jnp.cos(angles), 1.0)
        sine = jnp.where(lane < ROT_DIM, jnp.sin(angles), 0.0)
        rope[q, 1] = jnp.where(lane < half, -sine, sine)

    def hop_out(m):
        return send(y_b.at[m], rin.at[m], hx_s.at[m], hx_r.at[m], other)

    def hop_back(m):
        return send(y_b.at[m], dyr.at[m], hb_s.at[m], hb_r.at[m], other)

    def front(m):
        unit, _ = stats(rin[m].astype(F32))
        normed = unit * wide[0:1, :] + wide[1:2, :]
        xg[m, ring.block(ring.me)] = normed.astype(BF16)
        for copy in ring.gather(xg, m, (ag_s, ag_r)):
            copy.start()

    def front_back(m):
        gr[m, ring.block(ring.me)] = dyr[m]
        for copy in ring.gather(gr, m, (gg_s, gg_r)):
            copy.start()

    def mirror_copy(which, m):
        buf = (xg, gr)[which]
        return send(
            buf.at[m], buf.at[micro + m], mx_s.at[which, m], mx_r.at[which, m], mirror
        )

    def x_block(who):
        return fblock[2 * who] if isinstance(who, int) else jnp.where(who == 0, f, fblock[2])

    def x_dst(a, m, who):
        block = x_block(who)
        if a == 3:
            return dj_x.at[:, m, block]
        return (act_x, att_x, up_x)[a].at[m, block]

    def x_src(a, m, who):
        place = (m, micro)[who] if isinstance(who, int) else jnp.where(who == 0, m, micro)
        return (act, att, up, dj)[a].at[place]

    def x_local(a, m, who):
        return pltpu.make_async_copy(
            x_src(a, m, who), x_dst(a, m, who), xl_sem.at[a, m, who]
        )

    def x_send(a, m, who):
        return send(
            x_src(a, m, who), x_dst(a, m, who), xs_s.at[a, m, who], xs_r.at[a, m, who], sibling
        )

    def x_start(a, m, who):
        x_local(a, m, who).start()
        x_send(a, m, who).start()

    def x_sent(a, m, who):
        x_local(a, m, who).wait()
        x_send(a, m, who).wait_send()

    def c_pair(which, m, who):
        src, dst = ((xg, xc_x), (gr, gc_x))[which]
        block = x_block(who)
        q = who * micro + m
        mine = pltpu.make_async_copy(
            src.at[q, :, rows_at(f)], dst.at[m, block], cl_sem.at[which, m, who]
        )
        theirs = send(
            src.at[q, :, rows_at(fblock[1])],
            dst.at[m, block],
            ca_s.at[which, m, who],
            ca_r.at[which, m, who],
            sibling,
        )
        return mine, theirs

    def c_start(which, m, who):
        for copy in c_pair(which, m, who):
            copy.start()

    def attention_masks(q):
        low = low_half(length)
        lane = lax.broadcasted_iota(jnp.int32, (length, LANES), 1)
        tables = (rope[q, 0], rope[q, 1], lax.rem(lane, HEAD_DIM) < ROT_DIM // 2)
        return low, lane, tables, allowed_of(q)

    factor = HEAD_DIM ** (-0.5)

    def forward_stage(m, who, k, fresh):
        q = who * micro + m
        place = jnp.where(who == 0, m, micro)

        @pl.when(who == 0)
        def _():
            for copy in ring.gather(xg, m, (ag_s, ag_r)):
                copy.wait()
            c_start(0, m, 0)

            @pl.when(second | (k == 1))
            def _():
                mirror_copy(0, m).start()

        @pl.when(who == 1)
        def _():
            mirror_copy(0, m).wait_recv()
            c_start(0, m, 1)

            @pl.when(m == 1)
            def _():
                x_sent(0, 0, 1)
                x_sent(1, 0, 1)

        @pl.when(fresh)
        def _():
            for mask in order:
                w_ready(0, mask)
            w_start(2)
            w_start(3)

        low, lane, tables, allowed = attention_masks(q)
        for part in range(3):
            def qkv_tile(n, part=part):
                at = cols(n)
                acc = jnp.dot(xg[q], wq[part, :, at], preferred_element_type=F32)
                acc = acc + wide[3 + part:4 + part, pl.ds(
                    pl.multiple_of(t * own + n * TILE, TILE), TILE)]
                if part < 2:
                    acc = jnp.concatenate(
                        [
                            twist(acc[:, c:c + LANES], tables, 1.0)
                            for c in range(0, TILE, LANES)
                        ],
                        axis=1,
                    )
                qkv[q, part, :, at] = acc.astype(BF16)

            loop(own // TILE, qkv_tile)

        def pair(p):
            at = cols(p, LANES)
            query, key, value = qkv[q, 0, :, at], qkv[q, 1, :, at], qkv[q, 2, :, at]
            outs = []
            for h in range(2):
                mask = low if h == 0 else ~low
                one = jnp.where(mask, query, jnp.zeros_like(query))
                s = lax.dot_general(one, key, COLS, preferred_element_type=F32)
                s = jnp.where(allowed, s * factor, -1e30)
                top = jnp.max(s, axis=-1, keepdims=True)
                e = jnp.exp(s - top)
                total = jnp.sum(e, axis=-1, keepdims=True)
                probs = (e / total).astype(BF16)
                outs.append(jnp.dot(probs, value, preferred_element_type=F32))
                lse[q] = jnp.where(lane == 2 * p + h, top + jnp.log(total), lse[q])
            att[place, :, at] = jnp.where(low, outs[0], outs[1]).astype(BF16)

        lse[q] = jnp.zeros((length, LANES), F32)
        loop(own // LANES, pair)
        x_start(1, m, who)

        @pl.when(first & (k == 1))
        def _():
            output_finish(0)

        @pl.when(fresh)
        def _():
            for mask in order:
                w_ready(1, mask)

        def up_tile(n):
            at = cols(n)
            u = jnp.dot(xg[q], w1[:, at], preferred_element_type=F32) + fb[0:1, at]
            c = 0.7978845608028654
            square = u * u
            th = jnp.tanh(c * u * (1.0 + 0.044715 * square))
            act[place, :, at] = (0.5 * u * (1.0 + th)).astype(BF16)
            slope = 0.5 * (1.0 + th)
            slope = slope + 0.5 * u * (1.0 - th * th) * (c * (1.0 + 3 * 0.044715 * square))
            gp[q, :, at] = slope.astype(BF16)

        loop(hidden // TILE, up_tile)
        x_start(0, m, who)

    def output_stage(m, fresh):
        for mask in out_order:
            @pl.when(fresh)
            def _(mask=mask):
                w_ready(2, mask)
                w_ready(3, mask)

            def out_tile(n, mask=mask):
                start = pl.multiple_of(fblock[mask] * depth + n * TILE, TILE)
                at = pl.ds(start, TILE)
                acc = lax.dot_general(att[m], wo[at, :], COLS, preferred_element_type=F32)
                acc = acc + lax.dot_general(act[m], w2[at, :], COLS, preferred_element_type=F32)
                out_bf[m, :, at] = acc.astype(BF16)
                for copy in ring.scatter(out_bf, out_got, m, (rs_s, rs_r), at):
                    copy.start()

            loop(depth // TILE, out_tile)

        @pl.when(fresh)
        def _():
            mirror_copy(0, 0).start()

    def store_ends(m):
        return pltpu.make_async_copy(y_f.at[m], ends_o.at[m], o_sem.at[m])

    def output_finish(m):
        for copy in ring.scatter(out_bf, out_got, m, (rs_s, rs_r)):
            copy.wait()
        y = rin[m].astype(F32) + ring.total(out_bf, out_got, m) + wide[2:3, :]

        @pl.when(first)
        def _():
            y_b[m] = y.astype(BF16)
            hop_out(m).start()

        @pl.when(second)
        def _():
            y_f[m] = y
            store_ends(m).start()

    def backward_stage(m, who, k):
        q = who * micro + m
        place = jnp.where(who == 0, m, micro)

        @pl.when(first & (who == 0))
        def _():
            for copy in ring.gather(gr, m, (gg_s, gg_r)):
                copy.wait()
            mirror_copy(1, m).start()
            c_start(1, m, 0)

        @pl.when(who == 1)
        def _():
            mirror_copy(1, m).wait_recv()
            c_start(1, m, 1)

            @pl.when(m == 1)
            def _():
                x_sent(2, 0, 1)
                x_sent(3, 0, 1)

        def att_tile(n):
            at = cols(n)
            gatt[:, at] = jnp.dot(gr[q], wo[:, at], preferred_element_type=F32).astype(BF16)

        loop(own // TILE, att_tile)
        low, lane, tables, allowed = attention_masks(q)

        def pair(p):
            at = cols(p, LANES)
            query, key, value = qkv[q, 0, :, at], qkv[q, 1, :, at], qkv[q, 2, :, at]
            grad = gatt[:, at]
            dqs, dks, dvs = [], [], []
            for h in range(2):
                mask = low if h == 0 else ~low
                one = jnp.where(mask, query, jnp.zeros_like(query))
                s = lax.dot_general(one, key, COLS, preferred_element_type=F32)
                s = jnp.where(allowed, s * factor, -1e30)
                log_total = jnp.sum(
                    jnp.where(lane == 2 * p + h, lse[q], 0.0), axis=-1, keepdims=True
                )
                soft = jnp.exp(s - log_total)
                probs = soft.astype(BF16)
                one_grad = jnp.where(mask, grad, jnp.zeros_like(grad))
                dp = lax.dot_general(one_grad, value, COLS, preferred_element_type=F32)
                delta = jnp.sum(dp * soft, axis=-1, keepdims=True)
                ds = (soft * (dp - delta)).astype(BF16)
                dvs.append(lax.dot_general(probs, grad, ROWS, preferred_element_type=F32))
                dqs.append(jnp.dot(ds, key, preferred_element_type=F32))
                dks.append(lax.dot_general(ds, query, ROWS, preferred_element_type=F32))
            dq = jnp.where(low, dqs[0], dqs[1]) * factor
            dk = jnp.where(low, dks[0], dks[1]) * factor
            dj[place, 0, :, at] = twist(dq, tables, -1.0).astype(BF16)
            dj[place, 1, :, at] = twist(dk, tables, -1.0).astype(BF16)
            dj[place, 2, :, at] = jnp.where(low, dvs[0], dvs[1]).astype(BF16)

        loop(own // LANES, pair)
        x_start(3, m, who)

        @pl.when(second & (k == 3))
        def _():
            backward_finish(0)

        @pl.when(who == 0)
        def _():
            for part in range(3):
                head_sums[part:part + 1, :] += jnp.sum(
                    dj[m, part].astype(F32), axis=0, keepdims=True
                )

        def up_tile(n):
            at = cols(n)
            acc = jnp.dot(gr[q], w2[:, at], preferred_element_type=F32)
            rounded = (acc * gp[q, :, at].astype(F32)).astype(BF16)
            up[place, :, at] = rounded
            sums = jnp.sum(rounded.astype(F32), axis=0, keepdims=True)
            up_sums[0:1, at] += jnp.where(who == 0, sums, 0.0)

        loop(hidden // TILE, up_tile)
        x_start(2, m, who)

        @pl.when(first & (k == 4))
        def _():
            hop_back(1).wait_recv()
            front_back(1)

        def norm_tile(n):
            at = cols(n)
            acc = lax.dot_general(up[m], w1[at, :], COLS, preferred_element_type=F32)
            for part in range(3):
                acc = acc + lax.dot_general(
                    dj[m, part], wq[part, at, :], COLS, preferred_element_type=F32
                )
            in_bf[m, :, at] = acc.astype(BF16)
            for copy in ring.scatter(in_bf, in_got, m, (rb_s, rb_r), at):
                copy.start()

        @pl.when(who == 0)
        def _():
            loop(width // TILE, norm_tile)


    def backward_finish(m):
        for copy in ring.scatter(in_bf, in_got, m, (rb_s, rb_r)):
            copy.wait()
        grad_norm = ring.total(in_bf, in_got, m)
        unit, inv_root = stats(rin[m].astype(F32))
        scaled = grad_norm * wide[0:1, :]
        upstream = dyr[m].astype(F32)
        dx = upstream + inv_root * (
            scaled
            - jnp.mean(scaled, axis=-1, keepdims=True)
            - unit * jnp.mean(scaled * unit, axis=-1, keepdims=True)
        )

        @pl.when(second)
        def _():
            y_b[m] = dx.astype(BF16)
            hop_back(m).start()

        @pl.when(first)
        def _():
            y_f[m] = dx
            store_ends(m).start()

        for i, term in enumerate((grad_norm * unit, grad_norm, upstream)):
            own_sums[i:i + 1, :] += jnp.sum(term, axis=0, keepdims=True)

    own_sums[...] = jnp.zeros_like(own_sums)
    head_sums[...] = jnp.zeros_like(head_sums)
    up_sums[...] = jnp.zeros_like(up_sums)

    @pl.when(first)
    def _():
        load_rows.wait()
        loop(micro, front)

    @pl.when(second)
    def _():
        load_dy.wait()
        loop(micro, front_back)

    seg_copy.wait()
    loop(2 * micro, rope_of)

    @pl.when(second)
    def _():
        for mask in order:
            w_ready(0, mask)
        w_start(2)
        w_start(3)
        for a in (1, 2, 3):
            for mask in order:
                w_ready(a, mask)

        def dy_out(m):
            for copy in ring.gather(gr, m, (gg_s, gg_r)):
                copy.wait()
            mirror_copy(1, m).start()
            c_start(1, m, 0)

        loop(micro, dy_out)

    def slot(k):
        is_f = jnp.where(first, k < 4, (k < 8) & (lax.rem(k, 2) == 0))
        is_o = jnp.where(first, k < 2, (k == 5) | (k == 6))
        who = jnp.where(first, (k // 2) % 2 * (k < 4) + lax.rem(k, 2) * (k >= 4), k // 4)
        m = jnp.where(first, jnp.where(k < 4, lax.rem(k, 2), (k - 4) // 2), lax.rem(k // 2, 2))
        m_o = jnp.where(first, m, k - 5)
        fresh = first & (k == 0)

        @pl.when(second & ((k == 0) | (k == 1)))
        def _():
            hop_out(k).wait_recv()
            front(k)

        @pl.when(first & (k == 4))
        def _():
            hop_back(0).wait_recv()
            front_back(0)

        @pl.when(is_f)
        def _():
            forward_stage(m, who, k, fresh)

        @pl.when(is_o)
        def _():
            output_stage(m_o, fresh)

        @pl.when(jnp.logical_not(is_f))
        def _():
            backward_stage(m, who, k)

        @pl.when(first & (k == 2))
        def _():
            output_finish(1)

        @pl.when(first & (k == 6))
        def _():
            backward_finish(0)

        @pl.when((first & (k == 7)) | (second & (k == 4)))
        def _():
            backward_finish(1)

        @pl.when(second & (k == 7))
        def _():
            loop(micro, output_finish)

    loop(8, slot)

    s_src[...] = jnp.zeros_like(s_src)
    for j in range(count):
        s_src[j, 0:3, :] = own_sums[0:3, j * LANES:(j + 1) * LANES]
    for j in range(nf):
        s_src[t * nf + j, 3:6, :] = head_sums[0:3, j * LANES:(j + 1) * LANES]
        for r in range(per_row):
            c = (j * per_row + r) * LANES
            s_src[t * nf + j, 6 + r:7 + r, :] = up_sums[0:1, c:c + LANES]
    small = [
        send(s_src.at[to], s_got.at[k], sm_s.at[k], sm_r.at[k], peer) for k, to, peer in group
    ]
    for copy in small:
        copy.start()

    @pl.when(second)
    def _():
        for m in range(micro):
            hop_back(m).wait_send()

    @pl.when(first)
    def _():
        for m in range(micro):
            hop_out(m).wait_send()

    total = s_src[me]
    for k, copy in enumerate(small):
        copy.wait()
        total = total + s_got[k + 1]
    sums_o[...] = total
    for m in range(micro):
        for who in range(2):
            for a in range(4):
                if (m, who) != (0, 1):
                    x_sent(a, m, who)
                x_send(a, m, who).wait_recv()
            for which in range(2):
                mine, theirs = c_pair(which, m, who)
                mine.wait()
                theirs.wait()
        for which in range(2):
            mirror_copy(which, m).wait_send()
        store_ends(m).wait()
    for a in range(4):
        for mask in masks_of(nf):
            for i, bit in bits_below(mask, nf):
                w_send(a, mask, i, bit).wait_send()


def fused(ends, smalls, segments, wq, wo, w1, w2, nf, nt):
    micro, per, width = ends.shape
    length = per * nt
    own, hidden = wo.shape[1], w1.shape[1]
    depth = width // nf
    count = nf * nt
    bits = nf.bit_length() - 1
    anywhere = pl.BlockSpec(memory_space=pl.ANY)
    inside = pl.BlockSpec(memory_space=pltpu.VMEM)
    dma = pltpu.SemaphoreType.DMA
    vm = pltpu.VMEM
    piece = (ROWS_OF_PACK, LANES)
    packs = 2 * micro
    some = micro + 1
    out_shape = [
        jax.ShapeDtypeStruct(ends.shape, F32),
        jax.ShapeDtypeStruct(piece, F32),
        jax.ShapeDtypeStruct((micro, nf, length, hidden), BF16),
        jax.ShapeDtypeStruct((micro, nf, length, own), BF16),
        jax.ShapeDtypeStruct((micro, nf, length, hidden), BF16),
        jax.ShapeDtypeStruct((3, micro, nf, length, own), BF16),
        jax.ShapeDtypeStruct((micro, nf, length, depth), BF16),
        jax.ShapeDtypeStruct((micro, nf, length, depth), BF16),
    ]
    scratch = [
        vm((3, width, own), BF16), vm((width, own), BF16),
        vm((width, hidden), BF16), vm((width, hidden), BF16),
        vm(piece, F32), vm((count,) + piece, F32),
        vm((ROWS_OF_PACK, width), F32), vm((8, hidden), F32),
        vm((2, 8, length), F32), vm((packs, 2, length, LANES), F32),
        vm(ends.shape, BF16), vm(ends.shape, BF16),
        vm((packs, length, width), BF16), vm((packs, 3, length, own), BF16),
        vm((packs, length, LANES), F32), vm((some, length, own), BF16),
        vm((packs, length, hidden), BF16), vm((some, length, hidden), BF16),
        vm((packs, length, width), BF16), vm((length, own), BF16),
        vm((some, length, hidden), BF16), vm((some, 3, length, own), BF16),
        vm((micro, length, width), BF16), vm((micro, nt - 1, per, width), BF16),
        vm((micro, length, width), BF16), vm((micro, nt - 1, per, width), BF16),
        vm(ends.shape, F32), vm(ends.shape, BF16),
        vm((8, width), F32), vm((8, own), F32), vm((8, hidden), F32),
        vm((count,) + piece, F32), vm((count,) + piece, F32),
        dma, dma((4,)), dma((4, nf, bits)), dma((4, nf)),
        dma((count,)), dma((count,)), dma((count,)), dma((count,)),
        dma((micro, nt)), dma((micro, nt)), dma((micro, nt)), dma((micro, nt)),
        dma((micro, nt)), dma((micro, nt)), dma((micro, nt)), dma((micro, nt)),
        dma((micro,)), dma((micro,)), dma((micro,)), dma((micro,)),
        dma((4, micro, 2)), dma((4, micro, 2)), dma((4, micro, 2)),
        dma((2, micro, 2)), dma((2, micro, 2)), dma((2, micro, 2)),
        dma((3, micro)), dma((3, micro)), dma((micro,)),
    ]
    return pl.pallas_call(
        functools.partial(fused_kernel, nf, nt),
        out_shape=out_shape,
        in_specs=[anywhere] + [inside] * 7 + [anywhere] * 4,
        out_specs=[anywhere, inside] + [anywhere] * 6,
        scratch_shapes=scratch,
        compiler_params=pltpu.CompilerParams(
            collective_id=4, has_side_effects=True, vmem_limit_bytes=VMEM_LIMIT
        ),
        name="fused",
    )(ends, *smalls, segments, wq, wo, w1, w2)


def padded(flat):
    size = -(-flat.shape[-1] // (8 * LANES)) * (8 * LANES)
    room = [(0, 0)] * (flat.ndim - 1) + [(0, size - flat.shape[-1])]
    flat = jnp.pad(flat, room)
    return flat.reshape(flat.shape[:-1] + (size // LANES, LANES))


def split_shards(
    ends_in, segments, ln_gain, ln_bias, w_qkv, w_out, w_fc1, w_fc2,
    bias_qkv, bias_out, bias_fc1, bias_fc2,
):
    nf, nt = lax.axis_size("fsdp"), lax.axis_size("tp")
    count = nf * nt
    section, tp_index = lax.axis_index("section"), lax.axis_index("tp")
    is_first = section == 0
    piece = ln_gain.shape[1]
    hidden_piece = bias_fc1.shape[1]
    own, hidden = w_out.shape[2], w_fc1.shape[2]
    width = piece * count

    pack = jnp.concatenate(
        [ln_gain[0], ln_bias[0], bias_out[0], bias_fc2[0], bias_qkv[0].reshape(-1), bias_fc1[0]]
    ).astype(F32)
    used = pack.shape[0]
    smalls = gather_small(padded(pack), nf, nt).reshape(count, -1)[:, :used]
    wide = smalls[:, :7 * piece].reshape(count, 7, piece).transpose(1, 0, 2).reshape(7, width)
    vec = jnp.stack([wide[0], wide[1], wide[2] + wide[3]])
    vec = jnp.pad(vec, ((0, 5), (0, 0)))
    qb = lax.dynamic_slice_in_dim(wide[4:7], tp_index * own, own, 1)
    qb = jnp.pad(qb, ((0, 5), (0, 0)))
    fb = lax.dynamic_slice_in_dim(smalls[:, 7 * piece:], tp_index * nf, nf, 0).reshape(1, hidden)
    fb = jnp.pad(fb, ((0, 7), (0, 0)))
    rope = rope_tables(segments)
    segc, segr = segments[:, :, None], segments[:, None, :]

    wq = lax.all_gather(w_qkv[0].transpose(1, 0, 2), "fsdp", axis=1, tiled=True)
    w1 = lax.all_gather(w_fc1[0], "fsdp", axis=0, tiled=True)
    wo = lax.all_gather(w_out[0], "fsdp", axis=0, tiled=True)
    w2 = lax.all_gather(w_fc2[0], "fsdp", axis=0, tiled=True)
    weights = (wq, wo, w1, w2)
    rows, xg, qkv, lse, att, gp, act, y = forward(
        ends_in[0], weights, vec, qb, fb, rope, segc, segr, nt
    )
    gr, up, dj, dx, own_sums, head_sums, up_sums = backward(
        ends_in[0], weights, rows, qkv, lse, gp, vec, rope, segc, segr, nt
    )

    def everywhere(arr):
        return lax.all_gather(arr, "fsdp", axis=arr.ndim - 2, tiled=True)

    def columns(arr):
        return lax.all_to_all(arr, "fsdp", split_axis=2, concat_axis=1, tiled=True)

    xc, gc = columns(xg), columns(gr)

    def product(left, right):
        return lax.dot_general(
            left, right, (((0, 1), (0, 1)), ((), ())), preferred_element_type=F32
        )

    act_all, att_all, up_all, dj_all = (everywhere(a) for a in (act, att, up, dj))
    grad_fc2 = product(gc, act_all)
    grad_out = product(gc, att_all)
    grad_fc1 = product(xc, up_all)
    grad_qkv = jnp.stack([product(xc, dj_all[:, part]) for part in range(3)], axis=1)

    mine = own_sums[:3].reshape(3, count, piece).transpose(1, 0, 2).reshape(count, 3 * piece)
    head = lax.dynamic_update_slice_in_dim(
        jnp.zeros((3, width), F32), head_sums[:3], tp_index * own, 1
    )
    head = head.reshape(3, count, piece).transpose(1, 0, 2).reshape(count, 3 * piece)
    ups = lax.dynamic_update_slice_in_dim(
        jnp.zeros((count, hidden_piece), F32),
        up_sums[0].reshape(nf, hidden_piece),
        tp_index * nf,
        0,
    )
    sums = sum_small(padded(jnp.concatenate([mine, head, ups], axis=1)), nf, nt).reshape(-1)
    gain_grad, bias_grad, row_grad = (sums[i * piece:(i + 1) * piece] for i in range(3))
    qkv_bias_grad = sums[3 * piece:6 * piece].reshape(3, piece)
    fc1_bias_grad = sums[6 * piece:6 * piece + hidden_piece]
    ends_out = jnp.where(is_first, dx, y)[None]
    return (
        ends_out,
        gain_grad[None],
        bias_grad[None],
        grad_qkv[None],
        grad_out[None],
        grad_fc1[None],
        grad_fc2[None],
        qkv_bias_grad[None],
        row_grad[None],
        fc1_bias_grad[None],
        row_grad[None],
    )


def fused_shards(
    ends_in, segments, ln_gain, ln_bias, w_qkv, w_out, w_fc1, w_fc2,
    bias_qkv, bias_out, bias_fc1, bias_fc2,
):
    nf, nt = lax.axis_size("fsdp"), lax.axis_size("tp")
    used = 6 + bias_fc1.shape[1] // LANES
    ends_out, sums, act_x, att_x, up_x, dj_x, xc, gc = fused(
        ends_in[0],
        (ln_gain, ln_bias, bias_out, bias_fc2, bias_qkv[0], bias_fc1),
        segments, w_qkv[0].transpose(1, 0, 2), w_out[0], w_fc1[0], w_fc2[0], nf, nt,
    )

    def product(left, right):
        left = left.reshape(-1, left.shape[-1])
        right = right.reshape(-1, right.shape[-1])
        return lax.dot_general(left, right, ROWS, preferred_element_type=F32)

    grad_fc2 = product(gc, act_x)
    grad_out = product(gc, att_x)
    grad_fc1 = product(xc, up_x)
    grad_qkv = jnp.stack([product(xc, dj_x[part]) for part in range(3)], axis=1)
    row_grad = sums[2:3]
    return (
        ends_out[None],
        sums[0:1],
        sums[1:2],
        grad_qkv[None],
        grad_out[None],
        grad_fc1[None],
        grad_fc2[None],
        sums[3:6][None],
        row_grad,
        sums[6:used].reshape(1, -1),
        row_grad,
    )


def shards(*args):
    rows, piece = args[0].shape[2], args[2].shape[1]
    small = rows * lax.axis_size("tp") <= 256
    tidy = piece == LANES and args[10].shape[1] // LANES <= ROWS_OF_PACK - 6
    square = lax.axis_size("fsdp") == 4 and args[0].shape[1] == 2
    return (fused_shards if small and tidy and square else split_shards)(*args)


def solution(mesh):
    both = P("section", ("fsdp", "tp"))
    square = P("section", "fsdp", "tp")
    tokens = P("section", None, ("fsdp", "tp"), None)
    heads = P("section", "fsdp", None, "tp")
    bias3 = P("section", None, ("fsdp", "tp"))
    return jax.shard_map(
        shards,
        mesh=mesh,
        in_specs=(
            tokens, P(None, "fsdp"), both, both, heads, square, square, square,
            bias3, both, both, both,
        ),
        out_specs=(
            tokens, both, both, heads, square, square, square, bias3, both, both, both,
        ),
        check_vma=False,
    )
```

```python
import functools

import jax
import jax.numpy as jnp
from jax import lax
from jax.experimental import pallas as pl
from jax.experimental.pallas import tpu as pltpu
from jax.sharding import PartitionSpec as P

HEAD_DIM = 64
ROT_DIM = 32
EPSILON = 1e-05
LANES = 128
TILE = 256
MESH = pl.DeviceIdType.MESH
F32 = jnp.float32
BF16 = jnp.bfloat16
COLS = (((1,), (1,)), ((), ()))
ROWS = (((0,), (0,)), ((), ()))
VMEM_LIMIT = 66_900_000


def positions_of(segment_ids):
    length = segment_ids.shape[-1]
    places = jnp.arange(length, dtype=jnp.int32)
    before = jnp.concatenate([segment_ids[..., :1] - 1, segment_ids[..., :-1]], axis=-1)
    starts = jnp.where(segment_ids != before, places, 0)
    starts = lax.cummax(starts, axis=segment_ids.ndim - 1)
    return places - starts


def rope_tables(segments):
    half = ROT_DIM // 2
    freq = jnp.exp(-jnp.log(10000.0) * (2.0 * jnp.arange(half, dtype=F32)) / ROT_DIM)
    angles = positions_of(segments).astype(F32)[..., None] * freq
    cosine, sine = jnp.cos(angles), jnp.sin(angles)
    none = jnp.zeros_like(sine)
    rest = jnp.zeros(angles.shape[:-1] + (HEAD_DIM - ROT_DIM,), F32)
    keep = jnp.concatenate([cosine, cosine, rest + 1.0], axis=-1)
    ahead = jnp.concatenate([-sine, none, rest], axis=-1)
    behind = jnp.concatenate([none, sine, rest], axis=-1)
    tables = jnp.stack([keep, ahead, behind], axis=1)
    return jnp.concatenate([tables, tables], axis=-1)


def send(src, dst, send_sem, recv_sem, device):
    return pltpu.make_async_remote_copy(
        src_ref=src,
        dst_ref=dst,
        send_sem=send_sem,
        recv_sem=recv_sem,
        device_id=device,
        device_id_type=MESH,
    )


def greet(peers):
    barrier = pltpu.get_barrier_semaphore()
    for peer in peers:
        pl.semaphore_signal(barrier, inc=1, device_id=peer, device_id_type=MESH)
    pl.semaphore_wait(barrier, len(peers))


def group_peers(nf, nt):
    me = lax.axis_index("fsdp") * nt + lax.axis_index("tp")
    found = []
    for k in range(1, nf * nt):
        to = lax.rem(me + k, nf * nt)
        found.append((k, to, {"fsdp": to // nt, "tp": lax.rem(to, nt)}))
    return me, found


def gather_small_kernel(nf, nt, own, out, send_sems, recv_sems, local_sem):
    me, peers = group_peers(nf, nt)
    greet([peer for _, _, peer in peers])
    mine = pltpu.make_async_copy(own, out.at[me], local_sem)
    mine.start()
    copies = []
    for k, _, peer in peers:
        copy = send(own, out.at[me], send_sems.at[k], recv_sems.at[k], peer)
        copy.start()
        copies.append(copy)
    mine.wait()
    for copy in copies:
        copy.wait()


def gather_small(own, nf, nt):
    count = nf * nt
    return pl.pallas_call(
        functools.partial(gather_small_kernel, nf, nt),
        out_shape=jax.ShapeDtypeStruct((count,) + own.shape, own.dtype),
        in_specs=[pl.BlockSpec(memory_space=pltpu.VMEM)],
        out_specs=pl.BlockSpec(memory_space=pltpu.VMEM),
        scratch_shapes=[
            pltpu.SemaphoreType.DMA((count,)),
            pltpu.SemaphoreType.DMA((count,)),
            pltpu.SemaphoreType.DMA,
        ],
        compiler_params=pltpu.CompilerParams(collective_id=0, has_side_effects=True),
        name="gather_small",
    )(own)


def sum_small_kernel(nf, nt, own, out, got, send_sems, recv_sems):
    me, peers = group_peers(nf, nt)
    greet([peer for _, _, peer in peers])
    copies = []
    for k, to, peer in peers:
        copy = send(own.at[to], got.at[k], send_sems.at[k], recv_sems.at[k], peer)
        copy.start()
        copies.append(copy)
    total = own[me]
    for k, copy in enumerate(copies):
        copy.wait()
        total = total + got[k + 1]
    out[...] = total


def sum_small(own, nf, nt):
    count = nf * nt
    return pl.pallas_call(
        functools.partial(sum_small_kernel, nf, nt),
        out_shape=jax.ShapeDtypeStruct(own.shape[1:], own.dtype),
        in_specs=[pl.BlockSpec(memory_space=pltpu.VMEM)],
        out_specs=pl.BlockSpec(memory_space=pltpu.VMEM),
        scratch_shapes=[
            pltpu.VMEM(own.shape, own.dtype),
            pltpu.SemaphoreType.DMA((count,)),
            pltpu.SemaphoreType.DMA((count,)),
        ],
        compiler_params=pltpu.CompilerParams(collective_id=1, has_side_effects=True),
        name="sum_small",
    )(own)


def cols(n, width=TILE):
    return pl.ds(pl.multiple_of(n * width, width), width)


def loop(count, body):
    def step(i, carry):
        body(i)
        return carry

    lax.fori_loop(0, count, step, 0)


def turn(x, tables, sign):
    keep, ahead, behind = tables
    left = pltpu.roll(x, LANES - ROT_DIM // 2, 1)
    right = pltpu.roll(x, ROT_DIM // 2, 1)
    return x * keep + sign * (left * ahead + right * behind)


def low_half(length):
    return lax.broadcasted_iota(jnp.int32, (length, LANES), 1) < HEAD_DIM


def allowed_mask(segc, segr, m, length):
    query = lax.broadcasted_iota(jnp.int32, (length, length), 0)
    key = lax.broadcasted_iota(jnp.int32, (length, length), 1)
    return (query >= key) & (segc[m] == segr[m])


class Ring:
    def __init__(self, nt, rows):
        self.nt, self.rows = nt, rows
        self.me = lax.axis_index("tp")
        self.others = [(k, lax.rem(self.me + k, nt)) for k in range(1, nt)]

    def block(self, who):
        return pl.ds(pl.multiple_of(who * self.rows, self.rows), self.rows)

    def gather(self, buf, m, sems):
        return [
            send(
                buf.at[m, self.block(self.me)],
                buf.at[m, self.block(self.me)],
                sems[0].at[m, k],
                sems[1].at[m, k],
                {"tp": to},
            )
            for k, to in self.others
        ]

    def scatter(self, buf, got, m, sems, part=None):
        at = slice(None) if part is None else part
        return [
            send(
                buf.at[m, self.block(to), at],
                got.at[m, k - 1, :, at],
                sems[0].at[m, k],
                sems[1].at[m, k],
                {"tp": to},
            )
            for k, to in self.others
        ]

    def total(self, buf, got, m):
        acc = buf[m, self.block(self.me)].astype(F32)
        for k, _ in self.others:
            acc = acc + got[m, k - 1].astype(F32)
        return acc


def stats(rows):
    mean = jnp.mean(rows, axis=-1, keepdims=True)
    centred = rows - mean
    variance = jnp.mean(centred * centred, axis=-1, keepdims=True)
    inv_root = lax.rsqrt(variance + EPSILON)
    return centred * inv_root, inv_root


def forward_kernel(
    nt,
    rows_h, wq_h, wo_h, w1_h, w2_h, vec, qb, fb, rope, segc, segr,
    rows_o, xg_o, qkv_o, lse_o, att_o, gp_o, act_o, y_o,
    wq, wo, w1, w2, rin, xg, qkv, lse, att, gp, act, branch, got, out_f, out_b,
    w_sem, in_sem, o_sem, ag_s, ag_r, rs_s, rs_r, x_s, x_r,
):
    micro, length, width = xg.shape
    section = lax.axis_index("section")
    first, second = section == 0, section == 1
    ring = Ring(nt, length // nt)
    own = wo.shape[1]
    loads = []
    for i, (src, dst) in enumerate(((wq_h, wq), (w1_h, w1), (wo_h, wo), (w2_h, w2))):
        loads.append(pltpu.make_async_copy(src, dst, w_sem.at[i]))
        loads[-1].start()
    mine = pltpu.make_async_copy(rows_h, rin, in_sem)

    @pl.when(first)
    def _():
        mine.start()

    greet([{"tp": to} for _, to in ring.others] + [{"section": 1 - section}])

    @pl.when(first)
    def _():
        mine.wait()

    def hop(m):
        return send(out_b.at[m], rin.at[m], x_s.at[m], x_r.at[m], {"section": 1 - section})

    def front(m):
        unit, _ = stats(rin[m].astype(F32))
        normed = unit * vec[0:1, :] + vec[1:2, :]
        xg[m, ring.block(ring.me)] = normed.astype(BF16)
        for copy in ring.gather(xg, m, (ag_s, ag_r)):
            copy.start()

    def arrive(m):
        @pl.when(second)
        def _():
            hop(m).wait_recv()
            front(m)

    stores = []

    def store(src, dst, m, i):
        copy = pltpu.make_async_copy(src.at[m], dst.at[m], o_sem.at[m, i])
        copy.start()
        stores.append(copy)

    def body(m):
        for copy in ring.gather(xg, m, (ag_s, ag_r)):
            copy.wait()
        store(xg, xg_o, m, 0)
        store(rin, rows_o, m, 1)
        tables = (rope[m, 0], rope[m, 1], rope[m, 2])
        if m == 0:
            loads[0].wait()
        per = own // TILE
        for part in range(3):
            def qkv_tile(n, part=part):
                at = cols(n)
                acc = jnp.dot(xg[m], wq[part, :, at], preferred_element_type=F32)
                acc = acc + qb[part:part + 1, at]
                if part < 2:
                    acc = jnp.concatenate(
                        [
                            turn(acc[:, c:c + LANES], tables, 1.0)
                            for c in range(0, TILE, LANES)
                        ],
                        axis=1,
                    )
                qkv[m, part, :, at] = acc.astype(BF16)

            loop(per, qkv_tile)
        store(qkv, qkv_o, m, 2)
        allowed = allowed_mask(segc, segr, m, length)
        low = low_half(length)
        lane = lax.broadcasted_iota(jnp.int32, (length, LANES), 1)

        def pair(p):
            at = cols(p, LANES)
            query, key, value = qkv[m, 0, :, at], qkv[m, 1, :, at], qkv[m, 2, :, at]
            outs = []
            for h in range(2):
                mask = low if h == 0 else ~low
                one = jnp.where(mask, query, jnp.zeros_like(query))
                s = lax.dot_general(one, key, COLS, preferred_element_type=F32)
                s = jnp.where(allowed, s * HEAD_DIM ** (-0.5), -1e30)
                top = jnp.max(s, axis=-1, keepdims=True)
                e = jnp.exp(s - top)
                total = jnp.sum(e, axis=-1, keepdims=True)
                probs = (e / total).astype(BF16)
                outs.append(jnp.dot(probs, value, preferred_element_type=F32))
                lse[m] = jnp.where(lane == 2 * p + h, top + jnp.log(total), lse[m])
            att[m, :, at] = jnp.where(low, outs[0], outs[1]).astype(BF16)

        lse[m] = jnp.zeros((length, LANES), F32)
        loop(own // LANES, pair)
        store(lse, lse_o, m, 3)
        store(att, att_o, m, 4)
        if m == 0:
            loads[1].wait()

        def up_tile(n):
            at = cols(n)
            u = jnp.dot(xg[m], w1[:, at], preferred_element_type=F32) + fb[0:1, at]
            c = 0.7978845608028654
            square = u * u
            t = jnp.tanh(c * u * (1.0 + 0.044715 * square))
            act[m, :, at] = (0.5 * u * (1.0 + t)).astype(BF16)
            slope = 0.5 * (1.0 + t) + 0.5 * u * (1.0 - t * t) * (c * (1.0 + 3 * 0.044715 * square))
            gp[m, :, at] = slope.astype(BF16)

        loop(act.shape[2] // TILE, up_tile)
        store(act, act_o, m, 5)
        store(gp, gp_o, m, 6)
        if m == 0:
            loads[2].wait()
            loads[3].wait()

        def out_tile(n):
            at = cols(n)
            acc = lax.dot_general(att[m], wo[at, :], COLS, preferred_element_type=F32)
            acc = acc + lax.dot_general(act[m], w2[at, :], COLS, preferred_element_type=F32)
            branch[m, :, at] = acc.astype(BF16)
            for copy in ring.scatter(branch, got, m, (rs_s, rs_r), at):
                copy.start()

        loop(width // TILE, out_tile)

    def finish(m):
        for copy in ring.scatter(branch, got, m, (rs_s, rs_r)):
            copy.wait()
        y = rin[m].astype(F32) + ring.total(branch, got, m) + vec[2:3, :]
        out_f[m] = y
        out_b[m] = y.astype(BF16)
        store(out_f, y_o, m, 7)

        @pl.when(first)
        def _():
            hop(m).start()

    @pl.when(first)
    def _():
        for m in range(micro):
            front(m)

    for m in range(micro):
        arrive(m)
        body(m)
    for m in range(micro):
        finish(m)
    for copy in stores:
        copy.wait()

    @pl.when(first)
    def _():
        for m in range(micro):
            hop(m).wait_send()


def forward(rows, weights, vec, qb, fb, rope, segc, segr, nt):
    wq, wo, w1, w2 = weights
    micro, per, width = rows.shape
    length = per * nt
    own, hidden = wo.shape[1], w1.shape[1]
    anywhere = pl.BlockSpec(memory_space=pl.ANY)
    inside = pl.BlockSpec(memory_space=pltpu.VMEM)
    out_shape = [
        jax.ShapeDtypeStruct(rows.shape, BF16),
        jax.ShapeDtypeStruct((micro, length, width), BF16),
        jax.ShapeDtypeStruct((micro, 3, length, own), BF16),
        jax.ShapeDtypeStruct((micro, length, LANES), F32),
        jax.ShapeDtypeStruct((micro, length, own), BF16),
        jax.ShapeDtypeStruct((micro, length, hidden), BF16),
        jax.ShapeDtypeStruct((micro, length, hidden), BF16),
        jax.ShapeDtypeStruct(rows.shape, F32),
    ]
    dma = pltpu.SemaphoreType.DMA
    return pl.pallas_call(
        functools.partial(forward_kernel, nt),
        out_shape=out_shape,
        in_specs=[anywhere] * 5 + [inside] * 6,
        out_specs=[anywhere] * 8,
        scratch_shapes=[
            pltpu.VMEM(wq.shape, BF16),
            pltpu.VMEM(wo.shape, BF16),
            pltpu.VMEM(w1.shape, BF16),
            pltpu.VMEM(w2.shape, BF16),
            pltpu.VMEM(rows.shape, BF16),
            pltpu.VMEM((micro, length, width), BF16),
            pltpu.VMEM((micro, 3, length, own), BF16),
            pltpu.VMEM((micro, length, LANES), F32),
            pltpu.VMEM((micro, length, own), BF16),
            pltpu.VMEM((micro, length, hidden), BF16),
            pltpu.VMEM((micro, length, hidden), BF16),
            pltpu.VMEM((micro, length, width), BF16),
            pltpu.VMEM((micro, nt - 1, per, width), BF16),
            pltpu.VMEM(rows.shape, F32),
            pltpu.VMEM(rows.shape, BF16),
            dma((4,)),
            dma,
            dma((micro, 8)),
            dma((micro, nt)),
            dma((micro, nt)),
            dma((micro, nt)),
            dma((micro, nt)),
            dma((micro,)),
            dma((micro,)),
        ],
        compiler_params=pltpu.CompilerParams(
            collective_id=2, has_side_effects=True, vmem_limit_bytes=VMEM_LIMIT
        ),
        name="forward",
    )(rows, wq, wo, w1, w2, vec, qb, fb, rope, segc, segr)


def backward_kernel(
    nt,
    dy_h, wq_h, wo_h, w1_h, w2_h, rows_h, qkv_h, lse_h, gp_h, vec, rope, segc, segr,
    gr_o, up_o, dj_o, dx_o, own_sums, head_sums, up_sums,
    wq, wo, w1, w2, dyr, rin, qkv, lse, gp, gr, gatt, up, dj, branch, got, out_f, out_b,
    w_sem, in_sem, o_sem, ag_s, ag_r, rs_s, rs_r, x_s, x_r,
):
    micro, length, width = gr.shape
    section = lax.axis_index("section")
    first, second = section == 0, section == 1
    ring = Ring(nt, length // nt)
    own = wo.shape[1]
    mine = pltpu.make_async_copy(dy_h, dyr, in_sem.at[4])

    @pl.when(second)
    def _():
        mine.start()

    loads = []
    for i, (src, dst) in enumerate(((wo_h, wo), (w2_h, w2), (wq_h, wq), (w1_h, w1))):
        loads.append(pltpu.make_async_copy(src, dst, w_sem.at[i]))
    kept = []
    for i, (src, dst) in enumerate(((qkv_h, qkv), (lse_h, lse), (gp_h, gp), (rows_h, rin))):
        kept.append(pltpu.make_async_copy(src, dst, in_sem.at[i]))
    for copy in (loads[0], kept[0], kept[1], loads[1], kept[2], loads[2], loads[3], kept[3]):
        copy.start()
    greet([{"tp": to} for _, to in ring.others] + [{"section": 1 - section}])

    @pl.when(second)
    def _():
        mine.wait()

    def hop(m):
        return send(out_b.at[m], dyr.at[m], x_s.at[m], x_r.at[m], {"section": 1 - section})

    def front(m):
        gr[m, ring.block(ring.me)] = dyr[m]
        for copy in ring.gather(gr, m, (ag_s, ag_r)):
            copy.start()

    def arrive(m):
        @pl.when(first)
        def _():
            hop(m).wait_recv()
            front(m)

    stores = []

    def store(src, dst, m, i):
        copy = pltpu.make_async_copy(src.at[m], dst.at[m], o_sem.at[m, i])
        copy.start()
        stores.append(copy)

    def body(m):
        for copy in ring.gather(gr, m, (ag_s, ag_r)):
            copy.wait()
        store(gr, gr_o, m, 0)
        if m == 0:
            loads[0].wait()

        def att_tile(n):
            at = cols(n)
            gatt[:, at] = jnp.dot(gr[m], wo[:, at], preferred_element_type=F32).astype(BF16)

        loop(own // TILE, att_tile)
        if m == 0:
            kept[0].wait()
            kept[1].wait()
        tables = (rope[m, 0], rope[m, 1], rope[m, 2])
        allowed = allowed_mask(segc, segr, m, length)
        low = low_half(length)
        lane = lax.broadcasted_iota(jnp.int32, (length, LANES), 1)
        factor = HEAD_DIM ** (-0.5)

        def pair(p):
            at = cols(p, LANES)
            query, key, value = qkv[m, 0, :, at], qkv[m, 1, :, at], qkv[m, 2, :, at]
            grad = gatt[:, at]
            dqs, dks, dvs = [], [], []
            for h in range(2):
                mask = low if h == 0 else ~low
                one = jnp.where(mask, query, jnp.zeros_like(query))
                s = lax.dot_general(one, key, COLS, preferred_element_type=F32)
                s = jnp.where(allowed, s * factor, -1e30)
                log_total = jnp.sum(
                    jnp.where(lane == 2 * p + h, lse[m], 0.0), axis=-1, keepdims=True
                )
                soft = jnp.exp(s - log_total)
                probs = soft.astype(BF16)
                one_grad = jnp.where(mask, grad, jnp.zeros_like(grad))
                dp = lax.dot_general(one_grad, value, COLS, preferred_element_type=F32)
                delta = jnp.sum(dp * soft, axis=-1, keepdims=True)
                ds = (soft * (dp - delta)).astype(BF16)
                dvs.append(lax.dot_general(probs, grad, ROWS, preferred_element_type=F32))
                dqs.append(jnp.dot(ds, key, preferred_element_type=F32))
                dks.append(lax.dot_general(ds, query, ROWS, preferred_element_type=F32))
            dq = jnp.where(low, dqs[0], dqs[1]) * factor
            dk = jnp.where(low, dks[0], dks[1]) * factor
            dj[m, 0, :, at] = turn(dq, tables, -1.0).astype(BF16)
            dj[m, 1, :, at] = turn(dk, tables, -1.0).astype(BF16)
            dj[m, 2, :, at] = jnp.where(low, dvs[0], dvs[1]).astype(BF16)

        loop(own // LANES, pair)
        store(dj, dj_o, m, 1)
        for part in range(3):
            sums = jnp.sum(dj[m, part].astype(F32), axis=0, keepdims=True)
            if m == 0:
                head_sums[part:part + 1, :] = sums
            else:
                head_sums[part:part + 1, :] += sums
        if m == 0:
            loads[1].wait()
            kept[2].wait()

        def up_tile(n):
            at = cols(n)
            acc = jnp.dot(gr[m], w2[:, at], preferred_element_type=F32)
            rounded = (acc * gp[m, :, at].astype(F32)).astype(BF16)
            up[m, :, at] = rounded
            sums = jnp.sum(rounded.astype(F32), axis=0, keepdims=True)
            if m == 0:
                up_sums[0:1, at] = sums
            else:
                up_sums[0:1, at] += sums

        loop(up.shape[2] // TILE, up_tile)
        store(up, up_o, m, 2)
        if m == 0:
            loads[2].wait()
            loads[3].wait()

        def norm_tile(n):
            at = cols(n)
            acc = lax.dot_general(up[m], w1[at, :], COLS, preferred_element_type=F32)
            for part in range(3):
                acc = acc + lax.dot_general(
                    dj[m, part], wq[part, at, :], COLS, preferred_element_type=F32
                )
            branch[m, :, at] = acc.astype(BF16)
            for copy in ring.scatter(branch, got, m, (rs_s, rs_r), at):
                copy.start()

        loop(width // TILE, norm_tile)

    def finish(m):
        for copy in ring.scatter(branch, got, m, (rs_s, rs_r)):
            copy.wait()
        if m == 0:
            kept[3].wait()
        grad_norm = ring.total(branch, got, m)
        unit, inv_root = stats(rin[m].astype(F32))
        scaled = grad_norm * vec[0:1, :]
        upstream = dyr[m].astype(F32)
        dx = upstream + inv_root * (
            scaled
            - jnp.mean(scaled, axis=-1, keepdims=True)
            - unit * jnp.mean(scaled * unit, axis=-1, keepdims=True)
        )
        out_f[m] = dx
        out_b[m] = dx.astype(BF16)

        @pl.when(second)
        def _():
            hop(m).start()

        store(out_f, dx_o, m, 3)
        for i, term in enumerate((grad_norm * unit, grad_norm, upstream)):
            sums = jnp.sum(term, axis=0, keepdims=True)
            if m == 0:
                own_sums[i:i + 1, :] = sums
            else:
                own_sums[i:i + 1, :] += sums

    @pl.when(second)
    def _():
        for m in range(micro):
            front(m)

    for m in range(micro):
        arrive(m)
        body(m)
    for m in range(micro):
        finish(m)
    for copy in stores:
        copy.wait()

    @pl.when(second)
    def _():
        for m in range(micro):
            hop(m).wait_send()


def backward(dy, weights, rows, qkv, lse, gp, vec, rope, segc, segr, nt):
    wq, wo, w1, w2 = weights
    micro, per, width = rows.shape
    length = per * nt
    own, hidden = wo.shape[1], w1.shape[1]
    anywhere = pl.BlockSpec(memory_space=pl.ANY)
    inside = pl.BlockSpec(memory_space=pltpu.VMEM)
    out_shape = [
        jax.ShapeDtypeStruct((micro, length, width), BF16),
        jax.ShapeDtypeStruct((micro, length, hidden), BF16),
        jax.ShapeDtypeStruct((micro, 3, length, own), BF16),
        jax.ShapeDtypeStruct(rows.shape, F32),
        jax.ShapeDtypeStruct((8, width), F32),
        jax.ShapeDtypeStruct((8, own), F32),
        jax.ShapeDtypeStruct((8, hidden), F32),
    ]
    dma = pltpu.SemaphoreType.DMA
    return pl.pallas_call(
        functools.partial(backward_kernel, nt),
        out_shape=out_shape,
        in_specs=[anywhere] * 9 + [inside] * 4,
        out_specs=[anywhere] * 4 + [inside] * 3,
        scratch_shapes=[
            pltpu.VMEM(wq.shape, BF16),
            pltpu.VMEM(wo.shape, BF16),
            pltpu.VMEM(w1.shape, BF16),
            pltpu.VMEM(w2.shape, BF16),
            pltpu.VMEM(rows.shape, BF16),
            pltpu.VMEM(rows.shape, BF16),
            pltpu.VMEM(qkv.shape, BF16),
            pltpu.VMEM(lse.shape, F32),
            pltpu.VMEM(gp.shape, BF16),
            pltpu.VMEM((micro, length, width), BF16),
            pltpu.VMEM((length, own), BF16),
            pltpu.VMEM((micro, length, hidden), BF16),
            pltpu.VMEM((micro, 3, length, own), BF16),
            pltpu.VMEM((micro, length, width), BF16),
            pltpu.VMEM((micro, nt - 1, per, width), BF16),
            pltpu.VMEM(rows.shape, F32),
            pltpu.VMEM(rows.shape, BF16),
            dma((4,)),
            dma((5,)),
            dma((micro, 4)),
            dma((micro, nt)),
            dma((micro, nt)),
            dma((micro, nt)),
            dma((micro, nt)),
            dma((micro,)),
            dma((micro,)),
        ],
        compiler_params=pltpu.CompilerParams(
            collective_id=3, has_side_effects=True, vmem_limit_bytes=VMEM_LIMIT
        ),
        name="backward",
    )(dy, wq, wo, w1, w2, rows, qkv, lse, gp, vec, rope, segc, segr)


ROWS_OF_PACK = 16
PIECES = 4


def twist(x, tables, sign):
    keep, sine, ahead = tables
    left = pltpu.roll(x, LANES - ROT_DIM // 2, 1)
    right = pltpu.roll(x, ROT_DIM // 2, 1)
    return x * keep + jnp.where(ahead, left, right) * (sign * sine)


def masks_of(nf):
    return range(nf)


def bits_below(mask, nf):
    low = mask & -mask if mask else nf
    return [(i, 1 << i) for i in range(nf.bit_length() - 1) if (1 << i) < low]


def flipped(index, mask, nf):
    for i in range(nf.bit_length() - 1):
        if mask >> i & 1:
            index = index + (1 << i) * (1 - 2 * lax.rem(index // (1 << i), 2))
    return index


def fused_kernel(
    nf, nt,
    ends_h, gain, shift, b_out, b_fc2, b_qkv, b_fc1, seg_in, wq_h, wo_h, w1_h, w2_h,
    ends_o, sums_o, act_x, att_x, up_x, dj_x, xc_x, gc_x,
    wq, wo, w1, w2, pack, packs, wide, fb, segs, rope, rin, dyr, xg, qkv, lse, att, gp, act,
    gr, gatt, up, dj, out_bf, out_got, in_bf, in_got, y_f, y_b,
    own_sums, head_sums, up_sums, s_src, s_got,
    in_sem, wl_sem, ws_sem, wr_sem, pk_s, pk_r, sm_s, sm_r,
    ag_s, ag_r, gg_s, gg_r, rs_s, rs_r, rb_s, rb_r, hx_s, hx_r, hb_s, hb_r,
    xl_sem, xs_s, xs_r, cl_sem, ca_s, ca_r, mx_s, mx_r, o_sem,
    l1_s, l1_r, l2_s, l2_r, fw_s, fw_r, go_sem,
):
    micro, per, width = rin.shape
    length = per * nt
    section, f, t = (lax.axis_index(a) for a in ("section", "fsdp", "tp"))
    first, second = section == 0, section == 1
    ring = Ring(nt, per)
    own, hidden = wo.shape[1], w1.shape[1]
    depth = width // nf
    mirror, sibling = {"fsdp": flipped(f, 2, nf)}, {"fsdp": flipped(f, 1, nf)}
    count = nf * nt
    other = {"section": 1 - section}
    across = {"section": 1 - section, "fsdp": flipped(f, 2, nf)}
    me, group = group_peers(nf, nt)
    fblock = [flipped(f, mask, nf) for mask in masks_of(nf)]

    def rows_at(block):
        return pl.ds(pl.multiple_of(block * depth, depth), depth)

    load_rows = pltpu.make_async_copy(ends_h, rin, in_sem)
    load_dy = pltpu.make_async_copy(ends_h, dyr, in_sem)

    @pl.when(first)
    def _():
        load_rows.start()

    @pl.when(second)
    def _():
        load_dy.start()

    greet([peer for _, _, peer in group] + [other, across])

    per_row = hidden // nf // LANES
    segs[0] = jnp.zeros((8, length), F32)
    segs[0, 0:micro, :] = seg_in[...].astype(F32)
    pack[...] = jnp.zeros_like(pack)
    pack[0:1, :] = gain[...].astype(F32)
    pack[1:2, :] = shift[...].astype(F32)
    pack[2:3, :] = b_out[...].astype(F32) + b_fc2[...].astype(F32)
    pack[3:6, :] = b_qkv[...].astype(F32)
    for r in range(per_row):
        pack[6 + r:7 + r, :] = b_fc1[:, r * LANES:(r + 1) * LANES].astype(F32)
    seg_copy = send(segs.at[0], segs.at[1], mx_s.at[2, 0], mx_r.at[2, 0], mirror)
    pack_local = pltpu.make_async_copy(pack, packs.at[me], pk_s.at[0])
    pack_copies = [
        send(pack, packs.at[me], pk_s.at[k], pk_r.at[k], peer) for k, _, peer in group
    ]
    pack_local.start()
    seg_copy.start()
    for copy in pack_copies:
        copy.start()

    table = ((wq_h, wq), (w1_h, w1), (wo_h, wo), (w2_h, w2))

    def w_at(ref, block):
        return ref.at[:, rows_at(block), :] if len(ref.shape) == 3 else ref.at[rows_at(block), :]

    def w_local(a):
        return pltpu.make_async_copy(table[a][0], w_at(table[a][1], f), wl_sem.at[a])

    def w_send(a, mask, i, bit):
        block = w_at(table[a][1], fblock[mask])
        src = table[a][0] if mask == 0 else block
        peer = {"fsdp": flipped(f, bit, nf)}
        return send(src, block, ws_sem.at[a, mask, i], wr_sem.at[a, mask | bit], peer)

    def w_recv(a, mask):
        block = w_at(table[a][1], fblock[mask])
        return send(block, block, ws_sem.at[a, mask, 0], wr_sem.at[a, mask], other)

    def w_near(a):
        w_local(a).start()
        w_send(a, 0, 0, 1).start()

    def w_far(a):
        w_send(a, 0, 1, 2).start()

    part_rows = depth // PIECES
    per_slot = length // part_rows

    def stage(p):
        return up.at[p // per_slot, pl.ds(p % per_slot * part_rows, part_rows), :]

    def piece_at(a, mask, p):
        start = pl.multiple_of(fblock[mask] * depth + p * part_rows, part_rows)
        return table[a][1].at[pl.ds(start, part_rows), :]

    def leg_one(a, p):
        src = table[a][0].at[pl.ds(p * part_rows, part_rows), :]
        return send(src, stage(p), l1_s.at[p], l1_r.at[p], across)

    def leg_two(a, p):
        return send(stage(p), piece_at(a, 2, p), l2_s.at[p], l2_r.at[p], other)

    def passed_on(a, mask, p):
        block = piece_at(a, mask, p)
        return send(block, block, fw_s.at[p], fw_r.at[p], sibling)

    def relay(a, p):
        leg_one(a, p).wait_recv()
        leg_two(a, p).start()

    def via_ready(a):
        for p in range(PIECES):
            leg_two(a, p).wait_recv()
            passed_on(a, 2, p).start()
        for p in range(PIECES):
            passed_on(a, 3, p).wait_recv()

    def w_ready(a, mask):
        if mask == 0:
            w_local(a).wait()
            return
        w_recv(a, mask).wait_recv()
        for i, bit in bits_below(mask, nf):
            w_send(a, mask, i, bit).start()

    order = sorted(masks_of(nf), key=lambda m: (m != 0, -(m & -m), m))
    out_order = list(masks_of(nf))
    for a in range(4):
        w_near(a)

    @pl.when(first)
    def _():
        w_far(0)
        w_far(2)
        for p in range(PIECES):
            leg_one(1, p).start()

    def small_arrive():
        pack_local.wait()
        for copy in pack_copies:
            copy.wait()
        for j in range(count):
            wide[:, j * LANES:(j + 1) * LANES] = packs[j]
        for j in range(nf):
            for r in range(per_row):
                c = (j * per_row + r) * LANES
                fb[0:1, c:c + LANES] = packs[t * nf + j, 6 + r:7 + r, :]

    def segment_parts(q):
        row = segs[q // micro, pl.ds(lax.rem(q, micro), 1), :]
        query = lax.broadcasted_iota(jnp.int32, (length, length), 0)
        key = lax.broadcasted_iota(jnp.int32, (length, length), 1)
        column = jnp.sum(jnp.where(query == key, row, 0.0), axis=1, keepdims=True)
        return row, column, query >= key

    def allowed_of(q):
        row, column, causal = segment_parts(q)
        return causal & (row == column)

    def rope_of(q):
        row, column, _ = segment_parts(q)
        before = jnp.sum(jnp.where(row < column, 1.0, 0.0), axis=1, keepdims=True)
        lane = lax.rem(lax.broadcasted_iota(jnp.int32, (length, LANES), 1), HEAD_DIM)
        place = lax.broadcasted_iota(jnp.int32, (length, LANES), 0).astype(F32) - before
        half = ROT_DIM // 2
        power = lax.rem(lane, half).astype(F32)
        freq = jnp.exp(-jnp.log(10000.0) * (2.0 * power) / ROT_DIM)
        angles = place * freq
        rope[q, 0] = jnp.where(lane < ROT_DIM, jnp.cos(angles), 1.0)
        sine = jnp.where(lane < ROT_DIM, jnp.sin(angles), 0.0)
        rope[q, 1] = jnp.where(lane < half, -sine, sine)

    def hop_out(m):
        return send(y_b.at[m], rin.at[m], hx_s.at[m], hx_r.at[m], other)

    def hop_back(m):
        return send(y_b.at[m], dyr.at[m], hb_s.at[m], hb_r.at[m], other)

    def front(m):
        unit, _ = stats(rin[m].astype(F32))
        normed = unit * wide[0:1, :] + wide[1:2, :]
        xg[m, ring.block(ring.me)] = normed.astype(BF16)
        for copy in ring.gather(xg, m, (ag_s, ag_r)):
            copy.start()

    def front_back(m):
        gr[m, ring.block(ring.me)] = dyr[m]
        for copy in ring.gather(gr, m, (gg_s, gg_r)):
            copy.start()

    def mirror_copy(which, m):
        buf = (xg, gr)[which]
        return send(
            buf.at[m], buf.at[micro + m], mx_s.at[which, m], mx_r.at[which, m], mirror
        )

    def x_block(who):
        return fblock[2 * who] if isinstance(who, int) else jnp.where(who == 0, f, fblock[2])

    def x_dst(a, m, who):
        block = x_block(who)
        if a == 3:
            return dj_x.at[:, m, block]
        return (act_x, att_x, up_x)[a].at[m, block]

    def x_src(a, m, who):
        place = (m, micro)[who] if isinstance(who, int) else jnp.where(who == 0, m, micro)
        return (act, att, up, dj)[a].at[place]

    def x_local(a, m, who):
        return pltpu.make_async_copy(
            x_src(a, m, who), x_dst(a, m, who), xl_sem.at[a, m, who]
        )

    def x_send(a, m, who):
        return send(
            x_src(a, m, who), x_dst(a, m, who), xs_s.at[a, m, who], xs_r.at[a, m, who], sibling
        )

    def x_start(a, m, who):
        x_local(a, m, who).start()
        x_send(a, m, who).start()

    def x_sent(a, m, who):
        x_local(a, m, who).wait()
        x_send(a, m, who).wait_send()

    def c_pair(which, m, who):
        src, dst = ((xg, xc_x), (gr, gc_x))[which]
        block = x_block(who)
        q = who * micro + m
        mine = pltpu.make_async_copy(
            src.at[q, :, rows_at(f)], dst.at[m, block], cl_sem.at[which, m, who]
        )
        theirs = send(
            src.at[q, :, rows_at(fblock[1])],
            dst.at[m, block],
            ca_s.at[which, m, who],
            ca_r.at[which, m, who],
            sibling,
        )
        return mine, theirs

    def c_start(which, m, who):
        for copy in c_pair(which, m, who):
            copy.start()

    def attention_masks(q):
        low = low_half(length)
        lane = lax.broadcasted_iota(jnp.int32, (length, LANES), 1)
        tables = (rope[q, 0], rope[q, 1], lax.rem(lane, HEAD_DIM) < ROT_DIM // 2)
        return low, lane, tables, allowed_of(q)

    factor = HEAD_DIM ** (-0.5)

    def forward_stage(m, who, k, fresh):
        q = who * micro + m
        place = jnp.where(who == 0, m, micro)

        @pl.when(who == 0)
        def _():
            for copy in ring.gather(xg, m, (ag_s, ag_r)):
                copy.wait()
            c_start(0, m, 0)

            @pl.when(second)
            def _():
                mirror_copy(0, m).start()

        @pl.when(who == 1)
        def _():
            mirror_copy(0, m).wait_recv()
            c_start(0, m, 1)

            @pl.when(m == 1)
            def _():
                x_sent(0, 0, 1)
                x_sent(1, 0, 1)

        @pl.when(fresh)
        def _():
            for mask in order:
                w_ready(0, mask)
            w_far(3)

        low, lane, tables, allowed = attention_masks(q)
        for part in range(3):
            def qkv_tile(n, part=part):
                at = cols(n)
                acc = jnp.dot(xg[q], wq[part, :, at], preferred_element_type=F32)
                acc = acc + wide[3 + part:4 + part, pl.ds(
                    pl.multiple_of(t * own + n * TILE, TILE), TILE)]
                if part < 2:
                    acc = jnp.concatenate(
                        [
                            twist(acc[:, c:c + LANES], tables, 1.0)
                            for c in range(0, TILE, LANES)
                        ],
                        axis=1,
                    )
                qkv[q, part, :, at] = acc.astype(BF16)

            loop(own // TILE, qkv_tile)

        def pair(p):
            at = cols(p, LANES)
            query, key, value = qkv[q, 0, :, at], qkv[q, 1, :, at], qkv[q, 2, :, at]
            outs = []
            for h in range(2):
                mask = low if h == 0 else ~low
                one = jnp.where(mask, query, jnp.zeros_like(query))
                s = lax.dot_general(one, key, COLS, preferred_element_type=F32)
                s = jnp.where(allowed, s * factor, -1e30)
                top = jnp.max(s, axis=-1, keepdims=True)
                e = jnp.exp(s - top)
                total = jnp.sum(e, axis=-1, keepdims=True)
                probs = (e / total).astype(BF16)
                outs.append(jnp.dot(probs, value, preferred_element_type=F32))
                lse[q] = jnp.where(lane == 2 * p + h, top + jnp.log(total), lse[q])
            att[place, :, at] = jnp.where(low, outs[0], outs[1]).astype(BF16)

        lse[q] = jnp.zeros((length, LANES), F32)
        loop(own // LANES, pair)
        x_start(1, m, who)

        @pl.when(first & (k == 1))
        def _():
            output_finish(0)
            relay(3, 0)

        @pl.when(k == 0)
        def _():
            w_ready(1, 0)
            w_ready(1, 1)

        @pl.when(fresh)
        def _():
            via_ready(1)

        @pl.when(second & (k == 0))
        def _():
            w_ready(1, 3)

        def up_tile(n):
            at = cols(n)
            u = jnp.dot(xg[q], w1[:, at], preferred_element_type=F32) + fb[0:1, at]
            c = 0.7978845608028654
            square = u * u
            th = jnp.tanh(c * u * (1.0 + 0.044715 * square))
            act[place, :, at] = (0.5 * u * (1.0 + th)).astype(BF16)
            slope = 0.5 * (1.0 + th)
            slope = slope + 0.5 * u * (1.0 - th * th) * (c * (1.0 + 3 * 0.044715 * square))
            gp[q, :, at] = slope.astype(BF16)

        loop(hidden // TILE, up_tile)
        x_start(0, m, who)

    def output_stage(m, fresh):
        for mask in out_order:
            @pl.when(fresh)
            def _(mask=mask):
                w_ready(2, mask)
                w_ready(3, mask)

            def out_tile(n, mask=mask):
                start = pl.multiple_of(fblock[mask] * depth + n * TILE, TILE)
                at = pl.ds(start, TILE)
                acc = lax.dot_general(att[m], wo[at, :], COLS, preferred_element_type=F32)
                acc = acc + lax.dot_general(act[m], w2[at, :], COLS, preferred_element_type=F32)
                out_bf[m, :, at] = acc.astype(BF16)
                for copy in ring.scatter(out_bf, out_got, m, (rs_s, rs_r), at):
                    copy.start()

            loop(depth // TILE, out_tile)

        @pl.when(fresh)
        def _():
            pl.semaphore_signal(go_sem, inc=1, device_id=other, device_id_type=MESH)

    def store_ends(m):
        return pltpu.make_async_copy(y_f.at[m], ends_o.at[m], o_sem.at[m])

    def output_finish(m):
        for copy in ring.scatter(out_bf, out_got, m, (rs_s, rs_r)):
            copy.wait()
        y = rin[m].astype(F32) + ring.total(out_bf, out_got, m) + wide[2:3, :]

        @pl.when(first)
        def _():
            y_b[m] = y.astype(BF16)
            hop_out(m).start()

        @pl.when(second)
        def _():
            y_f[m] = y
            store_ends(m).start()

    def backward_stage(m, who, k):
        q = who * micro + m
        place = jnp.where(who == 0, m, micro)

        @pl.when(first & (who == 0))
        def _():
            for copy in ring.gather(gr, m, (gg_s, gg_r)):
                copy.wait()
            mirror_copy(1, m).start()
            c_start(1, m, 0)

        @pl.when(who == 1)
        def _():
            mirror_copy(1, m).wait_recv()
            c_start(1, m, 1)

            @pl.when(m == 1)
            def _():
                x_sent(2, 0, 1)
                x_sent(3, 0, 1)

        def att_tile(n):
            at = cols(n)
            gatt[:, at] = jnp.dot(gr[q], wo[:, at], preferred_element_type=F32).astype(BF16)

        loop(own // TILE, att_tile)
        low, lane, tables, allowed = attention_masks(q)

        def pair(p):
            at = cols(p, LANES)
            query, key, value = qkv[q, 0, :, at], qkv[q, 1, :, at], qkv[q, 2, :, at]
            grad = gatt[:, at]
            dqs, dks, dvs = [], [], []
            for h in range(2):
                mask = low if h == 0 else ~low
                one = jnp.where(mask, query, jnp.zeros_like(query))
                s = lax.dot_general(one, key, COLS, preferred_element_type=F32)
                s = jnp.where(allowed, s * factor, -1e30)
                log_total = jnp.sum(
                    jnp.where(lane == 2 * p + h, lse[q], 0.0), axis=-1, keepdims=True
                )
                soft = jnp.exp(s - log_total)
                probs = soft.astype(BF16)
                one_grad = jnp.where(mask, grad, jnp.zeros_like(grad))
                dp = lax.dot_general(one_grad, value, COLS, preferred_element_type=F32)
                delta = jnp.sum(dp * soft, axis=-1, keepdims=True)
                ds = (soft * (dp - delta)).astype(BF16)
                dvs.append(lax.dot_general(probs, grad, ROWS, preferred_element_type=F32))
                dqs.append(jnp.dot(ds, key, preferred_element_type=F32))
                dks.append(lax.dot_general(ds, query, ROWS, preferred_element_type=F32))
            dq = jnp.where(low, dqs[0], dqs[1]) * factor
            dk = jnp.where(low, dks[0], dks[1]) * factor
            dj[place, 0, :, at] = twist(dq, tables, -1.0).astype(BF16)
            dj[place, 1, :, at] = twist(dk, tables, -1.0).astype(BF16)
            dj[place, 2, :, at] = jnp.where(low, dvs[0], dvs[1]).astype(BF16)

        loop(own // LANES, pair)
        x_start(3, m, who)

        @pl.when(who == 0)
        def _():
            for part in range(3):
                head_sums[part:part + 1, :] += jnp.sum(
                    dj[m, part].astype(F32), axis=0, keepdims=True
                )

        @pl.when(second & (k == 1))
        def _():
            w_ready(3, 0)
            w_ready(3, 1)
            via_ready(3)

        def up_tile(n):
            at = cols(n)
            acc = jnp.dot(gr[q], w2[:, at], preferred_element_type=F32)
            rounded = (acc * gp[q, :, at].astype(F32)).astype(BF16)
            up[place, :, at] = rounded
            sums = jnp.sum(rounded.astype(F32), axis=0, keepdims=True)
            up_sums[0:1, at] += jnp.where(who == 0, sums, 0.0)

        loop(hidden // TILE, up_tile)
        x_start(2, m, who)

        @pl.when(second & (k == 3))
        def _():
            backward_finish(0)

        @pl.when(first & (k == 4))
        def _():
            hop_back(1).wait_recv()
            front_back(1)

        def norm_tile(n):
            at = cols(n)
            acc = lax.dot_general(up[m], w1[at, :], COLS, preferred_element_type=F32)
            for part in range(3):
                acc = acc + lax.dot_general(
                    dj[m, part], wq[part, at, :], COLS, preferred_element_type=F32
                )
            in_bf[m, :, at] = acc.astype(BF16)
            for copy in ring.scatter(in_bf, in_got, m, (rb_s, rb_r), at):
                copy.start()

        @pl.when(who == 0)
        def _():
            loop(width // TILE, norm_tile)


    def backward_finish(m):
        for copy in ring.scatter(in_bf, in_got, m, (rb_s, rb_r)):
            copy.wait()
        grad_norm = ring.total(in_bf, in_got, m)
        unit, inv_root = stats(rin[m].astype(F32))
        scaled = grad_norm * wide[0:1, :]
        upstream = dyr[m].astype(F32)
        dx = upstream + inv_root * (
            scaled
            - jnp.mean(scaled, axis=-1, keepdims=True)
            - unit * jnp.mean(scaled * unit, axis=-1, keepdims=True)
        )

        @pl.when(second)
        def _():
            y_b[m] = dx.astype(BF16)
            hop_back(m).start()

        @pl.when(first)
        def _():
            y_f[m] = dx
            store_ends(m).start()

        for i, term in enumerate((grad_norm * unit, grad_norm, upstream)):
            own_sums[i:i + 1, :] += jnp.sum(term, axis=0, keepdims=True)

    own_sums[...] = jnp.zeros_like(own_sums)
    head_sums[...] = jnp.zeros_like(head_sums)
    up_sums[...] = jnp.zeros_like(up_sums)

    @pl.when(first)
    def _():
        small_arrive()
        load_rows.wait()
        loop(micro, front)
        seg_copy.wait()
        loop(2 * micro, rope_of)

    @pl.when(second)
    def _():
        load_dy.wait()
        loop(micro, front_back)

    @pl.when(second)
    def _():
        for p in range(PIECES):
            relay(1, p)
        w_far(0)
        w_far(1)
        small_arrive()
        seg_copy.wait()
        loop(2 * micro, rope_of)
        for mask in order:
            w_ready(0, mask)
        w_far(2)
        for p in range(PIECES):
            leg_two(1, p).wait_send()
        pl.semaphore_wait(go_sem, 1)
        for p in range(PIECES):
            leg_one(3, p).start()

        def dy_in(m):
            for copy in ring.gather(gr, m, (gg_s, gg_r)):
                copy.wait()
            c_start(1, m, 0)

        loop(micro, dy_in)

    def slot(k):
        is_f = jnp.where(first, k < 4, (k < 8) & (lax.rem(k, 2) == 0))
        is_o = jnp.where(first, k < 2, (k == 5) | (k == 6))
        who = jnp.where(first, (k // 2) % 2 * (k < 4) + lax.rem(k, 2) * (k >= 4), k // 4)
        m = jnp.where(first, jnp.where(k < 4, lax.rem(k, 2), (k - 4) // 2), lax.rem(k // 2, 2))
        m_o = jnp.where(first, m, k - 5)
        fresh = first & (k == 0)

        @pl.when(second & ((k == 0) | (k == 1)))
        def _():
            hop_out(k).wait_recv()
            front(k)

        @pl.when(second & (k == 0))
        def _():
            w_ready(1, 2)

        @pl.when(second & (k == 1))
        def _():
            for i in range(micro):
                mirror_copy(1, i).start()
            for mask in order:
                w_ready(2, mask)

        @pl.when(first & (k == 4))
        def _():
            for p in range(PIECES):
                leg_two(3, p).wait_send()
            hop_back(0).wait_recv()
            front_back(0)

        @pl.when(is_f)
        def _():
            forward_stage(m, who, k, fresh)

        @pl.when(is_o)
        def _():
            output_stage(m_o, fresh)

        @pl.when(jnp.logical_not(is_f))
        def _():
            backward_stage(m, who, k)

        @pl.when(first & (k == 1))
        def _():
            relay(3, 1)
            relay(3, 2)
            output_finish(1)
            relay(3, 3)
            for i in range(micro):
                mirror_copy(0, i).start()

        @pl.when(first & (k == 7))
        def _():
            backward_finish(0)

        @pl.when((first & (k == 7)) | (second & (k == 4)))
        def _():
            backward_finish(1)

        @pl.when(second & (k == 7))
        def _():
            loop(micro, output_finish)

    loop(8, slot)

    s_src[...] = jnp.zeros_like(s_src)
    for j in range(count):
        s_src[j, 0:3, :] = own_sums[0:3, j * LANES:(j + 1) * LANES]
    for j in range(nf):
        s_src[t * nf + j, 3:6, :] = head_sums[0:3, j * LANES:(j + 1) * LANES]
        for r in range(per_row):
            c = (j * per_row + r) * LANES
            s_src[t * nf + j, 6 + r:7 + r, :] = up_sums[0:1, c:c + LANES]
    small = [
        send(s_src.at[to], s_got.at[k], sm_s.at[k], sm_r.at[k], peer) for k, to, peer in group
    ]
    for copy in small:
        copy.start()

    @pl.when(second)
    def _():
        for m in range(micro):
            hop_back(m).wait_send()

    @pl.when(first)
    def _():
        for m in range(micro):
            hop_out(m).wait_send()

    total = s_src[me]
    for k, copy in enumerate(small):
        copy.wait()
        total = total + s_got[k + 1]
    sums_o[...] = total
    for m in range(micro):
        for who in range(2):
            for a in range(4):
                if (m, who) != (0, 1):
                    x_sent(a, m, who)
                x_send(a, m, who).wait_recv()
            for which in range(2):
                mine, theirs = c_pair(which, m, who)
                mine.wait()
                theirs.wait()
        for which in range(2):
            mirror_copy(which, m).wait_send()
        store_ends(m).wait()
    for a in range(4):
        w_send(a, 0, 0, 1).wait_send()
    for side, via in ((first, 1), (second, 3)):
        @pl.when(side)
        def _(via=via):
            for a in range(4):
                if a != via:
                    w_send(a, 0, 1, 2).wait_send()
                    w_send(a, 2, 0, 1).wait_send()
            for p in range(PIECES):
                leg_one(via, p).wait_send()
                passed_on(via, 2, p).wait_send()


def fused(ends, smalls, segments, wq, wo, w1, w2, nf, nt):
    micro, per, width = ends.shape
    length = per * nt
    own, hidden = wo.shape[1], w1.shape[1]
    depth = width // nf
    count = nf * nt
    bits = nf.bit_length() - 1
    anywhere = pl.BlockSpec(memory_space=pl.ANY)
    inside = pl.BlockSpec(memory_space=pltpu.VMEM)
    dma = pltpu.SemaphoreType.DMA
    vm = pltpu.VMEM
    piece = (ROWS_OF_PACK, LANES)
    packs = 2 * micro
    some = micro + 1
    out_shape = [
        jax.ShapeDtypeStruct(ends.shape, F32),
        jax.ShapeDtypeStruct(piece, F32),
        jax.ShapeDtypeStruct((micro, nf, length, hidden), BF16),
        jax.ShapeDtypeStruct((micro, nf, length, own), BF16),
        jax.ShapeDtypeStruct((micro, nf, length, hidden), BF16),
        jax.ShapeDtypeStruct((3, micro, nf, length, own), BF16),
        jax.ShapeDtypeStruct((micro, nf, length, depth), BF16),
        jax.ShapeDtypeStruct((micro, nf, length, depth), BF16),
    ]
    scratch = [
        vm((3, width, own), BF16), vm((width, own), BF16),
        vm((width, hidden), BF16), vm((width, hidden), BF16),
        vm(piece, F32), vm((count,) + piece, F32),
        vm((ROWS_OF_PACK, width), F32), vm((8, hidden), F32),
        vm((2, 8, length), F32), vm((packs, 2, length, LANES), F32),
        vm(ends.shape, BF16), vm(ends.shape, BF16),
        vm((packs, length, width), BF16), vm((packs, 3, length, own), BF16),
        vm((packs, length, LANES), F32), vm((some, length, own), BF16),
        vm((packs, length, hidden), BF16), vm((some, length, hidden), BF16),
        vm((packs, length, width), BF16), vm((length, own), BF16),
        vm((some, length, hidden), BF16), vm((some, 3, length, own), BF16),
        vm((micro, length, width), BF16), vm((micro, nt - 1, per, width), BF16),
        vm((micro, length, width), BF16), vm((micro, nt - 1, per, width), BF16),
        vm(ends.shape, F32), vm(ends.shape, BF16),
        vm((8, width), F32), vm((8, own), F32), vm((8, hidden), F32),
        vm((count,) + piece, F32), vm((count,) + piece, F32),
        dma, dma((4,)), dma((4, nf, bits)), dma((4, nf)),
        dma((count,)), dma((count,)), dma((count,)), dma((count,)),
        dma((micro, nt)), dma((micro, nt)), dma((micro, nt)), dma((micro, nt)),
        dma((micro, nt)), dma((micro, nt)), dma((micro, nt)), dma((micro, nt)),
        dma((micro,)), dma((micro,)), dma((micro,)), dma((micro,)),
        dma((4, micro, 2)), dma((4, micro, 2)), dma((4, micro, 2)),
        dma((2, micro, 2)), dma((2, micro, 2)), dma((2, micro, 2)),
        dma((3, micro)), dma((3, micro)), dma((micro,)),
        dma((PIECES,)), dma((PIECES,)), dma((PIECES,)), dma((PIECES,)),
        dma((PIECES,)), dma((PIECES,)), pltpu.SemaphoreType.REGULAR,
    ]
    return pl.pallas_call(
        functools.partial(fused_kernel, nf, nt),
        out_shape=out_shape,
        in_specs=[anywhere] + [inside] * 7 + [anywhere] * 4,
        out_specs=[anywhere, inside] + [anywhere] * 6,
        scratch_shapes=scratch,
        compiler_params=pltpu.CompilerParams(
            collective_id=4, has_side_effects=True, vmem_limit_bytes=VMEM_LIMIT
        ),
        name="fused",
    )(ends, *smalls, segments, wq, wo, w1, w2)


def padded(flat):
    size = -(-flat.shape[-1] // (8 * LANES)) * (8 * LANES)
    room = [(0, 0)] * (flat.ndim - 1) + [(0, size - flat.shape[-1])]
    flat = jnp.pad(flat, room)
    return flat.reshape(flat.shape[:-1] + (size // LANES, LANES))


def split_shards(
    ends_in, segments, ln_gain, ln_bias, w_qkv, w_out, w_fc1, w_fc2,
    bias_qkv, bias_out, bias_fc1, bias_fc2,
):
    nf, nt = lax.axis_size("fsdp"), lax.axis_size("tp")
    count = nf * nt
    section, tp_index = lax.axis_index("section"), lax.axis_index("tp")
    is_first = section == 0
    piece = ln_gain.shape[1]
    hidden_piece = bias_fc1.shape[1]
    own, hidden = w_out.shape[2], w_fc1.shape[2]
    width = piece * count

    pack = jnp.concatenate(
        [ln_gain[0], ln_bias[0], bias_out[0], bias_fc2[0], bias_qkv[0].reshape(-1), bias_fc1[0]]
    ).astype(F32)
    used = pack.shape[0]
    smalls = gather_small(padded(pack), nf, nt).reshape(count, -1)[:, :used]
    wide = smalls[:, :7 * piece].reshape(count, 7, piece).transpose(1, 0, 2).reshape(7, width)
    vec = jnp.stack([wide[0], wide[1], wide[2] + wide[3]])
    vec = jnp.pad(vec, ((0, 5), (0, 0)))
    qb = lax.dynamic_slice_in_dim(wide[4:7], tp_index * own, own, 1)
    qb = jnp.pad(qb, ((0, 5), (0, 0)))
    fb = lax.dynamic_slice_in_dim(smalls[:, 7 * piece:], tp_index * nf, nf, 0).reshape(1, hidden)
    fb = jnp.pad(fb, ((0, 7), (0, 0)))
    rope = rope_tables(segments)
    segc, segr = segments[:, :, None], segments[:, None, :]

    wq = lax.all_gather(w_qkv[0].transpose(1, 0, 2), "fsdp", axis=1, tiled=True)
    w1 = lax.all_gather(w_fc1[0], "fsdp", axis=0, tiled=True)
    wo = lax.all_gather(w_out[0], "fsdp", axis=0, tiled=True)
    w2 = lax.all_gather(w_fc2[0], "fsdp", axis=0, tiled=True)
    weights = (wq, wo, w1, w2)
    rows, xg, qkv, lse, att, gp, act, y = forward(
        ends_in[0], weights, vec, qb, fb, rope, segc, segr, nt
    )
    gr, up, dj, dx, own_sums, head_sums, up_sums = backward(
        ends_in[0], weights, rows, qkv, lse, gp, vec, rope, segc, segr, nt
    )

    def everywhere(arr):
        return lax.all_gather(arr, "fsdp", axis=arr.ndim - 2, tiled=True)

    def columns(arr):
        return lax.all_to_all(arr, "fsdp", split_axis=2, concat_axis=1, tiled=True)

    xc, gc = columns(xg), columns(gr)

    def product(left, right):
        return lax.dot_general(
            left, right, (((0, 1), (0, 1)), ((), ())), preferred_element_type=F32
        )

    act_all, att_all, up_all, dj_all = (everywhere(a) for a in (act, att, up, dj))
    grad_fc2 = product(gc, act_all)
    grad_out = product(gc, att_all)
    grad_fc1 = product(xc, up_all)
    grad_qkv = jnp.stack([product(xc, dj_all[:, part]) for part in range(3)], axis=1)

    mine = own_sums[:3].reshape(3, count, piece).transpose(1, 0, 2).reshape(count, 3 * piece)
    head = lax.dynamic_update_slice_in_dim(
        jnp.zeros((3, width), F32), head_sums[:3], tp_index * own, 1
    )
    head = head.reshape(3, count, piece).transpose(1, 0, 2).reshape(count, 3 * piece)
    ups = lax.dynamic_update_slice_in_dim(
        jnp.zeros((count, hidden_piece), F32),
        up_sums[0].reshape(nf, hidden_piece),
        tp_index * nf,
        0,
    )
    sums = sum_small(padded(jnp.concatenate([mine, head, ups], axis=1)), nf, nt).reshape(-1)
    gain_grad, bias_grad, row_grad = (sums[i * piece:(i + 1) * piece] for i in range(3))
    qkv_bias_grad = sums[3 * piece:6 * piece].reshape(3, piece)
    fc1_bias_grad = sums[6 * piece:6 * piece + hidden_piece]
    ends_out = jnp.where(is_first, dx, y)[None]
    return (
        ends_out,
        gain_grad[None],
        bias_grad[None],
        grad_qkv[None],
        grad_out[None],
        grad_fc1[None],
        grad_fc2[None],
        qkv_bias_grad[None],
        row_grad[None],
        fc1_bias_grad[None],
        row_grad[None],
    )


def fused_shards(
    ends_in, segments, ln_gain, ln_bias, w_qkv, w_out, w_fc1, w_fc2,
    bias_qkv, bias_out, bias_fc1, bias_fc2,
):
    nf, nt = lax.axis_size("fsdp"), lax.axis_size("tp")
    used = 6 + bias_fc1.shape[1] // LANES
    ends_out, sums, act_x, att_x, up_x, dj_x, xc, gc = fused(
        ends_in[0],
        (ln_gain, ln_bias, bias_out, bias_fc2, bias_qkv[0], bias_fc1),
        segments, w_qkv[0].transpose(1, 0, 2), w_out[0], w_fc1[0], w_fc2[0], nf, nt,
    )

    def product(left, right):
        left = left.reshape(-1, left.shape[-1])
        right = right.reshape(-1, right.shape[-1])
        return lax.dot_general(left, right, ROWS, preferred_element_type=F32)

    grad_fc2 = product(gc, act_x)
    grad_out = product(gc, att_x)
    grad_fc1 = product(xc, up_x)
    grad_qkv = jnp.stack([product(xc, dj_x[part]) for part in range(3)], axis=1)
    row_grad = sums[2:3]
    return (
        ends_out[None],
        sums[0:1],
        sums[1:2],
        grad_qkv[None],
        grad_out[None],
        grad_fc1[None],
        grad_fc2[None],
        sums[3:6][None],
        row_grad,
        sums[6:used].reshape(1, -1),
        row_grad,
    )


def shards(*args):
    rows, piece = args[0].shape[2], args[2].shape[1]
    small = rows * lax.axis_size("tp") <= 256
    tidy = piece == LANES and args[10].shape[1] // LANES <= ROWS_OF_PACK - 6
    square = lax.axis_size("fsdp") == 4 and args[0].shape[1] == 2
    return (fused_shards if small and tidy and square else split_shards)(*args)


def solution(mesh):
    both = P("section", ("fsdp", "tp"))
    square = P("section", "fsdp", "tp")
    tokens = P("section", None, ("fsdp", "tp"), None)
    heads = P("section", "fsdp", None, "tp")
    bias3 = P("section", None, ("fsdp", "tp"))
    return jax.shard_map(
        shards,
        mesh=mesh,
        in_specs=(
            tokens, P(None, "fsdp"), both, both, heads, square, square, square,
            bias3, both, both, both,
        ),
        out_specs=(
            tokens, both, both, heads, square, square, square, bias3, both, both, both,
        ),
        check_vma=False,
    )
```

```python
import functools

import jax
import jax.numpy as jnp
from jax import lax
from jax.experimental import pallas as pl
from jax.experimental.pallas import tpu as pltpu
from jax.sharding import PartitionSpec as P

HEAD_DIM = 64
ROT_DIM = 32
EPSILON = 1e-05
LANES = 128
TILE = 256
MESH = pl.DeviceIdType.MESH
F32 = jnp.float32
BF16 = jnp.bfloat16
COLS = (((1,), (1,)), ((), ()))
ROWS = (((0,), (0,)), ((), ()))
VMEM_LIMIT = 66_900_000


def positions_of(segment_ids):
    length = segment_ids.shape[-1]
    places = jnp.arange(length, dtype=jnp.int32)
    before = jnp.concatenate([segment_ids[..., :1] - 1, segment_ids[..., :-1]], axis=-1)
    starts = jnp.where(segment_ids != before, places, 0)
    starts = lax.cummax(starts, axis=segment_ids.ndim - 1)
    return places - starts


def rope_tables(segments):
    half = ROT_DIM // 2
    freq = jnp.exp(-jnp.log(10000.0) * (2.0 * jnp.arange(half, dtype=F32)) / ROT_DIM)
    angles = positions_of(segments).astype(F32)[..., None] * freq
    cosine, sine = jnp.cos(angles), jnp.sin(angles)
    none = jnp.zeros_like(sine)
    rest = jnp.zeros(angles.shape[:-1] + (HEAD_DIM - ROT_DIM,), F32)
    keep = jnp.concatenate([cosine, cosine, rest + 1.0], axis=-1)
    ahead = jnp.concatenate([-sine, none, rest], axis=-1)
    behind = jnp.concatenate([none, sine, rest], axis=-1)
    tables = jnp.stack([keep, ahead, behind], axis=1)
    return jnp.concatenate([tables, tables], axis=-1)


def send(src, dst, send_sem, recv_sem, device):
    return pltpu.make_async_remote_copy(
        src_ref=src,
        dst_ref=dst,
        send_sem=send_sem,
        recv_sem=recv_sem,
        device_id=device,
        device_id_type=MESH,
    )


def greet(peers):
    barrier = pltpu.get_barrier_semaphore()
    for peer in peers:
        pl.semaphore_signal(barrier, inc=1, device_id=peer, device_id_type=MESH)
    pl.semaphore_wait(barrier, len(peers))


def group_peers(nf, nt):
    me = lax.axis_index("fsdp") * nt + lax.axis_index("tp")
    found = []
    for k in range(1, nf * nt):
        to = lax.rem(me + k, nf * nt)
        found.append((k, to, {"fsdp": to // nt, "tp": lax.rem(to, nt)}))
    return me, found


def gather_small_kernel(nf, nt, own, out, send_sems, recv_sems, local_sem):
    me, peers = group_peers(nf, nt)
    greet([peer for _, _, peer in peers])
    mine = pltpu.make_async_copy(own, out.at[me], local_sem)
    mine.start()
    copies = []
    for k, _, peer in peers:
        copy = send(own, out.at[me], send_sems.at[k], recv_sems.at[k], peer)
        copy.start()
        copies.append(copy)
    mine.wait()
    for copy in copies:
        copy.wait()


def gather_small(own, nf, nt):
    count = nf * nt
    return pl.pallas_call(
        functools.partial(gather_small_kernel, nf, nt),
        out_shape=jax.ShapeDtypeStruct((count,) + own.shape, own.dtype),
        in_specs=[pl.BlockSpec(memory_space=pltpu.VMEM)],
        out_specs=pl.BlockSpec(memory_space=pltpu.VMEM),
        scratch_shapes=[
            pltpu.SemaphoreType.DMA((count,)),
            pltpu.SemaphoreType.DMA((count,)),
            pltpu.SemaphoreType.DMA,
        ],
        compiler_params=pltpu.CompilerParams(collective_id=0, has_side_effects=True),
        name="gather_small",
    )(own)


def sum_small_kernel(nf, nt, own, out, got, send_sems, recv_sems):
    me, peers = group_peers(nf, nt)
    greet([peer for _, _, peer in peers])
    copies = []
    for k, to, peer in peers:
        copy = send(own.at[to], got.at[k], send_sems.at[k], recv_sems.at[k], peer)
        copy.start()
        copies.append(copy)
    total = own[me]
    for k, copy in enumerate(copies):
        copy.wait()
        total = total + got[k + 1]
    out[...] = total


def sum_small(own, nf, nt):
    count = nf * nt
    return pl.pallas_call(
        functools.partial(sum_small_kernel, nf, nt),
        out_shape=jax.ShapeDtypeStruct(own.shape[1:], own.dtype),
        in_specs=[pl.BlockSpec(memory_space=pltpu.VMEM)],
        out_specs=pl.BlockSpec(memory_space=pltpu.VMEM),
        scratch_shapes=[
            pltpu.VMEM(own.shape, own.dtype),
            pltpu.SemaphoreType.DMA((count,)),
            pltpu.SemaphoreType.DMA((count,)),
        ],
        compiler_params=pltpu.CompilerParams(collective_id=1, has_side_effects=True),
        name="sum_small",
    )(own)


def cols(n, width=TILE):
    return pl.ds(pl.multiple_of(n * width, width), width)


def loop(count, body):
    def step(i, carry):
        body(i)
        return carry

    lax.fori_loop(0, count, step, 0)


def turn(x, tables, sign):
    keep, ahead, behind = tables
    left = pltpu.roll(x, LANES - ROT_DIM // 2, 1)
    right = pltpu.roll(x, ROT_DIM // 2, 1)
    return x * keep + sign * (left * ahead + right * behind)


def low_half(length):
    return lax.broadcasted_iota(jnp.int32, (length, LANES), 1) < HEAD_DIM


def allowed_mask(segc, segr, m, length):
    query = lax.broadcasted_iota(jnp.int32, (length, length), 0)
    key = lax.broadcasted_iota(jnp.int32, (length, length), 1)
    return (query >= key) & (segc[m] == segr[m])


class Ring:
    def __init__(self, nt, rows):
        self.nt, self.rows = nt, rows
        self.me = lax.axis_index("tp")
        self.others = [(k, lax.rem(self.me + k, nt)) for k in range(1, nt)]

    def block(self, who):
        return pl.ds(pl.multiple_of(who * self.rows, self.rows), self.rows)

    def gather(self, buf, m, sems):
        return [
            send(
                buf.at[m, self.block(self.me)],
                buf.at[m, self.block(self.me)],
                sems[0].at[m, k],
                sems[1].at[m, k],
                {"tp": to},
            )
            for k, to in self.others
        ]

    def scatter(self, buf, got, m, sems, part=None):
        at = slice(None) if part is None else part
        return [
            send(
                buf.at[m, self.block(to), at],
                got.at[m, k - 1, :, at],
                sems[0].at[m, k],
                sems[1].at[m, k],
                {"tp": to},
            )
            for k, to in self.others
        ]

    def total(self, buf, got, m):
        acc = buf[m, self.block(self.me)].astype(F32)
        for k, _ in self.others:
            acc = acc + got[m, k - 1].astype(F32)
        return acc


def stats(rows):
    mean = jnp.mean(rows, axis=-1, keepdims=True)
    centred = rows - mean
    variance = jnp.mean(centred * centred, axis=-1, keepdims=True)
    inv_root = lax.rsqrt(variance + EPSILON)
    return centred * inv_root, inv_root


def forward_kernel(
    nt,
    rows_h, wq_h, wo_h, w1_h, w2_h, vec, qb, fb, rope, segc, segr,
    rows_o, xg_o, qkv_o, lse_o, att_o, gp_o, act_o, y_o,
    wq, wo, w1, w2, rin, xg, qkv, lse, att, gp, act, branch, got, out_f, out_b,
    w_sem, in_sem, o_sem, ag_s, ag_r, rs_s, rs_r, x_s, x_r,
):
    micro, length, width = xg.shape
    section = lax.axis_index("section")
    first, second = section == 0, section == 1
    ring = Ring(nt, length // nt)
    own = wo.shape[1]
    loads = []
    for i, (src, dst) in enumerate(((wq_h, wq), (w1_h, w1), (wo_h, wo), (w2_h, w2))):
        loads.append(pltpu.make_async_copy(src, dst, w_sem.at[i]))
        loads[-1].start()
    mine = pltpu.make_async_copy(rows_h, rin, in_sem)

    @pl.when(first)
    def _():
        mine.start()

    greet([{"tp": to} for _, to in ring.others] + [{"section": 1 - section}])

    @pl.when(first)
    def _():
        mine.wait()

    def hop(m):
        return send(out_b.at[m], rin.at[m], x_s.at[m], x_r.at[m], {"section": 1 - section})

    def front(m):
        unit, _ = stats(rin[m].astype(F32))
        normed = unit * vec[0:1, :] + vec[1:2, :]
        xg[m, ring.block(ring.me)] = normed.astype(BF16)
        for copy in ring.gather(xg, m, (ag_s, ag_r)):
            copy.start()

    def arrive(m):
        @pl.when(second)
        def _():
            hop(m).wait_recv()
            front(m)

    stores = []

    def store(src, dst, m, i):
        copy = pltpu.make_async_copy(src.at[m], dst.at[m], o_sem.at[m, i])
        copy.start()
        stores.append(copy)

    def body(m):
        for copy in ring.gather(xg, m, (ag_s, ag_r)):
            copy.wait()
        store(xg, xg_o, m, 0)
        store(rin, rows_o, m, 1)
        tables = (rope[m, 0], rope[m, 1], rope[m, 2])
        if m == 0:
            loads[0].wait()
        per = own // TILE
        for part in range(3):
            def qkv_tile(n, part=part):
                at = cols(n)
                acc = jnp.dot(xg[m], wq[part, :, at], preferred_element_type=F32)
                acc = acc + qb[part:part + 1, at]
                if part < 2:
                    acc = jnp.concatenate(
                        [
                            turn(acc[:, c:c + LANES], tables, 1.0)
                            for c in range(0, TILE, LANES)
                        ],
                        axis=1,
                    )
                qkv[m, part, :, at] = acc.astype(BF16)

            loop(per, qkv_tile)
        store(qkv, qkv_o, m, 2)
        allowed = allowed_mask(segc, segr, m, length)
        low = low_half(length)
        lane = lax.broadcasted_iota(jnp.int32, (length, LANES), 1)

        def pair(p):
            at = cols(p, LANES)
            query, key, value = qkv[m, 0, :, at], qkv[m, 1, :, at], qkv[m, 2, :, at]
            outs = []
            for h in range(2):
                mask = low if h == 0 else ~low
                one = jnp.where(mask, query, jnp.zeros_like(query))
                s = lax.dot_general(one, key, COLS, preferred_element_type=F32)
                s = jnp.where(allowed, s * HEAD_DIM ** (-0.5), -1e30)
                top = jnp.max(s, axis=-1, keepdims=True)
                e = jnp.exp(s - top)
                total = jnp.sum(e, axis=-1, keepdims=True)
                probs = (e / total).astype(BF16)
                outs.append(jnp.dot(probs, value, preferred_element_type=F32))
                lse[m] = jnp.where(lane == 2 * p + h, top + jnp.log(total), lse[m])
            att[m, :, at] = jnp.where(low, outs[0], outs[1]).astype(BF16)

        lse[m] = jnp.zeros((length, LANES), F32)
        loop(own // LANES, pair)
        store(lse, lse_o, m, 3)
        store(att, att_o, m, 4)
        if m == 0:
            loads[1].wait()

        def up_tile(n):
            at = cols(n)
            u = jnp.dot(xg[m], w1[:, at], preferred_element_type=F32) + fb[0:1, at]
            c = 0.7978845608028654
            square = u * u
            t = jnp.tanh(c * u * (1.0 + 0.044715 * square))
            act[m, :, at] = (0.5 * u * (1.0 + t)).astype(BF16)
            slope = 0.5 * (1.0 + t) + 0.5 * u * (1.0 - t * t) * (c * (1.0 + 3 * 0.044715 * square))
            gp[m, :, at] = slope.astype(BF16)

        loop(act.shape[2] // TILE, up_tile)
        store(act, act_o, m, 5)
        store(gp, gp_o, m, 6)
        if m == 0:
            loads[2].wait()
            loads[3].wait()

        def out_tile(n):
            at = cols(n)
            acc = lax.dot_general(att[m], wo[at, :], COLS, preferred_element_type=F32)
            acc = acc + lax.dot_general(act[m], w2[at, :], COLS, preferred_element_type=F32)
            branch[m, :, at] = acc.astype(BF16)
            for copy in ring.scatter(branch, got, m, (rs_s, rs_r), at):
                copy.start()

        loop(width // TILE, out_tile)

    def finish(m):
        for copy in ring.scatter(branch, got, m, (rs_s, rs_r)):
            copy.wait()
        y = rin[m].astype(F32) + ring.total(branch, got, m) + vec[2:3, :]
        out_f[m] = y
        out_b[m] = y.astype(BF16)
        store(out_f, y_o, m, 7)

        @pl.when(first)
        def _():
            hop(m).start()

    @pl.when(first)
    def _():
        for m in range(micro):
            front(m)

    for m in range(micro):
        arrive(m)
        body(m)
    for m in range(micro):
        finish(m)
    for copy in stores:
        copy.wait()

    @pl.when(first)
    def _():
        for m in range(micro):
            hop(m).wait_send()


def forward(rows, weights, vec, qb, fb, rope, segc, segr, nt):
    wq, wo, w1, w2 = weights
    micro, per, width = rows.shape
    length = per * nt
    own, hidden = wo.shape[1], w1.shape[1]
    anywhere = pl.BlockSpec(memory_space=pl.ANY)
    inside = pl.BlockSpec(memory_space=pltpu.VMEM)
    out_shape = [
        jax.ShapeDtypeStruct(rows.shape, BF16),
        jax.ShapeDtypeStruct((micro, length, width), BF16),
        jax.ShapeDtypeStruct((micro, 3, length, own), BF16),
        jax.ShapeDtypeStruct((micro, length, LANES), F32),
        jax.ShapeDtypeStruct((micro, length, own), BF16),
        jax.ShapeDtypeStruct((micro, length, hidden), BF16),
        jax.ShapeDtypeStruct((micro, length, hidden), BF16),
        jax.ShapeDtypeStruct(rows.shape, F32),
    ]
    dma = pltpu.SemaphoreType.DMA
    return pl.pallas_call(
        functools.partial(forward_kernel, nt),
        out_shape=out_shape,
        in_specs=[anywhere] * 5 + [inside] * 6,
        out_specs=[anywhere] * 8,
        scratch_shapes=[
            pltpu.VMEM(wq.shape, BF16),
            pltpu.VMEM(wo.shape, BF16),
            pltpu.VMEM(w1.shape, BF16),
            pltpu.VMEM(w2.shape, BF16),
            pltpu.VMEM(rows.shape, BF16),
            pltpu.VMEM((micro, length, width), BF16),
            pltpu.VMEM((micro, 3, length, own), BF16),
            pltpu.VMEM((micro, length, LANES), F32),
            pltpu.VMEM((micro, length, own), BF16),
            pltpu.VMEM((micro, length, hidden), BF16),
            pltpu.VMEM((micro, length, hidden), BF16),
            pltpu.VMEM((micro, length, width), BF16),
            pltpu.VMEM((micro, nt - 1, per, width), BF16),
            pltpu.VMEM(rows.shape, F32),
            pltpu.VMEM(rows.shape, BF16),
            dma((4,)),
            dma,
            dma((micro, 8)),
            dma((micro, nt)),
            dma((micro, nt)),
            dma((micro, nt)),
            dma((micro, nt)),
            dma((micro,)),
            dma((micro,)),
        ],
        compiler_params=pltpu.CompilerParams(
            collective_id=2, has_side_effects=True, vmem_limit_bytes=VMEM_LIMIT
        ),
        name="forward",
    )(rows, wq, wo, w1, w2, vec, qb, fb, rope, segc, segr)


def backward_kernel(
    nt,
    dy_h, wq_h, wo_h, w1_h, w2_h, rows_h, qkv_h, lse_h, gp_h, vec, rope, segc, segr,
    gr_o, up_o, dj_o, dx_o, own_sums, head_sums, up_sums,
    wq, wo, w1, w2, dyr, rin, qkv, lse, gp, gr, gatt, up, dj, branch, got, out_f, out_b,
    w_sem, in_sem, o_sem, ag_s, ag_r, rs_s, rs_r, x_s, x_r,
):
    micro, length, width = gr.shape
    section = lax.axis_index("section")
    first, second = section == 0, section == 1
    ring = Ring(nt, length // nt)
    own = wo.shape[1]
    mine = pltpu.make_async_copy(dy_h, dyr, in_sem.at[4])

    @pl.when(second)
    def _():
        mine.start()

    loads = []
    for i, (src, dst) in enumerate(((wo_h, wo), (w2_h, w2), (wq_h, wq), (w1_h, w1))):
        loads.append(pltpu.make_async_copy(src, dst, w_sem.at[i]))
    kept = []
    for i, (src, dst) in enumerate(((qkv_h, qkv), (lse_h, lse), (gp_h, gp), (rows_h, rin))):
        kept.append(pltpu.make_async_copy(src, dst, in_sem.at[i]))
    for copy in (loads[0], kept[0], kept[1], loads[1], kept[2], loads[2], loads[3], kept[3]):
        copy.start()
    greet([{"tp": to} for _, to in ring.others] + [{"section": 1 - section}])

    @pl.when(second)
    def _():
        mine.wait()

    def hop(m):
        return send(out_b.at[m], dyr.at[m], x_s.at[m], x_r.at[m], {"section": 1 - section})

    def front(m):
        gr[m, ring.block(ring.me)] = dyr[m]
        for copy in ring.gather(gr, m, (ag_s, ag_r)):
            copy.start()

    def arrive(m):
        @pl.when(first)
        def _():
            hop(m).wait_recv()
            front(m)

    stores = []

    def store(src, dst, m, i):
        copy = pltpu.make_async_copy(src.at[m], dst.at[m], o_sem.at[m, i])
        copy.start()
        stores.append(copy)

    def body(m):
        for copy in ring.gather(gr, m, (ag_s, ag_r)):
            copy.wait()
        store(gr, gr_o, m, 0)
        if m == 0:
            loads[0].wait()

        def att_tile(n):
            at = cols(n)
            gatt[:, at] = jnp.dot(gr[m], wo[:, at], preferred_element_type=F32).astype(BF16)

        loop(own // TILE, att_tile)
        if m == 0:
            kept[0].wait()
            kept[1].wait()
        tables = (rope[m, 0], rope[m, 1], rope[m, 2])
        allowed = allowed_mask(segc, segr, m, length)
        low = low_half(length)
        lane = lax.broadcasted_iota(jnp.int32, (length, LANES), 1)
        factor = HEAD_DIM ** (-0.5)

        def pair(p):
            at = cols(p, LANES)
            query, key, value = qkv[m, 0, :, at], qkv[m, 1, :, at], qkv[m, 2, :, at]
            grad = gatt[:, at]
            dqs, dks, dvs = [], [], []
            for h in range(2):
                mask = low if h == 0 else ~low
                one = jnp.where(mask, query, jnp.zeros_like(query))
                s = lax.dot_general(one, key, COLS, preferred_element_type=F32)
                s = jnp.where(allowed, s * factor, -1e30)
                log_total = jnp.sum(
                    jnp.where(lane == 2 * p + h, lse[m], 0.0), axis=-1, keepdims=True
                )
                soft = jnp.exp(s - log_total)
                probs = soft.astype(BF16)
                one_grad = jnp.where(mask, grad, jnp.zeros_like(grad))
                dp = lax.dot_general(one_grad, value, COLS, preferred_element_type=F32)
                delta = jnp.sum(dp * soft, axis=-1, keepdims=True)
                ds = (soft * (dp - delta)).astype(BF16)
                dvs.append(lax.dot_general(probs, grad, ROWS, preferred_element_type=F32))
                dqs.append(jnp.dot(ds, key, preferred_element_type=F32))
                dks.append(lax.dot_general(ds, query, ROWS, preferred_element_type=F32))
            dq = jnp.where(low, dqs[0], dqs[1]) * factor
            dk = jnp.where(low, dks[0], dks[1]) * factor
            dj[m, 0, :, at] = turn(dq, tables, -1.0).astype(BF16)
            dj[m, 1, :, at] = turn(dk, tables, -1.0).astype(BF16)
            dj[m, 2, :, at] = jnp.where(low, dvs[0], dvs[1]).astype(BF16)

        loop(own // LANES, pair)
        store(dj, dj_o, m, 1)
        for part in range(3):
            sums = jnp.sum(dj[m, part].astype(F32), axis=0, keepdims=True)
            if m == 0:
                head_sums[part:part + 1, :] = sums
            else:
                head_sums[part:part + 1, :] += sums
        if m == 0:
            loads[1].wait()
            kept[2].wait()

        def up_tile(n):
            at = cols(n)
            acc = jnp.dot(gr[m], w2[:, at], preferred_element_type=F32)
            rounded = (acc * gp[m, :, at].astype(F32)).astype(BF16)
            up[m, :, at] = rounded
            sums = jnp.sum(rounded.astype(F32), axis=0, keepdims=True)
            if m == 0:
                up_sums[0:1, at] = sums
            else:
                up_sums[0:1, at] += sums

        loop(up.shape[2] // TILE, up_tile)
        store(up, up_o, m, 2)
        if m == 0:
            loads[2].wait()
            loads[3].wait()

        def norm_tile(n):
            at = cols(n)
            acc = lax.dot_general(up[m], w1[at, :], COLS, preferred_element_type=F32)
            for part in range(3):
                acc = acc + lax.dot_general(
                    dj[m, part], wq[part, at, :], COLS, preferred_element_type=F32
                )
            branch[m, :, at] = acc.astype(BF16)
            for copy in ring.scatter(branch, got, m, (rs_s, rs_r), at):
                copy.start()

        loop(width // TILE, norm_tile)

    def finish(m):
        for copy in ring.scatter(branch, got, m, (rs_s, rs_r)):
            copy.wait()
        if m == 0:
            kept[3].wait()
        grad_norm = ring.total(branch, got, m)
        unit, inv_root = stats(rin[m].astype(F32))
        scaled = grad_norm * vec[0:1, :]
        upstream = dyr[m].astype(F32)
        dx = upstream + inv_root * (
            scaled
            - jnp.mean(scaled, axis=-1, keepdims=True)
            - unit * jnp.mean(scaled * unit, axis=-1, keepdims=True)
        )
        out_f[m] = dx
        out_b[m] = dx.astype(BF16)

        @pl.when(second)
        def _():
            hop(m).start()

        store(out_f, dx_o, m, 3)
        for i, term in enumerate((grad_norm * unit, grad_norm, upstream)):
            sums = jnp.sum(term, axis=0, keepdims=True)
            if m == 0:
                own_sums[i:i + 1, :] = sums
            else:
                own_sums[i:i + 1, :] += sums

    @pl.when(second)
    def _():
        for m in range(micro):
            front(m)

    for m in range(micro):
        arrive(m)
        body(m)
    for m in range(micro):
        finish(m)
    for copy in stores:
        copy.wait()

    @pl.when(second)
    def _():
        for m in range(micro):
            hop(m).wait_send()


def backward(dy, weights, rows, qkv, lse, gp, vec, rope, segc, segr, nt):
    wq, wo, w1, w2 = weights
    micro, per, width = rows.shape
    length = per * nt
    own, hidden = wo.shape[1], w1.shape[1]
    anywhere = pl.BlockSpec(memory_space=pl.ANY)
    inside = pl.BlockSpec(memory_space=pltpu.VMEM)
    out_shape = [
        jax.ShapeDtypeStruct((micro, length, width), BF16),
        jax.ShapeDtypeStruct((micro, length, hidden), BF16),
        jax.ShapeDtypeStruct((micro, 3, length, own), BF16),
        jax.ShapeDtypeStruct(rows.shape, F32),
        jax.ShapeDtypeStruct((8, width), F32),
        jax.ShapeDtypeStruct((8, own), F32),
        jax.ShapeDtypeStruct((8, hidden), F32),
    ]
    dma = pltpu.SemaphoreType.DMA
    return pl.pallas_call(
        functools.partial(backward_kernel, nt),
        out_shape=out_shape,
        in_specs=[anywhere] * 9 + [inside] * 4,
        out_specs=[anywhere] * 4 + [inside] * 3,
        scratch_shapes=[
            pltpu.VMEM(wq.shape, BF16),
            pltpu.VMEM(wo.shape, BF16),
            pltpu.VMEM(w1.shape, BF16),
            pltpu.VMEM(w2.shape, BF16),
            pltpu.VMEM(rows.shape, BF16),
            pltpu.VMEM(rows.shape, BF16),
            pltpu.VMEM(qkv.shape, BF16),
            pltpu.VMEM(lse.shape, F32),
            pltpu.VMEM(gp.shape, BF16),
            pltpu.VMEM((micro, length, width), BF16),
            pltpu.VMEM((length, own), BF16),
            pltpu.VMEM((micro, length, hidden), BF16),
            pltpu.VMEM((micro, 3, length, own), BF16),
            pltpu.VMEM((micro, length, width), BF16),
            pltpu.VMEM((micro, nt - 1, per, width), BF16),
            pltpu.VMEM(rows.shape, F32),
            pltpu.VMEM(rows.shape, BF16),
            dma((4,)),
            dma((5,)),
            dma((micro, 4)),
            dma((micro, nt)),
            dma((micro, nt)),
            dma((micro, nt)),
            dma((micro, nt)),
            dma((micro,)),
            dma((micro,)),
        ],
        compiler_params=pltpu.CompilerParams(
            collective_id=3, has_side_effects=True, vmem_limit_bytes=VMEM_LIMIT
        ),
        name="backward",
    )(dy, wq, wo, w1, w2, rows, qkv, lse, gp, vec, rope, segc, segr)


ROWS_OF_PACK = 16
PIECES = 8
DIRECT = 2
LINE_SUMS = False
LINE_ROWS = False
WIDE = 512


def twist(x, tables, sign):
    keep, sine, ahead = tables
    left = pltpu.roll(x, LANES - ROT_DIM // 2, 1)
    right = pltpu.roll(x, ROT_DIM // 2, 1)
    return x * keep + jnp.where(ahead, left, right) * (sign * sine)


def masks_of(nf):
    return range(nf)


def bits_below(mask, nf):
    low = mask & -mask if mask else nf
    return [(i, 1 << i) for i in range(nf.bit_length() - 1) if (1 << i) < low]


def flipped(index, mask, nf):
    for i in range(nf.bit_length() - 1):
        if mask >> i & 1:
            index = index + (1 << i) * (1 - 2 * lax.rem(index // (1 << i), 2))
    return index


def fused_kernel(
    nf, nt,
    ends_h, gain, shift, b_out, b_fc2, b_qkv, b_fc1, seg_in, wq_h, wo_h, w1_h, w2_h,
    ends_o, sums_o, act_x, att_x, up_x, dj_x, xc_x, gc_x,
    wq, wo, w1, w2, pack, packs, wide, fb, segs, rope, rin, dyr, xg, qkv, lse, att, gp, act,
    gr, gatt, up, dj, out_bf, out_got, in_bf, in_got, y_f, y_b,
    own_sums, head_sums, up_sums, s_src, s_got,
    in_sem, wl_sem, ws_sem, wr_sem, pk_s, pk_r, sm_s, sm_r,
    ag_s, ag_r, gg_s, gg_r, rs_s, rs_r, rb_s, rb_r, hx_s, hx_r, hb_s, hb_r,
    xl_sem, xs_s, xs_r, cl_sem, ca_s, ca_r, mx_s, mx_r, o_sem,
    l1_s, l1_r, l2_s, l2_r, fw_s, fw_r, go_sem, nb, wide_b, mf_s, mb_s, wb_sem,
    out_via, in_via, rv_s, rv_r, bv_s, bv_r,
):
    micro, per, width = rin.shape
    length = per * nt
    section, f, t = (lax.axis_index(a) for a in ("section", "fsdp", "tp"))
    first, second = section == 0, section == 1
    ring = Ring(nt, per)
    own, hidden = wo.shape[1], w1.shape[1]
    depth = width // nf
    mirror, sibling = {"fsdp": flipped(f, 2, nf)}, {"fsdp": flipped(f, 1, nf)}
    count = nf * nt
    other = {"section": 1 - section}
    across = {"section": 1 - section, "fsdp": flipped(f, 2, nf)}
    me, group = group_peers(nf, nt)
    fblock = [flipped(f, mask, nf) for mask in masks_of(nf)]

    def rows_at(block):
        return pl.ds(pl.multiple_of(block * depth, depth), depth)

    load_rows = pltpu.make_async_copy(ends_h, rin, in_sem)
    load_dy = pltpu.make_async_copy(ends_h, dyr, in_sem)

    @pl.when(first)
    def _():
        load_rows.start()

    @pl.when(second)
    def _():
        load_dy.start()

    greet(
        [peer for _, _, peer in group]
        + [across, other]
        + [{"section": 1 - section, "tp": to} for _, to in ring.others]
    )

    per_row = hidden // nf // LANES
    segs[0] = jnp.zeros((8, length), F32)
    segs[0, 0:micro, :] = seg_in[...].astype(F32)
    pack[...] = jnp.zeros_like(pack)
    pack[0:1, :] = gain[...].astype(F32)
    pack[1:2, :] = shift[...].astype(F32)
    pack[2:3, :] = b_out[...].astype(F32) + b_fc2[...].astype(F32)
    pack[3:6, :] = b_qkv[...].astype(F32)
    for r in range(per_row):
        pack[6 + r:7 + r, :] = b_fc1[:, r * LANES:(r + 1) * LANES].astype(F32)
    seg_copy = send(segs.at[0], segs.at[1], mx_s.at[2, 0], mx_r.at[2, 0], mirror)
    pack_local = pltpu.make_async_copy(pack, packs.at[me], pk_s.at[0])
    pack_copies = [
        send(pack, packs.at[me], pk_s.at[k], pk_r.at[k], peer) for k, _, peer in group
    ]
    pack_local.start()
    seg_copy.start()
    for copy in pack_copies:
        copy.start()

    table = ((wq_h, wq), (w1_h, w1), (wo_h, wo), (w2_h, w2))

    def w_at(ref, block):
        return ref.at[:, rows_at(block), :] if len(ref.shape) == 3 else ref.at[rows_at(block), :]

    def w_local(a):
        return pltpu.make_async_copy(table[a][0], w_at(table[a][1], f), wl_sem.at[a])

    def w_send(a, mask, i, bit):
        block = w_at(table[a][1], fblock[mask])
        src = table[a][0] if mask == 0 else block
        peer = {"fsdp": flipped(f, bit, nf)}
        return send(src, block, ws_sem.at[a, mask, i], wr_sem.at[a, mask | bit], peer)

    def w_recv(a, mask):
        block = w_at(table[a][1], fblock[mask])
        return send(block, block, ws_sem.at[a, mask, 0], wr_sem.at[a, mask], other)

    def w_near(a):
        w_local(a).start()
        w_send(a, 0, 0, 1).start()

    def w_far(a):
        w_send(a, 0, 1, 2).start()

    part_rows = depth // PIECES
    per_slot = length // part_rows

    def stage(p):
        return up.at[p // per_slot, pl.ds(p % per_slot * part_rows, part_rows), :]

    def piece_at(a, mask, p):
        start = pl.multiple_of(fblock[mask] * depth + p * part_rows, part_rows)
        return table[a][1].at[pl.ds(start, part_rows), :]

    def leg_one(a, p):
        src = table[a][0].at[pl.ds(p * part_rows, part_rows), :]
        return send(src, stage(p), l1_s.at[p], l1_r.at[p], across)

    def leg_two(a, p):
        return send(stage(p), piece_at(a, 2, p), l2_s.at[p], l2_r.at[p], other)

    def passed_on(a, mask, p):
        block = piece_at(a, mask, p)
        return send(block, block, fw_s.at[p], fw_r.at[p], sibling)

    def straight(p):
        src = table[3][0].at[pl.ds(p * part_rows, part_rows), :]
        return send(src, piece_at(3, 0, p), l1_s.at[p], l2_r.at[p], mirror)

    def relay(a, p):
        leg_one(a, p).wait_recv()
        leg_two(a, p).start()

    def via_ready(a):
        for p in range(PIECES):
            leg_two(a, p).wait_recv()
            passed_on(a, 2, p).start()
        for p in range(PIECES):
            passed_on(a, 3, p).wait_recv()

    def w_ready(a, mask):
        if mask == 0:
            w_local(a).wait()
            return
        w_recv(a, mask).wait_recv()
        for i, bit in bits_below(mask, nf):
            w_send(a, mask, i, bit).start()

    order = sorted(masks_of(nf), key=lambda m: (m != 0, -(m & -m), m))
    out_order = list(masks_of(nf))
    for a in range(4):
        w_near(a)

    @pl.when(first)
    def _():
        w_far(0)
        w_far(2)
        for p in range(PIECES):
            leg_one(1, p).start()

    def small_arrive():
        pack_local.wait()
        for copy in pack_copies:
            copy.wait()
        for j in range(count):
            wide[:, j * LANES:(j + 1) * LANES] = packs[j]
        for j in range(nf):
            for r in range(per_row):
                c = (j * per_row + r) * LANES
                fb[0:1, c:c + LANES] = packs[t * nf + j, 6 + r:7 + r, :]

    def segment_parts(q):
        row = segs[q // micro, pl.ds(lax.rem(q, micro), 1), :]
        query = lax.broadcasted_iota(jnp.int32, (length, length), 0)
        key = lax.broadcasted_iota(jnp.int32, (length, length), 1)
        column = jnp.sum(jnp.where(query == key, row, 0.0), axis=1, keepdims=True)
        return row, column, query >= key

    def allowed_of(q):
        row, column, causal = segment_parts(q)
        return causal & (row == column)

    def rope_of(q):
        row, column, _ = segment_parts(q)
        before = jnp.sum(jnp.where(row < column, 1.0, 0.0), axis=1, keepdims=True)
        lane = lax.rem(lax.broadcasted_iota(jnp.int32, (length, LANES), 1), HEAD_DIM)
        place = lax.broadcasted_iota(jnp.int32, (length, LANES), 0).astype(F32) - before
        half = ROT_DIM // 2
        power = lax.rem(lane, half).astype(F32)
        freq = jnp.exp(-jnp.log(10000.0) * (2.0 * power) / ROT_DIM)
        angles = place * freq
        rope[q, 0] = jnp.where(lane < ROT_DIM, jnp.cos(angles), 1.0)
        sine = jnp.where(lane < ROT_DIM, jnp.sin(angles), 0.0)
        rope[q, 1] = jnp.where(lane < half, -sine, sine)

    def hop_out(m):
        return send(y_b.at[m], rin.at[m], hx_s.at[m], hx_r.at[m], other)

    def hop_back(m):
        return send(y_b.at[m], dyr.at[m], hb_s.at[m], hb_r.at[m], other)

    line = LINE_SUMS and nt == 4
    line_rows = LINE_ROWS and nt == 4
    inner = (t == 1) | (t == 2)
    far_end = jnp.where(t == 1, 3, 0)
    near_end = jnp.where(t == 1, 0, 3)

    def is_far(a, b, on=line):
        return (jnp.abs(a - b) == nt - 1) if on else False

    def unless(flag, do):
        if flag is False:
            do()
        else:
            pl.when(jnp.logical_not(flag))(do)

    def spread(buf, m, send_sems, recv_sems):
        here = ring.block(t)
        return [
            (
                is_far(t, to, line_rows),
                send(
                    buf.at[m, here], buf.at[m, here], send_sems.at[m, k], recv_sems.at[m, t],
                    {"tp": to},
                ),
            )
            for k, to in ring.others
        ]

    def block_wait(buf, m, recv_sems, who):
        at = ring.block(who)
        send(buf.at[m, at], buf.at[m, at], o_sem.at[m], recv_sems.at[m, who], other).wait_recv()

    def onward(buf, m, send_sems, recv_sems):
        at = ring.block(far_end)
        return send(
            buf.at[m, at], buf.at[m, at], send_sems.at[m, 0], recv_sems.at[m, far_end],
            {"tp": near_end},
        )

    def blocks_wait(buf, m, send_sems, recv_sems):
        if line_rows:
            @pl.when(inner)
            def _():
                block_wait(buf, m, recv_sems, far_end)
                onward(buf, m, send_sems, recv_sems).start()

        for _, who in ring.others:
            unless(
                (inner & (who == far_end)) if line_rows else False,
                functools.partial(block_wait, buf, m, recv_sems, who),
            )
        if line_rows:
            @pl.when(inner)
            def _():
                onward(buf, m, send_sems, recv_sems).wait_send()

    def spread_start(buf, m, send_sems, recv_sems):
        for skip, copy in spread(buf, m, send_sems, recv_sems):
            unless(skip, copy.start)

    def spread_wait(buf, m, send_sems, recv_sems):
        blocks_wait(buf, m, send_sems, recv_sems)
        for skip, copy in spread(buf, m, send_sems, recv_sems):
            unless(skip, copy.wait_send)

    last = micro - 1

    def cast(src, buf, send_sems, recv_sems):
        here = ring.block(t)
        return [
            (
                is_far(t, to, line_rows),
                send(
                    src, buf.at[last, here], send_sems.at[k], recv_sems.at[last, t],
                    {"section": 1 - section, "tp": to},
                ),
            )
            for k, to in [(0, t)] + ring.others
        ]

    def cast_wait(buf, send_sems, recv_sems):
        blocks_wait(buf, last, send_sems, recv_sems)
        block_wait(buf, last, recv_sems, t)

    def cast_rows():
        return cast(nb, xg, mf_s, ag_r)

    def cast_back():
        return cast(y_b.at[last], gr, mb_s, gg_r)

    def wide_copy():
        return send(wide.at[0:8], wide_b, wb_sem.at[0], wb_sem.at[1], other)

    def front(m):
        unit, _ = stats(rin[m].astype(F32))
        normed = unit * wide[0:1, :] + wide[1:2, :]
        xg[m, ring.block(ring.me)] = normed.astype(BF16)
        spread_start(xg, m, ag_s, ag_r)

    def front_back(m):
        gr[m, ring.block(ring.me)] = dyr[m]
        spread_start(gr, m, gg_s, gg_r)

    def mirror_copy(which, m):
        buf = (xg, gr)[which]
        return send(
            buf.at[m], buf.at[micro + m], mx_s.at[which, m], mx_r.at[which, m], mirror
        )

    def x_block(who):
        return fblock[2 * who] if isinstance(who, int) else jnp.where(who == 0, f, fblock[2])

    def x_dst(a, m, who):
        block = x_block(who)
        if a == 3:
            return dj_x.at[:, m, block]
        return (act_x, att_x, up_x)[a].at[m, block]

    def x_src(a, m, who):
        place = (m, micro)[who] if isinstance(who, int) else jnp.where(who == 0, m, micro)
        return (act, att, up, dj)[a].at[place]

    def x_local(a, m, who):
        return pltpu.make_async_copy(
            x_src(a, m, who), x_dst(a, m, who), xl_sem.at[a, m, who]
        )

    def x_send(a, m, who):
        return send(
            x_src(a, m, who), x_dst(a, m, who), xs_s.at[a, m, who], xs_r.at[a, m, who], sibling
        )

    def x_start(a, m, who):
        x_local(a, m, who).start()
        x_send(a, m, who).start()

    def x_sent(a, m, who):
        x_local(a, m, who).wait()
        x_send(a, m, who).wait_send()

    def c_pair(which, m, who):
        src, dst = ((xg, xc_x), (gr, gc_x))[which]
        block = x_block(who)
        q = who * micro + m
        mine = pltpu.make_async_copy(
            src.at[q, :, rows_at(f)], dst.at[m, block], cl_sem.at[which, m, who]
        )
        theirs = send(
            src.at[q, :, rows_at(fblock[1])],
            dst.at[m, block],
            ca_s.at[which, m, who],
            ca_r.at[which, m, who],
            sibling,
        )
        return mine, theirs

    def c_start(which, m, who):
        for copy in c_pair(which, m, who):
            copy.start()

    def sum_set(buf, got, via, sems, m, at):
        send_sems, recv_sems, via_s, via_r = sems
        found = []
        for k, to in ring.others:
            held = (inner & (to == far_end)) if line else False
            copy = send(
                buf.at[m, ring.block(to), at], got.at[m, k - 1, :, at],
                send_sems.at[m, k], recv_sems.at[m, k], {"tp": to},
            )
            found.append((k, is_far(t, to), held, copy))
        detour = send(
            buf.at[m, ring.block(nt - 1 - t), at], via.at[m, :, at],
            via_s.at[m], via_r.at[m], {"tp": jnp.where(t == 0, 1, 2)},
        )
        return found, detour

    everything = slice(None)

    def sum_tile(buf, got, via, sems, m, at, eager):
        found, detour = sum_set(buf, got, via, sems, m, at)
        if line:
            pl.when(jnp.logical_not(inner))(detour.start)
        for _, far, held, copy in found:
            skip = (far | held) if line else False
            if line and not eager:
                skip = skip | jnp.logical_not(inner)
            unless(skip, copy.start)

    def sum_after(buf, got, via, sems, m, eager):
        if not line:
            return
        found, detour = sum_set(buf, got, via, sems, m, everything)

        @pl.when(inner)
        def _():
            detour.wait_recv()
            at = ring.block(far_end)
            buf[m, at] = (buf[m, at].astype(F32) + via[m].astype(F32)).astype(BF16)
            for _, _, held, copy in found:
                pl.when(held)(copy.start)

        if not eager:
            @pl.when(jnp.logical_not(inner))
            def _():
                for _, far, _, copy in found:
                    unless(far, copy.start)

    def sum_wait(buf, got, via, sems, m):
        found, detour = sum_set(buf, got, via, sems, m, everything)
        for k, far, _, copy in found:
            unless(far, copy.wait_send)
            unless(is_far(lax.rem(t - k + nt, nt), t), copy.wait_recv)
        if line:
            pl.when(jnp.logical_not(inner))(detour.wait_send)
        total = buf[m, ring.block(t)].astype(F32)
        for k, _ in ring.others:
            part = got[m, k - 1].astype(F32)
            if line:
                part = jnp.where(is_far(lax.rem(t - k + nt, nt), t), 0.0, part)
            total = total + part
        return total

    out_set = (out_bf, out_got, out_via, (rs_s, rs_r, rv_s, rv_r))
    in_set = (in_bf, in_got, in_via, (rb_s, rb_r, bv_s, bv_r))

    def attention_masks(q):
        low = low_half(length)
        lane = lax.broadcasted_iota(jnp.int32, (length, LANES), 1)
        tables = (rope[q, 0], rope[q, 1], lax.rem(lane, HEAD_DIM) < ROT_DIM // 2)
        return low, lane, tables, allowed_of(q)

    factor = HEAD_DIM ** (-0.5)

    def forward_stage(m, who, k, fresh):
        q = who * micro + m
        place = jnp.where(who == 0, m, micro)

        @pl.when(who == 0)
        def _():
            @pl.when(first | (m < last))
            def _():
                spread_wait(xg, m, ag_s, ag_r)

            @pl.when(second & (m == last))
            def _():
                hop_out(last).wait_recv()
                cast_wait(xg, ag_s, ag_r)

            c_start(0, m, 0)

            @pl.when(second)
            def _():
                mirror_copy(0, m).start()

        @pl.when(who == 1)
        def _():
            mirror_copy(0, m).wait_recv()
            c_start(0, m, 1)

            @pl.when(m == 1)
            def _():
                x_sent(0, 0, 1)
                x_sent(1, 0, 1)

        @pl.when(fresh)
        def _():
            for mask in order:
                w_ready(0, mask)
            w_far(3)

        low, lane, tables, allowed = attention_masks(q)
        for part in range(3):
            def qkv_tile(n, part=part):
                at = cols(n, WIDE)
                acc = jnp.dot(xg[q], wq[part, :, at], preferred_element_type=F32)
                acc = acc + wide[3 + part:4 + part, pl.ds(
                    pl.multiple_of(t * own + n * WIDE, WIDE), WIDE)]
                if part < 2:
                    acc = jnp.concatenate(
                        [
                            twist(acc[:, c:c + LANES], tables, 1.0)
                            for c in range(0, WIDE, LANES)
                        ],
                        axis=1,
                    )
                qkv[q, part, :, at] = acc.astype(BF16)

            loop(own // WIDE, qkv_tile)

        def pair(p):
            at = cols(p, LANES)
            query, key, value = qkv[q, 0, :, at], qkv[q, 1, :, at], qkv[q, 2, :, at]
            outs = []
            for h in range(2):
                mask = low if h == 0 else ~low
                one = jnp.where(mask, query, jnp.zeros_like(query))
                s = lax.dot_general(one, key, COLS, preferred_element_type=F32)
                s = jnp.where(allowed, s * factor, -1e30)
                top = jnp.max(s, axis=-1, keepdims=True)
                e = jnp.exp(s - top)
                total = jnp.sum(e, axis=-1, keepdims=True)
                probs = (e / total).astype(BF16)
                outs.append(jnp.dot(probs, value, preferred_element_type=F32))
                lse[q] = jnp.where(lane == 2 * p + h, top + jnp.log(total), lse[q])
            att[place, :, at] = jnp.where(low, outs[0], outs[1]).astype(BF16)

        lse[q] = jnp.zeros((length, LANES), F32)
        loop(own // LANES, pair)
        x_start(1, m, who)

        @pl.when(first & (k == 1))
        def _():
            output_finish(0)
            relay(3, 0)
            relay(3, 1)

        @pl.when(k == 0)
        def _():
            w_ready(1, 0)
            w_ready(1, 1)

        @pl.when(fresh)
        def _():
            via_ready(1)

        @pl.when(second & (k == 0))
        def _():
            w_ready(1, 3)

        def up_tile(n):
            at = cols(n, WIDE)
            u = jnp.dot(xg[q], w1[:, at], preferred_element_type=F32) + fb[0:1, at]
            c = 0.7978845608028654
            square = u * u
            th = jnp.tanh(c * u * (1.0 + 0.044715 * square))
            act[place, :, at] = (0.5 * u * (1.0 + th)).astype(BF16)
            slope = 0.5 * (1.0 + th)
            slope = slope + 0.5 * u * (1.0 - th * th) * (c * (1.0 + 3 * 0.044715 * square))
            gp[q, :, at] = slope.astype(BF16)

        loop(hidden // WIDE, up_tile)
        x_start(0, m, who)

    def differ(a, b):
        return a + b - 2 * a * b

    def output_stage(m, lo, hi, fresh, now):
        def block(j):
            if fresh is not None:
                for mask in masks_of(nf):
                    @pl.when(fresh & (j == mask))
                    def _(mask=mask):
                        w_ready(2, mask)
                        w_ready(3, mask)
                        if mask == 2:
                            pl.semaphore_signal(
                                go_sem, inc=1, device_id=other, device_id_type=MESH
                            )

            owner = 2 * differ(f // 2, j // 2) + differ(lax.rem(f, 2), lax.rem(j, 2))

            def out_tile(n):
                at = pl.ds(pl.multiple_of(owner * depth + n * WIDE, WIDE), WIDE)
                acc = lax.dot_general(att[m], wo[at, :], COLS, preferred_element_type=F32)
                acc = acc + lax.dot_general(act[m], w2[at, :], COLS, preferred_element_type=F32)
                out_bf[m, :, at] = acc.astype(BF16)
                if now is True:
                    sum_tile(*out_set, m, at, True)
                else:
                    pl.when(now)(lambda: sum_tile(*out_set, m, at, True))

            loop(depth // WIDE, out_tile)

        def step(j, carry):
            block(j)
            return carry

        lax.fori_loop(lo, hi, step, 0)

    def output_rest(m):
        half = width // 2
        start = pl.multiple_of((1 - f // 2) * half, half)
        sum_tile(*out_set, m, pl.ds(start, half), True)

    def store_ends(m):
        return pltpu.make_async_copy(y_f.at[m], ends_o.at[m], o_sem.at[m])

    def output_finish(m):
        total = sum_wait(*out_set, m)
        y = rin[m].astype(F32) + total + wide[2:3, :]

        @pl.when(first)
        def _():
            y_b[m] = y.astype(BF16)
            hop_out(m).start()

        @pl.when(first & (m == last))
        def _():
            wide_copy().wait_recv()
            unit, _ = stats(y_b[m].astype(F32))
            nb[...] = (unit * wide_b[0:1, :] + wide_b[1:2, :]).astype(BF16)
            for skip, copy in cast_rows():
                unless(skip, copy.start)

        @pl.when(second)
        def _():
            y_f[m] = y
            store_ends(m).start()

    def backward_stage(m, who, k):
        q = who * micro + m
        place = jnp.where(who == 0, m, micro)

        @pl.when(first & (who == 0))
        def _():
            @pl.when(m < last)
            def _():
                spread_wait(gr, m, gg_s, gg_r)

            @pl.when(m == last)
            def _():
                cast_wait(gr, gg_s, gg_r)
                dyr[m] = gr[m, ring.block(t)]

            mirror_copy(1, m).start()
            c_start(1, m, 0)

        @pl.when(who == 1)
        def _():
            mirror_copy(1, m).wait_recv()
            c_start(1, m, 1)

            @pl.when(m == 1)
            def _():
                x_sent(2, 0, 1)
                x_sent(3, 0, 1)

        def att_tile(n):
            at = cols(n, WIDE)
            gatt[:, at] = jnp.dot(gr[q], wo[:, at], preferred_element_type=F32).astype(BF16)

        loop(own // WIDE, att_tile)
        low, lane, tables, allowed = attention_masks(q)

        def pair(p):
            at = cols(p, LANES)
            query, key, value = qkv[q, 0, :, at], qkv[q, 1, :, at], qkv[q, 2, :, at]
            grad = gatt[:, at]
            dqs, dks, dvs = [], [], []
            for h in range(2):
                mask = low if h == 0 else ~low
                one = jnp.where(mask, query, jnp.zeros_like(query))
                s = lax.dot_general(one, key, COLS, preferred_element_type=F32)
                s = jnp.where(allowed, s * factor, -1e30)
                log_total = jnp.sum(
                    jnp.where(lane == 2 * p + h, lse[q], 0.0), axis=-1, keepdims=True
                )
                soft = jnp.exp(s - log_total)
                probs = soft.astype(BF16)
                one_grad = jnp.where(mask, grad, jnp.zeros_like(grad))
                dp = lax.dot_general(one_grad, value, COLS, preferred_element_type=F32)
                delta = jnp.sum(dp * soft, axis=-1, keepdims=True)
                ds = (soft * (dp - delta)).astype(BF16)
                dvs.append(lax.dot_general(probs, grad, ROWS, preferred_element_type=F32))
                dqs.append(jnp.dot(ds, key, preferred_element_type=F32))
                dks.append(lax.dot_general(ds, query, ROWS, preferred_element_type=F32))
            dq = jnp.where(low, dqs[0], dqs[1]) * factor
            dk = jnp.where(low, dks[0], dks[1]) * factor
            dj[place, 0, :, at] = twist(dq, tables, -1.0).astype(BF16)
            dj[place, 1, :, at] = twist(dk, tables, -1.0).astype(BF16)
            dj[place, 2, :, at] = jnp.where(low, dvs[0], dvs[1]).astype(BF16)

        loop(own // LANES, pair)
        x_start(3, m, who)

        @pl.when(who == 0)
        def _():
            for part in range(3):
                head_sums[part:part + 1, :] += jnp.sum(
                    dj[m, part].astype(F32), axis=0, keepdims=True
                )

        @pl.when(second & (k == 1))
        def _():
            w_ready(3, 0)
            w_ready(3, 1)
            output_stage(0, 0, 2, None, True)
            via_ready(3)

        def up_tile(n):
            at = cols(n, WIDE)
            acc = jnp.dot(gr[q], w2[:, at], preferred_element_type=F32)
            rounded = (acc * gp[q, :, at].astype(F32)).astype(BF16)
            up[place, :, at] = rounded
            sums = jnp.sum(rounded.astype(F32), axis=0, keepdims=True)
            up_sums[0:1, at] += jnp.where(who == 0, sums, 0.0)

        loop(hidden // WIDE, up_tile)
        x_start(2, m, who)

        def norm_tile(n):
            at = cols(n, WIDE)
            acc = lax.dot_general(up[m], w1[at, :], COLS, preferred_element_type=F32)
            for part in range(3):
                acc = acc + lax.dot_general(
                    dj[m, part], wq[part, at, :], COLS, preferred_element_type=F32
                )
            in_bf[m, :, at] = acc.astype(BF16)
            sum_tile(*in_set, m, at, False)

        @pl.when(who == 0)
        def _():
            loop(width // WIDE, norm_tile)
            sum_after(*in_set, m, False)


    def backward_finish(m):
        grad_norm = sum_wait(*in_set, m)
        unit, inv_root = stats(rin[m].astype(F32))
        scaled = grad_norm * wide[0:1, :]
        upstream = dyr[m].astype(F32)
        dx = upstream + inv_root * (
            scaled
            - jnp.mean(scaled, axis=-1, keepdims=True)
            - unit * jnp.mean(scaled * unit, axis=-1, keepdims=True)
        )

        @pl.when(second)
        def _():
            y_b[m] = dx.astype(BF16)

        @pl.when(second & (m < last))
        def _():
            hop_back(m).start()

        @pl.when(second & (m == last))
        def _():
            for skip, copy in cast_back():
                unless(skip, copy.start)

        @pl.when(first)
        def _():
            y_f[m] = dx
            store_ends(m).start()

        for i, term in enumerate((grad_norm * unit, grad_norm, upstream)):
            own_sums[i:i + 1, :] += jnp.sum(term, axis=0, keepdims=True)

    own_sums[...] = jnp.zeros_like(own_sums)
    head_sums[...] = jnp.zeros_like(head_sums)
    up_sums[...] = jnp.zeros_like(up_sums)

    @pl.when(first)
    def _():
        small_arrive()
        load_rows.wait()
        loop(micro, front)
        seg_copy.wait()
        loop(2 * micro, rope_of)

    @pl.when(second)
    def _():
        load_dy.wait()
        loop(micro, front_back)

    @pl.when(second)
    def _():
        for p in range(PIECES):
            relay(1, p)
        w_far(0)
        w_far(1)
        small_arrive()
        wide_copy().start()
        seg_copy.wait()
        loop(2 * micro, rope_of)
        for mask in order:
            w_ready(0, mask)
        w_far(2)
        for p in range(PIECES):
            leg_two(1, p).wait_send()
        pl.semaphore_wait(go_sem, 1)
        for p in range(PIECES - DIRECT):
            leg_one(3, p).start()

        def dy_in(m):
            spread_wait(gr, m, gg_s, gg_r)
            c_start(1, m, 0)

        loop(micro, dy_in)


    def slot(k):
        is_f = jnp.where(first, k < 4, (k < 8) & (lax.rem(k, 2) == 0))
        is_o = jnp.where(first, k < 2, (k == 1) | (k == 6))
        who = jnp.where(first, (k // 2) % 2 * (k < 4) + lax.rem(k, 2) * (k >= 4), k // 4)
        m = jnp.where(first, jnp.where(k < 4, lax.rem(k, 2), (k - 4) // 2), lax.rem(k // 2, 2))
        m_o = jnp.where(first, m, k // 6)
        fresh = first & (k == 0)

        @pl.when(second & (k == 0))
        def _():
            hop_out(0).wait_recv()
            front(0)
            w_ready(1, 2)
            for p in range(PIECES - DIRECT, PIECES):
                straight(p).start()

        @pl.when(second & (k == 1))
        def _():
            for i in range(micro):
                mirror_copy(1, i).start()
            for mask in order:
                w_ready(2, mask)

        @pl.when(first & (k == 3))
        def _():
            hop_back(0).wait_recv()
            front_back(0)

        @pl.when(is_f)
        def _():
            forward_stage(m, who, k, fresh)

        @pl.when(jnp.logical_not(is_f))
        def _():
            backward_stage(m, who, k)

        @pl.when(second & (k == 6))
        def _():
            for skip, copy in cast_back():
                unless(skip, copy.wait_send)

        @pl.when(is_o)
        def _():
            held_back = second & (k == 1)
            output_stage(
                m_o, jnp.where(held_back, 2, 0), nf, fresh, jnp.logical_not(held_back)
            )

        @pl.when(first & (k < 2))
        def _():
            sum_after(*out_set, m, True)

        @pl.when(second & (k == 6))
        def _():
            sum_after(*out_set, 1, True)

        @pl.when(second & (k == 2))
        def _():
            backward_finish(0)
            output_rest(0)
            sum_after(*out_set, 0, True)

        @pl.when(first & (k == 1))
        def _():
            for p in range(2, PIECES - DIRECT):
                relay(3, p)
            for i in range(micro):
                mirror_copy(0, i).start()
            for p in range(PIECES - DIRECT):
                leg_two(3, p).wait_send()
            output_finish(1)

        @pl.when(first & (k == 7))
        def _():
            backward_finish(0)

        @pl.when((first & (k == 7)) | (second & (k == 4)))
        def _():
            backward_finish(1)

        @pl.when(second & (k == 7))
        def _():
            loop(micro, output_finish)

    loop(8, slot)

    s_src[...] = jnp.zeros_like(s_src)
    for j in range(count):
        s_src[j, 0:3, :] = own_sums[0:3, j * LANES:(j + 1) * LANES]
    for j in range(nf):
        s_src[t * nf + j, 3:6, :] = head_sums[0:3, j * LANES:(j + 1) * LANES]
        for r in range(per_row):
            c = (j * per_row + r) * LANES
            s_src[t * nf + j, 6 + r:7 + r, :] = up_sums[0:1, c:c + LANES]
    small = [
        send(s_src.at[to], s_got.at[k], sm_s.at[k], sm_r.at[k], peer) for k, to, peer in group
    ]
    for copy in small:
        copy.start()

    @pl.when(second)
    def _():
        for m in range(last):
            hop_back(m).wait_send()
        wide_copy().wait_send()

    @pl.when(first)
    def _():
        for m in range(micro):
            hop_out(m).wait_send()
        for skip, copy in cast_rows():
            unless(skip, copy.wait_send)

    total = s_src[me]
    for k, copy in enumerate(small):
        copy.wait()
        total = total + s_got[k + 1]
    sums_o[...] = total
    for m in range(micro):
        for who in range(2):
            for a in range(4):
                if (m, who) != (0, 1):
                    x_sent(a, m, who)
                x_send(a, m, who).wait_recv()
            for which in range(2):
                mine, theirs = c_pair(which, m, who)
                mine.wait()
                theirs.wait()
        for which in range(2):
            mirror_copy(which, m).wait_send()
        store_ends(m).wait()
    for a in range(4):
        w_send(a, 0, 0, 1).wait_send()
    for side, via in ((first, 1), (second, 3)):
        @pl.when(side)
        def _(via=via):
            for a in range(4):
                if a != via:
                    w_send(a, 0, 1, 2).wait_send()
                    w_send(a, 2, 0, 1).wait_send()
            for p in range(PIECES):
                if via == 3 and p >= PIECES - DIRECT:
                    straight(p).wait_send()
                else:
                    leg_one(via, p).wait_send()
                passed_on(via, 2, p).wait_send()


def fused(ends, smalls, segments, wq, wo, w1, w2, nf, nt):
    micro, per, width = ends.shape
    length = per * nt
    own, hidden = wo.shape[1], w1.shape[1]
    depth = width // nf
    count = nf * nt
    bits = nf.bit_length() - 1
    anywhere = pl.BlockSpec(memory_space=pl.ANY)
    inside = pl.BlockSpec(memory_space=pltpu.VMEM)
    dma = pltpu.SemaphoreType.DMA
    vm = pltpu.VMEM
    piece = (ROWS_OF_PACK, LANES)
    packs = 2 * micro
    some = micro + 1
    out_shape = [
        jax.ShapeDtypeStruct(ends.shape, F32),
        jax.ShapeDtypeStruct(piece, F32),
        jax.ShapeDtypeStruct((micro, nf, length, hidden), BF16),
        jax.ShapeDtypeStruct((micro, nf, length, own), BF16),
        jax.ShapeDtypeStruct((micro, nf, length, hidden), BF16),
        jax.ShapeDtypeStruct((3, micro, nf, length, own), BF16),
        jax.ShapeDtypeStruct((micro, nf, length, depth), BF16),
        jax.ShapeDtypeStruct((micro, nf, length, depth), BF16),
    ]
    scratch = [
        vm((3, width, own), BF16), vm((width, own), BF16),
        vm((width, hidden), BF16), vm((width, hidden), BF16),
        vm(piece, F32), vm((count,) + piece, F32),
        vm((ROWS_OF_PACK, width), F32), vm((8, hidden), F32),
        vm((2, 8, length), F32), vm((packs, 2, length, LANES), F32),
        vm(ends.shape, BF16), vm(ends.shape, BF16),
        vm((packs, length, width), BF16), vm((packs, 3, length, own), BF16),
        vm((packs, length, LANES), F32), vm((some, length, own), BF16),
        vm((packs, length, hidden), BF16), vm((some, length, hidden), BF16),
        vm((packs, length, width), BF16), vm((length, own), BF16),
        vm((some, length, hidden), BF16), vm((some, 3, length, own), BF16),
        vm((micro, length, width), BF16), vm((micro, nt - 1, per, width), BF16),
        vm((micro, length, width), BF16), vm((micro, nt - 1, per, width), BF16),
        vm(ends.shape, F32), vm(ends.shape, BF16),
        vm((8, width), F32), vm((8, own), F32), vm((8, hidden), F32),
        vm((count,) + piece, F32), vm((count,) + piece, F32),
        dma, dma((4,)), dma((4, nf, bits)), dma((4, nf)),
        dma((count,)), dma((count,)), dma((count,)), dma((count,)),
        dma((micro, nt)), dma((micro, nt)), dma((micro, nt)), dma((micro, nt)),
        dma((micro, nt)), dma((micro, nt)), dma((micro, nt)), dma((micro, nt)),
        dma((micro,)), dma((micro,)), dma((micro,)), dma((micro,)),
        dma((4, micro, 2)), dma((4, micro, 2)), dma((4, micro, 2)),
        dma((2, micro, 2)), dma((2, micro, 2)), dma((2, micro, 2)),
        dma((3, micro)), dma((3, micro)), dma((micro,)),
        dma((PIECES,)), dma((PIECES,)), dma((PIECES,)), dma((PIECES,)),
        dma((PIECES,)), dma((PIECES,)), pltpu.SemaphoreType.REGULAR,
        vm((per, width), BF16), vm((8, width), F32), dma((nt,)), dma((nt,)), dma((2,)),
        vm(ends.shape, BF16), vm(ends.shape, BF16),
        dma((micro,)), dma((micro,)), dma((micro,)), dma((micro,)),
    ]
    return pl.pallas_call(
        functools.partial(fused_kernel, nf, nt),
        out_shape=out_shape,
        in_specs=[anywhere] + [inside] * 7 + [anywhere] * 4,
        out_specs=[anywhere, inside] + [anywhere] * 6,
        scratch_shapes=scratch,
        compiler_params=pltpu.CompilerParams(
            collective_id=4, has_side_effects=True, vmem_limit_bytes=VMEM_LIMIT
        ),
        name="fused",
    )(ends, *smalls, segments, wq, wo, w1, w2)


def padded(flat):
    size = -(-flat.shape[-1] // (8 * LANES)) * (8 * LANES)
    room = [(0, 0)] * (flat.ndim - 1) + [(0, size - flat.shape[-1])]
    flat = jnp.pad(flat, room)
    return flat.reshape(flat.shape[:-1] + (size // LANES, LANES))


def split_shards(
    ends_in, segments, ln_gain, ln_bias, w_qkv, w_out, w_fc1, w_fc2,
    bias_qkv, bias_out, bias_fc1, bias_fc2,
):
    nf, nt = lax.axis_size("fsdp"), lax.axis_size("tp")
    count = nf * nt
    section, tp_index = lax.axis_index("section"), lax.axis_index("tp")
    is_first = section == 0
    piece = ln_gain.shape[1]
    hidden_piece = bias_fc1.shape[1]
    own, hidden = w_out.shape[2], w_fc1.shape[2]
    width = piece * count

    pack = jnp.concatenate(
        [ln_gain[0], ln_bias[0], bias_out[0], bias_fc2[0], bias_qkv[0].reshape(-1), bias_fc1[0]]
    ).astype(F32)
    used = pack.shape[0]
    smalls = gather_small(padded(pack), nf, nt).reshape(count, -1)[:, :used]
    wide = smalls[:, :7 * piece].reshape(count, 7, piece).transpose(1, 0, 2).reshape(7, width)
    vec = jnp.stack([wide[0], wide[1], wide[2] + wide[3]])
    vec = jnp.pad(vec, ((0, 5), (0, 0)))
    qb = lax.dynamic_slice_in_dim(wide[4:7], tp_index * own, own, 1)
    qb = jnp.pad(qb, ((0, 5), (0, 0)))
    fb = lax.dynamic_slice_in_dim(smalls[:, 7 * piece:], tp_index * nf, nf, 0).reshape(1, hidden)
    fb = jnp.pad(fb, ((0, 7), (0, 0)))
    rope = rope_tables(segments)
    segc, segr = segments[:, :, None], segments[:, None, :]

    wq = lax.all_gather(w_qkv[0].transpose(1, 0, 2), "fsdp", axis=1, tiled=True)
    w1 = lax.all_gather(w_fc1[0], "fsdp", axis=0, tiled=True)
    wo = lax.all_gather(w_out[0], "fsdp", axis=0, tiled=True)
    w2 = lax.all_gather(w_fc2[0], "fsdp", axis=0, tiled=True)
    weights = (wq, wo, w1, w2)
    rows, xg, qkv, lse, att, gp, act, y = forward(
        ends_in[0], weights, vec, qb, fb, rope, segc, segr, nt
    )
    gr, up, dj, dx, own_sums, head_sums, up_sums = backward(
        ends_in[0], weights, rows, qkv, lse, gp, vec, rope, segc, segr, nt
    )

    def everywhere(arr):
        return lax.all_gather(arr, "fsdp", axis=arr.ndim - 2, tiled=True)

    def columns(arr):
        return lax.all_to_all(arr, "fsdp", split_axis=2, concat_axis=1, tiled=True)

    xc, gc = columns(xg), columns(gr)

    def product(left, right):
        return lax.dot_general(
            left, right, (((0, 1), (0, 1)), ((), ())), preferred_element_type=F32
        )

    act_all, att_all, up_all, dj_all = (everywhere(a) for a in (act, att, up, dj))
    grad_fc2 = product(gc, act_all)
    grad_out = product(gc, att_all)
    grad_fc1 = product(xc, up_all)
    grad_qkv = jnp.stack([product(xc, dj_all[:, part]) for part in range(3)], axis=1)

    mine = own_sums[:3].reshape(3, count, piece).transpose(1, 0, 2).reshape(count, 3 * piece)
    head = lax.dynamic_update_slice_in_dim(
        jnp.zeros((3, width), F32), head_sums[:3], tp_index * own, 1
    )
    head = head.reshape(3, count, piece).transpose(1, 0, 2).reshape(count, 3 * piece)
    ups = lax.dynamic_update_slice_in_dim(
        jnp.zeros((count, hidden_piece), F32),
        up_sums[0].reshape(nf, hidden_piece),
        tp_index * nf,
        0,
    )
    sums = sum_small(padded(jnp.concatenate([mine, head, ups], axis=1)), nf, nt).reshape(-1)
    gain_grad, bias_grad, row_grad = (sums[i * piece:(i + 1) * piece] for i in range(3))
    qkv_bias_grad = sums[3 * piece:6 * piece].reshape(3, piece)
    fc1_bias_grad = sums[6 * piece:6 * piece + hidden_piece]
    ends_out = jnp.where(is_first, dx, y)[None]
    return (
        ends_out,
        gain_grad[None],
        bias_grad[None],
        grad_qkv[None],
        grad_out[None],
        grad_fc1[None],
        grad_fc2[None],
        qkv_bias_grad[None],
        row_grad[None],
        fc1_bias_grad[None],
        row_grad[None],
    )


def fused_shards(
    ends_in, segments, ln_gain, ln_bias, w_qkv, w_out, w_fc1, w_fc2,
    bias_qkv, bias_out, bias_fc1, bias_fc2,
):
    nf, nt = lax.axis_size("fsdp"), lax.axis_size("tp")
    used = 6 + bias_fc1.shape[1] // LANES
    ends_out, sums, act_x, att_x, up_x, dj_x, xc, gc = fused(
        ends_in[0],
        (ln_gain, ln_bias, bias_out, bias_fc2, bias_qkv[0], bias_fc1),
        segments, w_qkv[0].transpose(1, 0, 2), w_out[0], w_fc1[0], w_fc2[0], nf, nt,
    )

    def product(left, right):
        left = left.reshape(-1, left.shape[-1])
        right = right.reshape(-1, right.shape[-1])
        return lax.dot_general(left, right, ROWS, preferred_element_type=F32)

    grad_fc2 = product(gc, act_x)
    grad_out = product(gc, att_x)
    grad_fc1 = product(xc, up_x)
    left, right = xc.reshape(-1, xc.shape[-1]), dj_x.reshape(3, -1, dj_x.shape[-1])
    grad_qkv = lax.dot_general(
        left, right, (((0,), (1,)), ((), ())), preferred_element_type=F32
    )
    row_grad = sums[2:3]
    return (
        ends_out[None],
        sums[0:1],
        sums[1:2],
        grad_qkv[None],
        grad_out[None],
        grad_fc1[None],
        grad_fc2[None],
        sums[3:6][None],
        row_grad,
        sums[6:used].reshape(1, -1),
        row_grad,
    )


def shards(*args):
    rows, piece = args[0].shape[2], args[2].shape[1]
    small = rows * lax.axis_size("tp") <= 256
    tidy = piece == LANES and args[10].shape[1] // LANES <= ROWS_OF_PACK - 6
    square = lax.axis_size("fsdp") == 4 and args[0].shape[1] == 2
    return (fused_shards if small and tidy and square else split_shards)(*args)


def solution(mesh):
    both = P("section", ("fsdp", "tp"))
    square = P("section", "fsdp", "tp")
    tokens = P("section", None, ("fsdp", "tp"), None)
    heads = P("section", "fsdp", None, "tp")
    bias3 = P("section", None, ("fsdp", "tp"))
    return jax.shard_map(
        shards,
        mesh=mesh,
        in_specs=(
            tokens, P(None, "fsdp"), both, both, heads, square, square, square,
            bias3, both, both, both,
        ),
        out_specs=(
            tokens, both, both, heads, square, square, square, bias3, both, both, both,
        ),
        check_vma=False,
    )
```

```python
import functools

import jax
import jax.numpy as jnp
from jax import lax
from jax.experimental import pallas as pl
from jax.experimental.pallas import tpu as pltpu
from jax.sharding import PartitionSpec as P

HEAD_DIM = 64
ROT_DIM = 32
EPSILON = 1e-05
LANES = 128
TILE = 256
MESH = pl.DeviceIdType.MESH
F32 = jnp.float32
BF16 = jnp.bfloat16
COLS = (((1,), (1,)), ((), ()))
ROWS = (((0,), (0,)), ((), ()))
VMEM_LIMIT = 66_900_000


def positions_of(segment_ids):
    length = segment_ids.shape[-1]
    places = jnp.arange(length, dtype=jnp.int32)
    before = jnp.concatenate([segment_ids[..., :1] - 1, segment_ids[..., :-1]], axis=-1)
    starts = jnp.where(segment_ids != before, places, 0)
    starts = lax.cummax(starts, axis=segment_ids.ndim - 1)
    return places - starts


def rope_tables(segments):
    half = ROT_DIM // 2
    freq = jnp.exp(-jnp.log(10000.0) * (2.0 * jnp.arange(half, dtype=F32)) / ROT_DIM)
    angles = positions_of(segments).astype(F32)[..., None] * freq
    cosine, sine = jnp.cos(angles), jnp.sin(angles)
    none = jnp.zeros_like(sine)
    rest = jnp.zeros(angles.shape[:-1] + (HEAD_DIM - ROT_DIM,), F32)
    keep = jnp.concatenate([cosine, cosine, rest + 1.0], axis=-1)
    ahead = jnp.concatenate([-sine, none, rest], axis=-1)
    behind = jnp.concatenate([none, sine, rest], axis=-1)
    tables = jnp.stack([keep, ahead, behind], axis=1)
    return jnp.concatenate([tables, tables], axis=-1)


def send(src, dst, send_sem, recv_sem, device):
    return pltpu.make_async_remote_copy(
        src_ref=src,
        dst_ref=dst,
        send_sem=send_sem,
        recv_sem=recv_sem,
        device_id=device,
        device_id_type=MESH,
    )


def greet(peers):
    barrier = pltpu.get_barrier_semaphore()
    for peer in peers:
        pl.semaphore_signal(barrier, inc=1, device_id=peer, device_id_type=MESH)
    pl.semaphore_wait(barrier, len(peers))


def group_peers(nf, nt):
    me = lax.axis_index("fsdp") * nt + lax.axis_index("tp")
    found = []
    for k in range(1, nf * nt):
        to = lax.rem(me + k, nf * nt)
        found.append((k, to, {"fsdp": to // nt, "tp": lax.rem(to, nt)}))
    return me, found


def gather_small_kernel(nf, nt, own, out, send_sems, recv_sems, local_sem):
    me, peers = group_peers(nf, nt)
    greet([peer for _, _, peer in peers])
    mine = pltpu.make_async_copy(own, out.at[me], local_sem)
    mine.start()
    copies = []
    for k, _, peer in peers:
        copy = send(own, out.at[me], send_sems.at[k], recv_sems.at[k], peer)
        copy.start()
        copies.append(copy)
    mine.wait()
    for copy in copies:
        copy.wait()


def gather_small(own, nf, nt):
    count = nf * nt
    return pl.pallas_call(
        functools.partial(gather_small_kernel, nf, nt),
        out_shape=jax.ShapeDtypeStruct((count,) + own.shape, own.dtype),
        in_specs=[pl.BlockSpec(memory_space=pltpu.VMEM)],
        out_specs=pl.BlockSpec(memory_space=pltpu.VMEM),
        scratch_shapes=[
            pltpu.SemaphoreType.DMA((count,)),
            pltpu.SemaphoreType.DMA((count,)),
            pltpu.SemaphoreType.DMA,
        ],
        compiler_params=pltpu.CompilerParams(collective_id=0, has_side_effects=True),
        name="gather_small",
    )(own)


def sum_small_kernel(nf, nt, own, out, got, send_sems, recv_sems):
    me, peers = group_peers(nf, nt)
    greet([peer for _, _, peer in peers])
    copies = []
    for k, to, peer in peers:
        copy = send(own.at[to], got.at[k], send_sems.at[k], recv_sems.at[k], peer)
        copy.start()
        copies.append(copy)
    total = own[me]
    for k, copy in enumerate(copies):
        copy.wait()
        total = total + got[k + 1]
    out[...] = total


def sum_small(own, nf, nt):
    count = nf * nt
    return pl.pallas_call(
        functools.partial(sum_small_kernel, nf, nt),
        out_shape=jax.ShapeDtypeStruct(own.shape[1:], own.dtype),
        in_specs=[pl.BlockSpec(memory_space=pltpu.VMEM)],
        out_specs=pl.BlockSpec(memory_space=pltpu.VMEM),
        scratch_shapes=[
            pltpu.VMEM(own.shape, own.dtype),
            pltpu.SemaphoreType.DMA((count,)),
            pltpu.SemaphoreType.DMA((count,)),
        ],
        compiler_params=pltpu.CompilerParams(collective_id=1, has_side_effects=True),
        name="sum_small",
    )(own)


def cols(n, width=TILE):
    return pl.ds(pl.multiple_of(n * width, width), width)


def loop(count, body):
    def step(i, carry):
        body(i)
        return carry

    lax.fori_loop(0, count, step, 0)


def turn(x, tables, sign):
    keep, ahead, behind = tables
    left = pltpu.roll(x, LANES - ROT_DIM // 2, 1)
    right = pltpu.roll(x, ROT_DIM // 2, 1)
    return x * keep + sign * (left * ahead + right * behind)


def low_half(length):
    return lax.broadcasted_iota(jnp.int32, (length, LANES), 1) < HEAD_DIM


def allowed_mask(segc, segr, m, length):
    query = lax.broadcasted_iota(jnp.int32, (length, length), 0)
    key = lax.broadcasted_iota(jnp.int32, (length, length), 1)
    return (query >= key) & (segc[m] == segr[m])


class Ring:
    def __init__(self, nt, rows):
        self.nt, self.rows = nt, rows
        self.me = lax.axis_index("tp")
        self.others = [(k, lax.rem(self.me + k, nt)) for k in range(1, nt)]

    def block(self, who):
        return pl.ds(pl.multiple_of(who * self.rows, self.rows), self.rows)

    def gather(self, buf, m, sems):
        return [
            send(
                buf.at[m, self.block(self.me)],
                buf.at[m, self.block(self.me)],
                sems[0].at[m, k],
                sems[1].at[m, k],
                {"tp": to},
            )
            for k, to in self.others
        ]

    def scatter(self, buf, got, m, sems, part=None):
        at = slice(None) if part is None else part
        return [
            send(
                buf.at[m, self.block(to), at],
                got.at[m, k - 1, :, at],
                sems[0].at[m, k],
                sems[1].at[m, k],
                {"tp": to},
            )
            for k, to in self.others
        ]

    def total(self, buf, got, m):
        acc = buf[m, self.block(self.me)].astype(F32)
        for k, _ in self.others:
            acc = acc + got[m, k - 1].astype(F32)
        return acc


def stats(rows):
    mean = jnp.mean(rows, axis=-1, keepdims=True)
    centred = rows - mean
    variance = jnp.mean(centred * centred, axis=-1, keepdims=True)
    inv_root = lax.rsqrt(variance + EPSILON)
    return centred * inv_root, inv_root


def forward_kernel(
    nt,
    rows_h, wq_h, wo_h, w1_h, w2_h, vec, qb, fb, rope, segc, segr,
    rows_o, xg_o, qkv_o, lse_o, att_o, gp_o, act_o, y_o,
    wq, wo, w1, w2, rin, xg, qkv, lse, att, gp, act, branch, got, out_f, out_b,
    w_sem, in_sem, o_sem, ag_s, ag_r, rs_s, rs_r, x_s, x_r,
):
    micro, length, width = xg.shape
    section = lax.axis_index("section")
    first, second = section == 0, section == 1
    ring = Ring(nt, length // nt)
    own = wo.shape[1]
    loads = []
    for i, (src, dst) in enumerate(((wq_h, wq), (w1_h, w1), (wo_h, wo), (w2_h, w2))):
        loads.append(pltpu.make_async_copy(src, dst, w_sem.at[i]))
        loads[-1].start()
    mine = pltpu.make_async_copy(rows_h, rin, in_sem)

    @pl.when(first)
    def _():
        mine.start()

    greet([{"tp": to} for _, to in ring.others] + [{"section": 1 - section}])

    @pl.when(first)
    def _():
        mine.wait()

    def hop(m):
        return send(out_b.at[m], rin.at[m], x_s.at[m], x_r.at[m], {"section": 1 - section})

    def front(m):
        unit, _ = stats(rin[m].astype(F32))
        normed = unit * vec[0:1, :] + vec[1:2, :]
        xg[m, ring.block(ring.me)] = normed.astype(BF16)
        for copy in ring.gather(xg, m, (ag_s, ag_r)):
            copy.start()

    def arrive(m):
        @pl.when(second)
        def _():
            hop(m).wait_recv()
            front(m)

    stores = []

    def store(src, dst, m, i):
        copy = pltpu.make_async_copy(src.at[m], dst.at[m], o_sem.at[m, i])
        copy.start()
        stores.append(copy)

    def body(m):
        for copy in ring.gather(xg, m, (ag_s, ag_r)):
            copy.wait()
        store(xg, xg_o, m, 0)
        store(rin, rows_o, m, 1)
        tables = (rope[m, 0], rope[m, 1], rope[m, 2])
        if m == 0:
            loads[0].wait()
        per = own // TILE
        for part in range(3):
            def qkv_tile(n, part=part):
                at = cols(n)
                acc = jnp.dot(xg[m], wq[part, :, at], preferred_element_type=F32)
                acc = acc + qb[part:part + 1, at]
                if part < 2:
                    acc = jnp.concatenate(
                        [
                            turn(acc[:, c:c + LANES], tables, 1.0)
                            for c in range(0, TILE, LANES)
                        ],
                        axis=1,
                    )
                qkv[m, part, :, at] = acc.astype(BF16)

            loop(per, qkv_tile)
        store(qkv, qkv_o, m, 2)
        allowed = allowed_mask(segc, segr, m, length)
        low = low_half(length)
        lane = lax.broadcasted_iota(jnp.int32, (length, LANES), 1)

        def pair(p):
            at = cols(p, LANES)
            query, key, value = qkv[m, 0, :, at], qkv[m, 1, :, at], qkv[m, 2, :, at]
            outs = []
            for h in range(2):
                mask = low if h == 0 else ~low
                one = jnp.where(mask, query, jnp.zeros_like(query))
                s = lax.dot_general(one, key, COLS, preferred_element_type=F32)
                s = jnp.where(allowed, s * HEAD_DIM ** (-0.5), -1e30)
                top = jnp.max(s, axis=-1, keepdims=True)
                e = jnp.exp(s - top)
                total = jnp.sum(e, axis=-1, keepdims=True)
                probs = (e / total).astype(BF16)
                outs.append(jnp.dot(probs, value, preferred_element_type=F32))
                lse[m] = jnp.where(lane == 2 * p + h, top + jnp.log(total), lse[m])
            att[m, :, at] = jnp.where(low, outs[0], outs[1]).astype(BF16)

        lse[m] = jnp.zeros((length, LANES), F32)
        loop(own // LANES, pair)
        store(lse, lse_o, m, 3)
        store(att, att_o, m, 4)
        if m == 0:
            loads[1].wait()

        def up_tile(n):
            at = cols(n)
            u = jnp.dot(xg[m], w1[:, at], preferred_element_type=F32) + fb[0:1, at]
            c = 0.7978845608028654
            square = u * u
            t = jnp.tanh(c * u * (1.0 + 0.044715 * square))
            act[m, :, at] = (0.5 * u * (1.0 + t)).astype(BF16)
            slope = 0.5 * (1.0 + t) + 0.5 * u * (1.0 - t * t) * (c * (1.0 + 3 * 0.044715 * square))
            gp[m, :, at] = slope.astype(BF16)

        loop(act.shape[2] // TILE, up_tile)
        store(act, act_o, m, 5)
        store(gp, gp_o, m, 6)
        if m == 0:
            loads[2].wait()
            loads[3].wait()

        def out_tile(n):
            at = cols(n)
            acc = lax.dot_general(att[m], wo[at, :], COLS, preferred_element_type=F32)
            acc = acc + lax.dot_general(act[m], w2[at, :], COLS, preferred_element_type=F32)
            branch[m, :, at] = acc.astype(BF16)
            for copy in ring.scatter(branch, got, m, (rs_s, rs_r), at):
                copy.start()

        loop(width // TILE, out_tile)

    def finish(m):
        for copy in ring.scatter(branch, got, m, (rs_s, rs_r)):
            copy.wait()
        y = rin[m].astype(F32) + ring.total(branch, got, m) + vec[2:3, :]
        out_f[m] = y
        out_b[m] = y.astype(BF16)
        store(out_f, y_o, m, 7)

        @pl.when(first)
        def _():
            hop(m).start()

    @pl.when(first)
    def _():
        for m in range(micro):
            front(m)

    for m in range(micro):
        arrive(m)
        body(m)
    for m in range(micro):
        finish(m)
    for copy in stores:
        copy.wait()

    @pl.when(first)
    def _():
        for m in range(micro):
            hop(m).wait_send()


def forward(rows, weights, vec, qb, fb, rope, segc, segr, nt):
    wq, wo, w1, w2 = weights
    micro, per, width = rows.shape
    length = per * nt
    own, hidden = wo.shape[1], w1.shape[1]
    anywhere = pl.BlockSpec(memory_space=pl.ANY)
    inside = pl.BlockSpec(memory_space=pltpu.VMEM)
    out_shape = [
        jax.ShapeDtypeStruct(rows.shape, BF16),
        jax.ShapeDtypeStruct((micro, length, width), BF16),
        jax.ShapeDtypeStruct((micro, 3, length, own), BF16),
        jax.ShapeDtypeStruct((micro, length, LANES), F32),
        jax.ShapeDtypeStruct((micro, length, own), BF16),
        jax.ShapeDtypeStruct((micro, length, hidden), BF16),
        jax.ShapeDtypeStruct((micro, length, hidden), BF16),
        jax.ShapeDtypeStruct(rows.shape, F32),
    ]
    dma = pltpu.SemaphoreType.DMA
    return pl.pallas_call(
        functools.partial(forward_kernel, nt),
        out_shape=out_shape,
        in_specs=[anywhere] * 5 + [inside] * 6,
        out_specs=[anywhere] * 8,
        scratch_shapes=[
            pltpu.VMEM(wq.shape, BF16),
            pltpu.VMEM(wo.shape, BF16),
            pltpu.VMEM(w1.shape, BF16),
            pltpu.VMEM(w2.shape, BF16),
            pltpu.VMEM(rows.shape, BF16),
            pltpu.VMEM((micro, length, width), BF16),
            pltpu.VMEM((micro, 3, length, own), BF16),
            pltpu.VMEM((micro, length, LANES), F32),
            pltpu.VMEM((micro, length, own), BF16),
            pltpu.VMEM((micro, length, hidden), BF16),
            pltpu.VMEM((micro, length, hidden), BF16),
            pltpu.VMEM((micro, length, width), BF16),
            pltpu.VMEM((micro, nt - 1, per, width), BF16),
            pltpu.VMEM(rows.shape, F32),
            pltpu.VMEM(rows.shape, BF16),
            dma((4,)),
            dma,
            dma((micro, 8)),
            dma((micro, nt)),
            dma((micro, nt)),
            dma((micro, nt)),
            dma((micro, nt)),
            dma((micro,)),
            dma((micro,)),
        ],
        compiler_params=pltpu.CompilerParams(
            collective_id=2, has_side_effects=True, vmem_limit_bytes=VMEM_LIMIT
        ),
        name="forward",
    )(rows, wq, wo, w1, w2, vec, qb, fb, rope, segc, segr)


def backward_kernel(
    nt,
    dy_h, wq_h, wo_h, w1_h, w2_h, rows_h, qkv_h, lse_h, gp_h, vec, rope, segc, segr,
    gr_o, up_o, dj_o, dx_o, own_sums, head_sums, up_sums,
    wq, wo, w1, w2, dyr, rin, qkv, lse, gp, gr, gatt, up, dj, branch, got, out_f, out_b,
    w_sem, in_sem, o_sem, ag_s, ag_r, rs_s, rs_r, x_s, x_r,
):
    micro, length, width = gr.shape
    section = lax.axis_index("section")
    first, second = section == 0, section == 1
    ring = Ring(nt, length // nt)
    own = wo.shape[1]
    mine = pltpu.make_async_copy(dy_h, dyr, in_sem.at[4])

    @pl.when(second)
    def _():
        mine.start()

    loads = []
    for i, (src, dst) in enumerate(((wo_h, wo), (w2_h, w2), (wq_h, wq), (w1_h, w1))):
        loads.append(pltpu.make_async_copy(src, dst, w_sem.at[i]))
    kept = []
    for i, (src, dst) in enumerate(((qkv_h, qkv), (lse_h, lse), (gp_h, gp), (rows_h, rin))):
        kept.append(pltpu.make_async_copy(src, dst, in_sem.at[i]))
    for copy in (loads[0], kept[0], kept[1], loads[1], kept[2], loads[2], loads[3], kept[3]):
        copy.start()
    greet([{"tp": to} for _, to in ring.others] + [{"section": 1 - section}])

    @pl.when(second)
    def _():
        mine.wait()

    def hop(m):
        return send(out_b.at[m], dyr.at[m], x_s.at[m], x_r.at[m], {"section": 1 - section})

    def front(m):
        gr[m, ring.block(ring.me)] = dyr[m]
        for copy in ring.gather(gr, m, (ag_s, ag_r)):
            copy.start()

    def arrive(m):
        @pl.when(first)
        def _():
            hop(m).wait_recv()
            front(m)

    stores = []

    def store(src, dst, m, i):
        copy = pltpu.make_async_copy(src.at[m], dst.at[m], o_sem.at[m, i])
        copy.start()
        stores.append(copy)

    def body(m):
        for copy in ring.gather(gr, m, (ag_s, ag_r)):
            copy.wait()
        store(gr, gr_o, m, 0)
        if m == 0:
            loads[0].wait()

        def att_tile(n):
            at = cols(n)
            gatt[:, at] = jnp.dot(gr[m], wo[:, at], preferred_element_type=F32).astype(BF16)

        loop(own // TILE, att_tile)
        if m == 0:
            kept[0].wait()
            kept[1].wait()
        tables = (rope[m, 0], rope[m, 1], rope[m, 2])
        allowed = allowed_mask(segc, segr, m, length)
        low = low_half(length)
        lane = lax.broadcasted_iota(jnp.int32, (length, LANES), 1)
        factor = HEAD_DIM ** (-0.5)

        def pair(p):
            at = cols(p, LANES)
            query, key, value = qkv[m, 0, :, at], qkv[m, 1, :, at], qkv[m, 2, :, at]
            grad = gatt[:, at]
            dqs, dks, dvs = [], [], []
            for h in range(2):
                mask = low if h == 0 else ~low
                one = jnp.where(mask, query, jnp.zeros_like(query))
                s = lax.dot_general(one, key, COLS, preferred_element_type=F32)
                s = jnp.where(allowed, s * factor, -1e30)
                log_total = jnp.sum(
                    jnp.where(lane == 2 * p + h, lse[m], 0.0), axis=-1, keepdims=True
                )
                soft = jnp.exp(s - log_total)
                probs = soft.astype(BF16)
                one_grad = jnp.where(mask, grad, jnp.zeros_like(grad))
                dp = lax.dot_general(one_grad, value, COLS, preferred_element_type=F32)
                delta = jnp.sum(dp * soft, axis=-1, keepdims=True)
                ds = (soft * (dp - delta)).astype(BF16)
                dvs.append(lax.dot_general(probs, grad, ROWS, preferred_element_type=F32))
                dqs.append(jnp.dot(ds, key, preferred_element_type=F32))
                dks.append(lax.dot_general(ds, query, ROWS, preferred_element_type=F32))
            dq = jnp.where(low, dqs[0], dqs[1]) * factor
            dk = jnp.where(low, dks[0], dks[1]) * factor
            dj[m, 0, :, at] = turn(dq, tables, -1.0).astype(BF16)
            dj[m, 1, :, at] = turn(dk, tables, -1.0).astype(BF16)
            dj[m, 2, :, at] = jnp.where(low, dvs[0], dvs[1]).astype(BF16)

        loop(own // LANES, pair)
        store(dj, dj_o, m, 1)
        for part in range(3):
            sums = jnp.sum(dj[m, part].astype(F32), axis=0, keepdims=True)
            if m == 0:
                head_sums[part:part + 1, :] = sums
            else:
                head_sums[part:part + 1, :] += sums
        if m == 0:
            loads[1].wait()
            kept[2].wait()

        def up_tile(n):
            at = cols(n)
            acc = jnp.dot(gr[m], w2[:, at], preferred_element_type=F32)
            rounded = (acc * gp[m, :, at].astype(F32)).astype(BF16)
            up[m, :, at] = rounded
            sums = jnp.sum(rounded.astype(F32), axis=0, keepdims=True)
            if m == 0:
                up_sums[0:1, at] = sums
            else:
                up_sums[0:1, at] += sums

        loop(up.shape[2] // TILE, up_tile)
        store(up, up_o, m, 2)
        if m == 0:
            loads[2].wait()
            loads[3].wait()

        def norm_tile(n):
            at = cols(n)
            acc = lax.dot_general(up[m], w1[at, :], COLS, preferred_element_type=F32)
            for part in range(3):
                acc = acc + lax.dot_general(
                    dj[m, part], wq[part, at, :], COLS, preferred_element_type=F32
                )
            branch[m, :, at] = acc.astype(BF16)
            for copy in ring.scatter(branch, got, m, (rs_s, rs_r), at):
                copy.start()

        loop(width // TILE, norm_tile)

    def finish(m):
        for copy in ring.scatter(branch, got, m, (rs_s, rs_r)):
            copy.wait()
        if m == 0:
            kept[3].wait()
        grad_norm = ring.total(branch, got, m)
        unit, inv_root = stats(rin[m].astype(F32))
        scaled = grad_norm * vec[0:1, :]
        upstream = dyr[m].astype(F32)
        dx = upstream + inv_root * (
            scaled
            - jnp.mean(scaled, axis=-1, keepdims=True)
            - unit * jnp.mean(scaled * unit, axis=-1, keepdims=True)
        )
        out_f[m] = dx
        out_b[m] = dx.astype(BF16)

        @pl.when(second)
        def _():
            hop(m).start()

        store(out_f, dx_o, m, 3)
        for i, term in enumerate((grad_norm * unit, grad_norm, upstream)):
            sums = jnp.sum(term, axis=0, keepdims=True)
            if m == 0:
                own_sums[i:i + 1, :] = sums
            else:
                own_sums[i:i + 1, :] += sums

    @pl.when(second)
    def _():
        for m in range(micro):
            front(m)

    for m in range(micro):
        arrive(m)
        body(m)
    for m in range(micro):
        finish(m)
    for copy in stores:
        copy.wait()

    @pl.when(second)
    def _():
        for m in range(micro):
            hop(m).wait_send()


def backward(dy, weights, rows, qkv, lse, gp, vec, rope, segc, segr, nt):
    wq, wo, w1, w2 = weights
    micro, per, width = rows.shape
    length = per * nt
    own, hidden = wo.shape[1], w1.shape[1]
    anywhere = pl.BlockSpec(memory_space=pl.ANY)
    inside = pl.BlockSpec(memory_space=pltpu.VMEM)
    out_shape = [
        jax.ShapeDtypeStruct((micro, length, width), BF16),
        jax.ShapeDtypeStruct((micro, length, hidden), BF16),
        jax.ShapeDtypeStruct((micro, 3, length, own), BF16),
        jax.ShapeDtypeStruct(rows.shape, F32),
        jax.ShapeDtypeStruct((8, width), F32),
        jax.ShapeDtypeStruct((8, own), F32),
        jax.ShapeDtypeStruct((8, hidden), F32),
    ]
    dma = pltpu.SemaphoreType.DMA
    return pl.pallas_call(
        functools.partial(backward_kernel, nt),
        out_shape=out_shape,
        in_specs=[anywhere] * 9 + [inside] * 4,
        out_specs=[anywhere] * 4 + [inside] * 3,
        scratch_shapes=[
            pltpu.VMEM(wq.shape, BF16),
            pltpu.VMEM(wo.shape, BF16),
            pltpu.VMEM(w1.shape, BF16),
            pltpu.VMEM(w2.shape, BF16),
            pltpu.VMEM(rows.shape, BF16),
            pltpu.VMEM(rows.shape, BF16),
            pltpu.VMEM(qkv.shape, BF16),
            pltpu.VMEM(lse.shape, F32),
            pltpu.VMEM(gp.shape, BF16),
            pltpu.VMEM((micro, length, width), BF16),
            pltpu.VMEM((length, own), BF16),
            pltpu.VMEM((micro, length, hidden), BF16),
            pltpu.VMEM((micro, 3, length, own), BF16),
            pltpu.VMEM((micro, length, width), BF16),
            pltpu.VMEM((micro, nt - 1, per, width), BF16),
            pltpu.VMEM(rows.shape, F32),
            pltpu.VMEM(rows.shape, BF16),
            dma((4,)),
            dma((5,)),
            dma((micro, 4)),
            dma((micro, nt)),
            dma((micro, nt)),
            dma((micro, nt)),
            dma((micro, nt)),
            dma((micro,)),
            dma((micro,)),
        ],
        compiler_params=pltpu.CompilerParams(
            collective_id=3, has_side_effects=True, vmem_limit_bytes=VMEM_LIMIT
        ),
        name="backward",
    )(dy, wq, wo, w1, w2, rows, qkv, lse, gp, vec, rope, segc, segr)


ROWS_OF_PACK = 16
PIECES = 8
DIRECT = 2
STRIPS = 4
WIDE = 512


def twist(x, tables, sign):
    keep, sine, ahead = tables
    left = pltpu.roll(x, LANES - ROT_DIM // 2, 1)
    right = pltpu.roll(x, ROT_DIM // 2, 1)
    return x * keep + jnp.where(ahead, left, right) * (sign * sine)


def masks_of(nf):
    return range(nf)


def bits_below(mask, nf):
    low = mask & -mask if mask else nf
    return [(i, 1 << i) for i in range(nf.bit_length() - 1) if (1 << i) < low]


def flipped(index, mask, nf):
    for i in range(nf.bit_length() - 1):
        if mask >> i & 1:
            index = index + (1 << i) * (1 - 2 * lax.rem(index // (1 << i), 2))
    return index


def fused_kernel(
    nf, nt,
    ends_h, gain, shift, b_out, b_fc2, b_qkv, b_fc1, seg_in, wq_h, wo_h, w1_h, w2_h,
    ends_o, sums_o, fc2_o, fc1_o, out_o, qkv_o, turned_o,
    act_x, att_x, up_x, dj_x, xc_x, gc_x,
    wq, wo, w1, w2, pack, packs, wide, fb, segs, rope, rin, dyr, xg, qkv, lse, att, gp, act,
    gr, gatt, up, dj, out_bf, out_got, in_bf, in_got, y_f, y_b,
    own_sums, head_sums, up_sums, s_src, s_got,
    in_sem, wl_sem, ws_sem, wr_sem, pk_s, pk_r, sm_s, sm_r,
    ag_s, ag_r, gg_s, gg_r, rs_s, rs_r, rb_s, rb_r, hx_s, hx_r, hb_s, hb_r,
    xl_sem, xs_s, xs_r, cl_sem, ca_s, ca_r, mx_s, mx_r, o_sem,
    l1_s, l1_r, l2_s, l2_r, fw_s, fw_r, go_sem, nb, wide_b, mf_s, mb_s, wb_sem,
    dl_sem, ds_sem,
):
    micro, per, width = rin.shape
    length = per * nt
    section, f, t = (lax.axis_index(a) for a in ("section", "fsdp", "tp"))
    first, second = section == 0, section == 1
    ring = Ring(nt, per)
    own, hidden = wo.shape[1], w1.shape[1]
    depth = width // nf
    mirror, sibling = {"fsdp": flipped(f, 2, nf)}, {"fsdp": flipped(f, 1, nf)}
    count = nf * nt
    other = {"section": 1 - section}
    across = {"section": 1 - section, "fsdp": flipped(f, 2, nf)}
    me, group = group_peers(nf, nt)
    fblock = [flipped(f, mask, nf) for mask in masks_of(nf)]

    def rows_at(block):
        return pl.ds(pl.multiple_of(block * depth, depth), depth)

    load_rows = pltpu.make_async_copy(ends_h, rin, in_sem)
    load_dy = pltpu.make_async_copy(ends_h, dyr, in_sem)

    @pl.when(first)
    def _():
        load_rows.start()

    @pl.when(second)
    def _():
        load_dy.start()

    greet(
        [peer for _, _, peer in group]
        + [across, other]
        + [{"section": 1 - section, "tp": to} for _, to in ring.others]
    )

    per_row = hidden // nf // LANES
    segs[0] = jnp.zeros((8, length), F32)
    segs[0, 0:micro, :] = seg_in[...].astype(F32)
    pack[...] = jnp.zeros_like(pack)
    pack[0:1, :] = gain[...].astype(F32)
    pack[1:2, :] = shift[...].astype(F32)
    pack[2:3, :] = b_out[...].astype(F32) + b_fc2[...].astype(F32)
    pack[3:6, :] = b_qkv[...].astype(F32)
    for r in range(per_row):
        pack[6 + r:7 + r, :] = b_fc1[:, r * LANES:(r + 1) * LANES].astype(F32)
    seg_copy = send(segs.at[0], segs.at[1], mx_s.at[2, 0], mx_r.at[2, 0], mirror)
    pack_local = pltpu.make_async_copy(pack, packs.at[me], pk_s.at[0])
    pack_copies = [
        send(pack, packs.at[me], pk_s.at[k], pk_r.at[k], peer) for k, _, peer in group
    ]
    pack_local.start()
    seg_copy.start()
    for copy in pack_copies:
        copy.start()

    table = ((wq_h, wq), (w1_h, w1), (wo_h, wo), (w2_h, w2))

    def w_at(ref, block):
        return ref.at[:, rows_at(block), :] if len(ref.shape) == 3 else ref.at[rows_at(block), :]

    def w_local(a):
        return pltpu.make_async_copy(table[a][0], w_at(table[a][1], f), wl_sem.at[a])

    def w_send(a, mask, i, bit):
        block = w_at(table[a][1], fblock[mask])
        src = table[a][0] if mask == 0 else block
        peer = {"fsdp": flipped(f, bit, nf)}
        return send(src, block, ws_sem.at[a, mask, i], wr_sem.at[a, mask | bit], peer)

    def w_recv(a, mask):
        block = w_at(table[a][1], fblock[mask])
        return send(block, block, ws_sem.at[a, mask, 0], wr_sem.at[a, mask], other)

    def w_near(a):
        w_local(a).start()
        w_send(a, 0, 0, 1).start()

    def w_far(a):
        w_send(a, 0, 1, 2).start()

    part_rows = depth // PIECES
    per_slot = length // part_rows

    def stage(p):
        return up.at[p // per_slot, pl.ds(p % per_slot * part_rows, part_rows), :]

    def piece_at(a, mask, p):
        start = pl.multiple_of(fblock[mask] * depth + p * part_rows, part_rows)
        return table[a][1].at[pl.ds(start, part_rows), :]

    def leg_one(a, p):
        src = table[a][0].at[pl.ds(p * part_rows, part_rows), :]
        return send(src, stage(p), l1_s.at[p], l1_r.at[p], across)

    def leg_two(a, p):
        return send(stage(p), piece_at(a, 2, p), l2_s.at[p], l2_r.at[p], other)

    def passed_on(a, mask, p):
        block = piece_at(a, mask, p)
        return send(block, block, fw_s.at[p], fw_r.at[p], sibling)

    def straight(p):
        src = table[3][0].at[pl.ds(p * part_rows, part_rows), :]
        return send(src, piece_at(3, 0, p), l1_s.at[p], l2_r.at[p], mirror)

    def relay(a, p):
        leg_one(a, p).wait_recv()
        leg_two(a, p).start()

    def via_ready(a):
        for p in range(PIECES):
            leg_two(a, p).wait_recv()
            passed_on(a, 2, p).start()
        for p in range(PIECES):
            passed_on(a, 3, p).wait_recv()

    def w_ready(a, mask):
        if mask == 0:
            w_local(a).wait()
            return
        w_recv(a, mask).wait_recv()
        for i, bit in bits_below(mask, nf):
            w_send(a, mask, i, bit).start()

    order = sorted(masks_of(nf), key=lambda m: (m != 0, -(m & -m), m))
    out_order = list(masks_of(nf))
    for a in range(4):
        w_near(a)

    @pl.when(first)
    def _():
        w_far(0)
        w_far(2)
        for p in range(PIECES):
            leg_one(1, p).start()

    def small_arrive():
        pack_local.wait()
        for copy in pack_copies:
            copy.wait()
        for j in range(count):
            wide[:, j * LANES:(j + 1) * LANES] = packs[j]
        for j in range(nf):
            for r in range(per_row):
                c = (j * per_row + r) * LANES
                fb[0:1, c:c + LANES] = packs[t * nf + j, 6 + r:7 + r, :]

    def segment_parts(q):
        row = segs[q // micro, pl.ds(lax.rem(q, micro), 1), :]
        query = lax.broadcasted_iota(jnp.int32, (length, length), 0)
        key = lax.broadcasted_iota(jnp.int32, (length, length), 1)
        column = jnp.sum(jnp.where(query == key, row, 0.0), axis=1, keepdims=True)
        return row, column, query >= key

    def allowed_of(q):
        row, column, causal = segment_parts(q)
        return causal & (row == column)

    def rope_of(q):
        row, column, _ = segment_parts(q)
        before = jnp.sum(jnp.where(row < column, 1.0, 0.0), axis=1, keepdims=True)
        lane = lax.rem(lax.broadcasted_iota(jnp.int32, (length, LANES), 1), HEAD_DIM)
        place = lax.broadcasted_iota(jnp.int32, (length, LANES), 0).astype(F32) - before
        half = ROT_DIM // 2
        power = lax.rem(lane, half).astype(F32)
        freq = jnp.exp(-jnp.log(10000.0) * (2.0 * power) / ROT_DIM)
        angles = place * freq
        rope[q, 0] = jnp.where(lane < ROT_DIM, jnp.cos(angles), 1.0)
        sine = jnp.where(lane < ROT_DIM, jnp.sin(angles), 0.0)
        rope[q, 1] = jnp.where(lane < half, -sine, sine)

    def hop_out(m):
        return send(y_b.at[m], rin.at[m], hx_s.at[m], hx_r.at[m], other)

    def hop_back(m):
        return send(y_b.at[m], dyr.at[m], hb_s.at[m], hb_r.at[m], other)

    def spread(buf, m, send_sems, recv_sems):
        here = ring.block(t)
        return [
            send(
                buf.at[m, here], buf.at[m, here], send_sems.at[m, k], recv_sems.at[m, t],
                {"tp": to},
            )
            for k, to in ring.others
        ]

    def block_wait(buf, m, recv_sems, who):
        at = ring.block(who)
        send(buf.at[m, at], buf.at[m, at], o_sem.at[m], recv_sems.at[m, who], other).wait_recv()

    def spread_start(buf, m, send_sems, recv_sems):
        for copy in spread(buf, m, send_sems, recv_sems):
            copy.start()

    def spread_wait(buf, m, send_sems, recv_sems):
        for _, who in ring.others:
            block_wait(buf, m, recv_sems, who)
        for copy in spread(buf, m, send_sems, recv_sems):
            copy.wait_send()

    last = micro - 1

    def cast(src, buf, send_sems, recv_sems):
        here = ring.block(t)
        return [
            send(
                src, buf.at[last, here], send_sems.at[k], recv_sems.at[last, t],
                {"section": 1 - section, "tp": to},
            )
            for k, to in [(0, t)] + ring.others
        ]

    def cast_wait(buf, recv_sems):
        for who in range(nt):
            block_wait(buf, last, recv_sems, who)

    def cast_rows():
        return cast(nb, xg, mf_s, ag_r)

    def cast_back():
        return cast(y_b.at[last], gr, mb_s, gg_r)

    def wide_copy():
        return send(wide.at[0:8], wide_b, wb_sem.at[0], wb_sem.at[1], other)

    def front(m):
        unit, _ = stats(rin[m].astype(F32))
        normed = unit * wide[0:1, :] + wide[1:2, :]
        xg[m, ring.block(ring.me)] = normed.astype(BF16)
        spread_start(xg, m, ag_s, ag_r)

    def front_back(m):
        gr[m, ring.block(ring.me)] = dyr[m]
        spread_start(gr, m, gg_s, gg_r)

    def mirror_copy(which, m):
        buf = (xg, gr)[which]
        return send(
            buf.at[m], buf.at[micro + m], mx_s.at[which, m], mx_r.at[which, m], mirror
        )

    def x_block(who):
        return fblock[2 * who] if isinstance(who, int) else jnp.where(who == 0, f, fblock[2])

    def x_dst(a, m, who):
        block = x_block(who)
        if a == 3:
            return dj_x.at[m, :, block]
        return (act_x, att_x, up_x)[a].at[m, block]

    def x_src(a, m, who):
        place = (m, micro)[who] if isinstance(who, int) else jnp.where(who == 0, m, micro)
        return (act, att, up, dj)[a].at[place]

    def x_local(a, m, who):
        return pltpu.make_async_copy(
            x_src(a, m, who), x_dst(a, m, who), xl_sem.at[a, m, who]
        )

    def x_send(a, m, who):
        return send(
            x_src(a, m, who), x_dst(a, m, who), xs_s.at[a, m, who], xs_r.at[a, m, who], sibling
        )

    def x_start(a, m, who):
        x_local(a, m, who).start()
        x_send(a, m, who).start()

    def x_sent(a, m, who):
        x_local(a, m, who).wait()
        x_send(a, m, who).wait_send()

    def c_pair(which, m, who):
        src, dst = ((xg, xc_x), (gr, gc_x))[which]
        block = x_block(who)
        q = who * micro + m
        mine = pltpu.make_async_copy(
            src.at[q, :, rows_at(f)], dst.at[m, block], cl_sem.at[which, m, who]
        )
        theirs = send(
            src.at[q, :, rows_at(fblock[1])],
            dst.at[m, block],
            ca_s.at[which, m, who],
            ca_r.at[which, m, who],
            sibling,
        )
        return mine, theirs

    def c_start(which, m, who):
        for copy in c_pair(which, m, who):
            copy.start()

    def sum_start(buf, got, sems, m, at):
        for copy in ring.scatter(buf, got, m, sems, at):
            copy.start()

    def sum_wait(buf, got, sems, m):
        for copy in ring.scatter(buf, got, m, sems):
            copy.wait()
        return ring.total(buf, got, m)

    out_set = (out_bf, out_got, (rs_s, rs_r))
    in_set = (in_bf, in_got, (rb_s, rb_r))

    def attention_masks(q):
        low = low_half(length)
        lane = lax.broadcasted_iota(jnp.int32, (length, LANES), 1)
        tables = (rope[q, 0], rope[q, 1], lax.rem(lane, HEAD_DIM) < ROT_DIM // 2)
        return low, lane, tables, allowed_of(q)

    factor = HEAD_DIM ** (-0.5)

    def forward_stage(m, who, k, fresh):
        q = who * micro + m
        place = jnp.where(who == 0, m, micro)

        @pl.when(who == 0)
        def _():
            @pl.when(first | (m < last))
            def _():
                spread_wait(xg, m, ag_s, ag_r)

            @pl.when(second & (m == last))
            def _():
                hop_out(last).wait_recv()
                cast_wait(xg, ag_r)

            c_start(0, m, 0)

            @pl.when(second)
            def _():
                mirror_copy(0, m).start()

        @pl.when(who == 1)
        def _():
            mirror_copy(0, m).wait_recv()
            c_start(0, m, 1)

            @pl.when(m == 1)
            def _():
                x_sent(0, 0, 1)
                x_sent(1, 0, 1)

        @pl.when(fresh)
        def _():
            for mask in order:
                w_ready(0, mask)
            w_far(3)

        low, lane, tables, allowed = attention_masks(q)
        for part in range(3):
            def qkv_tile(n, part=part):
                at = cols(n, WIDE)
                acc = jnp.dot(xg[q], wq[part, :, at], preferred_element_type=F32)
                acc = acc + wide[3 + part:4 + part, pl.ds(
                    pl.multiple_of(t * own + n * WIDE, WIDE), WIDE)]
                if part < 2:
                    acc = jnp.concatenate(
                        [
                            twist(acc[:, c:c + LANES], tables, 1.0)
                            for c in range(0, WIDE, LANES)
                        ],
                        axis=1,
                    )
                qkv[q, part, :, at] = acc.astype(BF16)

            loop(own // WIDE, qkv_tile)

        def pair(p):
            at = cols(p, LANES)
            query, key, value = qkv[q, 0, :, at], qkv[q, 1, :, at], qkv[q, 2, :, at]
            outs = []
            for h in range(2):
                mask = low if h == 0 else ~low
                one = jnp.where(mask, query, jnp.zeros_like(query))
                s = lax.dot_general(one, key, COLS, preferred_element_type=F32)
                s = jnp.where(allowed, s * factor, -1e30)
                top = jnp.max(s, axis=-1, keepdims=True)
                e = jnp.exp(s - top)
                total = jnp.sum(e, axis=-1, keepdims=True)
                probs = (e / total).astype(BF16)
                outs.append(jnp.dot(probs, value, preferred_element_type=F32))
                lse[q] = jnp.where(lane == 2 * p + h, top + jnp.log(total), lse[q])
            att[place, :, at] = jnp.where(low, outs[0], outs[1]).astype(BF16)

        lse[q] = jnp.zeros((length, LANES), F32)
        loop(own // LANES, pair)
        x_start(1, m, who)

        @pl.when(first & (k == 1))
        def _():
            output_finish(0)
            relay(3, 0)
            relay(3, 1)

        @pl.when(k == 0)
        def _():
            w_ready(1, 0)
            w_ready(1, 1)

        @pl.when(fresh)
        def _():
            via_ready(1)

        @pl.when(second & (k == 0))
        def _():
            w_ready(1, 3)

        def up_tile(n):
            at = cols(n, WIDE)
            u = jnp.dot(xg[q], w1[:, at], preferred_element_type=F32) + fb[0:1, at]
            c = 0.7978845608028654
            square = u * u
            th = jnp.tanh(c * u * (1.0 + 0.044715 * square))
            act[place, :, at] = (0.5 * u * (1.0 + th)).astype(BF16)
            slope = 0.5 * (1.0 + th)
            slope = slope + 0.5 * u * (1.0 - th * th) * (c * (1.0 + 3 * 0.044715 * square))
            gp[q, :, at] = slope.astype(BF16)

        loop(hidden // WIDE, up_tile)
        x_start(0, m, who)

    def differ(a, b):
        return a + b - 2 * a * b

    def output_stage(m, lo, hi, fresh, now):
        def block(j):
            if fresh is not None:
                for mask in masks_of(nf):
                    @pl.when(fresh & (j == mask))
                    def _(mask=mask):
                        w_ready(2, mask)
                        w_ready(3, mask)
                        if mask == 2:
                            pl.semaphore_signal(
                                go_sem, inc=1, device_id=other, device_id_type=MESH
                            )

            owner = 2 * differ(f // 2, j // 2) + differ(lax.rem(f, 2), lax.rem(j, 2))

            def out_tile(n):
                at = pl.ds(pl.multiple_of(owner * depth + n * WIDE, WIDE), WIDE)
                acc = lax.dot_general(att[m], wo[at, :], COLS, preferred_element_type=F32)
                acc = acc + lax.dot_general(act[m], w2[at, :], COLS, preferred_element_type=F32)
                out_bf[m, :, at] = acc.astype(BF16)
                if now is True:
                    sum_start(*out_set, m, at)
                else:
                    pl.when(now)(lambda: sum_start(*out_set, m, at))

            loop(depth // WIDE, out_tile)

        def step(j, carry):
            block(j)
            return carry

        lax.fori_loop(lo, hi, step, 0)

    def output_rest(m):
        half = width // 2
        start = pl.multiple_of((1 - f // 2) * half, half)
        sum_start(*out_set, m, pl.ds(start, half))

    def store_ends(m):
        return pltpu.make_async_copy(y_f.at[m], ends_o.at[m], o_sem.at[m])

    def output_finish(m):
        total = sum_wait(*out_set, m)
        y = rin[m].astype(F32) + total + wide[2:3, :]

        @pl.when(first)
        def _():
            y_b[m] = y.astype(BF16)
            hop_out(m).start()

        @pl.when(first & (m == last))
        def _():
            wide_copy().wait_recv()
            unit, _ = stats(y_b[m].astype(F32))
            nb[...] = (unit * wide_b[0:1, :] + wide_b[1:2, :]).astype(BF16)
            for copy in cast_rows():
                copy.start()

        @pl.when(second)
        def _():
            y_f[m] = y
            store_ends(m).start()

    def backward_stage(m, who, k):
        q = who * micro + m
        place = jnp.where(who == 0, m, micro)

        @pl.when(first & (who == 0))
        def _():
            @pl.when(m < last)
            def _():
                spread_wait(gr, m, gg_s, gg_r)

            @pl.when(m == last)
            def _():
                cast_wait(gr, gg_r)
                dyr[m] = gr[m, ring.block(t)]

            mirror_copy(1, m).start()
            c_start(1, m, 0)

        @pl.when(who == 1)
        def _():
            mirror_copy(1, m).wait_recv()
            c_start(1, m, 1)

            @pl.when(second & (m == 1))
            def _():
                x_sent(2, 0, 1)
                x_sent(3, 0, 1)

        def att_tile(n):
            at = cols(n, WIDE)
            gatt[:, at] = jnp.dot(gr[q], wo[:, at], preferred_element_type=F32).astype(BF16)

        loop(own // WIDE, att_tile)
        low, lane, tables, allowed = attention_masks(q)

        def pair(p):
            at = cols(p, LANES)
            query, key, value = qkv[q, 0, :, at], qkv[q, 1, :, at], qkv[q, 2, :, at]
            grad = gatt[:, at]
            dqs, dks, dvs = [], [], []
            for h in range(2):
                mask = low if h == 0 else ~low
                one = jnp.where(mask, query, jnp.zeros_like(query))
                s = lax.dot_general(one, key, COLS, preferred_element_type=F32)
                s = jnp.where(allowed, s * factor, -1e30)
                log_total = jnp.sum(
                    jnp.where(lane == 2 * p + h, lse[q], 0.0), axis=-1, keepdims=True
                )
                soft = jnp.exp(s - log_total)
                probs = soft.astype(BF16)
                one_grad = jnp.where(mask, grad, jnp.zeros_like(grad))
                dp = lax.dot_general(one_grad, value, COLS, preferred_element_type=F32)
                delta = jnp.sum(dp * soft, axis=-1, keepdims=True)
                ds = (soft * (dp - delta)).astype(BF16)
                dvs.append(lax.dot_general(probs, grad, ROWS, preferred_element_type=F32))
                dqs.append(jnp.dot(ds, key, preferred_element_type=F32))
                dks.append(lax.dot_general(ds, query, ROWS, preferred_element_type=F32))
            dq = jnp.where(low, dqs[0], dqs[1]) * factor
            dk = jnp.where(low, dks[0], dks[1]) * factor
            dj[place, 0, :, at] = twist(dq, tables, -1.0).astype(BF16)
            dj[place, 1, :, at] = twist(dk, tables, -1.0).astype(BF16)
            dj[place, 2, :, at] = jnp.where(low, dvs[0], dvs[1]).astype(BF16)

        loop(own // LANES, pair)
        x_start(3, m, who)

        @pl.when(who == 0)
        def _():
            for part in range(3):
                head_sums[part:part + 1, :] += jnp.sum(
                    dj[m, part].astype(F32), axis=0, keepdims=True
                )

        @pl.when(second & (k == 1))
        def _():
            w_ready(3, 0)
            w_ready(3, 1)
            output_stage(0, 0, 2, None, True)
            via_ready(3)

        def up_tile(n):
            at = cols(n, WIDE)
            acc = jnp.dot(gr[q], w2[:, at], preferred_element_type=F32)
            rounded = (acc * gp[q, :, at].astype(F32)).astype(BF16)
            up[place, :, at] = rounded
            sums = jnp.sum(rounded.astype(F32), axis=0, keepdims=True)
            up_sums[0:1, at] += jnp.where(who == 0, sums, 0.0)

        loop(hidden // WIDE, up_tile)
        x_start(2, m, who)

        def norm_tile(n):
            at = cols(n, WIDE)
            acc = lax.dot_general(up[m], w1[at, :], COLS, preferred_element_type=F32)
            for part in range(3):
                acc = acc + lax.dot_general(
                    dj[m, part], wq[part, at, :], COLS, preferred_element_type=F32
                )
            in_bf[m, :, at] = acc.astype(BF16)
            sum_start(*in_set, m, at)

        @pl.when(who == 0)
        def _():
            loop(width // WIDE, norm_tile)


    def backward_finish(m):
        grad_norm = sum_wait(*in_set, m)
        unit, inv_root = stats(rin[m].astype(F32))
        scaled = grad_norm * wide[0:1, :]
        upstream = dyr[m].astype(F32)
        dx = upstream + inv_root * (
            scaled
            - jnp.mean(scaled, axis=-1, keepdims=True)
            - unit * jnp.mean(scaled * unit, axis=-1, keepdims=True)
        )

        @pl.when(second)
        def _():
            y_b[m] = dx.astype(BF16)

        @pl.when(second & (m < last))
        def _():
            hop_back(m).start()

        @pl.when(second & (m == last))
        def _():
            for copy in cast_back():
                copy.start()

        @pl.when(first)
        def _():
            y_f[m] = dx
            store_ends(m).start()

        for i, term in enumerate((grad_norm * unit, grad_norm, upstream)):
            own_sums[i:i + 1, :] += jnp.sum(term, axis=0, keepdims=True)

    def strip(slot):
        return xg.at[:, :, pl.ds(pl.multiple_of(slot * own, own), own)]

    def strip_copy(src, slot):
        return pltpu.make_async_copy(src, strip(slot), dl_sem.at[slot])

    wide_strips = hidden // own
    kinds = 2 * wide_strips

    def strip_start(i, m):
        slot = lax.rem(i, STRIPS)

        @pl.when(i < wide_strips)
        def _():
            strip_copy(act_x.at[m, :, :, cols(i, own)], slot).start()

        @pl.when((i >= wide_strips) & (i < kinds))
        def _():
            strip_copy(up_x.at[m, :, :, cols(i - wide_strips, own)], slot).start()

        @pl.when(i == kinds)
        def _():
            strip_copy(att_x.at[m], slot).start()

        @pl.when(i > kinds)
        def _():
            strip_copy(dj_x.at[m, i - kinds - 1], slot).start()

    half = depth // 2

    def result_copy(dst, h):
        return pltpu.make_async_copy(att.at[h], dst, ds_sem.at[h])

    def turn_rows(m):
        strip_copy(xc_x.at[m], 2).start()
        strip_copy(gc_x.at[m], 3).start()
        for which in range(2):
            strip_copy(xc_x.at[m], 2 + which).wait()
            for b in range(nf):
                for h in range(2):
                    block = xg[b, :, pl.ds((2 + which) * own + h * half, half)]
                    c = (h * nf + b) * length
                    act[which, :, c:c + length] = block.T

    def turned_copies():
        span = nf * length
        return [
            pltpu.make_async_copy(
                act.at[which, :, pl.ds(h * span, span)],
                turned_o.at[which, pl.ds(h * half, half), :],
                dl_sem.at[2 * which + h],
            )
            for which in range(2)
            for h in range(2)
        ]

    def weight_stage():
        m = 0
        for i in range(micro):
            for a in (0, 1):
                x_sent(a, i, 0)
            mirror_copy(0, i).wait_send()
            for who in range(2):
                mine, theirs = c_pair(0, i, who)
                mine.wait()
                theirs.wait()
        for a in (2, 3):
            x_sent(a, 0, 0)

        @pl.when(first)
        def _():
            for a in (2, 3):
                x_sent(a, 0, 1)

        for who in range(2):
            for a in range(4):
                x_send(a, 0, who).wait_recv()
            mine, theirs = c_pair(1, 0, who)
            mine.wait()
            theirs.wait()
        strip_start(0, m)
        strip_start(1, m)
        turn_rows(m)
        strip_start(2, m)
        strip_start(3, m)

        def step(i):
            slot = lax.rem(i, STRIPS)
            strip_copy(xc_x.at[m], slot).wait()
            use_dy = (i < wide_strips) | (i == kinds)
            right = xg[:, :, cols(slot, own)].reshape(nf * length, own)
            which = jnp.where(use_dy, 1, 0)
            span = nf * length
            left = jnp.concatenate([act[which, :, :span], act[which, :, span:]], axis=0)
            value = jnp.dot(left, right, preferred_element_type=F32)
            for h in range(2):
                rows = pl.ds(h * half, half)

                @pl.when(i > 0)
                def _(h=h):
                    result_copy(out_o.at[pl.ds(0, half), :], h).wait()

                att[h] = value[h * half:(h + 1) * half].astype(BF16)

                @pl.when(i < wide_strips)
                def _(h=h, rows=rows):
                    result_copy(fc2_o.at[rows, cols(i, own)], h).start()

                @pl.when((i >= wide_strips) & (i < kinds))
                def _(h=h, rows=rows):
                    result_copy(fc1_o.at[rows, cols(i - wide_strips, own)], h).start()

                @pl.when(i == kinds)
                def _(h=h, rows=rows):
                    result_copy(out_o.at[rows, :], h).start()

                @pl.when(i > kinds)
                def _(h=h, rows=rows):
                    result_copy(qkv_o.at[i - kinds - 1, rows, :], h).start()

            @pl.when(i + STRIPS < kinds + 4)
            def _():
                strip_start(i + STRIPS, m)

        loop(kinds + 4, step)
        for h in range(2):
            result_copy(out_o.at[pl.ds(0, half), :], h).wait()

    own_sums[...] = jnp.zeros_like(own_sums)
    head_sums[...] = jnp.zeros_like(head_sums)
    up_sums[...] = jnp.zeros_like(up_sums)

    @pl.when(first)
    def _():
        small_arrive()
        load_rows.wait()
        loop(micro, front)
        seg_copy.wait()
        loop(2 * micro, rope_of)

    @pl.when(second)
    def _():
        load_dy.wait()
        loop(micro, front_back)

    @pl.when(second)
    def _():
        for p in range(PIECES):
            relay(1, p)
        w_far(0)
        w_far(1)
        small_arrive()
        wide_copy().start()
        seg_copy.wait()
        loop(2 * micro, rope_of)
        for mask in order:
            w_ready(0, mask)
        w_far(2)
        for p in range(PIECES):
            leg_two(1, p).wait_send()
        pl.semaphore_wait(go_sem, 1)
        for p in range(PIECES - DIRECT):
            leg_one(3, p).start()

        def dy_in(m):
            spread_wait(gr, m, gg_s, gg_r)
            c_start(1, m, 0)

        loop(micro, dy_in)


    small = [
        send(s_src.at[to], s_got.at[k], sm_s.at[k], sm_r.at[k], peer) for k, to, peer in group
    ]

    def small_start():
        s_src[...] = jnp.zeros_like(s_src)
        for j in range(count):
            s_src[j, 0:3, :] = own_sums[0:3, j * LANES:(j + 1) * LANES]
        for j in range(nf):
            s_src[t * nf + j, 3:6, :] = head_sums[0:3, j * LANES:(j + 1) * LANES]
            for r in range(per_row):
                c = (j * per_row + r) * LANES
                s_src[t * nf + j, 6 + r:7 + r, :] = up_sums[0:1, c:c + LANES]
        for copy in small:
            copy.start()

    def slot(k):
        is_f = jnp.where(first, k < 4, (k < 8) & (lax.rem(k, 2) == 0))
        is_o = jnp.where(first, k < 2, (k == 1) | (k == 6))
        who = jnp.where(first, (k // 2) % 2 * (k < 4) + lax.rem(k, 2) * (k >= 4), k // 4)
        m = jnp.where(first, jnp.where(k < 4, lax.rem(k, 2), (k - 4) // 2), lax.rem(k // 2, 2))
        m_o = jnp.where(first, m, k // 6)
        fresh = first & (k == 0)

        @pl.when(second & (k == 0))
        def _():
            hop_out(0).wait_recv()
            front(0)
            w_ready(1, 2)
            for p in range(PIECES - DIRECT, PIECES):
                straight(p).start()

        @pl.when(second & (k == 1))
        def _():
            for i in range(micro):
                mirror_copy(1, i).start()
            for mask in order:
                w_ready(2, mask)

        @pl.when(first & (k == 3))
        def _():
            hop_back(0).wait_recv()
            front_back(0)

        @pl.when(is_f)
        def _():
            forward_stage(m, who, k, fresh)

        @pl.when(jnp.logical_not(is_f))
        def _():
            backward_stage(m, who, k)

        @pl.when(second & (k == 6))
        def _():
            for copy in cast_back():
                copy.wait_send()

        @pl.when(is_o)
        def _():
            held_back = second & (k == 1)
            output_stage(
                m_o, jnp.where(held_back, 2, 0), nf, fresh, jnp.logical_not(held_back)
            )


        @pl.when(second & (k == 2))
        def _():
            backward_finish(0)
            output_rest(0)

        @pl.when(first & (k == 1))
        def _():
            for p in range(2, PIECES - DIRECT):
                relay(3, p)
            for i in range(micro):
                mirror_copy(0, i).start()
            for p in range(PIECES - DIRECT):
                leg_two(3, p).wait_send()
            output_finish(1)

        @pl.when(second & (k == 4))
        def _():
            backward_finish(1)

        @pl.when(second & (k == 7))
        def _():
            small_start()

        @pl.when((first & (k == 6)) | (second & (k == 7)))
        def _():
            weight_stage()

        @pl.when(k == 7)
        def _():
            for who in range(2):
                mine, theirs = c_pair(1, last, who)
                mine.wait()
                theirs.wait()
            turn_rows(last)
            for copy in turned_copies():
                copy.start()

        @pl.when(first & (k == 7))
        def _():
            loop(micro, backward_finish)
            small_start()

        @pl.when(second & (k == 7))
        def _():
            loop(micro, output_finish)

    loop(8, slot)

    for a in (2, 3):
        x_sent(a, last, 0)
    for who in range(2):
        for a in range(4):
            if who == 1:
                x_sent(a, last, 1)
            x_send(a, last, who).wait_recv()

    @pl.when(second)
    def _():
        for m in range(last):
            hop_back(m).wait_send()
        wide_copy().wait_send()

    @pl.when(first)
    def _():
        for m in range(micro):
            hop_out(m).wait_send()
        for copy in cast_rows():
            copy.wait_send()

    total = s_src[me]
    for k, copy in enumerate(small):
        copy.wait()
        total = total + s_got[k + 1]
    sums_o[...] = total
    for copy in turned_copies():
        copy.wait()
    for m in range(micro):
        mirror_copy(1, m).wait_send()
    for m in range(micro):
        store_ends(m).wait()
    for a in range(4):
        w_send(a, 0, 0, 1).wait_send()
    for side, via in ((first, 1), (second, 3)):
        @pl.when(side)
        def _(via=via):
            for a in range(4):
                if a != via:
                    w_send(a, 0, 1, 2).wait_send()
                    w_send(a, 2, 0, 1).wait_send()
            for p in range(PIECES):
                if via == 3 and p >= PIECES - DIRECT:
                    straight(p).wait_send()
                else:
                    leg_one(via, p).wait_send()
                passed_on(via, 2, p).wait_send()


def fused(ends, smalls, segments, wq, wo, w1, w2, nf, nt):
    micro, per, width = ends.shape
    length = per * nt
    own, hidden = wo.shape[1], w1.shape[1]
    depth = width // nf
    count = nf * nt
    bits = nf.bit_length() - 1
    anywhere = pl.BlockSpec(memory_space=pl.ANY)
    inside = pl.BlockSpec(memory_space=pltpu.VMEM)
    dma = pltpu.SemaphoreType.DMA
    vm = pltpu.VMEM
    piece = (ROWS_OF_PACK, LANES)
    packs = 2 * micro
    some = micro + 1
    out_shape = [
        jax.ShapeDtypeStruct(ends.shape, F32),
        jax.ShapeDtypeStruct(piece, F32),
        jax.ShapeDtypeStruct((depth, hidden), BF16),
        jax.ShapeDtypeStruct((depth, hidden), BF16),
        jax.ShapeDtypeStruct((depth, own), BF16),
        jax.ShapeDtypeStruct((3, depth, own), BF16),
        jax.ShapeDtypeStruct((2, depth, nf * length), BF16),
        jax.ShapeDtypeStruct((micro, nf, length, hidden), BF16),
        jax.ShapeDtypeStruct((micro, nf, length, own), BF16),
        jax.ShapeDtypeStruct((micro, nf, length, hidden), BF16),
        jax.ShapeDtypeStruct((micro, 3, nf, length, own), BF16),
        jax.ShapeDtypeStruct((micro, nf, length, depth), BF16),
        jax.ShapeDtypeStruct((micro, nf, length, depth), BF16),
    ]
    scratch = [
        vm((3, width, own), BF16), vm((width, own), BF16),
        vm((width, hidden), BF16), vm((width, hidden), BF16),
        vm(piece, F32), vm((count,) + piece, F32),
        vm((ROWS_OF_PACK, width), F32), vm((8, hidden), F32),
        vm((2, 8, length), F32), vm((packs, 2, length, LANES), F32),
        vm(ends.shape, BF16), vm(ends.shape, BF16),
        vm((packs, length, width), BF16), vm((packs, 3, length, own), BF16),
        vm((packs, length, LANES), F32), vm((some, length, own), BF16),
        vm((packs, length, hidden), BF16), vm((some, length, hidden), BF16),
        vm((packs, length, width), BF16), vm((length, own), BF16),
        vm((some, length, hidden), BF16), vm((some, 3, length, own), BF16),
        vm((micro, length, width), BF16), vm((micro, nt - 1, per, width), BF16),
        vm((micro, length, width), BF16), vm((micro, nt - 1, per, width), BF16),
        vm(ends.shape, F32), vm(ends.shape, BF16),
        vm((8, width), F32), vm((8, own), F32), vm((8, hidden), F32),
        vm((count,) + piece, F32), vm((count,) + piece, F32),
        dma, dma((4,)), dma((4, nf, bits)), dma((4, nf)),
        dma((count,)), dma((count,)), dma((count,)), dma((count,)),
        dma((micro, nt)), dma((micro, nt)), dma((micro, nt)), dma((micro, nt)),
        dma((micro, nt)), dma((micro, nt)), dma((micro, nt)), dma((micro, nt)),
        dma((micro,)), dma((micro,)), dma((micro,)), dma((micro,)),
        dma((4, micro, 2)), dma((4, micro, 2)), dma((4, micro, 2)),
        dma((2, micro, 2)), dma((2, micro, 2)), dma((2, micro, 2)),
        dma((3, micro)), dma((3, micro)), dma((micro,)),
        dma((PIECES,)), dma((PIECES,)), dma((PIECES,)), dma((PIECES,)),
        dma((PIECES,)), dma((PIECES,)), pltpu.SemaphoreType.REGULAR,
        vm((per, width), BF16), vm((8, width), F32), dma((nt,)), dma((nt,)), dma((2,)),
        dma((STRIPS,)), dma((2,)),
    ]
    return pl.pallas_call(
        functools.partial(fused_kernel, nf, nt),
        out_shape=out_shape,
        in_specs=[anywhere] + [inside] * 7 + [anywhere] * 4,
        out_specs=[anywhere, inside] + [anywhere] * 11,
        scratch_shapes=scratch,
        compiler_params=pltpu.CompilerParams(
            collective_id=4, has_side_effects=True, vmem_limit_bytes=VMEM_LIMIT
        ),
        name="fused",
    )(ends, *smalls, segments, wq, wo, w1, w2)


def padded(flat):
    size = -(-flat.shape[-1] // (8 * LANES)) * (8 * LANES)
    room = [(0, 0)] * (flat.ndim - 1) + [(0, size - flat.shape[-1])]
    flat = jnp.pad(flat, room)
    return flat.reshape(flat.shape[:-1] + (size // LANES, LANES))


def split_shards(
    ends_in, segments, ln_gain, ln_bias, w_qkv, w_out, w_fc1, w_fc2,
    bias_qkv, bias_out, bias_fc1, bias_fc2,
):
    nf, nt = lax.axis_size("fsdp"), lax.axis_size("tp")
    count = nf * nt
    section, tp_index = lax.axis_index("section"), lax.axis_index("tp")
    is_first = section == 0
    piece = ln_gain.shape[1]
    hidden_piece = bias_fc1.shape[1]
    own, hidden = w_out.shape[2], w_fc1.shape[2]
    width = piece * count

    pack = jnp.concatenate(
        [ln_gain[0], ln_bias[0], bias_out[0], bias_fc2[0], bias_qkv[0].reshape(-1), bias_fc1[0]]
    ).astype(F32)
    used = pack.shape[0]
    smalls = gather_small(padded(pack), nf, nt).reshape(count, -1)[:, :used]
    wide = smalls[:, :7 * piece].reshape(count, 7, piece).transpose(1, 0, 2).reshape(7, width)
    vec = jnp.stack([wide[0], wide[1], wide[2] + wide[3]])
    vec = jnp.pad(vec, ((0, 5), (0, 0)))
    qb = lax.dynamic_slice_in_dim(wide[4:7], tp_index * own, own, 1)
    qb = jnp.pad(qb, ((0, 5), (0, 0)))
    fb = lax.dynamic_slice_in_dim(smalls[:, 7 * piece:], tp_index * nf, nf, 0).reshape(1, hidden)
    fb = jnp.pad(fb, ((0, 7), (0, 0)))
    rope = rope_tables(segments)
    segc, segr = segments[:, :, None], segments[:, None, :]

    wq = lax.all_gather(w_qkv[0].transpose(1, 0, 2), "fsdp", axis=1, tiled=True)
    w1 = lax.all_gather(w_fc1[0], "fsdp", axis=0, tiled=True)
    wo = lax.all_gather(w_out[0], "fsdp", axis=0, tiled=True)
    w2 = lax.all_gather(w_fc2[0], "fsdp", axis=0, tiled=True)
    weights = (wq, wo, w1, w2)
    rows, xg, qkv, lse, att, gp, act, y = forward(
        ends_in[0], weights, vec, qb, fb, rope, segc, segr, nt
    )
    gr, up, dj, dx, own_sums, head_sums, up_sums = backward(
        ends_in[0], weights, rows, qkv, lse, gp, vec, rope, segc, segr, nt
    )

    def everywhere(arr):
        return lax.all_gather(arr, "fsdp", axis=arr.ndim - 2, tiled=True)

    def columns(arr):
        return lax.all_to_all(arr, "fsdp", split_axis=2, concat_axis=1, tiled=True)

    xc, gc = columns(xg), columns(gr)

    def product(left, right):
        return lax.dot_general(
            left, right, (((0, 1), (0, 1)), ((), ())), preferred_element_type=F32
        )

    act_all, att_all, up_all, dj_all = (everywhere(a) for a in (act, att, up, dj))
    grad_fc2 = product(gc, act_all)
    grad_out = product(gc, att_all)
    grad_fc1 = product(xc, up_all)
    grad_qkv = jnp.stack([product(xc, dj_all[:, part]) for part in range(3)], axis=1)

    mine = own_sums[:3].reshape(3, count, piece).transpose(1, 0, 2).reshape(count, 3 * piece)
    head = lax.dynamic_update_slice_in_dim(
        jnp.zeros((3, width), F32), head_sums[:3], tp_index * own, 1
    )
    head = head.reshape(3, count, piece).transpose(1, 0, 2).reshape(count, 3 * piece)
    ups = lax.dynamic_update_slice_in_dim(
        jnp.zeros((count, hidden_piece), F32),
        up_sums[0].reshape(nf, hidden_piece),
        tp_index * nf,
        0,
    )
    sums = sum_small(padded(jnp.concatenate([mine, head, ups], axis=1)), nf, nt).reshape(-1)
    gain_grad, bias_grad, row_grad = (sums[i * piece:(i + 1) * piece] for i in range(3))
    qkv_bias_grad = sums[3 * piece:6 * piece].reshape(3, piece)
    fc1_bias_grad = sums[6 * piece:6 * piece + hidden_piece]
    ends_out = jnp.where(is_first, dx, y)[None]
    return (
        ends_out,
        gain_grad[None],
        bias_grad[None],
        grad_qkv[None],
        grad_out[None],
        grad_fc1[None],
        grad_fc2[None],
        qkv_bias_grad[None],
        row_grad[None],
        fc1_bias_grad[None],
        row_grad[None],
    )


def last_kernel(
    used, last,
    ends, sums, turned, fc2, fc1, out, qkv, act, up, att, dj,
    ends_o, gain_o, shift_o, row_o, row_b, qkv_b, fc1_b, fc2_o, fc1_o, out_o, qkv_o,
    ends_v, turned_v, early_v, right_v, done_v, e_sem, t_sem, p_sem, r_sem, d_sem,
):
    strips, _, own = early_v.shape
    wide = (strips - 4) // 2
    copy = pltpu.make_async_copy

    def part(ref, i):
        return ref.at[:, pl.ds(i * own, own)]

    table = []
    for i in range(wide):
        right = act.at[last, :, :, pl.ds(i * own, own)]
        table.append((1, part(fc2, i), right, part(fc2_o, i)))
    for i in range(wide):
        right = up.at[last, :, :, pl.ds(i * own, own)]
        table.append((0, part(fc1, i), right, part(fc1_o, i)))
    table.append((1, out, att.at[last], out_o))
    for i in range(3):
        table.append((0, qkv.at[i], dj.at[last, i], qkv_o.at[i]))
    for which in (1, 0):
        copy(turned.at[which], turned_v.at[which], t_sem.at[which]).start()
    loads = []
    for i, (_, early, right, _) in enumerate(table):
        loads.append((
            copy(right, right_v.at[i], r_sem.at[i]), copy(early, early_v.at[i], p_sem.at[i])
        ))
        for one in loads[-1]:
            one.start()
    ends_in = copy(ends, ends_v, e_sem.at[0])
    ends_in.start()
    gain_o[...] = sums[0:1, :]
    shift_o[...] = sums[1:2, :]
    row_o[...] = sums[2:3, :]
    row_b[...] = sums[2:3, :]
    for r in range(3):
        qkv_b[r] = sums[3 + r:4 + r, :]
    for r in range(6, used):
        fc1_b[:, (r - 6) * LANES:(r - 5) * LANES] = sums[r:r + 1, :]
    ready = set()
    stores = []
    for i, (which, _, _, target) in enumerate(table):
        if which not in ready:
            copy(turned.at[which], turned_v.at[which], t_sem.at[which]).wait()
            ready.add(which)
        for one in loads[i]:
            one.wait()
        right = right_v[i].reshape(-1, own)
        done_v[i] = early_v[i].astype(F32) + jnp.dot(
            turned_v[which], right, preferred_element_type=F32
        )
        stores.append(copy(done_v.at[i], target, d_sem.at[i]))
        stores[-1].start()
        if i == 0:
            ends_in.wait()
            stores.append(copy(ends_v, ends_o, e_sem.at[1]))
            stores[-1].start()
    for one in stores:
        one.wait()


def last_products(used, ends, sums, turned, fc2, fc1, out, qkv, act, up, att, dj):
    depth, hidden = fc2.shape
    own = out.shape[1]
    micro, nf, length = act.shape[:3]
    strips = 2 * (hidden // own) + 4
    anywhere = pl.BlockSpec(memory_space=pl.ANY)
    inside = pl.BlockSpec(memory_space=pltpu.VMEM)
    small = jax.ShapeDtypeStruct((1, LANES), F32)
    dma = pltpu.SemaphoreType.DMA
    return pl.pallas_call(
        functools.partial(last_kernel, used, micro - 1),
        out_shape=[
            jax.ShapeDtypeStruct(ends.shape, F32), small, small, small, small,
            jax.ShapeDtypeStruct((3, 1, LANES), F32),
            jax.ShapeDtypeStruct((1, (used - 6) * LANES), F32),
            jax.ShapeDtypeStruct(fc2.shape, F32), jax.ShapeDtypeStruct(fc1.shape, F32),
            jax.ShapeDtypeStruct(out.shape, F32), jax.ShapeDtypeStruct(qkv.shape, F32),
        ],
        in_specs=[anywhere, inside] + [anywhere] * 9,
        out_specs=[anywhere] + [inside] * 6 + [anywhere] * 4,
        scratch_shapes=[
            pltpu.VMEM(ends.shape, F32), pltpu.VMEM(turned.shape, BF16),
            pltpu.VMEM((strips, depth, own), BF16),
            pltpu.VMEM((strips, nf, length, own), BF16),
            pltpu.VMEM((strips, depth, own), F32),
            dma((2,)), dma((2,)), dma((strips,)), dma((strips,)), dma((strips,)),
        ],
        compiler_params=pltpu.CompilerParams(vmem_limit_bytes=VMEM_LIMIT),
        name="last_products",
    )(ends, sums, turned, fc2, fc1, out, qkv, act, up, att, dj)


def fused_shards(
    ends_in, segments, ln_gain, ln_bias, w_qkv, w_out, w_fc1, w_fc2,
    bias_qkv, bias_out, bias_fc1, bias_fc2,
):
    nf, nt = lax.axis_size("fsdp"), lax.axis_size("tp")
    used = 6 + bias_fc1.shape[1] // LANES
    ends_out, sums, fc2, fc1, out, qkv, turned, act_x, att_x, up_x, dj_x, *_ = fused(
        ends_in[0],
        (ln_gain, ln_bias, bias_out, bias_fc2, bias_qkv[0], bias_fc1),
        segments, w_qkv[0].transpose(1, 0, 2), w_out[0], w_fc1[0], w_fc2[0], nf, nt,
    )

    ends_out, gain, shift, row, row_again, qkv_bias, fc1_bias, fc2, fc1, out, qkv = (
        last_products(
            used, ends_out, sums, turned, fc2, fc1, out, qkv, act_x, up_x, att_x, dj_x
        )
    )
    return (
        ends_out[None],
        gain,
        shift,
        qkv.transpose(1, 0, 2)[None],
        out[None],
        fc1[None],
        fc2[None],
        qkv_bias.transpose(1, 0, 2),
        row,
        fc1_bias,
        row_again,
    )


def shards(*args):
    rows, piece = args[0].shape[2], args[2].shape[1]
    small = rows * lax.axis_size("tp") <= 256
    tidy = piece == LANES and args[10].shape[1] // LANES <= ROWS_OF_PACK - 6
    square = lax.axis_size("fsdp") == 4 and args[0].shape[1] == 2
    return (fused_shards if small and tidy and square else split_shards)(*args)


def solution(mesh):
    both = P("section", ("fsdp", "tp"))
    square = P("section", "fsdp", "tp")
    tokens = P("section", None, ("fsdp", "tp"), None)
    heads = P("section", "fsdp", None, "tp")
    bias3 = P("section", None, ("fsdp", "tp"))
    return jax.shard_map(
        shards,
        mesh=mesh,
        in_specs=(
            tokens, P(None, "fsdp"), both, both, heads, square, square, square,
            bias3, both, both, both,
        ),
        out_specs=(
            tokens, both, both, heads, square, square, square, bias3, both, both, both,
        ),
        check_vma=False,
    )
```

```python
import functools

import jax
import jax.numpy as jnp
from jax import lax
from jax.experimental import pallas as pl
from jax.experimental.pallas import tpu as pltpu
from jax.sharding import PartitionSpec as P

HEAD_DIM = 64
ROT_DIM = 32
EPSILON = 1e-05
LANES = 128
TILE = 256
MESH = pl.DeviceIdType.MESH
F32 = jnp.float32
BF16 = jnp.bfloat16
COLS = (((1,), (1,)), ((), ()))
ROWS = (((0,), (0,)), ((), ()))
VMEM_LIMIT = 66_900_000


def positions_of(segment_ids):
    length = segment_ids.shape[-1]
    places = jnp.arange(length, dtype=jnp.int32)
    before = jnp.concatenate([segment_ids[..., :1] - 1, segment_ids[..., :-1]], axis=-1)
    starts = jnp.where(segment_ids != before, places, 0)
    starts = lax.cummax(starts, axis=segment_ids.ndim - 1)
    return places - starts


def rope_tables(segments):
    half = ROT_DIM // 2
    freq = jnp.exp(-jnp.log(10000.0) * (2.0 * jnp.arange(half, dtype=F32)) / ROT_DIM)
    angles = positions_of(segments).astype(F32)[..., None] * freq
    cosine, sine = jnp.cos(angles), jnp.sin(angles)
    none = jnp.zeros_like(sine)
    rest = jnp.zeros(angles.shape[:-1] + (HEAD_DIM - ROT_DIM,), F32)
    keep = jnp.concatenate([cosine, cosine, rest + 1.0], axis=-1)
    ahead = jnp.concatenate([-sine, none, rest], axis=-1)
    behind = jnp.concatenate([none, sine, rest], axis=-1)
    tables = jnp.stack([keep, ahead, behind], axis=1)
    return jnp.concatenate([tables, tables], axis=-1)


def send(src, dst, send_sem, recv_sem, device):
    return pltpu.make_async_remote_copy(
        src_ref=src,
        dst_ref=dst,
        send_sem=send_sem,
        recv_sem=recv_sem,
        device_id=device,
        device_id_type=MESH,
    )


def greet(peers):
    barrier = pltpu.get_barrier_semaphore()
    for peer in peers:
        pl.semaphore_signal(barrier, inc=1, device_id=peer, device_id_type=MESH)
    pl.semaphore_wait(barrier, len(peers))


def group_peers(nf, nt):
    me = lax.axis_index("fsdp") * nt + lax.axis_index("tp")
    found = []
    for k in range(1, nf * nt):
        to = lax.rem(me + k, nf * nt)
        found.append((k, to, {"fsdp": to // nt, "tp": lax.rem(to, nt)}))
    return me, found


def gather_small_kernel(nf, nt, own, out, send_sems, recv_sems, local_sem):
    me, peers = group_peers(nf, nt)
    greet([peer for _, _, peer in peers])
    mine = pltpu.make_async_copy(own, out.at[me], local_sem)
    mine.start()
    copies = []
    for k, _, peer in peers:
        copy = send(own, out.at[me], send_sems.at[k], recv_sems.at[k], peer)
        copy.start()
        copies.append(copy)
    mine.wait()
    for copy in copies:
        copy.wait()


def gather_small(own, nf, nt):
    count = nf * nt
    return pl.pallas_call(
        functools.partial(gather_small_kernel, nf, nt),
        out_shape=jax.ShapeDtypeStruct((count,) + own.shape, own.dtype),
        in_specs=[pl.BlockSpec(memory_space=pltpu.VMEM)],
        out_specs=pl.BlockSpec(memory_space=pltpu.VMEM),
        scratch_shapes=[
            pltpu.SemaphoreType.DMA((count,)),
            pltpu.SemaphoreType.DMA((count,)),
            pltpu.SemaphoreType.DMA,
        ],
        compiler_params=pltpu.CompilerParams(collective_id=0, has_side_effects=True),
        name="gather_small",
    )(own)


def sum_small_kernel(nf, nt, own, out, got, send_sems, recv_sems):
    me, peers = group_peers(nf, nt)
    greet([peer for _, _, peer in peers])
    copies = []
    for k, to, peer in peers:
        copy = send(own.at[to], got.at[k], send_sems.at[k], recv_sems.at[k], peer)
        copy.start()
        copies.append(copy)
    total = own[me]
    for k, copy in enumerate(copies):
        copy.wait()
        total = total + got[k + 1]
    out[...] = total


def sum_small(own, nf, nt):
    count = nf * nt
    return pl.pallas_call(
        functools.partial(sum_small_kernel, nf, nt),
        out_shape=jax.ShapeDtypeStruct(own.shape[1:], own.dtype),
        in_specs=[pl.BlockSpec(memory_space=pltpu.VMEM)],
        out_specs=pl.BlockSpec(memory_space=pltpu.VMEM),
        scratch_shapes=[
            pltpu.VMEM(own.shape, own.dtype),
            pltpu.SemaphoreType.DMA((count,)),
            pltpu.SemaphoreType.DMA((count,)),
        ],
        compiler_params=pltpu.CompilerParams(collective_id=1, has_side_effects=True),
        name="sum_small",
    )(own)


def cols(n, width=TILE):
    return pl.ds(pl.multiple_of(n * width, width), width)


def loop(count, body):
    def step(i, carry):
        body(i)
        return carry

    lax.fori_loop(0, count, step, 0)


def turn(x, tables, sign):
    keep, ahead, behind = tables
    left = pltpu.roll(x, LANES - ROT_DIM // 2, 1)
    right = pltpu.roll(x, ROT_DIM // 2, 1)
    return x * keep + sign * (left * ahead + right * behind)


def low_half(length):
    return lax.broadcasted_iota(jnp.int32, (length, LANES), 1) < HEAD_DIM


def allowed_mask(segc, segr, m, length):
    query = lax.broadcasted_iota(jnp.int32, (length, length), 0)
    key = lax.broadcasted_iota(jnp.int32, (length, length), 1)
    return (query >= key) & (segc[m] == segr[m])


class Ring:
    def __init__(self, nt, rows):
        self.nt, self.rows = nt, rows
        self.me = lax.axis_index("tp")
        self.others = [(k, lax.rem(self.me + k, nt)) for k in range(1, nt)]

    def block(self, who):
        return pl.ds(pl.multiple_of(who * self.rows, self.rows), self.rows)

    def gather(self, buf, m, sems):
        return [
            send(
                buf.at[m, self.block(self.me)],
                buf.at[m, self.block(self.me)],
                sems[0].at[m, k],
                sems[1].at[m, k],
                {"tp": to},
            )
            for k, to in self.others
        ]

    def scatter(self, buf, got, m, sems, part=None):
        at = slice(None) if part is None else part
        return [
            send(
                buf.at[m, self.block(to), at],
                got.at[m, k - 1, :, at],
                sems[0].at[m, k],
                sems[1].at[m, k],
                {"tp": to},
            )
            for k, to in self.others
        ]

    def total(self, buf, got, m):
        acc = buf[m, self.block(self.me)].astype(F32)
        for k, _ in self.others:
            acc = acc + got[m, k - 1].astype(F32)
        return acc


def stats(rows):
    mean = jnp.mean(rows, axis=-1, keepdims=True)
    centred = rows - mean
    variance = jnp.mean(centred * centred, axis=-1, keepdims=True)
    inv_root = lax.rsqrt(variance + EPSILON)
    return centred * inv_root, inv_root


def forward_kernel(
    nt,
    rows_h, wq_h, wo_h, w1_h, w2_h, vec, qb, fb, rope, segc, segr,
    rows_o, xg_o, qkv_o, lse_o, att_o, gp_o, act_o, y_o,
    wq, wo, w1, w2, rin, xg, qkv, lse, att, gp, act, branch, got, out_f, out_b,
    w_sem, in_sem, o_sem, ag_s, ag_r, rs_s, rs_r, x_s, x_r,
):
    micro, length, width = xg.shape
    section = lax.axis_index("section")
    first, second = section == 0, section == 1
    ring = Ring(nt, length // nt)
    own = wo.shape[1]
    loads = []
    for i, (src, dst) in enumerate(((wq_h, wq), (w1_h, w1), (wo_h, wo), (w2_h, w2))):
        loads.append(pltpu.make_async_copy(src, dst, w_sem.at[i]))
        loads[-1].start()
    mine = pltpu.make_async_copy(rows_h, rin, in_sem)

    @pl.when(first)
    def _():
        mine.start()

    greet([{"tp": to} for _, to in ring.others] + [{"section": 1 - section}])

    @pl.when(first)
    def _():
        mine.wait()

    def hop(m):
        return send(out_b.at[m], rin.at[m], x_s.at[m], x_r.at[m], {"section": 1 - section})

    def front(m):
        unit, _ = stats(rin[m].astype(F32))
        normed = unit * vec[0:1, :] + vec[1:2, :]
        xg[m, ring.block(ring.me)] = normed.astype(BF16)
        for copy in ring.gather(xg, m, (ag_s, ag_r)):
            copy.start()

    def arrive(m):
        @pl.when(second)
        def _():
            hop(m).wait_recv()
            front(m)

    stores = []

    def store(src, dst, m, i):
        copy = pltpu.make_async_copy(src.at[m], dst.at[m], o_sem.at[m, i])
        copy.start()
        stores.append(copy)

    def body(m):
        for copy in ring.gather(xg, m, (ag_s, ag_r)):
            copy.wait()
        store(xg, xg_o, m, 0)
        store(rin, rows_o, m, 1)
        tables = (rope[m, 0], rope[m, 1], rope[m, 2])
        if m == 0:
            loads[0].wait()
        per = own // TILE
        for part in range(3):
            def qkv_tile(n, part=part):
                at = cols(n)
                acc = jnp.dot(xg[m], wq[part, :, at], preferred_element_type=F32)
                acc = acc + qb[part:part + 1, at]
                if part < 2:
                    acc = jnp.concatenate(
                        [
                            turn(acc[:, c:c + LANES], tables, 1.0)
                            for c in range(0, TILE, LANES)
                        ],
                        axis=1,
                    )
                qkv[m, part, :, at] = acc.astype(BF16)

            loop(per, qkv_tile)
        store(qkv, qkv_o, m, 2)
        allowed = allowed_mask(segc, segr, m, length)
        low = low_half(length)
        lane = lax.broadcasted_iota(jnp.int32, (length, LANES), 1)

        def pair(p):
            at = cols(p, LANES)
            query, key, value = qkv[m, 0, :, at], qkv[m, 1, :, at], qkv[m, 2, :, at]
            outs = []
            for h in range(2):
                mask = low if h == 0 else ~low
                one = jnp.where(mask, query, jnp.zeros_like(query))
                s = lax.dot_general(one, key, COLS, preferred_element_type=F32)
                s = jnp.where(allowed, s * HEAD_DIM ** (-0.5), -1e30)
                top = jnp.max(s, axis=-1, keepdims=True)
                e = jnp.exp(s - top)
                total = jnp.sum(e, axis=-1, keepdims=True)
                probs = (e / total).astype(BF16)
                outs.append(jnp.dot(probs, value, preferred_element_type=F32))
                lse[m] = jnp.where(lane == 2 * p + h, top + jnp.log(total), lse[m])
            att[m, :, at] = jnp.where(low, outs[0], outs[1]).astype(BF16)

        lse[m] = jnp.zeros((length, LANES), F32)
        loop(own // LANES, pair)
        store(lse, lse_o, m, 3)
        store(att, att_o, m, 4)
        if m == 0:
            loads[1].wait()

        def up_tile(n):
            at = cols(n)
            u = jnp.dot(xg[m], w1[:, at], preferred_element_type=F32) + fb[0:1, at]
            c = 0.7978845608028654
            square = u * u
            t = jnp.tanh(c * u * (1.0 + 0.044715 * square))
            act[m, :, at] = (0.5 * u * (1.0 + t)).astype(BF16)
            slope = 0.5 * (1.0 + t) + 0.5 * u * (1.0 - t * t) * (c * (1.0 + 3 * 0.044715 * square))
            gp[m, :, at] = slope.astype(BF16)

        loop(act.shape[2] // TILE, up_tile)
        store(act, act_o, m, 5)
        store(gp, gp_o, m, 6)
        if m == 0:
            loads[2].wait()
            loads[3].wait()

        def out_tile(n):
            at = cols(n)
            acc = lax.dot_general(att[m], wo[at, :], COLS, preferred_element_type=F32)
            acc = acc + lax.dot_general(act[m], w2[at, :], COLS, preferred_element_type=F32)
            branch[m, :, at] = acc.astype(BF16)
            for copy in ring.scatter(branch, got, m, (rs_s, rs_r), at):
                copy.start()

        loop(width // TILE, out_tile)

    def finish(m):
        for copy in ring.scatter(branch, got, m, (rs_s, rs_r)):
            copy.wait()
        y = rin[m].astype(F32) + ring.total(branch, got, m) + vec[2:3, :]
        out_f[m] = y
        out_b[m] = y.astype(BF16)
        store(out_f, y_o, m, 7)

        @pl.when(first)
        def _():
            hop(m).start()

    @pl.when(first)
    def _():
        for m in range(micro):
            front(m)

    for m in range(micro):
        arrive(m)
        body(m)
    for m in range(micro):
        finish(m)
    for copy in stores:
        copy.wait()

    @pl.when(first)
    def _():
        for m in range(micro):
            hop(m).wait_send()


def forward(rows, weights, vec, qb, fb, rope, segc, segr, nt):
    wq, wo, w1, w2 = weights
    micro, per, width = rows.shape
    length = per * nt
    own, hidden = wo.shape[1], w1.shape[1]
    anywhere = pl.BlockSpec(memory_space=pl.ANY)
    inside = pl.BlockSpec(memory_space=pltpu.VMEM)
    out_shape = [
        jax.ShapeDtypeStruct(rows.shape, BF16),
        jax.ShapeDtypeStruct((micro, length, width), BF16),
        jax.ShapeDtypeStruct((micro, 3, length, own), BF16),
        jax.ShapeDtypeStruct((micro, length, LANES), F32),
        jax.ShapeDtypeStruct((micro, length, own), BF16),
        jax.ShapeDtypeStruct((micro, length, hidden), BF16),
        jax.ShapeDtypeStruct((micro, length, hidden), BF16),
        jax.ShapeDtypeStruct(rows.shape, F32),
    ]
    dma = pltpu.SemaphoreType.DMA
    return pl.pallas_call(
        functools.partial(forward_kernel, nt),
        out_shape=out_shape,
        in_specs=[anywhere] * 5 + [inside] * 6,
        out_specs=[anywhere] * 8,
        scratch_shapes=[
            pltpu.VMEM(wq.shape, BF16),
            pltpu.VMEM(wo.shape, BF16),
            pltpu.VMEM(w1.shape, BF16),
            pltpu.VMEM(w2.shape, BF16),
            pltpu.VMEM(rows.shape, BF16),
            pltpu.VMEM((micro, length, width), BF16),
            pltpu.VMEM((micro, 3, length, own), BF16),
            pltpu.VMEM((micro, length, LANES), F32),
            pltpu.VMEM((micro, length, own), BF16),
            pltpu.VMEM((micro, length, hidden), BF16),
            pltpu.VMEM((micro, length, hidden), BF16),
            pltpu.VMEM((micro, length, width), BF16),
            pltpu.VMEM((micro, nt - 1, per, width), BF16),
            pltpu.VMEM(rows.shape, F32),
            pltpu.VMEM(rows.shape, BF16),
            dma((4,)),
            dma,
            dma((micro, 8)),
            dma((micro, nt)),
            dma((micro, nt)),
            dma((micro, nt)),
            dma((micro, nt)),
            dma((micro,)),
            dma((micro,)),
        ],
        compiler_params=pltpu.CompilerParams(
            collective_id=2, has_side_effects=True, vmem_limit_bytes=VMEM_LIMIT
        ),
        name="forward",
    )(rows, wq, wo, w1, w2, vec, qb, fb, rope, segc, segr)


def backward_kernel(
    nt,
    dy_h, wq_h, wo_h, w1_h, w2_h, rows_h, qkv_h, lse_h, gp_h, vec, rope, segc, segr,
    gr_o, up_o, dj_o, dx_o, own_sums, head_sums, up_sums,
    wq, wo, w1, w2, dyr, rin, qkv, lse, gp, gr, gatt, up, dj, branch, got, out_f, out_b,
    w_sem, in_sem, o_sem, ag_s, ag_r, rs_s, rs_r, x_s, x_r,
):
    micro, length, width = gr.shape
    section = lax.axis_index("section")
    first, second = section == 0, section == 1
    ring = Ring(nt, length // nt)
    own = wo.shape[1]
    mine = pltpu.make_async_copy(dy_h, dyr, in_sem.at[4])

    @pl.when(second)
    def _():
        mine.start()

    loads = []
    for i, (src, dst) in enumerate(((wo_h, wo), (w2_h, w2), (wq_h, wq), (w1_h, w1))):
        loads.append(pltpu.make_async_copy(src, dst, w_sem.at[i]))
    kept = []
    for i, (src, dst) in enumerate(((qkv_h, qkv), (lse_h, lse), (gp_h, gp), (rows_h, rin))):
        kept.append(pltpu.make_async_copy(src, dst, in_sem.at[i]))
    for copy in (loads[0], kept[0], kept[1], loads[1], kept[2], loads[2], loads[3], kept[3]):
        copy.start()
    greet([{"tp": to} for _, to in ring.others] + [{"section": 1 - section}])

    @pl.when(second)
    def _():
        mine.wait()

    def hop(m):
        return send(out_b.at[m], dyr.at[m], x_s.at[m], x_r.at[m], {"section": 1 - section})

    def front(m):
        gr[m, ring.block(ring.me)] = dyr[m]
        for copy in ring.gather(gr, m, (ag_s, ag_r)):
            copy.start()

    def arrive(m):
        @pl.when(first)
        def _():
            hop(m).wait_recv()
            front(m)

    stores = []

    def store(src, dst, m, i):
        copy = pltpu.make_async_copy(src.at[m], dst.at[m], o_sem.at[m, i])
        copy.start()
        stores.append(copy)

    def body(m):
        for copy in ring.gather(gr, m, (ag_s, ag_r)):
            copy.wait()
        store(gr, gr_o, m, 0)
        if m == 0:
            loads[0].wait()

        def att_tile(n):
            at = cols(n)
            gatt[:, at] = jnp.dot(gr[m], wo[:, at], preferred_element_type=F32).astype(BF16)

        loop(own // TILE, att_tile)
        if m == 0:
            kept[0].wait()
            kept[1].wait()
        tables = (rope[m, 0], rope[m, 1], rope[m, 2])
        allowed = allowed_mask(segc, segr, m, length)
        low = low_half(length)
        lane = lax.broadcasted_iota(jnp.int32, (length, LANES), 1)
        factor = HEAD_DIM ** (-0.5)

        def pair(p):
            at = cols(p, LANES)
            query, key, value = qkv[m, 0, :, at], qkv[m, 1, :, at], qkv[m, 2, :, at]
            grad = gatt[:, at]
            dqs, dks, dvs = [], [], []
            for h in range(2):
                mask = low if h == 0 else ~low
                one = jnp.where(mask, query, jnp.zeros_like(query))
                s = lax.dot_general(one, key, COLS, preferred_element_type=F32)
                s = jnp.where(allowed, s * factor, -1e30)
                log_total = jnp.sum(
                    jnp.where(lane == 2 * p + h, lse[m], 0.0), axis=-1, keepdims=True
                )
                soft = jnp.exp(s - log_total)
                probs = soft.astype(BF16)
                one_grad = jnp.where(mask, grad, jnp.zeros_like(grad))
                dp = lax.dot_general(one_grad, value, COLS, preferred_element_type=F32)
                delta = jnp.sum(dp * soft, axis=-1, keepdims=True)
                ds = (soft * (dp - delta)).astype(BF16)
                dvs.append(lax.dot_general(probs, grad, ROWS, preferred_element_type=F32))
                dqs.append(jnp.dot(ds, key, preferred_element_type=F32))
                dks.append(lax.dot_general(ds, query, ROWS, preferred_element_type=F32))
            dq = jnp.where(low, dqs[0], dqs[1]) * factor
            dk = jnp.where(low, dks[0], dks[1]) * factor
            dj[m, 0, :, at] = turn(dq, tables, -1.0).astype(BF16)
            dj[m, 1, :, at] = turn(dk, tables, -1.0).astype(BF16)
            dj[m, 2, :, at] = jnp.where(low, dvs[0], dvs[1]).astype(BF16)

        loop(own // LANES, pair)
        store(dj, dj_o, m, 1)
        for part in range(3):
            sums = jnp.sum(dj[m, part].astype(F32), axis=0, keepdims=True)
            if m == 0:
                head_sums[part:part + 1, :] = sums
            else:
                head_sums[part:part + 1, :] += sums
        if m == 0:
            loads[1].wait()
            kept[2].wait()

        def up_tile(n):
            at = cols(n)
            acc = jnp.dot(gr[m], w2[:, at], preferred_element_type=F32)
            rounded = (acc * gp[m, :, at].astype(F32)).astype(BF16)
            up[m, :, at] = rounded
            sums = jnp.sum(rounded.astype(F32), axis=0, keepdims=True)
            if m == 0:
                up_sums[0:1, at] = sums
            else:
                up_sums[0:1, at] += sums

        loop(up.shape[2] // TILE, up_tile)
        store(up, up_o, m, 2)
        if m == 0:
            loads[2].wait()
            loads[3].wait()

        def norm_tile(n):
            at = cols(n)
            acc = lax.dot_general(up[m], w1[at, :], COLS, preferred_element_type=F32)
            for part in range(3):
                acc = acc + lax.dot_general(
                    dj[m, part], wq[part, at, :], COLS, preferred_element_type=F32
                )
            branch[m, :, at] = acc.astype(BF16)
            for copy in ring.scatter(branch, got, m, (rs_s, rs_r), at):
                copy.start()

        loop(width // TILE, norm_tile)

    def finish(m):
        for copy in ring.scatter(branch, got, m, (rs_s, rs_r)):
            copy.wait()
        if m == 0:
            kept[3].wait()
        grad_norm = ring.total(branch, got, m)
        unit, inv_root = stats(rin[m].astype(F32))
        scaled = grad_norm * vec[0:1, :]
        upstream = dyr[m].astype(F32)
        dx = upstream + inv_root * (
            scaled
            - jnp.mean(scaled, axis=-1, keepdims=True)
            - unit * jnp.mean(scaled * unit, axis=-1, keepdims=True)
        )
        out_f[m] = dx
        out_b[m] = dx.astype(BF16)

        @pl.when(second)
        def _():
            hop(m).start()

        store(out_f, dx_o, m, 3)
        for i, term in enumerate((grad_norm * unit, grad_norm, upstream)):
            sums = jnp.sum(term, axis=0, keepdims=True)
            if m == 0:
                own_sums[i:i + 1, :] = sums
            else:
                own_sums[i:i + 1, :] += sums

    @pl.when(second)
    def _():
        for m in range(micro):
            front(m)

    for m in range(micro):
        arrive(m)
        body(m)
    for m in range(micro):
        finish(m)
    for copy in stores:
        copy.wait()

    @pl.when(second)
    def _():
        for m in range(micro):
            hop(m).wait_send()


def backward(dy, weights, rows, qkv, lse, gp, vec, rope, segc, segr, nt):
    wq, wo, w1, w2 = weights
    micro, per, width = rows.shape
    length = per * nt
    own, hidden = wo.shape[1], w1.shape[1]
    anywhere = pl.BlockSpec(memory_space=pl.ANY)
    inside = pl.BlockSpec(memory_space=pltpu.VMEM)
    out_shape = [
        jax.ShapeDtypeStruct((micro, length, width), BF16),
        jax.ShapeDtypeStruct((micro, length, hidden), BF16),
        jax.ShapeDtypeStruct((micro, 3, length, own), BF16),
        jax.ShapeDtypeStruct(rows.shape, F32),
        jax.ShapeDtypeStruct((8, width), F32),
        jax.ShapeDtypeStruct((8, own), F32),
        jax.ShapeDtypeStruct((8, hidden), F32),
    ]
    dma = pltpu.SemaphoreType.DMA
    return pl.pallas_call(
        functools.partial(backward_kernel, nt),
        out_shape=out_shape,
        in_specs=[anywhere] * 9 + [inside] * 4,
        out_specs=[anywhere] * 4 + [inside] * 3,
        scratch_shapes=[
            pltpu.VMEM(wq.shape, BF16),
            pltpu.VMEM(wo.shape, BF16),
            pltpu.VMEM(w1.shape, BF16),
            pltpu.VMEM(w2.shape, BF16),
            pltpu.VMEM(rows.shape, BF16),
            pltpu.VMEM(rows.shape, BF16),
            pltpu.VMEM(qkv.shape, BF16),
            pltpu.VMEM(lse.shape, F32),
            pltpu.VMEM(gp.shape, BF16),
            pltpu.VMEM((micro, length, width), BF16),
            pltpu.VMEM((length, own), BF16),
            pltpu.VMEM((micro, length, hidden), BF16),
            pltpu.VMEM((micro, 3, length, own), BF16),
            pltpu.VMEM((micro, length, width), BF16),
            pltpu.VMEM((micro, nt - 1, per, width), BF16),
            pltpu.VMEM(rows.shape, F32),
            pltpu.VMEM(rows.shape, BF16),
            dma((4,)),
            dma((5,)),
            dma((micro, 4)),
            dma((micro, nt)),
            dma((micro, nt)),
            dma((micro, nt)),
            dma((micro, nt)),
            dma((micro,)),
            dma((micro,)),
        ],
        compiler_params=pltpu.CompilerParams(
            collective_id=3, has_side_effects=True, vmem_limit_bytes=VMEM_LIMIT
        ),
        name="backward",
    )(dy, wq, wo, w1, w2, rows, qkv, lse, gp, vec, rope, segc, segr)


ROWS_OF_PACK = 16
PIECES = 8
DIRECT = 2
STRIPS = 4
WIDE = 512


def twist(x, tables, sign):
    keep, sine, ahead = tables
    left = pltpu.roll(x, LANES - ROT_DIM // 2, 1)
    right = pltpu.roll(x, ROT_DIM // 2, 1)
    return x * keep + jnp.where(ahead, left, right) * (sign * sine)


def masks_of(nf):
    return range(nf)


def bits_below(mask, nf):
    low = mask & -mask if mask else nf
    return [(i, 1 << i) for i in range(nf.bit_length() - 1) if (1 << i) < low]


def flipped(index, mask, nf):
    for i in range(nf.bit_length() - 1):
        if mask >> i & 1:
            index = index + (1 << i) * (1 - 2 * lax.rem(index // (1 << i), 2))
    return index


def fused_kernel(
    nf, nt,
    ends_h, gain, shift, b_out, b_fc2, b_qkv, b_fc1, seg_in, wq_h, wo_h, w1_h, w2_h,
    ends_o, sums_o, fc2_o, fc1_o, out_o, qkv_o, turned_o,
    act_x, att_x, up_x, dj_x, xc_x, gc_x,
    wq, wo, w1, w2, pack, packs, wide, fb, segs, rope, rin, dyr, xg, qkv, lse, att, gp, act,
    gr, gatt, up, dj, out_bf, out_got, in_bf, in_got, y_f, y_b,
    own_sums, head_sums, up_sums, s_src, s_got,
    in_sem, wl_sem, ws_sem, wr_sem, pk_s, pk_r, sm_s, sm_r,
    ag_s, ag_r, gg_s, gg_r, rs_s, rs_r, rb_s, rb_r, hx_s, hx_r, hb_s, hb_r,
    xl_sem, xs_s, xs_r, cl_sem, ca_s, ca_r, mx_s, mx_r, o_sem,
    mg_s, mg_r, l1_s, l1_r, l2_s, l2_r, fw_s, fw_r, go_sem, nb, wide_b, mf_s, mb_s, wb_sem,
    dl_sem, ds_sem,
):
    micro, per, width = rin.shape
    length = per * nt
    section, f, t = (lax.axis_index(a) for a in ("section", "fsdp", "tp"))
    first, second = section == 0, section == 1
    ring = Ring(nt, per)
    own, hidden = wo.shape[1], w1.shape[1]
    depth = width // nf
    mirror, sibling = {"fsdp": flipped(f, 2, nf)}, {"fsdp": flipped(f, 1, nf)}
    count = nf * nt
    other = {"section": 1 - section}
    across = {"section": 1 - section, "fsdp": flipped(f, 2, nf)}
    me, group = group_peers(nf, nt)
    fblock = [flipped(f, mask, nf) for mask in masks_of(nf)]

    def rows_at(block):
        return pl.ds(pl.multiple_of(block * depth, depth), depth)

    load_rows = pltpu.make_async_copy(ends_h, rin, in_sem)
    load_dy = pltpu.make_async_copy(ends_h, dyr, in_sem)

    @pl.when(first)
    def _():
        load_rows.start()

    @pl.when(second)
    def _():
        load_dy.start()

    greet(
        [peer for _, _, peer in group]
        + [across, other]
        + [{"section": 1 - section, "tp": to} for _, to in ring.others]
    )

    per_row = hidden // nf // LANES
    segs[0] = jnp.zeros((8, length), F32)
    segs[0, 0:micro, :] = seg_in[...].astype(F32)
    pack[...] = jnp.zeros_like(pack)
    pack[0:1, :] = gain[...].astype(F32)
    pack[1:2, :] = shift[...].astype(F32)
    pack[2:3, :] = b_out[...].astype(F32) + b_fc2[...].astype(F32)
    pack[3:6, :] = b_qkv[...].astype(F32)
    for r in range(per_row):
        pack[6 + r:7 + r, :] = b_fc1[:, r * LANES:(r + 1) * LANES].astype(F32)
    seg_copy = send(segs.at[0], segs.at[1], mx_s.at[2, 0], mx_r.at[2, 0], mirror)
    pack_local = pltpu.make_async_copy(pack, packs.at[me], pk_s.at[0])
    pack_copies = [
        send(pack, packs.at[me], pk_s.at[k], pk_r.at[k], peer) for k, _, peer in group
    ]
    pack_local.start()
    seg_copy.start()
    for copy in pack_copies:
        copy.start()

    table = ((wq_h, wq), (w1_h, w1), (wo_h, wo), (w2_h, w2))

    def w_at(ref, block):
        return ref.at[:, rows_at(block), :] if len(ref.shape) == 3 else ref.at[rows_at(block), :]

    def w_local(a):
        return pltpu.make_async_copy(table[a][0], w_at(table[a][1], f), wl_sem.at[a])

    def w_send(a, mask, i, bit):
        block = w_at(table[a][1], fblock[mask])
        src = table[a][0] if mask == 0 else block
        peer = {"fsdp": flipped(f, bit, nf)}
        return send(src, block, ws_sem.at[a, mask, i], wr_sem.at[a, mask | bit], peer)

    def w_recv(a, mask):
        block = w_at(table[a][1], fblock[mask])
        return send(block, block, ws_sem.at[a, mask, 0], wr_sem.at[a, mask], other)

    def w_near(a):
        w_local(a).start()
        w_send(a, 0, 0, 1).start()

    def w_far(a):
        w_send(a, 0, 1, 2).start()

    part_rows = depth // PIECES
    per_slot = length // part_rows

    def stage(p):
        return up.at[p // per_slot, pl.ds(p % per_slot * part_rows, part_rows), :]

    def piece_at(a, mask, p):
        start = pl.multiple_of(fblock[mask] * depth + p * part_rows, part_rows)
        return table[a][1].at[pl.ds(start, part_rows), :]

    def leg_one(a, p):
        src = table[a][0].at[pl.ds(p * part_rows, part_rows), :]
        return send(src, stage(p), l1_s.at[p], l1_r.at[p], across)

    def leg_two(a, p):
        return send(stage(p), piece_at(a, 2, p), l2_s.at[p], l2_r.at[p], other)

    def passed_on(a, mask, p):
        block = piece_at(a, mask, p)
        return send(block, block, fw_s.at[p], fw_r.at[p], sibling)

    def straight(p):
        src = table[3][0].at[pl.ds(p * part_rows, part_rows), :]
        return send(src, piece_at(3, 0, p), l1_s.at[p], l2_r.at[p], mirror)

    def relay(a, p):
        leg_one(a, p).wait_recv()
        leg_two(a, p).start()

    def via_ready(a):
        for p in range(PIECES):
            leg_two(a, p).wait_recv()
            passed_on(a, 2, p).start()
        for p in range(PIECES):
            passed_on(a, 3, p).wait_recv()

    def w_ready(a, mask):
        if mask == 0:
            w_local(a).wait()
            return
        w_recv(a, mask).wait_recv()
        for i, bit in bits_below(mask, nf):
            w_send(a, mask, i, bit).start()

    order = sorted(masks_of(nf), key=lambda m: (m != 0, -(m & -m), m))
    out_order = list(masks_of(nf))
    for a in range(4):
        w_near(a)

    @pl.when(first)
    def _():
        w_far(0)
        w_far(2)
        for p in range(PIECES):
            leg_one(1, p).start()

    def small_arrive():
        pack_local.wait()
        for copy in pack_copies:
            copy.wait()
        for j in range(count):
            wide[:, j * LANES:(j + 1) * LANES] = packs[j]
        for j in range(nf):
            for r in range(per_row):
                c = (j * per_row + r) * LANES
                fb[0:1, c:c + LANES] = packs[t * nf + j, 6 + r:7 + r, :]

    def segment_parts(q):
        row = segs[q // micro, pl.ds(lax.rem(q, micro), 1), :]
        query = lax.broadcasted_iota(jnp.int32, (length, length), 0)
        key = lax.broadcasted_iota(jnp.int32, (length, length), 1)
        column = jnp.sum(jnp.where(query == key, row, 0.0), axis=1, keepdims=True)
        return row, column, query >= key

    def allowed_of(q):
        row, column, causal = segment_parts(q)
        return causal & (row == column)

    def rope_of(q):
        row, column, _ = segment_parts(q)
        before = jnp.sum(jnp.where(row < column, 1.0, 0.0), axis=1, keepdims=True)
        lane = lax.rem(lax.broadcasted_iota(jnp.int32, (length, LANES), 1), HEAD_DIM)
        place = lax.broadcasted_iota(jnp.int32, (length, LANES), 0).astype(F32) - before
        half = ROT_DIM // 2
        power = lax.rem(lane, half).astype(F32)
        freq = jnp.exp(-jnp.log(10000.0) * (2.0 * power) / ROT_DIM)
        angles = place * freq
        rope[q, 0] = jnp.where(lane < ROT_DIM, jnp.cos(angles), 1.0)
        sine = jnp.where(lane < ROT_DIM, jnp.sin(angles), 0.0)
        rope[q, 1] = jnp.where(lane < half, -sine, sine)

    def hop_out(m):
        return send(y_b.at[m], rin.at[m], hx_s.at[m], hx_r.at[m], other)

    def hop_back(m):
        return send(y_b.at[m], dyr.at[m], hb_s.at[m], hb_r.at[m], other)

    def spread(buf, m, send_sems, recv_sems):
        here = ring.block(t)
        return [
            send(
                buf.at[m, here], buf.at[m, here], send_sems.at[m, k], recv_sems.at[m, t],
                {"tp": to},
            )
            for k, to in ring.others
        ]

    def block_wait(buf, m, recv_sems, who):
        at = ring.block(who)
        send(buf.at[m, at], buf.at[m, at], o_sem.at[m], recv_sems.at[m, who], other).wait_recv()

    def spread_start(buf, m, send_sems, recv_sems):
        for copy in spread(buf, m, send_sems, recv_sems):
            copy.start()

    def spread_wait(buf, m, send_sems, recv_sems):
        for _, who in ring.others:
            block_wait(buf, m, recv_sems, who)
        for copy in spread(buf, m, send_sems, recv_sems):
            copy.wait_send()

    last = micro - 1

    def cast(src, buf, send_sems, recv_sems):
        here = ring.block(t)
        return [
            send(
                src, buf.at[last, here], send_sems.at[k], recv_sems.at[last, t],
                {"section": 1 - section, "tp": to},
            )
            for k, to in [(0, t)] + ring.others
        ]

    def cast_wait(buf, recv_sems):
        for who in range(nt):
            block_wait(buf, last, recv_sems, who)

    def cast_rows():
        return cast(nb, xg, mf_s, ag_r)

    def cast_back():
        return cast(y_b.at[last], gr, mb_s, gg_r)

    def wide_copy():
        return send(wide.at[0:8], wide_b, wb_sem.at[0], wb_sem.at[1], other)

    def front(m):
        unit, _ = stats(rin[m].astype(F32))
        normed = unit * wide[0:1, :] + wide[1:2, :]
        xg[m, ring.block(ring.me)] = normed.astype(BF16)
        spread_start(xg, m, ag_s, ag_r)

    def front_back(m):
        gr[m, ring.block(ring.me)] = dyr[m]

        @pl.when(first)
        def _():
            mirror_rows(m, t).start()

        spread_start(gr, m, gg_s, gg_r)

    def mirror_copy(m):
        return send(xg.at[m], xg.at[micro + m], mx_s.at[0, m], mx_r.at[0, m], mirror)

    def mirror_rows(m, who):
        at = ring.block(who)
        return send(
            gr.at[m, at], gr.at[micro + m, at], mg_s.at[m, who], mg_r.at[m, who], mirror
        )

    def x_block(who):
        return fblock[2 * who] if isinstance(who, int) else jnp.where(who == 0, f, fblock[2])

    def x_dst(a, m, who):
        block = x_block(who)
        if a == 3:
            return dj_x.at[m, :, block]
        return (act_x, att_x, up_x)[a].at[m, block]

    def x_src(a, m, who):
        place = (m, micro)[who] if isinstance(who, int) else jnp.where(who == 0, m, micro)
        return (act, att, up, dj)[a].at[place]

    def x_local(a, m, who):
        return pltpu.make_async_copy(
            x_src(a, m, who), x_dst(a, m, who), xl_sem.at[a, m, who]
        )

    def x_send(a, m, who):
        return send(
            x_src(a, m, who), x_dst(a, m, who), xs_s.at[a, m, who], xs_r.at[a, m, who], sibling
        )

    def x_start(a, m, who):
        x_local(a, m, who).start()
        x_send(a, m, who).start()

    def x_sent(a, m, who):
        x_local(a, m, who).wait()
        x_send(a, m, who).wait_send()

    def c_pair(which, m, who):
        src, dst = ((xg, xc_x), (gr, gc_x))[which]
        block = x_block(who)
        q = who * micro + m
        mine = pltpu.make_async_copy(
            src.at[q, :, rows_at(f)], dst.at[m, block], cl_sem.at[which, m, who]
        )
        theirs = send(
            src.at[q, :, rows_at(fblock[1])],
            dst.at[m, block],
            ca_s.at[which, m, who],
            ca_r.at[which, m, who],
            sibling,
        )
        return mine, theirs

    def c_start(which, m, who):
        for copy in c_pair(which, m, who):
            copy.start()

    def sum_start(buf, got, sems, m, at):
        for copy in ring.scatter(buf, got, m, sems, at):
            copy.start()

    def sum_wait(buf, got, sems, m):
        for copy in ring.scatter(buf, got, m, sems):
            copy.wait()
        return ring.total(buf, got, m)

    out_set = (out_bf, out_got, (rs_s, rs_r))
    in_set = (in_bf, in_got, (rb_s, rb_r))

    def attention_masks(q):
        low = low_half(length)
        lane = lax.broadcasted_iota(jnp.int32, (length, LANES), 1)
        tables = (rope[q, 0], rope[q, 1], lax.rem(lane, HEAD_DIM) < ROT_DIM // 2)
        return low, lane, tables, allowed_of(q)

    factor = HEAD_DIM ** (-0.5)

    def forward_stage(m, who, k, fresh):
        q = who * micro + m
        place = jnp.where(who == 0, m, micro)

        @pl.when(who == 0)
        def _():
            @pl.when(first | (m < last))
            def _():
                spread_wait(xg, m, ag_s, ag_r)

            @pl.when(second & (m == last))
            def _():
                hop_out(last).wait_recv()
                cast_wait(xg, ag_r)

            c_start(0, m, 0)

            @pl.when(second)
            def _():
                mirror_copy(m).start()

        @pl.when(who == 1)
        def _():
            mirror_copy(m).wait_recv()
            c_start(0, m, 1)

            @pl.when(m == 1)
            def _():
                x_sent(0, 0, 1)
                x_sent(1, 0, 1)

        @pl.when(fresh)
        def _():
            for mask in order:
                w_ready(0, mask)
            w_far(3)

        low, lane, tables, allowed = attention_masks(q)
        for part in range(3):
            def qkv_tile(n, part=part):
                at = cols(n, WIDE)
                acc = jnp.dot(xg[q], wq[part, :, at], preferred_element_type=F32)
                acc = acc + wide[3 + part:4 + part, pl.ds(
                    pl.multiple_of(t * own + n * WIDE, WIDE), WIDE)]
                if part < 2:
                    acc = jnp.concatenate(
                        [
                            twist(acc[:, c:c + LANES], tables, 1.0)
                            for c in range(0, WIDE, LANES)
                        ],
                        axis=1,
                    )
                qkv[q, part, :, at] = acc.astype(BF16)

            loop(own // WIDE, qkv_tile)

        def pair(p):
            at = cols(p, LANES)
            query, key, value = qkv[q, 0, :, at], qkv[q, 1, :, at], qkv[q, 2, :, at]
            outs = []
            for h in range(2):
                mask = low if h == 0 else ~low
                one = jnp.where(mask, query, jnp.zeros_like(query))
                s = lax.dot_general(one, key, COLS, preferred_element_type=F32)
                s = jnp.where(allowed, s * factor, -1e30)
                top = jnp.max(s, axis=-1, keepdims=True)
                e = jnp.exp(s - top)
                total = jnp.sum(e, axis=-1, keepdims=True)
                probs = (e / total).astype(BF16)
                outs.append(jnp.dot(probs, value, preferred_element_type=F32))
                lse[q] = jnp.where(lane == 2 * p + h, top + jnp.log(total), lse[q])
            att[place, :, at] = jnp.where(low, outs[0], outs[1]).astype(BF16)

        lse[q] = jnp.zeros((length, LANES), F32)
        loop(own // LANES, pair)
        x_start(1, m, who)

        @pl.when(first & (k == 1))
        def _():
            output_finish(0)
            relay(3, 0)
            relay(3, 1)

        @pl.when(k == 0)
        def _():
            w_ready(1, 0)
            w_ready(1, 1)

        @pl.when(fresh)
        def _():
            via_ready(1)

        @pl.when(second & (k == 0))
        def _():
            w_ready(1, 3)

        def up_tile(n):
            at = cols(n, WIDE)
            u = jnp.dot(xg[q], w1[:, at], preferred_element_type=F32) + fb[0:1, at]
            c = 0.7978845608028654
            square = u * u
            th = jnp.tanh(c * u * (1.0 + 0.044715 * square))
            act[place, :, at] = (0.5 * u * (1.0 + th)).astype(BF16)
            slope = 0.5 * (1.0 + th)
            slope = slope + 0.5 * u * (1.0 - th * th) * (c * (1.0 + 3 * 0.044715 * square))
            gp[q, :, at] = slope.astype(BF16)

        loop(hidden // WIDE, up_tile)
        x_start(0, m, who)

    def differ(a, b):
        return a + b - 2 * a * b

    def output_stage(m, lo, hi, fresh, now):
        def block(j):
            if fresh is not None:
                for mask in masks_of(nf):
                    @pl.when(fresh & (j == mask))
                    def _(mask=mask):
                        w_ready(2, mask)
                        w_ready(3, mask)
                        if mask == 2:
                            pl.semaphore_signal(
                                go_sem, inc=1, device_id=other, device_id_type=MESH
                            )

            owner = 2 * differ(f // 2, j // 2) + differ(lax.rem(f, 2), lax.rem(j, 2))

            def out_tile(n):
                at = pl.ds(pl.multiple_of(owner * depth + n * WIDE, WIDE), WIDE)
                acc = lax.dot_general(att[m], wo[at, :], COLS, preferred_element_type=F32)
                acc = acc + lax.dot_general(act[m], w2[at, :], COLS, preferred_element_type=F32)
                out_bf[m, :, at] = acc.astype(BF16)
                if now is True:
                    sum_start(*out_set, m, at)
                else:
                    pl.when(now)(lambda: sum_start(*out_set, m, at))

            loop(depth // WIDE, out_tile)

        def step(j, carry):
            block(j)
            return carry

        lax.fori_loop(lo, hi, step, 0)

    def output_rest(m):
        half = width // 2
        start = pl.multiple_of((1 - f // 2) * half, half)
        sum_start(*out_set, m, pl.ds(start, half))

    def store_ends(m):
        return pltpu.make_async_copy(y_f.at[m], ends_o.at[m], o_sem.at[m])

    def output_finish(m):
        total = sum_wait(*out_set, m)
        y = rin[m].astype(F32) + total + wide[2:3, :]

        @pl.when(first)
        def _():
            y_b[m] = y.astype(BF16)
            hop_out(m).start()

        @pl.when(first & (m == last))
        def _():
            wide_copy().wait_recv()
            unit, _ = stats(y_b[m].astype(F32))
            nb[...] = (unit * wide_b[0:1, :] + wide_b[1:2, :]).astype(BF16)
            for copy in cast_rows():
                copy.start()

        @pl.when(second)
        def _():
            y_f[m] = y
            store_ends(m).start()

    def backward_stage(m, who, k):
        q = who * micro + m
        place = jnp.where(who == 0, m, micro)

        @pl.when(first & (who == 0))
        def _():
            @pl.when(m < last)
            def _():
                for _, who in ring.others:
                    block_wait(gr, m, gg_r, who)
                    mirror_rows(m, who).start()
                for copy in spread(gr, m, gg_s, gg_r):
                    copy.wait_send()

            @pl.when(m == last)
            def _():
                for who in range(nt):
                    block_wait(gr, last, gg_r, who)
                    mirror_rows(last, who).start()
                dyr[m] = gr[m, ring.block(t)]

            c_start(1, m, 0)

        @pl.when(who == 1)
        def _():
            for who in range(nt):
                mirror_rows(m, who).wait_recv()
            c_start(1, m, 1)

            @pl.when(second & (m == 1))
            def _():
                x_sent(2, 0, 1)
                x_sent(3, 0, 1)

        def att_tile(n):
            at = cols(n, WIDE)
            gatt[:, at] = jnp.dot(gr[q], wo[:, at], preferred_element_type=F32).astype(BF16)

        loop(own // WIDE, att_tile)
        low, lane, tables, allowed = attention_masks(q)

        def pair(p):
            at = cols(p, LANES)
            query, key, value = qkv[q, 0, :, at], qkv[q, 1, :, at], qkv[q, 2, :, at]
            grad = gatt[:, at]
            dqs, dks, dvs = [], [], []
            for h in range(2):
                mask = low if h == 0 else ~low
                one = jnp.where(mask, query, jnp.zeros_like(query))
                s = lax.dot_general(one, key, COLS, preferred_element_type=F32)
                s = jnp.where(allowed, s * factor, -1e30)
                log_total = jnp.sum(
                    jnp.where(lane == 2 * p + h, lse[q], 0.0), axis=-1, keepdims=True
                )
                soft = jnp.exp(s - log_total)
                probs = soft.astype(BF16)
                one_grad = jnp.where(mask, grad, jnp.zeros_like(grad))
                dp = lax.dot_general(one_grad, value, COLS, preferred_element_type=F32)
                delta = jnp.sum(dp * soft, axis=-1, keepdims=True)
                ds = (soft * (dp - delta)).astype(BF16)
                dvs.append(lax.dot_general(probs, grad, ROWS, preferred_element_type=F32))
                dqs.append(jnp.dot(ds, key, preferred_element_type=F32))
                dks.append(lax.dot_general(ds, query, ROWS, preferred_element_type=F32))
            dq = jnp.where(low, dqs[0], dqs[1]) * factor
            dk = jnp.where(low, dks[0], dks[1]) * factor
            dj[place, 0, :, at] = twist(dq, tables, -1.0).astype(BF16)
            dj[place, 1, :, at] = twist(dk, tables, -1.0).astype(BF16)
            dj[place, 2, :, at] = jnp.where(low, dvs[0], dvs[1]).astype(BF16)

        loop(own // LANES, pair)
        x_start(3, m, who)

        @pl.when(second & (k == 3))
        def _():
            backward_finish(0)

        @pl.when(who == 0)
        def _():
            for part in range(3):
                head_sums[part:part + 1, :] += jnp.sum(
                    dj[m, part].astype(F32), axis=0, keepdims=True
                )

        @pl.when(second & (k == 1))
        def _():
            w_ready(3, 0)
            w_ready(3, 1)
            output_stage(0, 0, 2, None, True)
            via_ready(3)

        def up_tile(n):
            at = cols(n, WIDE)
            acc = jnp.dot(gr[q], w2[:, at], preferred_element_type=F32)
            rounded = (acc * gp[q, :, at].astype(F32)).astype(BF16)
            up[place, :, at] = rounded
            sums = jnp.sum(rounded.astype(F32), axis=0, keepdims=True)
            up_sums[0:1, at] += jnp.where(who == 0, sums, 0.0)

        loop(hidden // WIDE, up_tile)
        x_start(2, m, who)

        def norm_tile(n):
            at = cols(n, WIDE)
            acc = lax.dot_general(up[m], w1[at, :], COLS, preferred_element_type=F32)
            for part in range(3):
                acc = acc + lax.dot_general(
                    dj[m, part], wq[part, at, :], COLS, preferred_element_type=F32
                )
            in_bf[m, :, at] = acc.astype(BF16)
            sum_start(*in_set, m, at)

        @pl.when(who == 0)
        def _():
            loop(width // WIDE, norm_tile)


    def backward_finish(m):
        grad_norm = sum_wait(*in_set, m)
        unit, inv_root = stats(rin[m].astype(F32))
        scaled = grad_norm * wide[0:1, :]
        upstream = dyr[m].astype(F32)
        dx = upstream + inv_root * (
            scaled
            - jnp.mean(scaled, axis=-1, keepdims=True)
            - unit * jnp.mean(scaled * unit, axis=-1, keepdims=True)
        )

        @pl.when(second)
        def _():
            y_b[m] = dx.astype(BF16)

        @pl.when(second & (m < last))
        def _():
            hop_back(m).start()

        @pl.when(second & (m == last))
        def _():
            for copy in cast_back():
                copy.start()

        @pl.when(first)
        def _():
            y_f[m] = dx
            store_ends(m).start()

        for i, term in enumerate((grad_norm * unit, grad_norm, upstream)):
            own_sums[i:i + 1, :] += jnp.sum(term, axis=0, keepdims=True)

    def strip(slot):
        return xg.at[:, :, pl.ds(pl.multiple_of(slot * own, own), own)]

    def strip_copy(src, slot):
        return pltpu.make_async_copy(src, strip(slot), dl_sem.at[slot])

    wide_strips = hidden // own
    kinds = 2 * wide_strips

    def strip_start(i, m):
        slot = lax.rem(i, STRIPS)

        @pl.when(i < wide_strips)
        def _():
            strip_copy(act_x.at[m, :, :, cols(i, own)], slot).start()

        @pl.when((i >= wide_strips) & (i < kinds))
        def _():
            strip_copy(up_x.at[m, :, :, cols(i - wide_strips, own)], slot).start()

        @pl.when(i == kinds)
        def _():
            strip_copy(att_x.at[m], slot).start()

        @pl.when(i > kinds)
        def _():
            strip_copy(dj_x.at[m, i - kinds - 1], slot).start()

    half = depth // 2

    def result_copy(dst, h):
        return pltpu.make_async_copy(att.at[h], dst, ds_sem.at[h])

    def turn_rows(m):
        strip_copy(xc_x.at[m], 2).start()
        strip_copy(gc_x.at[m], 3).start()
        for which in range(2):
            strip_copy(xc_x.at[m], 2 + which).wait()
            for b in range(nf):
                for h in range(2):
                    block = xg[b, :, pl.ds((2 + which) * own + h * half, half)]
                    c = (h * nf + b) * length
                    act[which, :, c:c + length] = block.T

    def turned_copies():
        span = nf * length
        return [
            pltpu.make_async_copy(
                act.at[which, :, pl.ds(h * span, span)],
                turned_o.at[which, pl.ds(h * half, half), :],
                dl_sem.at[2 * which + h],
            )
            for which in range(2)
            for h in range(2)
        ]

    def weight_stage():
        m = 0
        for i in range(micro):
            for a in (0, 1):
                x_sent(a, i, 0)
            mirror_copy(i).wait_send()
            for who in range(2):
                mine, theirs = c_pair(0, i, who)
                mine.wait()
                theirs.wait()
        for a in (2, 3):
            x_sent(a, 0, 0)

        @pl.when(first)
        def _():
            for a in (2, 3):
                x_sent(a, 0, 1)

        for who in range(2):
            for a in range(4):
                x_send(a, 0, who).wait_recv()
            mine, theirs = c_pair(1, 0, who)
            mine.wait()
            theirs.wait()
        strip_start(0, m)
        strip_start(1, m)
        turn_rows(m)
        strip_start(2, m)
        strip_start(3, m)

        def step(i):
            slot = lax.rem(i, STRIPS)
            strip_copy(xc_x.at[m], slot).wait()
            use_dy = (i < wide_strips) | (i == kinds)
            right = xg[:, :, cols(slot, own)].reshape(nf * length, own)
            which = jnp.where(use_dy, 1, 0)
            span = nf * length
            left = jnp.concatenate([act[which, :, :span], act[which, :, span:]], axis=0)
            value = jnp.dot(left, right, preferred_element_type=F32)
            for h in range(2):
                rows = pl.ds(h * half, half)

                @pl.when(i > 0)
                def _(h=h):
                    result_copy(out_o.at[pl.ds(0, half), :], h).wait()

                att[h] = value[h * half:(h + 1) * half].astype(BF16)

                @pl.when(i < wide_strips)
                def _(h=h, rows=rows):
                    result_copy(fc2_o.at[rows, cols(i, own)], h).start()

                @pl.when((i >= wide_strips) & (i < kinds))
                def _(h=h, rows=rows):
                    result_copy(fc1_o.at[rows, cols(i - wide_strips, own)], h).start()

                @pl.when(i == kinds)
                def _(h=h, rows=rows):
                    result_copy(out_o.at[rows, :], h).start()

                @pl.when(i > kinds)
                def _(h=h, rows=rows):
                    result_copy(qkv_o.at[i - kinds - 1, rows, :], h).start()

            @pl.when(i + STRIPS < kinds + 4)
            def _():
                strip_start(i + STRIPS, m)

        loop(kinds + 4, step)
        for h in range(2):
            result_copy(out_o.at[pl.ds(0, half), :], h).wait()

    own_sums[...] = jnp.zeros_like(own_sums)
    head_sums[...] = jnp.zeros_like(head_sums)
    up_sums[...] = jnp.zeros_like(up_sums)

    @pl.when(first)
    def _():
        small_arrive()
        load_rows.wait()
        loop(micro, front)
        seg_copy.wait()
        loop(2 * micro, rope_of)

    @pl.when(second)
    def _():
        load_dy.wait()
        loop(micro, front_back)

    @pl.when(second)
    def _():
        for p in range(PIECES):
            relay(1, p)
        w_far(0)
        w_far(1)
        small_arrive()
        wide_copy().start()
        seg_copy.wait()
        loop(2 * micro, rope_of)
        for mask in order:
            w_ready(0, mask)
        w_far(2)
        for p in range(PIECES):
            leg_two(1, p).wait_send()
        pl.semaphore_wait(go_sem, 1)
        for p in range(PIECES - DIRECT):
            leg_one(3, p).start()

        def dy_in(m):
            spread_wait(gr, m, gg_s, gg_r)
            c_start(1, m, 0)

        loop(micro, dy_in)


    small = [
        send(s_src.at[to], s_got.at[k], sm_s.at[k], sm_r.at[k], peer) for k, to, peer in group
    ]

    def small_start():
        s_src[...] = jnp.zeros_like(s_src)
        for j in range(count):
            s_src[j, 0:3, :] = own_sums[0:3, j * LANES:(j + 1) * LANES]
        for j in range(nf):
            s_src[t * nf + j, 3:6, :] = head_sums[0:3, j * LANES:(j + 1) * LANES]
            for r in range(per_row):
                c = (j * per_row + r) * LANES
                s_src[t * nf + j, 6 + r:7 + r, :] = up_sums[0:1, c:c + LANES]
        for copy in small:
            copy.start()

    def slot(k):
        is_f = jnp.where(first, k < 4, (k < 8) & (lax.rem(k, 2) == 0))
        is_o = jnp.where(first, k < 2, (k == 1) | (k == 6))
        who = jnp.where(first, (k // 2) % 2 * (k < 4) + lax.rem(k, 2) * (k >= 4), k // 4)
        m = jnp.where(first, jnp.where(k < 4, lax.rem(k, 2), (k - 4) // 2), lax.rem(k // 2, 2))
        m_o = jnp.where(first, m, k // 6)
        fresh = first & (k == 0)

        @pl.when(second & (k == 0))
        def _():
            hop_out(0).wait_recv()
            front(0)
            w_ready(1, 2)
            for p in range(PIECES - DIRECT, PIECES):
                straight(p).start()

        @pl.when(second & (k == 1))
        def _():
            for i in range(micro):
                for who in range(nt):
                    mirror_rows(i, who).start()
            for mask in order:
                w_ready(2, mask)

        @pl.when(first & (k == 3))
        def _():
            hop_back(0).wait_recv()
            front_back(0)

        @pl.when(is_f)
        def _():
            forward_stage(m, who, k, fresh)

        @pl.when(jnp.logical_not(is_f))
        def _():
            backward_stage(m, who, k)

        @pl.when(second & (k == 6))
        def _():
            for copy in cast_back():
                copy.wait_send()

        @pl.when(is_o)
        def _():
            held_back = second & (k == 1)
            output_stage(
                m_o, jnp.where(held_back, 2, 0), nf, fresh, jnp.logical_not(held_back)
            )


        @pl.when(first & (k == 1))
        def _():
            for p in range(2, PIECES - DIRECT):
                relay(3, p)
            for i in range(micro):
                mirror_copy(i).start()
            for p in range(PIECES - DIRECT):
                leg_two(3, p).wait_send()
            output_finish(1)

        @pl.when(second & (k == 2))
        def _():
            output_rest(0)

        @pl.when(second & (k == 4))
        def _():
            backward_finish(1)

        @pl.when(second & (k == 7))
        def _():
            small_start()

        @pl.when((first & (k == 6)) | (second & (k == 7)))
        def _():
            weight_stage()

        @pl.when(first & (k == 7))
        def _():
            loop(micro, backward_finish)
            small_start()

        @pl.when(k == 7)
        def _():
            for who in range(2):
                mine, theirs = c_pair(1, last, who)
                mine.wait()
                theirs.wait()
            turn_rows(last)
            for copy in turned_copies():
                copy.start()

        @pl.when(second & (k == 7))
        def _():
            loop(micro, output_finish)

    loop(8, slot)

    for a in (2, 3):
        x_sent(a, last, 0)
    for who in range(2):
        for a in range(4):
            if who == 1:
                x_sent(a, last, 1)
            x_send(a, last, who).wait_recv()

    @pl.when(second)
    def _():
        for m in range(last):
            hop_back(m).wait_send()
        wide_copy().wait_send()

    @pl.when(first)
    def _():
        for m in range(micro):
            hop_out(m).wait_send()
        for copy in cast_rows():
            copy.wait_send()

    for m in range(micro):
        for who in range(nt):
            mirror_rows(m, who).wait_send()
    for m in range(micro):
        store_ends(m).wait()
    for a in range(4):
        w_send(a, 0, 0, 1).wait_send()
    for side, via in ((first, 1), (second, 3)):
        @pl.when(side)
        def _(via=via):
            for a in range(4):
                if a != via:
                    w_send(a, 0, 1, 2).wait_send()
                    w_send(a, 2, 0, 1).wait_send()
            for p in range(PIECES):
                if via == 3 and p >= PIECES - DIRECT:
                    straight(p).wait_send()
                else:
                    leg_one(via, p).wait_send()
                passed_on(via, 2, p).wait_send()
    total = s_src[me]
    for k, copy in enumerate(small):
        copy.wait()
        total = total + s_got[k + 1]
    sums_o[...] = total
    for copy in turned_copies():
        copy.wait()


def fused(ends, smalls, segments, wq, wo, w1, w2, nf, nt):
    micro, per, width = ends.shape
    length = per * nt
    own, hidden = wo.shape[1], w1.shape[1]
    depth = width // nf
    count = nf * nt
    bits = nf.bit_length() - 1
    anywhere = pl.BlockSpec(memory_space=pl.ANY)
    inside = pl.BlockSpec(memory_space=pltpu.VMEM)
    dma = pltpu.SemaphoreType.DMA
    vm = pltpu.VMEM
    piece = (ROWS_OF_PACK, LANES)
    packs = 2 * micro
    some = micro + 1
    out_shape = [
        jax.ShapeDtypeStruct(ends.shape, F32),
        jax.ShapeDtypeStruct(piece, F32),
        jax.ShapeDtypeStruct((depth, hidden), BF16),
        jax.ShapeDtypeStruct((depth, hidden), BF16),
        jax.ShapeDtypeStruct((depth, own), BF16),
        jax.ShapeDtypeStruct((3, depth, own), BF16),
        jax.ShapeDtypeStruct((2, depth, nf * length), BF16),
        jax.ShapeDtypeStruct((micro, nf, length, hidden), BF16),
        jax.ShapeDtypeStruct((micro, nf, length, own), BF16),
        jax.ShapeDtypeStruct((micro, nf, length, hidden), BF16),
        jax.ShapeDtypeStruct((micro, 3, nf, length, own), BF16),
        jax.ShapeDtypeStruct((micro, nf, length, depth), BF16),
        jax.ShapeDtypeStruct((micro, nf, length, depth), BF16),
    ]
    scratch = [
        vm((3, width, own), BF16), vm((width, own), BF16),
        vm((width, hidden), BF16), vm((width, hidden), BF16),
        vm(piece, F32), vm((count,) + piece, F32),
        vm((ROWS_OF_PACK, width), F32), vm((8, hidden), F32),
        vm((2, 8, length), F32), vm((packs, 2, length, LANES), F32),
        vm(ends.shape, BF16), vm(ends.shape, BF16),
        vm((packs, length, width), BF16), vm((packs, 3, length, own), BF16),
        vm((packs, length, LANES), F32), vm((some, length, own), BF16),
        vm((packs, length, hidden), BF16), vm((some, length, hidden), BF16),
        vm((packs, length, width), BF16), vm((length, own), BF16),
        vm((some, length, hidden), BF16), vm((some, 3, length, own), BF16),
        vm((micro, length, width), BF16), vm((micro, nt - 1, per, width), BF16),
        vm((micro, length, width), BF16), vm((micro, nt - 1, per, width), BF16),
        vm(ends.shape, F32), vm(ends.shape, BF16),
        vm((8, width), F32), vm((8, own), F32), vm((8, hidden), F32),
        vm((count,) + piece, F32), vm((count,) + piece, F32),
        dma, dma((4,)), dma((4, nf, bits)), dma((4, nf)),
        dma((count,)), dma((count,)), dma((count,)), dma((count,)),
        dma((micro, nt)), dma((micro, nt)), dma((micro, nt)), dma((micro, nt)),
        dma((micro, nt)), dma((micro, nt)), dma((micro, nt)), dma((micro, nt)),
        dma((micro,)), dma((micro,)), dma((micro,)), dma((micro,)),
        dma((4, micro, 2)), dma((4, micro, 2)), dma((4, micro, 2)),
        dma((2, micro, 2)), dma((2, micro, 2)), dma((2, micro, 2)),
        dma((3, micro)), dma((3, micro)), dma((micro,)),
        dma((micro, nt)), dma((micro, nt)),
        dma((PIECES,)), dma((PIECES,)), dma((PIECES,)), dma((PIECES,)),
        dma((PIECES,)), dma((PIECES,)), pltpu.SemaphoreType.REGULAR,
        vm((per, width), BF16), vm((8, width), F32), dma((nt,)), dma((nt,)), dma((2,)),
        dma((STRIPS,)), dma((2,)),
    ]
    return pl.pallas_call(
        functools.partial(fused_kernel, nf, nt),
        out_shape=out_shape,
        in_specs=[anywhere] + [inside] * 7 + [anywhere] * 4,
        out_specs=[anywhere, inside] + [anywhere] * 11,
        scratch_shapes=scratch,
        compiler_params=pltpu.CompilerParams(
            collective_id=4, has_side_effects=True, vmem_limit_bytes=VMEM_LIMIT
        ),
        name="fused",
    )(ends, *smalls, segments, wq, wo, w1, w2)


def padded(flat):
    size = -(-flat.shape[-1] // (8 * LANES)) * (8 * LANES)
    room = [(0, 0)] * (flat.ndim - 1) + [(0, size - flat.shape[-1])]
    flat = jnp.pad(flat, room)
    return flat.reshape(flat.shape[:-1] + (size // LANES, LANES))


def split_shards(
    ends_in, segments, ln_gain, ln_bias, w_qkv, w_out, w_fc1, w_fc2,
    bias_qkv, bias_out, bias_fc1, bias_fc2,
):
    nf, nt = lax.axis_size("fsdp"), lax.axis_size("tp")
    count = nf * nt
    section, tp_index = lax.axis_index("section"), lax.axis_index("tp")
    is_first = section == 0
    piece = ln_gain.shape[1]
    hidden_piece = bias_fc1.shape[1]
    own, hidden = w_out.shape[2], w_fc1.shape[2]
    width = piece * count

    pack = jnp.concatenate(
        [ln_gain[0], ln_bias[0], bias_out[0], bias_fc2[0], bias_qkv[0].reshape(-1), bias_fc1[0]]
    ).astype(F32)
    used = pack.shape[0]
    smalls = gather_small(padded(pack), nf, nt).reshape(count, -1)[:, :used]
    wide = smalls[:, :7 * piece].reshape(count, 7, piece).transpose(1, 0, 2).reshape(7, width)
    vec = jnp.stack([wide[0], wide[1], wide[2] + wide[3]])
    vec = jnp.pad(vec, ((0, 5), (0, 0)))
    qb = lax.dynamic_slice_in_dim(wide[4:7], tp_index * own, own, 1)
    qb = jnp.pad(qb, ((0, 5), (0, 0)))
    fb = lax.dynamic_slice_in_dim(smalls[:, 7 * piece:], tp_index * nf, nf, 0).reshape(1, hidden)
    fb = jnp.pad(fb, ((0, 7), (0, 0)))
    rope = rope_tables(segments)
    segc, segr = segments[:, :, None], segments[:, None, :]

    wq = lax.all_gather(w_qkv[0].transpose(1, 0, 2), "fsdp", axis=1, tiled=True)
    w1 = lax.all_gather(w_fc1[0], "fsdp", axis=0, tiled=True)
    wo = lax.all_gather(w_out[0], "fsdp", axis=0, tiled=True)
    w2 = lax.all_gather(w_fc2[0], "fsdp", axis=0, tiled=True)
    weights = (wq, wo, w1, w2)
    rows, xg, qkv, lse, att, gp, act, y = forward(
        ends_in[0], weights, vec, qb, fb, rope, segc, segr, nt
    )
    gr, up, dj, dx, own_sums, head_sums, up_sums = backward(
        ends_in[0], weights, rows, qkv, lse, gp, vec, rope, segc, segr, nt
    )

    def everywhere(arr):
        return lax.all_gather(arr, "fsdp", axis=arr.ndim - 2, tiled=True)

    def columns(arr):
        return lax.all_to_all(arr, "fsdp", split_axis=2, concat_axis=1, tiled=True)

    xc, gc = columns(xg), columns(gr)

    def product(left, right):
        return lax.dot_general(
            left, right, (((0, 1), (0, 1)), ((), ())), preferred_element_type=F32
        )

    act_all, att_all, up_all, dj_all = (everywhere(a) for a in (act, att, up, dj))
    grad_fc2 = product(gc, act_all)
    grad_out = product(gc, att_all)
    grad_fc1 = product(xc, up_all)
    grad_qkv = jnp.stack([product(xc, dj_all[:, part]) for part in range(3)], axis=1)

    mine = own_sums[:3].reshape(3, count, piece).transpose(1, 0, 2).reshape(count, 3 * piece)
    head = lax.dynamic_update_slice_in_dim(
        jnp.zeros((3, width), F32), head_sums[:3], tp_index * own, 1
    )
    head = head.reshape(3, count, piece).transpose(1, 0, 2).reshape(count, 3 * piece)
    ups = lax.dynamic_update_slice_in_dim(
        jnp.zeros((count, hidden_piece), F32),
        up_sums[0].reshape(nf, hidden_piece),
        tp_index * nf,
        0,
    )
    sums = sum_small(padded(jnp.concatenate([mine, head, ups], axis=1)), nf, nt).reshape(-1)
    gain_grad, bias_grad, row_grad = (sums[i * piece:(i + 1) * piece] for i in range(3))
    qkv_bias_grad = sums[3 * piece:6 * piece].reshape(3, piece)
    fc1_bias_grad = sums[6 * piece:6 * piece + hidden_piece]
    ends_out = jnp.where(is_first, dx, y)[None]
    return (
        ends_out,
        gain_grad[None],
        bias_grad[None],
        grad_qkv[None],
        grad_out[None],
        grad_fc1[None],
        grad_fc2[None],
        qkv_bias_grad[None],
        row_grad[None],
        fc1_bias_grad[None],
        row_grad[None],
    )


AHEAD = 3


def last_kernel(
    used, last,
    ends, sums, turned, fc2, fc1, out, qkv, act, up, att, dj,
    ends_o, gain_o, shift_o, row_o, row_b, qkv_b, fc1_b, fc2_o, fc1_o, out_o, qkv_o,
    ends_v, turned_v, early_v, right_v, done_v, e_sem, t_sem, p_sem, r_sem, d_sem,
):
    strips, _, own = early_v.shape
    wide = (strips - 4) // 2
    copy = pltpu.make_async_copy

    def part(ref, i):
        return ref.at[:, pl.ds(i * own, own)]

    table = []
    for i in range(wide):
        right = act.at[last, :, :, pl.ds(i * own, own)]
        table.append((1, part(fc2, i), right, part(fc2_o, i)))
    for i in range(wide):
        right = up.at[last, :, :, pl.ds(i * own, own)]
        table.append((0, part(fc1, i), right, part(fc1_o, i)))
    table.append((1, out, att.at[last], out_o))
    for i in range(3):
        table.append((0, qkv.at[i], dj.at[last, i], qkv_o.at[i]))
    def turned_load(which):
        return copy(turned.at[which], turned_v.at[which], t_sem.at[which])

    def loads(i):
        _, early, right, _ = table[i]
        return copy(right, right_v.at[i], r_sem.at[i]), copy(early, early_v.at[i], p_sem.at[i])

    turned_load(table[0][0]).start()
    for i in range(AHEAD):
        for one in loads(i):
            one.start()
    ends_in = copy(ends, ends_v, e_sem.at[0])
    gain_o[...] = sums[0:1, :]
    shift_o[...] = sums[1:2, :]
    row_o[...] = sums[2:3, :]
    row_b[...] = sums[2:3, :]
    for r in range(3):
        qkv_b[r] = sums[3 + r:4 + r, :]
    for r in range(6, used):
        fc1_b[:, (r - 6) * LANES:(r - 5) * LANES] = sums[r:r + 1, :]
    ready = set()
    stores = []
    for i, (which, _, _, target) in enumerate(table):
        if which not in ready:
            turned_load(which).wait()
            ready.add(which)
        for one in loads(i):
            one.wait()
        if i + AHEAD < strips:
            for one in loads(i + AHEAD):
                one.start()
        if i == 0:
            turned_load(1 - which).start()
        if i == 1:
            ends_in.start()
        right = right_v[i].reshape(-1, own)
        done_v[i] = early_v[i].astype(F32) + jnp.dot(
            turned_v[which], right, preferred_element_type=F32
        )
        stores.append(copy(done_v.at[i], target, d_sem.at[i]))
        stores[-1].start()
        if i == strips - 3:
            ends_in.wait()
            stores.append(copy(ends_v, ends_o, e_sem.at[1]))
            stores[-1].start()
    for one in stores:
        one.wait()


def last_products(used, ends, sums, turned, fc2, fc1, out, qkv, act, up, att, dj):
    depth, hidden = fc2.shape
    own = out.shape[1]
    micro, nf, length = act.shape[:3]
    strips = 2 * (hidden // own) + 4
    anywhere = pl.BlockSpec(memory_space=pl.ANY)
    inside = pl.BlockSpec(memory_space=pltpu.VMEM)
    small = jax.ShapeDtypeStruct((1, LANES), F32)
    dma = pltpu.SemaphoreType.DMA
    return pl.pallas_call(
        functools.partial(last_kernel, used, micro - 1),
        out_shape=[
            jax.ShapeDtypeStruct(ends.shape, F32), small, small, small, small,
            jax.ShapeDtypeStruct((3, 1, LANES), F32),
            jax.ShapeDtypeStruct((1, (used - 6) * LANES), F32),
            jax.ShapeDtypeStruct(fc2.shape, F32), jax.ShapeDtypeStruct(fc1.shape, F32),
            jax.ShapeDtypeStruct(out.shape, F32), jax.ShapeDtypeStruct(qkv.shape, F32),
        ],
        in_specs=[anywhere, inside] + [anywhere] * 9,
        out_specs=[anywhere] + [inside] * 6 + [anywhere] * 4,
        scratch_shapes=[
            pltpu.VMEM(ends.shape, F32), pltpu.VMEM(turned.shape, BF16),
            pltpu.VMEM((strips, depth, own), BF16),
            pltpu.VMEM((strips, nf, length, own), BF16),
            pltpu.VMEM((strips, depth, own), F32),
            dma((2,)), dma((2,)), dma((strips,)), dma((strips,)), dma((strips,)),
        ],
        compiler_params=pltpu.CompilerParams(vmem_limit_bytes=VMEM_LIMIT),
        name="last_products",
    )(ends, sums, turned, fc2, fc1, out, qkv, act, up, att, dj)


def fused_shards(
    ends_in, segments, ln_gain, ln_bias, w_qkv, w_out, w_fc1, w_fc2,
    bias_qkv, bias_out, bias_fc1, bias_fc2,
):
    nf, nt = lax.axis_size("fsdp"), lax.axis_size("tp")
    used = 6 + bias_fc1.shape[1] // LANES
    ends_out, sums, fc2, fc1, out, qkv, turned, act_x, att_x, up_x, dj_x, *_ = fused(
        ends_in[0],
        (ln_gain, ln_bias, bias_out, bias_fc2, bias_qkv[0], bias_fc1),
        segments, w_qkv[0].transpose(1, 0, 2), w_out[0], w_fc1[0], w_fc2[0], nf, nt,
    )

    ends_out, gain, shift, row, row_again, qkv_bias, fc1_bias, fc2, fc1, out, qkv = (
        last_products(
            used, ends_out, sums, turned, fc2, fc1, out, qkv, act_x, up_x, att_x, dj_x
        )
    )
    return (
        ends_out[None],
        gain,
        shift,
        qkv.transpose(1, 0, 2)[None],
        out[None],
        fc1[None],
        fc2[None],
        qkv_bias.transpose(1, 0, 2),
        row,
        fc1_bias,
        row_again,
    )


def shards(*args):
    rows, piece = args[0].shape[2], args[2].shape[1]
    small = rows * lax.axis_size("tp") <= 256
    tidy = piece == LANES and args[10].shape[1] // LANES <= ROWS_OF_PACK - 6
    square = lax.axis_size("fsdp") == 4 and args[0].shape[1] == 2
    return (fused_shards if small and tidy and square else split_shards)(*args)


def solution(mesh):
    both = P("section", ("fsdp", "tp"))
    square = P("section", "fsdp", "tp")
    tokens = P("section", None, ("fsdp", "tp"), None)
    heads = P("section", "fsdp", None, "tp")
    bias3 = P("section", None, ("fsdp", "tp"))
    return jax.shard_map(
        shards,
        mesh=mesh,
        in_specs=(
            tokens, P(None, "fsdp"), both, both, heads, square, square, square,
            bias3, both, both, both,
        ),
        out_specs=(
            tokens, both, both, heads, square, square, square, bias3, both, both, both,
        ),
        check_vma=False,
    )
```

```python
import functools

import jax
import jax.numpy as jnp
from jax import lax
from jax.experimental import pallas as pl
from jax.experimental.pallas import tpu as pltpu
from jax.sharding import PartitionSpec as P

HEAD_DIM = 64
ROT_DIM = 32
EPSILON = 1e-05
LANES = 128
TILE = 256
MESH = pl.DeviceIdType.MESH
F32 = jnp.float32
BF16 = jnp.bfloat16
COLS = (((1,), (1,)), ((), ()))
ROWS = (((0,), (0,)), ((), ()))
VMEM_LIMIT = 66_900_000


def positions_of(segment_ids):
    length = segment_ids.shape[-1]
    places = jnp.arange(length, dtype=jnp.int32)
    before = jnp.concatenate([segment_ids[..., :1] - 1, segment_ids[..., :-1]], axis=-1)
    starts = jnp.where(segment_ids != before, places, 0)
    starts = lax.cummax(starts, axis=segment_ids.ndim - 1)
    return places - starts


def rope_tables(segments):
    half = ROT_DIM // 2
    freq = jnp.exp(-jnp.log(10000.0) * (2.0 * jnp.arange(half, dtype=F32)) / ROT_DIM)
    angles = positions_of(segments).astype(F32)[..., None] * freq
    cosine, sine = jnp.cos(angles), jnp.sin(angles)
    none = jnp.zeros_like(sine)
    rest = jnp.zeros(angles.shape[:-1] + (HEAD_DIM - ROT_DIM,), F32)
    keep = jnp.concatenate([cosine, cosine, rest + 1.0], axis=-1)
    ahead = jnp.concatenate([-sine, none, rest], axis=-1)
    behind = jnp.concatenate([none, sine, rest], axis=-1)
    tables = jnp.stack([keep, ahead, behind], axis=1)
    return jnp.concatenate([tables, tables], axis=-1)


def send(src, dst, send_sem, recv_sem, device):
    return pltpu.make_async_remote_copy(
        src_ref=src,
        dst_ref=dst,
        send_sem=send_sem,
        recv_sem=recv_sem,
        device_id=device,
        device_id_type=MESH,
    )


def greet(peers):
    barrier = pltpu.get_barrier_semaphore()
    for peer in peers:
        pl.semaphore_signal(barrier, inc=1, device_id=peer, device_id_type=MESH)
    pl.semaphore_wait(barrier, len(peers))


def group_peers(nf, nt):
    me = lax.axis_index("fsdp") * nt + lax.axis_index("tp")
    found = []
    for k in range(1, nf * nt):
        to = lax.rem(me + k, nf * nt)
        found.append((k, to, {"fsdp": to // nt, "tp": lax.rem(to, nt)}))
    return me, found


def gather_small_kernel(nf, nt, own, out, send_sems, recv_sems, local_sem):
    me, peers = group_peers(nf, nt)
    greet([peer for _, _, peer in peers])
    mine = pltpu.make_async_copy(own, out.at[me], local_sem)
    mine.start()
    copies = []
    for k, _, peer in peers:
        copy = send(own, out.at[me], send_sems.at[k], recv_sems.at[k], peer)
        copy.start()
        copies.append(copy)
    mine.wait()
    for copy in copies:
        copy.wait()


def gather_small(own, nf, nt):
    count = nf * nt
    return pl.pallas_call(
        functools.partial(gather_small_kernel, nf, nt),
        out_shape=jax.ShapeDtypeStruct((count,) + own.shape, own.dtype),
        in_specs=[pl.BlockSpec(memory_space=pltpu.VMEM)],
        out_specs=pl.BlockSpec(memory_space=pltpu.VMEM),
        scratch_shapes=[
            pltpu.SemaphoreType.DMA((count,)),
            pltpu.SemaphoreType.DMA((count,)),
            pltpu.SemaphoreType.DMA,
        ],
        compiler_params=pltpu.CompilerParams(collective_id=0, has_side_effects=True),
        name="gather_small",
    )(own)


def sum_small_kernel(nf, nt, own, out, got, send_sems, recv_sems):
    me, peers = group_peers(nf, nt)
    greet([peer for _, _, peer in peers])
    copies = []
    for k, to, peer in peers:
        copy = send(own.at[to], got.at[k], send_sems.at[k], recv_sems.at[k], peer)
        copy.start()
        copies.append(copy)
    total = own[me]
    for k, copy in enumerate(copies):
        copy.wait()
        total = total + got[k + 1]
    out[...] = total


def sum_small(own, nf, nt):
    count = nf * nt
    return pl.pallas_call(
        functools.partial(sum_small_kernel, nf, nt),
        out_shape=jax.ShapeDtypeStruct(own.shape[1:], own.dtype),
        in_specs=[pl.BlockSpec(memory_space=pltpu.VMEM)],
        out_specs=pl.BlockSpec(memory_space=pltpu.VMEM),
        scratch_shapes=[
            pltpu.VMEM(own.shape, own.dtype),
            pltpu.SemaphoreType.DMA((count,)),
            pltpu.SemaphoreType.DMA((count,)),
        ],
        compiler_params=pltpu.CompilerParams(collective_id=1, has_side_effects=True),
        name="sum_small",
    )(own)


def cols(n, width=TILE):
    return pl.ds(pl.multiple_of(n * width, width), width)


def loop(count, body):
    def step(i, carry):
        body(i)
        return carry

    lax.fori_loop(0, count, step, 0)


def turn(x, tables, sign):
    keep, ahead, behind = tables
    left = pltpu.roll(x, LANES - ROT_DIM // 2, 1)
    right = pltpu.roll(x, ROT_DIM // 2, 1)
    return x * keep + sign * (left * ahead + right * behind)


def low_half(length):
    return lax.broadcasted_iota(jnp.int32, (length, LANES), 1) < HEAD_DIM


def allowed_mask(segc, segr, m, length):
    query = lax.broadcasted_iota(jnp.int32, (length, length), 0)
    key = lax.broadcasted_iota(jnp.int32, (length, length), 1)
    return (query >= key) & (segc[m] == segr[m])


class Ring:
    def __init__(self, nt, rows):
        self.nt, self.rows = nt, rows
        self.me = lax.axis_index("tp")
        self.others = [(k, lax.rem(self.me + k, nt)) for k in range(1, nt)]

    def block(self, who):
        return pl.ds(pl.multiple_of(who * self.rows, self.rows), self.rows)

    def gather(self, buf, m, sems):
        return [
            send(
                buf.at[m, self.block(self.me)],
                buf.at[m, self.block(self.me)],
                sems[0].at[m, k],
                sems[1].at[m, k],
                {"tp": to},
            )
            for k, to in self.others
        ]

    def scatter(self, buf, got, m, sems, part=None):
        at = slice(None) if part is None else part
        return [
            send(
                buf.at[m, self.block(to), at],
                got.at[m, k - 1, :, at],
                sems[0].at[m, k],
                sems[1].at[m, k],
                {"tp": to},
            )
            for k, to in self.others
        ]

    def total(self, buf, got, m):
        acc = buf[m, self.block(self.me)].astype(F32)
        for k, _ in self.others:
            acc = acc + got[m, k - 1].astype(F32)
        return acc


def stats(rows):
    mean = jnp.mean(rows, axis=-1, keepdims=True)
    centred = rows - mean
    variance = jnp.mean(centred * centred, axis=-1, keepdims=True)
    inv_root = lax.rsqrt(variance + EPSILON)
    return centred * inv_root, inv_root


def forward_kernel(
    nt,
    rows_h, wq_h, wo_h, w1_h, w2_h, vec, qb, fb, rope, segc, segr,
    rows_o, xg_o, qkv_o, lse_o, att_o, gp_o, act_o, y_o,
    wq, wo, w1, w2, rin, xg, qkv, lse, att, gp, act, branch, got, out_f, out_b,
    w_sem, in_sem, o_sem, ag_s, ag_r, rs_s, rs_r, x_s, x_r,
):
    micro, length, width = xg.shape
    section = lax.axis_index("section")
    first, second = section == 0, section == 1
    ring = Ring(nt, length // nt)
    own = wo.shape[1]
    loads = []
    for i, (src, dst) in enumerate(((wq_h, wq), (w1_h, w1), (wo_h, wo), (w2_h, w2))):
        loads.append(pltpu.make_async_copy(src, dst, w_sem.at[i]))
        loads[-1].start()
    mine = pltpu.make_async_copy(rows_h, rin, in_sem)

    @pl.when(first)
    def _():
        mine.start()

    greet([{"tp": to} for _, to in ring.others] + [{"section": 1 - section}])

    @pl.when(first)
    def _():
        mine.wait()

    def hop(m):
        return send(out_b.at[m], rin.at[m], x_s.at[m], x_r.at[m], {"section": 1 - section})

    def front(m):
        unit, _ = stats(rin[m].astype(F32))
        normed = unit * vec[0:1, :] + vec[1:2, :]
        xg[m, ring.block(ring.me)] = normed.astype(BF16)
        for copy in ring.gather(xg, m, (ag_s, ag_r)):
            copy.start()

    def arrive(m):
        @pl.when(second)
        def _():
            hop(m).wait_recv()
            front(m)

    stores = []

    def store(src, dst, m, i):
        copy = pltpu.make_async_copy(src.at[m], dst.at[m], o_sem.at[m, i])
        copy.start()
        stores.append(copy)

    def body(m):
        for copy in ring.gather(xg, m, (ag_s, ag_r)):
            copy.wait()
        store(xg, xg_o, m, 0)
        store(rin, rows_o, m, 1)
        tables = (rope[m, 0], rope[m, 1], rope[m, 2])
        if m == 0:
            loads[0].wait()
        per = own // TILE
        for part in range(3):
            def qkv_tile(n, part=part):
                at = cols(n)
                acc = jnp.dot(xg[m], wq[part, :, at], preferred_element_type=F32)
                acc = acc + qb[part:part + 1, at]
                if part < 2:
                    acc = jnp.concatenate(
                        [
                            turn(acc[:, c:c + LANES], tables, 1.0)
                            for c in range(0, TILE, LANES)
                        ],
                        axis=1,
                    )
                qkv[m, part, :, at] = acc.astype(BF16)

            loop(per, qkv_tile)
        store(qkv, qkv_o, m, 2)
        allowed = allowed_mask(segc, segr, m, length)
        low = low_half(length)
        lane = lax.broadcasted_iota(jnp.int32, (length, LANES), 1)

        def pair(p):
            at = cols(p, LANES)
            query, key, value = qkv[m, 0, :, at], qkv[m, 1, :, at], qkv[m, 2, :, at]
            outs = []
            for h in range(2):
                mask = low if h == 0 else ~low
                one = jnp.where(mask, query, jnp.zeros_like(query))
                s = lax.dot_general(one, key, COLS, preferred_element_type=F32)
                s = jnp.where(allowed, s * HEAD_DIM ** (-0.5), -1e30)
                top = jnp.max(s, axis=-1, keepdims=True)
                e = jnp.exp(s - top)
                total = jnp.sum(e, axis=-1, keepdims=True)
                probs = (e / total).astype(BF16)
                outs.append(jnp.dot(probs, value, preferred_element_type=F32))
                lse[m] = jnp.where(lane == 2 * p + h, top + jnp.log(total), lse[m])
            att[m, :, at] = jnp.where(low, outs[0], outs[1]).astype(BF16)

        lse[m] = jnp.zeros((length, LANES), F32)
        loop(own // LANES, pair)
        store(lse, lse_o, m, 3)
        store(att, att_o, m, 4)
        if m == 0:
            loads[1].wait()

        def up_tile(n):
            at = cols(n)
            u = jnp.dot(xg[m], w1[:, at], preferred_element_type=F32) + fb[0:1, at]
            c = 0.7978845608028654
            square = u * u
            t = jnp.tanh(c * u * (1.0 + 0.044715 * square))
            act[m, :, at] = (0.5 * u * (1.0 + t)).astype(BF16)
            slope = 0.5 * (1.0 + t) + 0.5 * u * (1.0 - t * t) * (c * (1.0 + 3 * 0.044715 * square))
            gp[m, :, at] = slope.astype(BF16)

        loop(act.shape[2] // TILE, up_tile)
        store(act, act_o, m, 5)
        store(gp, gp_o, m, 6)
        if m == 0:
            loads[2].wait()
            loads[3].wait()

        def out_tile(n):
            at = cols(n)
            acc = lax.dot_general(att[m], wo[at, :], COLS, preferred_element_type=F32)
            acc = acc + lax.dot_general(act[m], w2[at, :], COLS, preferred_element_type=F32)
            branch[m, :, at] = acc.astype(BF16)
            for copy in ring.scatter(branch, got, m, (rs_s, rs_r), at):
                copy.start()

        loop(width // TILE, out_tile)

    def finish(m):
        for copy in ring.scatter(branch, got, m, (rs_s, rs_r)):
            copy.wait()
        y = rin[m].astype(F32) + ring.total(branch, got, m) + vec[2:3, :]
        out_f[m] = y
        out_b[m] = y.astype(BF16)
        store(out_f, y_o, m, 7)

        @pl.when(first)
        def _():
            hop(m).start()

    @pl.when(first)
    def _():
        for m in range(micro):
            front(m)

    for m in range(micro):
        arrive(m)
        body(m)
    for m in range(micro):
        finish(m)
    for copy in stores:
        copy.wait()

    @pl.when(first)
    def _():
        for m in range(micro):
            hop(m).wait_send()


def forward(rows, weights, vec, qb, fb, rope, segc, segr, nt):
    wq, wo, w1, w2 = weights
    micro, per, width = rows.shape
    length = per * nt
    own, hidden = wo.shape[1], w1.shape[1]
    anywhere = pl.BlockSpec(memory_space=pl.ANY)
    inside = pl.BlockSpec(memory_space=pltpu.VMEM)
    out_shape = [
        jax.ShapeDtypeStruct(rows.shape, BF16),
        jax.ShapeDtypeStruct((micro, length, width), BF16),
        jax.ShapeDtypeStruct((micro, 3, length, own), BF16),
        jax.ShapeDtypeStruct((micro, length, LANES), F32),
        jax.ShapeDtypeStruct((micro, length, own), BF16),
        jax.ShapeDtypeStruct((micro, length, hidden), BF16),
        jax.ShapeDtypeStruct((micro, length, hidden), BF16),
        jax.ShapeDtypeStruct(rows.shape, F32),
    ]
    dma = pltpu.SemaphoreType.DMA
    return pl.pallas_call(
        functools.partial(forward_kernel, nt),
        out_shape=out_shape,
        in_specs=[anywhere] * 5 + [inside] * 6,
        out_specs=[anywhere] * 8,
        scratch_shapes=[
            pltpu.VMEM(wq.shape, BF16),
            pltpu.VMEM(wo.shape, BF16),
            pltpu.VMEM(w1.shape, BF16),
            pltpu.VMEM(w2.shape, BF16),
            pltpu.VMEM(rows.shape, BF16),
            pltpu.VMEM((micro, length, width), BF16),
            pltpu.VMEM((micro, 3, length, own), BF16),
            pltpu.VMEM((micro, length, LANES), F32),
            pltpu.VMEM((micro, length, own), BF16),
            pltpu.VMEM((micro, length, hidden), BF16),
            pltpu.VMEM((micro, length, hidden), BF16),
            pltpu.VMEM((micro, length, width), BF16),
            pltpu.VMEM((micro, nt - 1, per, width), BF16),
            pltpu.VMEM(rows.shape, F32),
            pltpu.VMEM(rows.shape, BF16),
            dma((4,)),
            dma,
            dma((micro, 8)),
            dma((micro, nt)),
            dma((micro, nt)),
            dma((micro, nt)),
            dma((micro, nt)),
            dma((micro,)),
            dma((micro,)),
        ],
        compiler_params=pltpu.CompilerParams(
            collective_id=2, has_side_effects=True, vmem_limit_bytes=VMEM_LIMIT
        ),
        name="forward",
    )(rows, wq, wo, w1, w2, vec, qb, fb, rope, segc, segr)


def backward_kernel(
    nt,
    dy_h, wq_h, wo_h, w1_h, w2_h, rows_h, qkv_h, lse_h, gp_h, vec, rope, segc, segr,
    gr_o, up_o, dj_o, dx_o, own_sums, head_sums, up_sums,
    wq, wo, w1, w2, dyr, rin, qkv, lse, gp, gr, gatt, up, dj, branch, got, out_f, out_b,
    w_sem, in_sem, o_sem, ag_s, ag_r, rs_s, rs_r, x_s, x_r,
):
    micro, length, width = gr.shape
    section = lax.axis_index("section")
    first, second = section == 0, section == 1
    ring = Ring(nt, length // nt)
    own = wo.shape[1]
    mine = pltpu.make_async_copy(dy_h, dyr, in_sem.at[4])

    @pl.when(second)
    def _():
        mine.start()

    loads = []
    for i, (src, dst) in enumerate(((wo_h, wo), (w2_h, w2), (wq_h, wq), (w1_h, w1))):
        loads.append(pltpu.make_async_copy(src, dst, w_sem.at[i]))
    kept = []
    for i, (src, dst) in enumerate(((qkv_h, qkv), (lse_h, lse), (gp_h, gp), (rows_h, rin))):
        kept.append(pltpu.make_async_copy(src, dst, in_sem.at[i]))
    for copy in (loads[0], kept[0], kept[1], loads[1], kept[2], loads[2], loads[3], kept[3]):
        copy.start()
    greet([{"tp": to} for _, to in ring.others] + [{"section": 1 - section}])

    @pl.when(second)
    def _():
        mine.wait()

    def hop(m):
        return send(out_b.at[m], dyr.at[m], x_s.at[m], x_r.at[m], {"section": 1 - section})

    def front(m):
        gr[m, ring.block(ring.me)] = dyr[m]
        for copy in ring.gather(gr, m, (ag_s, ag_r)):
            copy.start()

    def arrive(m):
        @pl.when(first)
        def _():
            hop(m).wait_recv()
            front(m)

    stores = []

    def store(src, dst, m, i):
        copy = pltpu.make_async_copy(src.at[m], dst.at[m], o_sem.at[m, i])
        copy.start()
        stores.append(copy)

    def body(m):
        for copy in ring.gather(gr, m, (ag_s, ag_r)):
            copy.wait()
        store(gr, gr_o, m, 0)
        if m == 0:
            loads[0].wait()

        def att_tile(n):
            at = cols(n)
            gatt[:, at] = jnp.dot(gr[m], wo[:, at], preferred_element_type=F32).astype(BF16)

        loop(own // TILE, att_tile)
        if m == 0:
            kept[0].wait()
            kept[1].wait()
        tables = (rope[m, 0], rope[m, 1], rope[m, 2])
        allowed = allowed_mask(segc, segr, m, length)
        low = low_half(length)
        lane = lax.broadcasted_iota(jnp.int32, (length, LANES), 1)
        factor = HEAD_DIM ** (-0.5)

        def pair(p):
            at = cols(p, LANES)
            query, key, value = qkv[m, 0, :, at], qkv[m, 1, :, at], qkv[m, 2, :, at]
            grad = gatt[:, at]
            dqs, dks, dvs = [], [], []
            for h in range(2):
                mask = low if h == 0 else ~low
                one = jnp.where(mask, query, jnp.zeros_like(query))
                s = lax.dot_general(one, key, COLS, preferred_element_type=F32)
                s = jnp.where(allowed, s * factor, -1e30)
                log_total = jnp.sum(
                    jnp.where(lane == 2 * p + h, lse[m], 0.0), axis=-1, keepdims=True
                )
                soft = jnp.exp(s - log_total)
                probs = soft.astype(BF16)
                one_grad = jnp.where(mask, grad, jnp.zeros_like(grad))
                dp = lax.dot_general(one_grad, value, COLS, preferred_element_type=F32)
                delta = jnp.sum(dp * soft, axis=-1, keepdims=True)
                ds = (soft * (dp - delta)).astype(BF16)
                dvs.append(lax.dot_general(probs, grad, ROWS, preferred_element_type=F32))
                dqs.append(jnp.dot(ds, key, preferred_element_type=F32))
                dks.append(lax.dot_general(ds, query, ROWS, preferred_element_type=F32))
            dq = jnp.where(low, dqs[0], dqs[1]) * factor
            dk = jnp.where(low, dks[0], dks[1]) * factor
            dj[m, 0, :, at] = turn(dq, tables, -1.0).astype(BF16)
            dj[m, 1, :, at] = turn(dk, tables, -1.0).astype(BF16)
            dj[m, 2, :, at] = jnp.where(low, dvs[0], dvs[1]).astype(BF16)

        loop(own // LANES, pair)
        store(dj, dj_o, m, 1)
        for part in range(3):
            sums = jnp.sum(dj[m, part].astype(F32), axis=0, keepdims=True)
            if m == 0:
                head_sums[part:part + 1, :] = sums
            else:
                head_sums[part:part + 1, :] += sums
        if m == 0:
            loads[1].wait()
            kept[2].wait()

        def up_tile(n):
            at = cols(n)
            acc = jnp.dot(gr[m], w2[:, at], preferred_element_type=F32)
            rounded = (acc * gp[m, :, at].astype(F32)).astype(BF16)
            up[m, :, at] = rounded
            sums = jnp.sum(rounded.astype(F32), axis=0, keepdims=True)
            if m == 0:
                up_sums[0:1, at] = sums
            else:
                up_sums[0:1, at] += sums

        loop(up.shape[2] // TILE, up_tile)
        store(up, up_o, m, 2)
        if m == 0:
            loads[2].wait()
            loads[3].wait()

        def norm_tile(n):
            at = cols(n)
            acc = lax.dot_general(up[m], w1[at, :], COLS, preferred_element_type=F32)
            for part in range(3):
                acc = acc + lax.dot_general(
                    dj[m, part], wq[part, at, :], COLS, preferred_element_type=F32
                )
            branch[m, :, at] = acc.astype(BF16)
            for copy in ring.scatter(branch, got, m, (rs_s, rs_r), at):
                copy.start()

        loop(width // TILE, norm_tile)

    def finish(m):
        for copy in ring.scatter(branch, got, m, (rs_s, rs_r)):
            copy.wait()
        if m == 0:
            kept[3].wait()
        grad_norm = ring.total(branch, got, m)
        unit, inv_root = stats(rin[m].astype(F32))
        scaled = grad_norm * vec[0:1, :]
        upstream = dyr[m].astype(F32)
        dx = upstream + inv_root * (
            scaled
            - jnp.mean(scaled, axis=-1, keepdims=True)
            - unit * jnp.mean(scaled * unit, axis=-1, keepdims=True)
        )
        out_f[m] = dx
        out_b[m] = dx.astype(BF16)

        @pl.when(second)
        def _():
            hop(m).start()

        store(out_f, dx_o, m, 3)
        for i, term in enumerate((grad_norm * unit, grad_norm, upstream)):
            sums = jnp.sum(term, axis=0, keepdims=True)
            if m == 0:
                own_sums[i:i + 1, :] = sums
            else:
                own_sums[i:i + 1, :] += sums

    @pl.when(second)
    def _():
        for m in range(micro):
            front(m)

    for m in range(micro):
        arrive(m)
        body(m)
    for m in range(micro):
        finish(m)
    for copy in stores:
        copy.wait()

    @pl.when(second)
    def _():
        for m in range(micro):
            hop(m).wait_send()


def backward(dy, weights, rows, qkv, lse, gp, vec, rope, segc, segr, nt):
    wq, wo, w1, w2 = weights
    micro, per, width = rows.shape
    length = per * nt
    own, hidden = wo.shape[1], w1.shape[1]
    anywhere = pl.BlockSpec(memory_space=pl.ANY)
    inside = pl.BlockSpec(memory_space=pltpu.VMEM)
    out_shape = [
        jax.ShapeDtypeStruct((micro, length, width), BF16),
        jax.ShapeDtypeStruct((micro, length, hidden), BF16),
        jax.ShapeDtypeStruct((micro, 3, length, own), BF16),
        jax.ShapeDtypeStruct(rows.shape, F32),
        jax.ShapeDtypeStruct((8, width), F32),
        jax.ShapeDtypeStruct((8, own), F32),
        jax.ShapeDtypeStruct((8, hidden), F32),
    ]
    dma = pltpu.SemaphoreType.DMA
    return pl.pallas_call(
        functools.partial(backward_kernel, nt),
        out_shape=out_shape,
        in_specs=[anywhere] * 9 + [inside] * 4,
        out_specs=[anywhere] * 4 + [inside] * 3,
        scratch_shapes=[
            pltpu.VMEM(wq.shape, BF16),
            pltpu.VMEM(wo.shape, BF16),
            pltpu.VMEM(w1.shape, BF16),
            pltpu.VMEM(w2.shape, BF16),
            pltpu.VMEM(rows.shape, BF16),
            pltpu.VMEM(rows.shape, BF16),
            pltpu.VMEM(qkv.shape, BF16),
            pltpu.VMEM(lse.shape, F32),
            pltpu.VMEM(gp.shape, BF16),
            pltpu.VMEM((micro, length, width), BF16),
            pltpu.VMEM((length, own), BF16),
            pltpu.VMEM((micro, length, hidden), BF16),
            pltpu.VMEM((micro, 3, length, own), BF16),
            pltpu.VMEM((micro, length, width), BF16),
            pltpu.VMEM((micro, nt - 1, per, width), BF16),
            pltpu.VMEM(rows.shape, F32),
            pltpu.VMEM(rows.shape, BF16),
            dma((4,)),
            dma((5,)),
            dma((micro, 4)),
            dma((micro, nt)),
            dma((micro, nt)),
            dma((micro, nt)),
            dma((micro, nt)),
            dma((micro,)),
            dma((micro,)),
        ],
        compiler_params=pltpu.CompilerParams(
            collective_id=3, has_side_effects=True, vmem_limit_bytes=VMEM_LIMIT
        ),
        name="backward",
    )(dy, wq, wo, w1, w2, rows, qkv, lse, gp, vec, rope, segc, segr)


ROWS_OF_PACK = 16
PIECES = 8
DIRECT_FIRST = 0
DIRECT = 2
STRIPS = 4
WIDE = 512


def twist(x, tables, sign):
    keep, sine, ahead = tables
    left = pltpu.roll(x, LANES - ROT_DIM // 2, 1)
    right = pltpu.roll(x, ROT_DIM // 2, 1)
    return x * keep + jnp.where(ahead, left, right) * (sign * sine)


def masks_of(nf):
    return range(nf)


def bits_below(mask, nf):
    low = mask & -mask if mask else nf
    return [(i, 1 << i) for i in range(nf.bit_length() - 1) if (1 << i) < low]


def flipped(index, mask, nf):
    for i in range(nf.bit_length() - 1):
        if mask >> i & 1:
            index = index + (1 << i) * (1 - 2 * lax.rem(index // (1 << i), 2))
    return index


def fused_kernel(
    nf, nt,
    ends_h, gain, shift, b_out, b_fc2, b_qkv, b_fc1, seg_in, wq_h, wo_h, w1_h, w2_h,
    ends_o, sums_o, fc2_o, fc1_o, out_o, qkv_o, turned_o,
    act_x, att_x, up_x, dj_x, xc_x, gc_x,
    wq, wo, w1, w2, pack, packs, wide, fb, segs, rope, rin, dyr, xg, qkv, lse, att, gp, act,
    gr, gatt, up, dj, out_bf, out_got, in_bf, in_got, y_f, y_b,
    own_sums, head_sums, up_sums, s_src, s_got,
    in_sem, wl_sem, ws_sem, wr_sem, pk_s, pk_r, sm_s, sm_r,
    ag_s, ag_r, gg_s, gg_r, rs_s, rs_r, rb_s, rb_r, hx_s, hx_r, hb_s, hb_r,
    xl_sem, xs_s, xs_r, cl_sem, ca_s, ca_r, mx_s, mx_r, o_sem,
    mg_s, mg_r, l1_s, l1_r, l2_s, l2_r, fw_s, fw_r, go_sem, nb, wide_b, mf_s, mb_s, wb_sem,
    dl_sem, ds_sem,
):
    micro, per, width = rin.shape
    length = per * nt
    section, f, t = (lax.axis_index(a) for a in ("section", "fsdp", "tp"))
    first, second = section == 0, section == 1
    ring = Ring(nt, per)
    own, hidden = wo.shape[1], w1.shape[1]
    depth = width // nf
    mirror, sibling = {"fsdp": flipped(f, 2, nf)}, {"fsdp": flipped(f, 1, nf)}
    count = nf * nt
    other = {"section": 1 - section}
    across = {"section": 1 - section, "fsdp": flipped(f, 2, nf)}
    me, group = group_peers(nf, nt)
    fblock = [flipped(f, mask, nf) for mask in masks_of(nf)]

    def rows_at(block):
        return pl.ds(pl.multiple_of(block * depth, depth), depth)

    load_rows = pltpu.make_async_copy(ends_h, rin, in_sem)
    load_dy = pltpu.make_async_copy(ends_h, dyr, in_sem)

    @pl.when(first)
    def _():
        load_rows.start()

    @pl.when(second)
    def _():
        load_dy.start()

    greet(
        [peer for _, _, peer in group]
        + [across, other]
        + [{"section": 1 - section, "tp": to} for _, to in ring.others]
    )

    per_row = hidden // nf // LANES
    segs[0] = jnp.zeros((8, length), F32)
    segs[0, 0:micro, :] = seg_in[...].astype(F32)
    pack[...] = jnp.zeros_like(pack)
    pack[0:1, :] = gain[...].astype(F32)
    pack[1:2, :] = shift[...].astype(F32)
    pack[2:3, :] = b_out[...].astype(F32) + b_fc2[...].astype(F32)
    pack[3:6, :] = b_qkv[...].astype(F32)
    for r in range(per_row):
        pack[6 + r:7 + r, :] = b_fc1[:, r * LANES:(r + 1) * LANES].astype(F32)
    seg_copy = send(segs.at[0], segs.at[1], mx_s.at[2, 0], mx_r.at[2, 0], mirror)
    pack_local = pltpu.make_async_copy(pack, packs.at[me], pk_s.at[0])
    pack_copies = [
        send(pack, packs.at[me], pk_s.at[k], pk_r.at[k], peer) for k, _, peer in group
    ]
    pack_local.start()
    seg_copy.start()
    for copy in pack_copies:
        copy.start()

    table = ((wq_h, wq), (w1_h, w1), (wo_h, wo), (w2_h, w2))

    def w_at(ref, block):
        return ref.at[:, rows_at(block), :] if len(ref.shape) == 3 else ref.at[rows_at(block), :]

    def w_local(a):
        return pltpu.make_async_copy(table[a][0], w_at(table[a][1], f), wl_sem.at[a])

    def w_send(a, mask, i, bit):
        block = w_at(table[a][1], fblock[mask])
        src = table[a][0] if mask == 0 else block
        peer = {"fsdp": flipped(f, bit, nf)}
        return send(src, block, ws_sem.at[a, mask, i], wr_sem.at[a, mask | bit], peer)

    def w_recv(a, mask):
        block = w_at(table[a][1], fblock[mask])
        return send(block, block, ws_sem.at[a, mask, 0], wr_sem.at[a, mask], other)

    def w_near(a):
        w_local(a).start()
        w_send(a, 0, 0, 1).start()

    def w_far(a):
        w_send(a, 0, 1, 2).start()

    part_rows = depth // PIECES
    per_slot = length // part_rows

    def stage(p):
        return up.at[p // per_slot, pl.ds(p % per_slot * part_rows, part_rows), :]

    def piece_at(a, mask, p):
        start = pl.multiple_of(fblock[mask] * depth + p * part_rows, part_rows)
        return table[a][1].at[pl.ds(start, part_rows), :]

    def leg_one(a, p):
        src = table[a][0].at[pl.ds(p * part_rows, part_rows), :]
        return send(src, stage(p), l1_s.at[p], l1_r.at[p], across)

    def leg_two(a, p):
        return send(stage(p), piece_at(a, 2, p), l2_s.at[p], l2_r.at[p], other)

    def passed_on(a, mask, p):
        block = piece_at(a, mask, p)
        return send(block, block, fw_s.at[p], fw_r.at[p], sibling)

    def straight(a, p):
        src = table[a][0].at[pl.ds(p * part_rows, part_rows), :]
        return send(src, piece_at(a, 0, p), l1_s.at[p], l2_r.at[p], mirror)

    def relay(a, p):
        leg_one(a, p).wait_recv()
        leg_two(a, p).start()

    def via_ready(a):
        for p in range(PIECES):
            leg_two(a, p).wait_recv()
            passed_on(a, 2, p).start()
        for p in range(PIECES):
            passed_on(a, 3, p).wait_recv()

    def w_ready(a, mask):
        if mask == 0:
            w_local(a).wait()
            return
        w_recv(a, mask).wait_recv()
        for i, bit in bits_below(mask, nf):
            w_send(a, mask, i, bit).start()

    order = sorted(masks_of(nf), key=lambda m: (m != 0, -(m & -m), m))
    out_order = list(masks_of(nf))
    for a in range(4):
        w_near(a)

    @pl.when(first)
    def _():
        w_far(0)
        for p in range(PIECES - DIRECT_FIRST, PIECES):
            straight(1, p).start()
        w_far(2)
        for p in range(PIECES - DIRECT_FIRST):
            leg_one(1, p).start()

    def small_arrive():
        pack_local.wait()
        for copy in pack_copies:
            copy.wait()
        for j in range(count):
            wide[:, j * LANES:(j + 1) * LANES] = packs[j]
        for j in range(nf):
            for r in range(per_row):
                c = (j * per_row + r) * LANES
                fb[0:1, c:c + LANES] = packs[t * nf + j, 6 + r:7 + r, :]

    def segment_parts(q):
        row = segs[q // micro, pl.ds(lax.rem(q, micro), 1), :]
        query = lax.broadcasted_iota(jnp.int32, (length, length), 0)
        key = lax.broadcasted_iota(jnp.int32, (length, length), 1)
        column = jnp.sum(jnp.where(query == key, row, 0.0), axis=1, keepdims=True)
        return row, column, query >= key

    def allowed_of(q):
        row, column, causal = segment_parts(q)
        return causal & (row == column)

    def rope_of(q):
        row, column, _ = segment_parts(q)
        before = jnp.sum(jnp.where(row < column, 1.0, 0.0), axis=1, keepdims=True)
        lane = lax.rem(lax.broadcasted_iota(jnp.int32, (length, LANES), 1), HEAD_DIM)
        place = lax.broadcasted_iota(jnp.int32, (length, LANES), 0).astype(F32) - before
        half = ROT_DIM // 2
        power = lax.rem(lane, half).astype(F32)
        freq = jnp.exp(-jnp.log(10000.0) * (2.0 * power) / ROT_DIM)
        angles = place * freq
        rope[q, 0] = jnp.where(lane < ROT_DIM, jnp.cos(angles), 1.0)
        sine = jnp.where(lane < ROT_DIM, jnp.sin(angles), 0.0)
        rope[q, 1] = jnp.where(lane < half, -sine, sine)

    def hop_out(m):
        return send(y_b.at[m], rin.at[m], hx_s.at[m], hx_r.at[m], other)

    def hop_back(m):
        return send(y_b.at[m], dyr.at[m], hb_s.at[m], hb_r.at[m], other)

    def spread(buf, m, send_sems, recv_sems):
        here = ring.block(t)
        return [
            send(
                buf.at[m, here], buf.at[m, here], send_sems.at[m, k], recv_sems.at[m, t],
                {"tp": to},
            )
            for k, to in ring.others
        ]

    def block_wait(buf, m, recv_sems, who):
        at = ring.block(who)
        send(buf.at[m, at], buf.at[m, at], o_sem.at[m], recv_sems.at[m, who], other).wait_recv()

    def spread_start(buf, m, send_sems, recv_sems):
        for copy in spread(buf, m, send_sems, recv_sems):
            copy.start()

    def spread_wait(buf, m, send_sems, recv_sems):
        for _, who in ring.others:
            block_wait(buf, m, recv_sems, who)
        for copy in spread(buf, m, send_sems, recv_sems):
            copy.wait_send()

    last = micro - 1

    def cast(src, buf, send_sems, recv_sems):
        here = ring.block(t)
        return [
            send(
                src, buf.at[last, here], send_sems.at[k], recv_sems.at[last, t],
                {"section": 1 - section, "tp": to},
            )
            for k, to in [(0, t)] + ring.others
        ]

    def cast_wait(buf, recv_sems):
        for who in range(nt):
            block_wait(buf, last, recv_sems, who)

    def cast_rows():
        return cast(nb, xg, mf_s, ag_r)

    def cast_back():
        return cast(y_b.at[last], gr, mb_s, gg_r)

    def wide_copy():
        return send(wide.at[0:8], wide_b, wb_sem.at[0], wb_sem.at[1], other)

    def front(m):
        unit, _ = stats(rin[m].astype(F32))
        normed = unit * wide[0:1, :] + wide[1:2, :]
        xg[m, ring.block(ring.me)] = normed.astype(BF16)
        spread_start(xg, m, ag_s, ag_r)

    def front_back(m):
        gr[m, ring.block(ring.me)] = dyr[m]

        @pl.when(first)
        def _():
            mirror_rows(m, t).start()

        spread_start(gr, m, gg_s, gg_r)

    def mirror_copy(m):
        return send(xg.at[m], xg.at[micro + m], mx_s.at[0, m], mx_r.at[0, m], mirror)

    def mirror_rows(m, who):
        at = ring.block(who)
        return send(
            gr.at[m, at], gr.at[micro + m, at], mg_s.at[m, who], mg_r.at[m, who], mirror
        )

    def x_block(who):
        return fblock[2 * who] if isinstance(who, int) else jnp.where(who == 0, f, fblock[2])

    def x_dst(a, m, who):
        block = x_block(who)
        if a == 3:
            return dj_x.at[m, :, block]
        return (act_x, att_x, up_x)[a].at[m, block]

    def x_src(a, m, who):
        place = (m, micro)[who] if isinstance(who, int) else jnp.where(who == 0, m, micro)
        return (act, att, up, dj)[a].at[place]

    def x_local(a, m, who):
        return pltpu.make_async_copy(
            x_src(a, m, who), x_dst(a, m, who), xl_sem.at[a, m, who]
        )

    def x_send(a, m, who):
        return send(
            x_src(a, m, who), x_dst(a, m, who), xs_s.at[a, m, who], xs_r.at[a, m, who], sibling
        )

    def x_start(a, m, who):
        x_local(a, m, who).start()
        x_send(a, m, who).start()

    def x_sent(a, m, who):
        x_local(a, m, who).wait()
        x_send(a, m, who).wait_send()

    def c_pair(which, m, who):
        src, dst = ((xg, xc_x), (gr, gc_x))[which]
        block = x_block(who)
        q = who * micro + m
        mine = pltpu.make_async_copy(
            src.at[q, :, rows_at(f)], dst.at[m, block], cl_sem.at[which, m, who]
        )
        theirs = send(
            src.at[q, :, rows_at(fblock[1])],
            dst.at[m, block],
            ca_s.at[which, m, who],
            ca_r.at[which, m, who],
            sibling,
        )
        return mine, theirs

    def c_start(which, m, who):
        for copy in c_pair(which, m, who):
            copy.start()

    def sum_start(buf, got, sems, m, at):
        for copy in ring.scatter(buf, got, m, sems, at):
            copy.start()

    def sum_wait(buf, got, sems, m):
        for copy in ring.scatter(buf, got, m, sems):
            copy.wait()
        return ring.total(buf, got, m)

    out_set = (out_bf, out_got, (rs_s, rs_r))
    in_set = (in_bf, in_got, (rb_s, rb_r))

    def attention_masks(q):
        low = low_half(length)
        lane = lax.broadcasted_iota(jnp.int32, (length, LANES), 1)
        tables = (rope[q, 0], rope[q, 1], lax.rem(lane, HEAD_DIM) < ROT_DIM // 2)
        return low, lane, tables, allowed_of(q)

    factor = HEAD_DIM ** (-0.5)

    def forward_stage(m, who, k, fresh):
        q = who * micro + m
        place = jnp.where(who == 0, m, micro)

        @pl.when(who == 0)
        def _():
            @pl.when(first | (m < last))
            def _():
                spread_wait(xg, m, ag_s, ag_r)

            @pl.when(second & (m == last))
            def _():
                hop_out(last).wait_recv()
                cast_wait(xg, ag_r)

            c_start(0, m, 0)

            @pl.when(second)
            def _():
                mirror_copy(m).start()

        @pl.when(who == 1)
        def _():
            mirror_copy(m).wait_recv()
            c_start(0, m, 1)

            @pl.when(m == 1)
            def _():
                x_sent(0, 0, 1)
                x_sent(1, 0, 1)

        @pl.when(fresh)
        def _():
            for mask in order:
                w_ready(0, mask)
            w_far(3)

        low, lane, tables, allowed = attention_masks(q)
        for part in range(3):
            def qkv_tile(n, part=part):
                at = cols(n, WIDE)
                acc = jnp.dot(xg[q], wq[part, :, at], preferred_element_type=F32)
                acc = acc + wide[3 + part:4 + part, pl.ds(
                    pl.multiple_of(t * own + n * WIDE, WIDE), WIDE)]
                if part < 2:
                    acc = jnp.concatenate(
                        [
                            twist(acc[:, c:c + LANES], tables, 1.0)
                            for c in range(0, WIDE, LANES)
                        ],
                        axis=1,
                    )
                qkv[q, part, :, at] = acc.astype(BF16)

            loop(own // WIDE, qkv_tile)

        def pair(p):
            at = cols(p, LANES)
            query, key, value = qkv[q, 0, :, at], qkv[q, 1, :, at], qkv[q, 2, :, at]
            outs = []
            for h in range(2):
                mask = low if h == 0 else ~low
                one = jnp.where(mask, query, jnp.zeros_like(query))
                s = lax.dot_general(one, key, COLS, preferred_element_type=F32)
                s = jnp.where(allowed, s * factor, -1e30)
                top = jnp.max(s, axis=-1, keepdims=True)
                e = jnp.exp(s - top)
                total = jnp.sum(e, axis=-1, keepdims=True)
                probs = (e / total).astype(BF16)
                outs.append(jnp.dot(probs, value, preferred_element_type=F32))
                lse[q] = jnp.where(lane == 2 * p + h, top + jnp.log(total), lse[q])
            att[place, :, at] = jnp.where(low, outs[0], outs[1]).astype(BF16)

        lse[q] = jnp.zeros((length, LANES), F32)
        loop(own // LANES, pair)
        x_start(1, m, who)

        @pl.when(first & (k == 1))
        def _():
            output_finish(0)
            relay(3, 0)
            relay(3, 1)

        @pl.when(k == 0)
        def _():
            w_ready(1, 0)
            w_ready(1, 1)

        @pl.when(fresh)
        def _():
            via_ready(1)

        @pl.when(second & (k == 0))
        def _():
            w_ready(1, 3)

        def up_tile(n):
            at = cols(n, WIDE)
            u = jnp.dot(xg[q], w1[:, at], preferred_element_type=F32) + fb[0:1, at]
            c = 0.7978845608028654
            square = u * u
            th = jnp.tanh(c * u * (1.0 + 0.044715 * square))
            act[place, :, at] = (0.5 * u * (1.0 + th)).astype(BF16)
            slope = 0.5 * (1.0 + th)
            slope = slope + 0.5 * u * (1.0 - th * th) * (c * (1.0 + 3 * 0.044715 * square))
            gp[q, :, at] = slope.astype(BF16)

        loop(hidden // WIDE, up_tile)
        x_start(0, m, who)

    def differ(a, b):
        return a + b - 2 * a * b

    def output_stage(m, lo, hi, fresh, now):
        def block(j):
            if fresh is not None:
                for mask in masks_of(nf):
                    @pl.when(fresh & (j == mask))
                    def _(mask=mask):
                        w_ready(2, mask)
                        w_ready(3, mask)
                        if mask == 2:
                            pl.semaphore_signal(
                                go_sem, inc=1, device_id=other, device_id_type=MESH
                            )

            owner = 2 * differ(f // 2, j // 2) + differ(lax.rem(f, 2), lax.rem(j, 2))

            def out_tile(n):
                at = pl.ds(pl.multiple_of(owner * depth + n * WIDE, WIDE), WIDE)
                acc = lax.dot_general(att[m], wo[at, :], COLS, preferred_element_type=F32)
                acc = acc + lax.dot_general(act[m], w2[at, :], COLS, preferred_element_type=F32)
                out_bf[m, :, at] = acc.astype(BF16)
                if now is True:
                    sum_start(*out_set, m, at)
                else:
                    pl.when(now)(lambda: sum_start(*out_set, m, at))

            loop(depth // WIDE, out_tile)

        def step(j, carry):
            block(j)
            return carry

        lax.fori_loop(lo, hi, step, 0)

    def output_rest(m):
        half = width // 2
        start = pl.multiple_of((1 - f // 2) * half, half)
        sum_start(*out_set, m, pl.ds(start, half))

    def store_ends(m):
        return pltpu.make_async_copy(y_f.at[m], ends_o.at[m], o_sem.at[m])

    def output_finish(m):
        total = sum_wait(*out_set, m)
        y = rin[m].astype(F32) + total + wide[2:3, :]

        @pl.when(first)
        def _():
            y_b[m] = y.astype(BF16)
            hop_out(m).start()

        @pl.when(first & (m == last))
        def _():
            wide_copy().wait_recv()
            unit, _ = stats(y_b[m].astype(F32))
            nb[...] = (unit * wide_b[0:1, :] + wide_b[1:2, :]).astype(BF16)
            for copy in cast_rows():
                copy.start()

        @pl.when(second)
        def _():
            y_f[m] = y
            store_ends(m).start()

    def backward_stage(m, who, k):
        q = who * micro + m
        place = jnp.where(who == 0, m, micro)

        @pl.when(first & (who == 0))
        def _():
            @pl.when(m < last)
            def _():
                for _, who in ring.others:
                    block_wait(gr, m, gg_r, who)
                    mirror_rows(m, who).start()
                for copy in spread(gr, m, gg_s, gg_r):
                    copy.wait_send()

            @pl.when(m == last)
            def _():
                for who in range(nt):
                    block_wait(gr, last, gg_r, who)
                    mirror_rows(last, who).start()
                dyr[m] = gr[m, ring.block(t)]

            c_start(1, m, 0)

        @pl.when(who == 1)
        def _():
            for who in range(nt):
                mirror_rows(m, who).wait_recv()
            c_start(1, m, 1)

            @pl.when(second & (m == 1))
            def _():
                x_sent(2, 0, 1)
                x_sent(3, 0, 1)

        def att_tile(n):
            at = cols(n, WIDE)
            gatt[:, at] = jnp.dot(gr[q], wo[:, at], preferred_element_type=F32).astype(BF16)

        loop(own // WIDE, att_tile)
        low, lane, tables, allowed = attention_masks(q)

        def pair(p):
            at = cols(p, LANES)
            query, key, value = qkv[q, 0, :, at], qkv[q, 1, :, at], qkv[q, 2, :, at]
            grad = gatt[:, at]
            dqs, dks, dvs = [], [], []
            for h in range(2):
                mask = low if h == 0 else ~low
                one = jnp.where(mask, query, jnp.zeros_like(query))
                s = lax.dot_general(one, key, COLS, preferred_element_type=F32)
                s = jnp.where(allowed, s * factor, -1e30)
                log_total = jnp.sum(
                    jnp.where(lane == 2 * p + h, lse[q], 0.0), axis=-1, keepdims=True
                )
                soft = jnp.exp(s - log_total)
                probs = soft.astype(BF16)
                one_grad = jnp.where(mask, grad, jnp.zeros_like(grad))
                dp = lax.dot_general(one_grad, value, COLS, preferred_element_type=F32)
                delta = jnp.sum(dp * soft, axis=-1, keepdims=True)
                ds = (soft * (dp - delta)).astype(BF16)
                dvs.append(lax.dot_general(probs, grad, ROWS, preferred_element_type=F32))
                dqs.append(jnp.dot(ds, key, preferred_element_type=F32))
                dks.append(lax.dot_general(ds, query, ROWS, preferred_element_type=F32))
            dq = jnp.where(low, dqs[0], dqs[1]) * factor
            dk = jnp.where(low, dks[0], dks[1]) * factor
            dj[place, 0, :, at] = twist(dq, tables, -1.0).astype(BF16)
            dj[place, 1, :, at] = twist(dk, tables, -1.0).astype(BF16)
            dj[place, 2, :, at] = jnp.where(low, dvs[0], dvs[1]).astype(BF16)

        loop(own // LANES, pair)
        x_start(3, m, who)

        @pl.when(second & (k == 3))
        def _():
            backward_finish(0)

        @pl.when(who == 0)
        def _():
            for part in range(3):
                head_sums[part:part + 1, :] += jnp.sum(
                    dj[m, part].astype(F32), axis=0, keepdims=True
                )

        @pl.when(second & (k == 1))
        def _():
            w_ready(3, 0)
            w_ready(3, 1)
            output_stage(0, 0, 2, None, True)
            via_ready(3)

        def up_tile(n):
            at = cols(n, WIDE)
            acc = jnp.dot(gr[q], w2[:, at], preferred_element_type=F32)
            rounded = (acc * gp[q, :, at].astype(F32)).astype(BF16)
            up[place, :, at] = rounded
            sums = jnp.sum(rounded.astype(F32), axis=0, keepdims=True)
            up_sums[0:1, at] += jnp.where(who == 0, sums, 0.0)

        loop(hidden // WIDE, up_tile)
        x_start(2, m, who)

        def norm_tile(n):
            at = cols(n, WIDE)
            acc = lax.dot_general(up[m], w1[at, :], COLS, preferred_element_type=F32)
            for part in range(3):
                acc = acc + lax.dot_general(
                    dj[m, part], wq[part, at, :], COLS, preferred_element_type=F32
                )
            in_bf[m, :, at] = acc.astype(BF16)
            sum_start(*in_set, m, at)

        @pl.when(who == 0)
        def _():
            loop(width // WIDE, norm_tile)


    def backward_finish(m):
        grad_norm = sum_wait(*in_set, m)
        unit, inv_root = stats(rin[m].astype(F32))
        scaled = grad_norm * wide[0:1, :]
        upstream = dyr[m].astype(F32)
        dx = upstream + inv_root * (
            scaled
            - jnp.mean(scaled, axis=-1, keepdims=True)
            - unit * jnp.mean(scaled * unit, axis=-1, keepdims=True)
        )

        @pl.when(second)
        def _():
            y_b[m] = dx.astype(BF16)

        @pl.when(second & (m < last))
        def _():
            hop_back(m).start()

        @pl.when(second & (m == last))
        def _():
            for copy in cast_back():
                copy.start()

        @pl.when(first)
        def _():
            y_f[m] = dx
            store_ends(m).start()

        for i, term in enumerate((grad_norm * unit, grad_norm, upstream)):
            own_sums[i:i + 1, :] += jnp.sum(term, axis=0, keepdims=True)

    def strip(slot):
        return xg.at[:, :, pl.ds(pl.multiple_of(slot * own, own), own)]

    def strip_copy(src, slot):
        return pltpu.make_async_copy(src, strip(slot), dl_sem.at[slot])

    wide_strips = hidden // own
    kinds = 2 * wide_strips

    def strip_start(i, m):
        slot = lax.rem(i, STRIPS)

        @pl.when(i < wide_strips)
        def _():
            strip_copy(act_x.at[m, :, :, cols(i, own)], slot).start()

        @pl.when((i >= wide_strips) & (i < kinds))
        def _():
            strip_copy(up_x.at[m, :, :, cols(i - wide_strips, own)], slot).start()

        @pl.when(i == kinds)
        def _():
            strip_copy(att_x.at[m], slot).start()

        @pl.when(i > kinds)
        def _():
            strip_copy(dj_x.at[m, i - kinds - 1], slot).start()

    half = depth // 2

    def result_copy(dst, h):
        return pltpu.make_async_copy(att.at[h], dst, ds_sem.at[h])

    def turn_rows(m):
        strip_copy(xc_x.at[m], 2).start()
        strip_copy(gc_x.at[m], 3).start()
        for which in range(2):
            strip_copy(xc_x.at[m], 2 + which).wait()
            for b in range(nf):
                for h in range(2):
                    block = xg[b, :, pl.ds((2 + which) * own + h * half, half)]
                    c = (h * nf + b) * length
                    act[which, :, c:c + length] = block.T

    def turned_copies():
        span = nf * length
        return [
            pltpu.make_async_copy(
                act.at[which, :, pl.ds(h * span, span)],
                turned_o.at[which, pl.ds(h * half, half), :],
                dl_sem.at[2 * which + h],
            )
            for which in range(2)
            for h in range(2)
        ]

    def weight_stage():
        m = 0
        for i in range(micro):
            for a in (0, 1):
                x_sent(a, i, 0)
            mirror_copy(i).wait_send()
            for who in range(2):
                mine, theirs = c_pair(0, i, who)
                mine.wait()
                theirs.wait()
        for a in (2, 3):
            x_sent(a, 0, 0)

        @pl.when(first)
        def _():
            for a in (2, 3):
                x_sent(a, 0, 1)

        for who in range(2):
            for a in range(4):
                x_send(a, 0, who).wait_recv()
            mine, theirs = c_pair(1, 0, who)
            mine.wait()
            theirs.wait()
        strip_start(0, m)
        strip_start(1, m)
        turn_rows(m)
        strip_start(2, m)
        strip_start(3, m)

        def step(i):
            slot = lax.rem(i, STRIPS)
            strip_copy(xc_x.at[m], slot).wait()
            use_dy = (i < wide_strips) | (i == kinds)
            right = xg[:, :, cols(slot, own)].reshape(nf * length, own)
            which = jnp.where(use_dy, 1, 0)
            span = nf * length
            left = jnp.concatenate([act[which, :, :span], act[which, :, span:]], axis=0)
            value = jnp.dot(left, right, preferred_element_type=F32)
            for h in range(2):
                rows = pl.ds(h * half, half)

                @pl.when(i > 0)
                def _(h=h):
                    result_copy(out_o.at[pl.ds(0, half), :], h).wait()

                att[h] = value[h * half:(h + 1) * half].astype(BF16)

                @pl.when(i < wide_strips)
                def _(h=h, rows=rows):
                    result_copy(fc2_o.at[rows, cols(i, own)], h).start()

                @pl.when((i >= wide_strips) & (i < kinds))
                def _(h=h, rows=rows):
                    result_copy(fc1_o.at[rows, cols(i - wide_strips, own)], h).start()

                @pl.when(i == kinds)
                def _(h=h, rows=rows):
                    result_copy(out_o.at[rows, :], h).start()

                @pl.when(i > kinds)
                def _(h=h, rows=rows):
                    result_copy(qkv_o.at[i - kinds - 1, rows, :], h).start()

            @pl.when(i + STRIPS < kinds + 4)
            def _():
                strip_start(i + STRIPS, m)

        loop(kinds + 4, step)
        for h in range(2):
            result_copy(out_o.at[pl.ds(0, half), :], h).wait()

    own_sums[...] = jnp.zeros_like(own_sums)
    head_sums[...] = jnp.zeros_like(head_sums)
    up_sums[...] = jnp.zeros_like(up_sums)

    @pl.when(first)
    def _():
        small_arrive()
        load_rows.wait()
        loop(micro, front)
        seg_copy.wait()
        loop(2 * micro, rope_of)

    @pl.when(second)
    def _():
        load_dy.wait()
        loop(micro, front_back)

    @pl.when(second)
    def _():
        for p in range(PIECES - DIRECT_FIRST):
            relay(1, p)
        w_far(0)
        w_far(1)
        small_arrive()
        wide_copy().start()
        seg_copy.wait()
        loop(2 * micro, rope_of)
        for mask in order:
            w_ready(0, mask)
        w_far(2)
        for p in range(PIECES - DIRECT_FIRST):
            leg_two(1, p).wait_send()
        pl.semaphore_wait(go_sem, 1)
        for p in range(PIECES - DIRECT):
            leg_one(3, p).start()

        def dy_in(m):
            spread_wait(gr, m, gg_s, gg_r)
            c_start(1, m, 0)

        loop(micro, dy_in)


    small = [
        send(s_src.at[to], s_got.at[k], sm_s.at[k], sm_r.at[k], peer) for k, to, peer in group
    ]

    def small_start():
        s_src[...] = jnp.zeros_like(s_src)
        for j in range(count):
            s_src[j, 0:3, :] = own_sums[0:3, j * LANES:(j + 1) * LANES]
        for j in range(nf):
            s_src[t * nf + j, 3:6, :] = head_sums[0:3, j * LANES:(j + 1) * LANES]
            for r in range(per_row):
                c = (j * per_row + r) * LANES
                s_src[t * nf + j, 6 + r:7 + r, :] = up_sums[0:1, c:c + LANES]
        for copy in small:
            copy.start()

    def slot(k):
        is_f = jnp.where(first, k < 4, (k < 8) & (lax.rem(k, 2) == 0))
        is_o = jnp.where(first, k < 2, (k == 1) | (k == 6))
        who = jnp.where(first, (k // 2) % 2 * (k < 4) + lax.rem(k, 2) * (k >= 4), k // 4)
        m = jnp.where(first, jnp.where(k < 4, lax.rem(k, 2), (k - 4) // 2), lax.rem(k // 2, 2))
        m_o = jnp.where(first, m, k // 6)
        fresh = first & (k == 0)

        @pl.when(second & (k == 0))
        def _():
            hop_out(0).wait_recv()
            front(0)
            w_ready(1, 2)
            for p in range(PIECES - DIRECT, PIECES):
                straight(3, p).start()

        @pl.when(second & (k == 1))
        def _():
            for i in range(micro):
                for who in range(nt):
                    mirror_rows(i, who).start()
            for mask in order:
                w_ready(2, mask)

        @pl.when(first & (k == 3))
        def _():
            hop_back(0).wait_recv()
            front_back(0)

        @pl.when(is_f)
        def _():
            forward_stage(m, who, k, fresh)

        @pl.when(jnp.logical_not(is_f))
        def _():
            backward_stage(m, who, k)

        @pl.when(second & (k == 6))
        def _():
            for copy in cast_back():
                copy.wait_send()

        @pl.when(is_o)
        def _():
            held_back = second & (k == 1)
            output_stage(
                m_o, jnp.where(held_back, 2, 0), nf, fresh, jnp.logical_not(held_back)
            )


        @pl.when(first & (k == 1))
        def _():
            for p in range(2, PIECES - DIRECT):
                relay(3, p)
            for i in range(micro):
                mirror_copy(i).start()
            for p in range(PIECES - DIRECT):
                leg_two(3, p).wait_send()
            output_finish(1)

        @pl.when(second & (k == 2))
        def _():
            output_rest(0)

        @pl.when(second & (k == 4))
        def _():
            backward_finish(1)

        @pl.when(second & (k == 7))
        def _():
            small_start()

        @pl.when((first & (k == 6)) | (second & (k == 7)))
        def _():
            weight_stage()

        @pl.when(first & (k == 7))
        def _():
            loop(micro, backward_finish)
            small_start()

        @pl.when(k == 7)
        def _():
            for who in range(2):
                mine, theirs = c_pair(1, last, who)
                mine.wait()
                theirs.wait()
            turn_rows(last)
            for copy in turned_copies():
                copy.start()

        @pl.when(second & (k == 7))
        def _():
            loop(micro, output_finish)

    loop(8, slot)

    for a in (2, 3):
        x_sent(a, last, 0)
    for who in range(2):
        for a in range(4):
            if who == 1:
                x_sent(a, last, 1)
            x_send(a, last, who).wait_recv()

    @pl.when(second)
    def _():
        for m in range(last):
            hop_back(m).wait_send()
        wide_copy().wait_send()

    @pl.when(first)
    def _():
        for m in range(micro):
            hop_out(m).wait_send()
        for copy in cast_rows():
            copy.wait_send()

    for m in range(micro):
        for who in range(nt):
            mirror_rows(m, who).wait_send()
    for m in range(micro):
        store_ends(m).wait()
    for a in range(4):
        w_send(a, 0, 0, 1).wait_send()
    for side, via in ((first, 1), (second, 3)):
        @pl.when(side)
        def _(via=via):
            for a in range(4):
                if a != via:
                    w_send(a, 0, 1, 2).wait_send()
                    w_send(a, 2, 0, 1).wait_send()
            for p in range(PIECES):
                if p >= PIECES - (DIRECT if via == 3 else DIRECT_FIRST):
                    straight(via, p).wait_send()
                else:
                    leg_one(via, p).wait_send()
                passed_on(via, 2, p).wait_send()
    total = s_src[me]
    for k, copy in enumerate(small):
        copy.wait()
        total = total + s_got[k + 1]
    sums_o[...] = total
    for copy in turned_copies():
        copy.wait()


def fused(ends, smalls, segments, wq, wo, w1, w2, nf, nt):
    micro, per, width = ends.shape
    length = per * nt
    own, hidden = wo.shape[1], w1.shape[1]
    depth = width // nf
    count = nf * nt
    bits = nf.bit_length() - 1
    anywhere = pl.BlockSpec(memory_space=pl.ANY)
    inside = pl.BlockSpec(memory_space=pltpu.VMEM)
    dma = pltpu.SemaphoreType.DMA
    vm = pltpu.VMEM
    piece = (ROWS_OF_PACK, LANES)
    packs = 2 * micro
    some = micro + 1
    out_shape = [
        jax.ShapeDtypeStruct(ends.shape, F32),
        jax.ShapeDtypeStruct(piece, F32),
        jax.ShapeDtypeStruct((depth, hidden), BF16),
        jax.ShapeDtypeStruct((depth, hidden), BF16),
        jax.ShapeDtypeStruct((depth, own), BF16),
        jax.ShapeDtypeStruct((3, depth, own), BF16),
        jax.ShapeDtypeStruct((2, depth, nf * length), BF16),
        jax.ShapeDtypeStruct((micro, nf, length, hidden), BF16),
        jax.ShapeDtypeStruct((micro, nf, length, own), BF16),
        jax.ShapeDtypeStruct((micro, nf, length, hidden), BF16),
        jax.ShapeDtypeStruct((micro, 3, nf, length, own), BF16),
        jax.ShapeDtypeStruct((micro, nf, length, depth), BF16),
        jax.ShapeDtypeStruct((micro, nf, length, depth), BF16),
    ]
    scratch = [
        vm((3, width, own), BF16), vm((width, own), BF16),
        vm((width, hidden), BF16), vm((width, hidden), BF16),
        vm(piece, F32), vm((count,) + piece, F32),
        vm((ROWS_OF_PACK, width), F32), vm((8, hidden), F32),
        vm((2, 8, length), F32), vm((packs, 2, length, LANES), F32),
        vm(ends.shape, BF16), vm(ends.shape, BF16),
        vm((packs, length, width), BF16), vm((packs, 3, length, own), BF16),
        vm((packs, length, LANES), F32), vm((some, length, own), BF16),
        vm((packs, length, hidden), BF16), vm((some, length, hidden), BF16),
        vm((packs, length, width), BF16), vm((length, own), BF16),
        vm((some, length, hidden), BF16), vm((some, 3, length, own), BF16),
        vm((micro, length, width), BF16), vm((micro, nt - 1, per, width), BF16),
        vm((micro, length, width), BF16), vm((micro, nt - 1, per, width), BF16),
        vm(ends.shape, F32), vm(ends.shape, BF16),
        vm((8, width), F32), vm((8, own), F32), vm((8, hidden), F32),
        vm((count,) + piece, F32), vm((count,) + piece, F32),
        dma, dma((4,)), dma((4, nf, bits)), dma((4, nf)),
        dma((count,)), dma((count,)), dma((count,)), dma((count,)),
        dma((micro, nt)), dma((micro, nt)), dma((micro, nt)), dma((micro, nt)),
        dma((micro, nt)), dma((micro, nt)), dma((micro, nt)), dma((micro, nt)),
        dma((micro,)), dma((micro,)), dma((micro,)), dma((micro,)),
        dma((4, micro, 2)), dma((4, micro, 2)), dma((4, micro, 2)),
        dma((2, micro, 2)), dma((2, micro, 2)), dma((2, micro, 2)),
        dma((3, micro)), dma((3, micro)), dma((micro,)),
        dma((micro, nt)), dma((micro, nt)),
        dma((PIECES,)), dma((PIECES,)), dma((PIECES,)), dma((PIECES,)),
        dma((PIECES,)), dma((PIECES,)), pltpu.SemaphoreType.REGULAR,
        vm((per, width), BF16), vm((8, width), F32), dma((nt,)), dma((nt,)), dma((2,)),
        dma((STRIPS,)), dma((2,)),
    ]
    return pl.pallas_call(
        functools.partial(fused_kernel, nf, nt),
        out_shape=out_shape,
        in_specs=[anywhere] + [inside] * 7 + [anywhere] * 4,
        out_specs=[anywhere, inside] + [anywhere] * 11,
        scratch_shapes=scratch,
        compiler_params=pltpu.CompilerParams(
            collective_id=4, has_side_effects=True, vmem_limit_bytes=VMEM_LIMIT
        ),
        name="fused",
    )(ends, *smalls, segments, wq, wo, w1, w2)


def padded(flat):
    size = -(-flat.shape[-1] // (8 * LANES)) * (8 * LANES)
    room = [(0, 0)] * (flat.ndim - 1) + [(0, size - flat.shape[-1])]
    flat = jnp.pad(flat, room)
    return flat.reshape(flat.shape[:-1] + (size // LANES, LANES))


def split_shards(
    ends_in, segments, ln_gain, ln_bias, w_qkv, w_out, w_fc1, w_fc2,
    bias_qkv, bias_out, bias_fc1, bias_fc2,
):
    nf, nt = lax.axis_size("fsdp"), lax.axis_size("tp")
    count = nf * nt
    section, tp_index = lax.axis_index("section"), lax.axis_index("tp")
    is_first = section == 0
    piece = ln_gain.shape[1]
    hidden_piece = bias_fc1.shape[1]
    own, hidden = w_out.shape[2], w_fc1.shape[2]
    width = piece * count

    pack = jnp.concatenate(
        [ln_gain[0], ln_bias[0], bias_out[0], bias_fc2[0], bias_qkv[0].reshape(-1), bias_fc1[0]]
    ).astype(F32)
    used = pack.shape[0]
    smalls = gather_small(padded(pack), nf, nt).reshape(count, -1)[:, :used]
    wide = smalls[:, :7 * piece].reshape(count, 7, piece).transpose(1, 0, 2).reshape(7, width)
    vec = jnp.stack([wide[0], wide[1], wide[2] + wide[3]])
    vec = jnp.pad(vec, ((0, 5), (0, 0)))
    qb = lax.dynamic_slice_in_dim(wide[4:7], tp_index * own, own, 1)
    qb = jnp.pad(qb, ((0, 5), (0, 0)))
    fb = lax.dynamic_slice_in_dim(smalls[:, 7 * piece:], tp_index * nf, nf, 0).reshape(1, hidden)
    fb = jnp.pad(fb, ((0, 7), (0, 0)))
    rope = rope_tables(segments)
    segc, segr = segments[:, :, None], segments[:, None, :]

    wq = lax.all_gather(w_qkv[0].transpose(1, 0, 2), "fsdp", axis=1, tiled=True)
    w1 = lax.all_gather(w_fc1[0], "fsdp", axis=0, tiled=True)
    wo = lax.all_gather(w_out[0], "fsdp", axis=0, tiled=True)
    w2 = lax.all_gather(w_fc2[0], "fsdp", axis=0, tiled=True)
    weights = (wq, wo, w1, w2)
    rows, xg, qkv, lse, att, gp, act, y = forward(
        ends_in[0], weights, vec, qb, fb, rope, segc, segr, nt
    )
    gr, up, dj, dx, own_sums, head_sums, up_sums = backward(
        ends_in[0], weights, rows, qkv, lse, gp, vec, rope, segc, segr, nt
    )

    def everywhere(arr):
        return lax.all_gather(arr, "fsdp", axis=arr.ndim - 2, tiled=True)

    def columns(arr):
        return lax.all_to_all(arr, "fsdp", split_axis=2, concat_axis=1, tiled=True)

    xc, gc = columns(xg), columns(gr)

    def product(left, right):
        return lax.dot_general(
            left, right, (((0, 1), (0, 1)), ((), ())), preferred_element_type=F32
        )

    act_all, att_all, up_all, dj_all = (everywhere(a) for a in (act, att, up, dj))
    grad_fc2 = product(gc, act_all)
    grad_out = product(gc, att_all)
    grad_fc1 = product(xc, up_all)
    grad_qkv = jnp.stack([product(xc, dj_all[:, part]) for part in range(3)], axis=1)

    mine = own_sums[:3].reshape(3, count, piece).transpose(1, 0, 2).reshape(count, 3 * piece)
    head = lax.dynamic_update_slice_in_dim(
        jnp.zeros((3, width), F32), head_sums[:3], tp_index * own, 1
    )
    head = head.reshape(3, count, piece).transpose(1, 0, 2).reshape(count, 3 * piece)
    ups = lax.dynamic_update_slice_in_dim(
        jnp.zeros((count, hidden_piece), F32),
        up_sums[0].reshape(nf, hidden_piece),
        tp_index * nf,
        0,
    )
    sums = sum_small(padded(jnp.concatenate([mine, head, ups], axis=1)), nf, nt).reshape(-1)
    gain_grad, bias_grad, row_grad = (sums[i * piece:(i + 1) * piece] for i in range(3))
    qkv_bias_grad = sums[3 * piece:6 * piece].reshape(3, piece)
    fc1_bias_grad = sums[6 * piece:6 * piece + hidden_piece]
    ends_out = jnp.where(is_first, dx, y)[None]
    return (
        ends_out,
        gain_grad[None],
        bias_grad[None],
        grad_qkv[None],
        grad_out[None],
        grad_fc1[None],
        grad_fc2[None],
        qkv_bias_grad[None],
        row_grad[None],
        fc1_bias_grad[None],
        row_grad[None],
    )


AHEAD = 3


def last_kernel(
    used, last,
    ends, sums, turned, fc2, fc1, out, qkv, act, up, att, dj,
    ends_o, gain_o, shift_o, row_o, row_b, qkv_b, fc1_b, fc2_o, fc1_o, out_o, qkv_o,
    ends_v, turned_v, early_v, right_v, done_v, e_sem, t_sem, p_sem, r_sem, d_sem,
    sums_v, row_v, qkv_v, hidden_v, s_sem,
):
    strips, _, own = early_v.shape
    wide = (strips - 4) // 2
    copy = pltpu.make_async_copy

    def part(ref, i):
        return ref.at[:, pl.ds(i * own, own)]

    table = []
    for i in range(wide):
        right = act.at[last, :, :, pl.ds(i * own, own)]
        table.append((1, part(fc2, i), right, part(fc2_o, i)))
    for i in range(wide):
        right = up.at[last, :, :, pl.ds(i * own, own)]
        table.append((0, part(fc1, i), right, part(fc1_o, i)))
    table.append((1, out, att.at[last], out_o))
    for i in range(3):
        table.append((0, qkv.at[i], dj.at[last, i], qkv_o.at[i]))
    def turned_load(which):
        return copy(turned.at[which], turned_v.at[which], t_sem.at[which])

    def loads(i):
        _, early, right, _ = table[i]
        return copy(right, right_v.at[i], r_sem.at[i]), copy(early, early_v.at[i], p_sem.at[i])

    turned_load(table[0][0]).start()
    for i in range(AHEAD):
        for one in loads(i):
            one.start()
    ends_in = copy(ends, ends_v, e_sem.at[0])
    sums_in = copy(sums, sums_v, s_sem.at[0])
    sums_in.start()
    tiny = [
        copy(row_v.at[0], gain_o, s_sem.at[1]),
        copy(row_v.at[1], shift_o, s_sem.at[2]),
        copy(row_v.at[2], row_o, s_sem.at[3]),
        copy(row_v.at[2], row_b, s_sem.at[4]),
        copy(qkv_v, qkv_b, s_sem.at[5]),
        copy(hidden_v, fc1_b, s_sem.at[6]),
    ]
    ready = set()
    stores = []
    for i, (which, _, _, target) in enumerate(table):
        if which not in ready:
            turned_load(which).wait()
            ready.add(which)
        for one in loads(i):
            one.wait()
        if i + AHEAD < strips:
            for one in loads(i + AHEAD):
                one.start()
        if i == 0:
            turned_load(1 - which).start()
        if i == 1:
            ends_in.start()
        right = right_v[i].reshape(-1, own)
        done_v[i] = early_v[i].astype(F32) + jnp.dot(
            turned_v[which], right, preferred_element_type=F32
        )
        stores.append(copy(done_v.at[i], target, d_sem.at[i]))
        stores[-1].start()
        if i == 2:
            sums_in.wait()
            for r in range(3):
                row_v[r] = sums_v[r:r + 1, :]
                qkv_v[r] = sums_v[3 + r:4 + r, :]
            for r in range(6, used):
                hidden_v[:, (r - 6) * LANES:(r - 5) * LANES] = sums_v[r:r + 1, :]
            for one in tiny:
                one.start()
            stores.extend(tiny)
        if i == strips - 3:
            ends_in.wait()
            stores.append(copy(ends_v, ends_o, e_sem.at[1]))
            stores[-1].start()
    for one in stores:
        one.wait()


def last_products(used, ends, sums, turned, fc2, fc1, out, qkv, act, up, att, dj):
    depth, hidden = fc2.shape
    own = out.shape[1]
    micro, nf, length = act.shape[:3]
    strips = 2 * (hidden // own) + 4
    anywhere = pl.BlockSpec(memory_space=pl.ANY)
    small = jax.ShapeDtypeStruct((1, LANES), F32)
    dma = pltpu.SemaphoreType.DMA
    return pl.pallas_call(
        functools.partial(last_kernel, used, micro - 1),
        out_shape=[
            jax.ShapeDtypeStruct(ends.shape, F32), small, small, small, small,
            jax.ShapeDtypeStruct((3, 1, LANES), F32),
            jax.ShapeDtypeStruct((1, (used - 6) * LANES), F32),
            jax.ShapeDtypeStruct(fc2.shape, F32), jax.ShapeDtypeStruct(fc1.shape, F32),
            jax.ShapeDtypeStruct(out.shape, F32), jax.ShapeDtypeStruct(qkv.shape, F32),
        ],
        in_specs=[anywhere] * 11,
        out_specs=[anywhere] * 11,
        scratch_shapes=[
            pltpu.VMEM(ends.shape, F32), pltpu.VMEM(turned.shape, BF16),
            pltpu.VMEM((strips, depth, own), BF16),
            pltpu.VMEM((strips, nf, length, own), BF16),
            pltpu.VMEM((strips, depth, own), F32),
            dma((2,)), dma((2,)), dma((strips,)), dma((strips,)), dma((strips,)),
            pltpu.VMEM(sums.shape, F32), pltpu.VMEM((3, 1, LANES), F32),
            pltpu.VMEM((3, 1, LANES), F32), pltpu.VMEM((1, (used - 6) * LANES), F32),
            dma((7,)),
        ],
        compiler_params=pltpu.CompilerParams(vmem_limit_bytes=VMEM_LIMIT),
        name="last_products",
    )(ends, sums, turned, fc2, fc1, out, qkv, act, up, att, dj)


def fused_shards(
    ends_in, segments, ln_gain, ln_bias, w_qkv, w_out, w_fc1, w_fc2,
    bias_qkv, bias_out, bias_fc1, bias_fc2,
):
    nf, nt = lax.axis_size("fsdp"), lax.axis_size("tp")
    used = 6 + bias_fc1.shape[1] // LANES
    ends_out, sums, fc2, fc1, out, qkv, turned, act_x, att_x, up_x, dj_x, *_ = fused(
        ends_in[0],
        (ln_gain, ln_bias, bias_out, bias_fc2, bias_qkv[0], bias_fc1),
        segments, w_qkv[0].transpose(1, 0, 2), w_out[0], w_fc1[0], w_fc2[0], nf, nt,
    )

    ends_out, gain, shift, row, row_again, qkv_bias, fc1_bias, fc2, fc1, out, qkv = (
        last_products(
            used, ends_out, sums, turned, fc2, fc1, out, qkv, act_x, up_x, att_x, dj_x
        )
    )
    return (
        ends_out[None],
        gain,
        shift,
        qkv.transpose(1, 0, 2)[None],
        out[None],
        fc1[None],
        fc2[None],
        qkv_bias.transpose(1, 0, 2),
        row,
        fc1_bias,
        row_again,
    )


def shards(*args):
    rows, piece = args[0].shape[2], args[2].shape[1]
    small = rows * lax.axis_size("tp") <= 256
    tidy = piece == LANES and args[10].shape[1] // LANES <= ROWS_OF_PACK - 6
    square = lax.axis_size("fsdp") == 4 and args[0].shape[1] == 2
    return (fused_shards if small and tidy and square else split_shards)(*args)


def solution(mesh):
    both = P("section", ("fsdp", "tp"))
    square = P("section", "fsdp", "tp")
    tokens = P("section", None, ("fsdp", "tp"), None)
    heads = P("section", "fsdp", None, "tp")
    bias3 = P("section", None, ("fsdp", "tp"))
    return jax.shard_map(
        shards,
        mesh=mesh,
        in_specs=(
            tokens, P(None, "fsdp"), both, both, heads, square, square, square,
            bias3, both, both, both,
        ),
        out_specs=(
            tokens, both, both, heads, square, square, square, bias3, both, both, both,
        ),
        check_vma=False,
    )
```
